32 devices in a mesh: blk: 8 (over z, y), sp: 4 (over x, core).
Axes of the slice: x: 2, y: 2, z: 4, core: 2. Of those that a mesh axis runs over, the one named last changes fastest.
Arguments:
- tokens: bfloat16 [4096, 2304], P(('blk', 'sp')), may hold values from -6 to 6
- w_qkv: bfloat16 [4096, 2304], replicated, may hold values from -5 to 5
- w_out: bfloat16 [2048, 2304], replicated, may hold values from -0.125 to 0.125
- gains: float32 [4, 2304], replicated, may hold values from 0.1 to 1.9
- w_ffn: bfloat16 [9216, 3, 2304], P('blk'), may hold values from -0.125 to 0.125
- cotangent: bfloat16 [4096, 2304], P(('blk', 'sp')), may hold values from -6 to 6
Outputs:
- block_out: bfloat16 [4096, 2304], P(('blk', 'sp'))
- tokens_grad: bfloat16 [4096, 2304], P(('blk', 'sp'))
- qkv_grad: float32 [4096, 2304], P(('sp', 'blk'))
- out_grad: float32 [2048, 2304], P(('sp', 'blk'))
- gains_grad: float32 [4, 2304], P(None, ('sp', 'blk'))
- ffn_grad: float32 [9216, 3, 2304], P(('blk', 'sp'))
The draws below stay inside these ranges and needn't reach their ends.
All inputs are finite; a program needn't handle non-finite values.
Results may differ from the reference program's by a relative error of at most 0.025.
Values may be sent and summed in bfloat16 or wider, within the bound.
A program may use at most 320 MiB of HBM per device.

```python
import math
import jax
import jax.numpy as jnp
from jax import lax

D = 2304
HEADS = 8
KV_HEADS = 4
HEAD = 256
FF = 9216
SEQ = 4096


def draw_w_qkv(key, part):
    group_ratio = HEADS // KV_HEADS
    row_total = (HEADS + 2 * KV_HEADS) * HEAD
    seed_base, seed_query, seed_keys = jax.random.split(key, 3)
    base_values = jnp.clip(jax.random.normal(seed_base, (row_total, D), jnp.float32), -6.0, 6.0)
    query_factor = jnp.exp(jax.random.uniform(seed_query, (KV_HEADS, group_ratio), jnp.float32, math.log(0.5), math.log(2.0)))
    key_factor = jnp.exp(jax.random.uniform(seed_keys, (KV_HEADS, 1), jnp.float32, math.log(0.5), math.log(1.5)))
    value_factor = jnp.ones((KV_HEADS, 1), jnp.float32)
    factors = jnp.concatenate([query_factor, key_factor, value_factor], axis=1)
    row_factor = jnp.repeat(factors.reshape(-1), HEAD)
    return (base_values * row_factor[:, None] * D ** (-0.5)).astype(jnp.bfloat16)


def levels(stream_key, dims, shards, low, largest):
    level = 1.0
    for axis_at, shards_of in shards:
        steps = jax.random.uniform(jax.random.fold_in(jax.random.fold_in(stream_key, 6), axis_at), (shards_of,), jnp.float32, low / len(shards), largest / len(shards))
        level = level * jnp.repeat(jnp.exp(steps), dims[axis_at] // shards_of).reshape((-1,) + (1,) * (len(dims) - 1 - axis_at))
    return level


def gaussian(stream_key, dims, scale, reach, pieces=(), kind=jnp.bfloat16):
    array = jax.random.normal(stream_key, dims, jnp.float32) * scale
    if len(pieces) > 0:
        array = levels(stream_key, dims, pieces, -0.22, 0.18) * array
    return jnp.clip(array, min=-reach, max=reach).astype(kind)


def setup_inputs(seed: int = 0) -> dict:
    arg_keys = jax.random.split(jax.random.key(seed), 7)
    tokens = gaussian(arg_keys[0], (SEQ, D), 1.0, 6.0, ((0, 32),))
    w_qkv = draw_w_qkv(jax.random.fold_in(arg_keys[6], 71), 0)
    w_out = gaussian(arg_keys[2], (HEADS * HEAD, D), (HEADS * HEAD) ** -0.5, 0.125)
    gains = jnp.clip(1.0 + 0.18 * jax.random.normal(arg_keys[3], (4, D), jnp.float32), 0.1, 1.9)
    w_ffn = gaussian(arg_keys[4], (FF, 3, D), D ** -0.5, 0.125, ((0, 8),))
    cotangent = gaussian(arg_keys[5], (SEQ, D), 1.0, 6.0, ((0, 32),))
    return dict(tokens=tokens, w_qkv=w_qkv, w_out=w_out, gains=gains, w_ffn=w_ffn, cotangent=cotangent)


@jax.custom_vjp
def low(v):
    return lax.optimization_barrier(v.astype(jnp.bfloat16)).astype(jnp.float32)

@jax.custom_vjp
def low_back(v):
    return v

def low_keep(v):
    return (low(v), None)

def low_pass(kept, grad):
    return (grad,)

def back_keep(v):
    return (v, None)

def back_low(kept, grad):
    return (low(grad),)
low.defvjp(low_keep, low_pass)
low_back.defvjp(back_keep, back_low)
NORM_EPSILON = 1e-06
CAP_VALUE = 50.0
GELU_SCALE = 0.7978845608028654
GELU_CUBIC = 0.044715
HIGHEST = lax.Precision.HIGHEST

def norm_scale(values, gain):
    return values * lax.rsqrt(lax.optimization_barrier(jnp.mean(values * values, axis=-1, keepdims=True)) + NORM_EPSILON) * gain

def gelu_value(values):
    return 0.5 * values * (1.0 + jnp.tanh(GELU_SCALE * (values + GELU_CUBIC * values * values * values)))

def attend(queries, keys_all, values_all):
    total_rows = queries.shape[0]
    block_rows = 512 if total_rows % 512 == 0 else total_rows
    score_scale = HEAD ** (-0.5)
    key_places = jnp.arange(total_rows, dtype=jnp.int32)

    def one_block(block_index):
        first_row = block_index * block_rows
        query_block = lax.dynamic_slice_in_dim(queries, first_row, block_rows, 0)
        raw = low_back(jnp.einsum('qkgd,rkd->kgqr', query_block, keys_all, precision=HIGHEST))
        capped = CAP_VALUE * jnp.tanh(raw * score_scale / CAP_VALUE)
        query_places = first_row + jnp.arange(block_rows, dtype=jnp.int32)
        allowed = key_places[None, :] <= query_places[:, None]
        weights = jnp.where(allowed, jnp.exp(capped), 0.0)
        totals = lax.optimization_barrier(jnp.sum(weights, axis=-1))
        summed = low_back(jnp.einsum('kgqr,rkd->qkgd', low(weights), values_all, precision=HIGHEST))
        return summed / jnp.transpose(totals, (2, 0, 1))[..., None]
    blocks = lax.map(jax.checkpoint(one_block), jnp.arange(total_rows // block_rows, dtype=jnp.int32))
    return blocks.reshape(total_rows, HEADS * HEAD)

def layer(tokens, w_qkv, w_out, gains, w_ffn):
    seq_rows = tokens.shape[0]
    group_ratio = HEADS // KV_HEADS
    act_in = low(norm_scale(tokens, gains[0]))
    projected = low(low_back(jnp.dot(act_in, w_qkv.T, precision=HIGHEST)))
    grouped = projected.reshape(seq_rows, KV_HEADS, group_ratio + 2, HEAD)
    queries = grouped[:, :, :group_ratio]
    keys_all = grouped[:, :, group_ratio]
    values_all = grouped[:, :, group_ratio + 1]
    attended = low(low_back(attend(queries, keys_all, values_all)))
    attn = low_back(jnp.dot(attended, w_out, precision=HIGHEST))
    middle = tokens + norm_scale(attn, gains[1])
    act_ffn = low(norm_scale(middle, gains[2]))
    gate = low_back(jnp.dot(act_ffn, w_ffn[:, 0, :].T, precision=HIGHEST))
    up_proj = low_back(jnp.dot(act_ffn, w_ffn[:, 1, :].T, precision=HIGHEST))
    hidden = low(gelu_value(gate) * up_proj)
    ffn_out = low_back(jnp.dot(hidden, w_ffn[:, 2, :], precision=HIGHEST))
    return middle + norm_scale(ffn_out, gains[3])

def reference(tokens, w_qkv, w_out, gains, w_ffn, cotangent):
    primals = (tokens.astype(jnp.float32), w_qkv.astype(jnp.float32), w_out.astype(jnp.float32), gains.astype(jnp.float32), w_ffn.astype(jnp.float32))
    result, pullback = jax.vjp(layer, *primals)
    grad_list = pullback(cotangent.astype(jnp.float32))
    return (result.astype(jnp.bfloat16), grad_list[0].astype(jnp.bfloat16), grad_list[1], grad_list[2], grad_list[3], grad_list[4])
```

```python
import math

import jax
import jax.numpy as jnp
from jax import lax
from jax.sharding import PartitionSpec as P

HEADS = 8
KV_HEADS = 4
HEAD = 256


NORM_EPSILON = 1e-06
CAP_VALUE = 50.0
GELU_SCALE = 0.7978845608028654
GELU_CUBIC = 0.044715


def norm_parts(values):
    inverse = lax.rsqrt(jnp.mean(values * values, axis=-1, keepdims=True) + NORM_EPSILON)
    return (values * inverse, inverse)


def norm_back(grad_y, normed, inverse, gain):
    grad_n = grad_y * gain
    grad_v = inverse * (grad_n - normed * jnp.mean(grad_n * normed, axis=-1, keepdims=True))
    return (grad_v, jnp.sum(grad_y * normed, axis=0))


def gelu_value(values):
    return (
        0.5
        * values
        * (1.0 + jnp.tanh(GELU_SCALE * (values + GELU_CUBIC * values * values * values)))
    )


def gelu_slope(values):
    bent = jnp.tanh(GELU_SCALE * (values + GELU_CUBIC * values * values * values))
    return 0.5 * (1.0 + bent) + 0.5 * values * (1.0 - bent * bent) * GELU_SCALE * (
        1.0 + 3.0 * GELU_CUBIC * values * values
    )


def contract_last(left, right):
    return lax.dot_general(
        left, right, (((1,), (1,)), ((), ())), preferred_element_type=jnp.float32
    )


def body(tokens, w_qkv, w_out, gains, w_ffn, cotangent):
    row_count = tokens.shape[0]
    groups = lax.axis_size("sp")
    cycle_size = lax.axis_size("blk")
    heads_here = HEADS // groups
    kv_here = KV_HEADS // groups
    group_ratio = HEADS // KV_HEADS
    query_width = HEADS * HEAD
    score_scale = HEAD ** (-0.5)
    source = tokens.astype(jnp.float32)
    normed_in, inverse_in = norm_parts(source)
    act_in = (normed_in * gains[0]).astype(jnp.bfloat16)
    act_block = lax.all_gather(act_in, "sp", axis=0, tiled=True)
    group_cols = (group_ratio + 2) * HEAD * kv_here
    sp_at = lax.axis_index("sp")
    w_group = lax.dynamic_slice_in_dim(w_qkv, sp_at * group_cols, group_cols, 0)
    head_data = (
        contract_last(act_block, w_group)
        .astype(jnp.bfloat16)
        .reshape(act_block.shape[0], kv_here, group_ratio + 2, HEAD)
    )
    block_rows = head_data.shape[0]
    query_group = head_data[:, :, :group_ratio]
    key_heads = head_data[:, :, group_ratio]
    value_heads = head_data[:, :, group_ratio + 1]
    first_query = lax.axis_index("blk") * block_rows
    last_query = first_query + block_rows - 1
    query_places = first_query + jnp.arange(block_rows, dtype=jnp.int32)

    def tile_scores(key_tile, tile_first):
        tile_rows = key_tile.shape[0]
        raw = jnp.einsum(
            "qkgd,rkd->kgqr", query_group, key_tile, preferred_element_type=jnp.float32
        )
        squashed = jnp.tanh(raw * score_scale / CAP_VALUE)
        allowed = (tile_first + jnp.arange(tile_rows, dtype=jnp.int32))[None, :] <= query_places[
            :, None
        ]
        weights = jnp.where(allowed, jnp.exp(CAP_VALUE * squashed), 0.0)
        return (weights, squashed)

    def run_tiles(state_now, pieces, tile_step):
        key_piece, value_piece = pieces
        piece_rows = key_piece.shape[0]
        tile_rows = math.gcd(piece_rows, block_rows)
        tile_count = piece_rows // tile_rows
        key_tiles = key_piece.reshape(tile_count, tile_rows, kv_here, HEAD)
        value_tiles = value_piece.reshape(tile_count, tile_rows, kv_here, HEAD)

        def one_tile(state_in, items):
            key_tile, value_tile, tile_index = items
            return (tile_step(state_in, key_tile, value_tile, tile_index * tile_rows), None)

        state_out, unused = lax.scan(
            one_tile, state_now, (key_tiles, value_tiles, jnp.arange(tile_count, dtype=jnp.int32))
        )
        return state_out

    def forward_step(state_in, key_tile, value_tile, tile_first):

        def forward_compute(state_old):
            totals_old, summed_old = state_old
            weights, squashed = tile_scores(key_tile, tile_first)
            totals_new = totals_old + jnp.sum(weights, axis=-1)
            summed_new = summed_old + jnp.einsum(
                "kgqr,rkd->qkgd",
                weights.astype(jnp.bfloat16),
                value_tile,
                preferred_element_type=jnp.float32,
            )
            return (totals_new, summed_new)

        return lax.cond(
            tile_first <= last_query, forward_compute, lambda state_old: state_old, state_in
        )

    zero_totals = jnp.zeros((kv_here, group_ratio, block_rows), jnp.float32)
    zero_summed = jnp.zeros((block_rows, kv_here, group_ratio, HEAD), jnp.float32)
    totals, summed = run_tiles(
        (zero_totals, zero_summed),
        (
            lax.all_gather(key_heads, "blk", axis=0, tiled=True),
            lax.all_gather(value_heads, "blk", axis=0, tiled=True),
        ),
        forward_step,
    )
    totals_rows = jnp.transpose(totals, (2, 0, 1))[..., None]
    attended = summed / totals_rows
    attended_low = attended.reshape(block_rows, heads_here, HEAD).astype(jnp.bfloat16)
    attended_tokens = lax.all_to_all(
        attended_low, "sp", split_axis=0, concat_axis=1, tiled=True
    ).reshape(row_count, query_width)
    attn = jnp.dot(attended_tokens, w_out, preferred_element_type=jnp.float32)
    normed_attn, inverse_attn = norm_parts(attn)
    middle = source + normed_attn * gains[1]
    normed_mid, inverse_mid = norm_parts(middle)
    act_ffn = (normed_mid * gains[2]).astype(jnp.bfloat16)
    w_in = w_ffn[:, :2, :]
    w_down = w_ffn[:, 2, :]
    gate_up = jnp.einsum(
        "td,fkd->tkf",
        lax.all_gather(act_ffn, "blk", axis=0, tiled=True),
        w_in,
        preferred_element_type=jnp.float32,
    )
    hidden = (gelu_value(gate_up[:, 0]) * gate_up[:, 1]).astype(jnp.bfloat16)
    hidden_all = hidden
    part = hidden_all
    ffn_out = lax.psum_scatter(
        jnp.dot(part, w_down, preferred_element_type=jnp.float32).astype(jnp.bfloat16),
        "blk",
        scatter_dimension=0,
        tiled=True,
    ).astype(jnp.float32)
    normed_ffn, inverse_ffn = norm_parts(ffn_out)
    result = middle + normed_ffn * gains[3]
    grad_out = cotangent.astype(jnp.float32)
    grad_ffn_f, gain_grad3 = norm_back(grad_out, normed_ffn, inverse_ffn, gains[3])
    grad_ffn = grad_ffn_f.astype(jnp.bfloat16)
    act_piece = lax.all_gather(act_ffn, "blk", axis=0, tiled=True)
    grad_piece = lax.all_gather(grad_ffn, "blk", axis=0, tiled=True)
    gate_up = jnp.einsum("td,fkd->tkf", act_piece, w_in, preferred_element_type=jnp.float32)
    hidden = (gelu_value(gate_up[:, 0]) * gate_up[:, 1]).astype(jnp.bfloat16)
    grad_hidden = contract_last(grad_piece, w_down)
    grad_gate = grad_hidden * gate_up[:, 1] * gelu_slope(gate_up[:, 0])
    grad_up = grad_hidden * gelu_value(gate_up[:, 0])
    grad_pair = jnp.stack([grad_gate, grad_up], axis=1).astype(jnp.bfloat16)
    in_part = jnp.einsum("tkf,td->fkd", grad_pair, act_piece, preferred_element_type=jnp.float32)
    down_part = jnp.einsum("tf,td->fd", hidden, grad_piece, preferred_element_type=jnp.float32)
    weight_sum = jnp.concatenate([in_part, down_part[:, None, :]], axis=1)
    part = grad_pair
    grad_act_ffn = lax.psum_scatter(
        jnp.einsum("tkf,fkd->td", part, w_in, preferred_element_type=jnp.float32).astype(
            jnp.bfloat16
        ),
        "blk",
        scatter_dimension=0,
        tiled=True,
    ).astype(jnp.float32)
    grad_norm_mid, gain_grad2 = norm_back(grad_act_ffn, normed_mid, inverse_mid, gains[2])
    grad_middle = grad_out + grad_norm_mid
    grad_attn_f, gain_grad1 = norm_back(grad_middle, normed_attn, inverse_attn, gains[1])
    grad_attn = grad_attn_f.astype(jnp.bfloat16)
    grad_block = lax.all_gather(grad_attn, "sp", axis=0, tiled=True)
    attended_cols = attended_low.reshape(block_rows, heads_here * HEAD)
    out_term = jnp.einsum(
        "tc,td->cd", attended_cols, grad_block, preferred_element_type=jnp.float32
    )
    out_grad = lax.psum_scatter(
        out_term.astype(jnp.bfloat16), "blk", scatter_dimension=0, tiled=True
    ).astype(jnp.float32)
    w_out_group = lax.dynamic_slice_in_dim(w_out, sp_at * heads_here * HEAD, heads_here * HEAD, 0)
    grad_heads = (
        contract_last(grad_block, w_out_group)
        .astype(jnp.bfloat16)
        .reshape(block_rows, kv_here, group_ratio, HEAD)
    )
    grad_heads_f = grad_heads.astype(jnp.float32)
    scaled = (grad_heads_f / totals_rows).astype(jnp.bfloat16)
    row_delta = jnp.transpose(
        jnp.sum(grad_heads_f * attended, axis=-1) / totals_rows[..., 0], (1, 2, 0)
    )

    def backward_step(state_in, key_tile, value_tile, tile_first):
        tile_rows = key_tile.shape[0]

        def backward_compute(state_old):
            grad_query, grad_keys, grad_values = state_old
            weights, squashed = tile_scores(key_tile, tile_first)
            grad_weights = (
                jnp.einsum("qkgd,rkd->kgqr", scaled, value_tile, preferred_element_type=jnp.float32)
                - row_delta[..., None]
            )
            grad_raw = (weights * grad_weights * (1.0 - squashed * squashed) * score_scale).astype(
                jnp.bfloat16
            )
            grad_query = grad_query + jnp.einsum(
                "kgqr,rkd->qkgd", grad_raw, key_tile, preferred_element_type=jnp.float32
            )
            key_part = jnp.einsum(
                "kgqr,qkgd->rkd", grad_raw, query_group, preferred_element_type=jnp.float32
            )
            value_part = jnp.einsum(
                "kgqr,qkgd->rkd",
                weights.astype(jnp.bfloat16),
                scaled,
                preferred_element_type=jnp.float32,
            )
            old_keys = lax.dynamic_slice_in_dim(grad_keys, tile_first, tile_rows, 0)
            grad_keys = lax.dynamic_update_slice_in_dim(
                grad_keys, old_keys + key_part, tile_first, 0
            )
            old_values = lax.dynamic_slice_in_dim(grad_values, tile_first, tile_rows, 0)
            grad_values = lax.dynamic_update_slice_in_dim(
                grad_values, old_values + value_part, tile_first, 0
            )
            return (grad_query, grad_keys, grad_values)

        return lax.cond(
            tile_first <= last_query, backward_compute, lambda state_old: state_old, state_in
        )

    start_back = (
        jnp.zeros((block_rows, kv_here, group_ratio, HEAD), jnp.float32),
        jnp.zeros((cycle_size * block_rows, kv_here, HEAD), jnp.float32),
        jnp.zeros((cycle_size * block_rows, kv_here, HEAD), jnp.float32),
    )
    grad_query, grad_keys_all, grad_values_all = run_tiles(
        start_back,
        (
            lax.all_gather(key_heads, "blk", axis=0, tiled=True),
            lax.all_gather(value_heads, "blk", axis=0, tiled=True),
        ),
        backward_step,
    )
    grad_keys, grad_values = (
        lax.psum_scatter(
            grad_keys_all.astype(jnp.bfloat16), "blk", scatter_dimension=0, tiled=True
        ).astype(jnp.float32),
        lax.psum_scatter(
            grad_values_all.astype(jnp.bfloat16), "blk", scatter_dimension=0, tiled=True
        ).astype(jnp.float32),
    )
    grad_proj_heads = jnp.concatenate(
        [grad_query, grad_keys[:, :, None], grad_values[:, :, None]], axis=2
    ).astype(jnp.bfloat16)
    grad_cols = grad_proj_heads.reshape(block_rows, group_cols)
    qkv_term = jnp.einsum("tc,td->cd", grad_cols, act_block, preferred_element_type=jnp.float32)
    qkv_grad = lax.psum_scatter(
        qkv_term.astype(jnp.bfloat16), "blk", scatter_dimension=0, tiled=True
    ).astype(jnp.float32)
    grad_proj_tokens = lax.all_to_all(grad_proj_heads, "sp", split_axis=0, concat_axis=1, tiled=True)
    grad_projected = grad_proj_tokens.reshape(row_count, w_qkv.shape[0])
    grad_act_in = jnp.dot(grad_projected, w_qkv, preferred_element_type=jnp.float32)
    grad_source, gain_grad0 = norm_back(grad_act_in, normed_in, inverse_in, gains[0])
    tokens_grad = (grad_middle + grad_source).astype(jnp.bfloat16)
    gains_term = jnp.stack([gain_grad0, gain_grad1, gain_grad2, gain_grad3], axis=0)
    ffn_grad = lax.psum_scatter(
        weight_sum.astype(jnp.bfloat16), "sp", scatter_dimension=0, tiled=True
    ).astype(jnp.float32)
    gains_part = lax.psum_scatter(gains_term, "sp", scatter_dimension=1, tiled=True)
    gains_grad = lax.psum_scatter(gains_part, "blk", scatter_dimension=1, tiled=True)
    return (result.astype(jnp.bfloat16), tokens_grad, qkv_grad, out_grad, gains_grad, ffn_grad)


def solution(mesh):
    return jax.shard_map(
        body,
        mesh=mesh,
        in_specs=(
            P(("blk", "sp"), None),
            P(),
            P(),
            P(),
            P("blk", None, None),
            P(("blk", "sp"), None),
        ),
        out_specs=(
            P(("blk", "sp"), None),
            P(("blk", "sp"), None),
            P(("sp", "blk"), None),
            P(("sp", "blk"), None),
            P(None, ("sp", "blk")),
            P(("blk", "sp"), None, None),
        ),
        check_vma=False,
    )
```

```python
import functools

import jax
import jax.numpy as jnp
from jax import lax
from jax.experimental import pallas as pl
from jax.experimental.pallas import tpu as pltpu
from jax.sharding import PartitionSpec as P

HEADS = 8
KV_HEADS = 4
HEAD = 256


VMEM_BYTES = 62 * 1024 * 1024
NORM_EPSILON = 1e-06
CAP_VALUE = 50.0
GELU_SCALE = 0.7978845608028654
GELU_CUBIC = 0.044715


def norm_parts(values):
    inverse = lax.rsqrt(jnp.mean(values * values, axis=-1, keepdims=True) + NORM_EPSILON)
    return (values * inverse, inverse)


def norm_back(grad_y, normed, inverse, gain):
    grad_n = grad_y * gain
    grad_v = inverse * (grad_n - normed * jnp.mean(grad_n * normed, axis=-1, keepdims=True))
    return (grad_v, jnp.sum(grad_y * normed, axis=0))


def gelu_value(values):
    return (
        0.5
        * values
        * (1.0 + jnp.tanh(GELU_SCALE * (values + GELU_CUBIC * values * values * values)))
    )


def gelu_slope(values):
    bent = jnp.tanh(GELU_SCALE * (values + GELU_CUBIC * values * values * values))
    return 0.5 * (1.0 + bent) + 0.5 * values * (1.0 - bent * bent) * GELU_SCALE * (
        1.0 + 3.0 * GELU_CUBIC * values * values
    )


def contract_last(left, right):
    return lax.dot_general(
        left, right, (((1,), (1,)), ((), ())), preferred_element_type=jnp.float32
    )


def push(source, target, sent, landed, block):
    return pltpu.make_async_remote_copy(
        src_ref=source,
        dst_ref=target,
        send_sem=sent,
        recv_sem=landed,
        device_id={"blk": block},
        device_id_type=pl.DeviceIdType.MESH,
    )


def greet(at, line, rows):
    barrier = pltpu.get_barrier_semaphore()

    def tell(block):
        pl.semaphore_signal(
            barrier, inc=1, device_id={"blk": block}, device_id_type=pl.DeviceIdType.MESH
        )

    tell(at + 1 - 2 * (at % 2))
    pl.when(line > 0)(lambda: tell(at - 2))
    pl.when(line < rows - 1)(lambda: tell(at + 2))
    pl.semaphore_wait(barrier, 1 + jnp.minimum(line, 1) + jnp.minimum(rows - 1 - line, 1))


def both(*terms):
    result = terms[0]
    for term in terms[1:]:
        result = jnp.logical_and(result, term)
    return result


def attend_kernel(
    heads,
    x_ref,
    low_ref,
    att_ref,
    tot_ref,
    kv_ref,
    kv,
    acc,
    part,
    up_sent,
    up_landed,
    side_sent,
    side_landed,
    own_done,
    save_done,
):
    at = lax.axis_index("blk")
    blocks = lax.axis_size("blk")
    rows = blocks // 2
    line, column = at // 2, at % 2
    partner = at + 1 - 2 * column
    size = x_ref.shape[0]
    first = heads * HEAD
    own = x_ref.at[:, pl.ds(first, 2 * HEAD)]
    greet(at, line, rows)

    def up_copy(index, source):
        return push(source, kv.at[index], up_sent.at[index // 2], up_landed.at[index // 2], at + 2)

    def side_copy(index, source):
        return push(
            source, kv.at[index], side_sent.at[index // 2], side_landed.at[index // 2], partner
        )

    def save(index):
        return pltpu.make_async_copy(kv.at[index], kv_ref.at[index], save_done.at[index])

    pl.when(line < rows - 1)(lambda: up_copy(at, own).start())
    pl.when(column == 0)(lambda: side_copy(at, own).start())
    keep = pltpu.make_async_copy(own, kv.at[at], own_done)
    keep.start()
    acc[...] = jnp.zeros_like(acc)
    part[...] = jnp.zeros_like(part)
    keep.wait()
    ahead = lax.broadcasted_iota(jnp.int32, (size, size), 1) - lax.broadcasted_iota(
        jnp.int32, (size, size), 0
    )

    def compute(index):
        save(index).start()
        span = (at - index) * size
        for head in range(heads):
            raw = lax.dot_general(
                x_ref[:, head * HEAD : (head + 1) * HEAD],
                kv[index, :, :HEAD],
                (((1,), (1,)), ((), ())),
                preferred_element_type=jnp.float32,
            )
            weights = jnp.exp(CAP_VALUE * jnp.tanh(raw * (HEAD ** (-0.5) / CAP_VALUE)))
            weights = jnp.where(ahead <= span, weights, 0.0)
            total = weights[:, :128]
            for piece in range(1, size // 128):
                total = total + weights[:, piece * 128 : (piece + 1) * 128]
            part[head] += total
            acc[:, head * HEAD : (head + 1) * HEAD] += jnp.dot(
                weights.astype(jnp.bfloat16),
                kv[index, :, HEAD:],
                preferred_element_type=jnp.float32,
            )

    @pl.loop(0, rows + 1)
    def _(step):
        source = line - step
        index = 2 * source + column

        @pl.when(both(step > 0, source >= 0))
        def _():
            up_copy(index, kv.at[index]).wait_recv()
            pl.when(line < rows - 1)(lambda: up_copy(index, kv.at[index]).start())
            side_copy(index, kv.at[index]).start()

        pl.when(source >= 0)(lambda: compute(index))
        other = 2 * (source + 1) + 1 - column

        @pl.when(both(step > 0, source + 1 >= 0, jnp.logical_or(step > 1, column == 1)))
        def _():
            side_copy(other, kv.at[other]).wait_recv()
            compute(other)

    for head in range(heads):
        columns = slice(head * HEAD, (head + 1) * HEAD)
        total = jnp.sum(part[head], axis=1, keepdims=True)
        value = acc[:, columns] / total
        att_ref[:, columns] = value
        low_ref[:, columns] = value.astype(jnp.bfloat16)
        tot_ref[head] = jnp.sum(part[head].T, axis=0, keepdims=True)

    @pl.loop(0, rows)
    def _(source):
        index = 2 * source + column

        @pl.when(source <= line)
        def _():
            pl.when(line < rows - 1)(lambda: up_copy(index, kv.at[index]).wait_send())
            pl.when(jnp.logical_or(source < line, column == 0))(
                lambda: side_copy(index, kv.at[index]).wait_send()
            )

    @pl.loop(0, blocks)
    def _(index):
        pl.when(index <= at)(lambda: save(index).wait())


def attend(projected, heads):
    size = projected.shape[0]
    blocks = lax.axis_size("blk")
    whole = pl.BlockSpec(memory_space=pltpu.VMEM)
    return pl.pallas_call(
        functools.partial(attend_kernel, heads),
        out_shape=(
            jax.ShapeDtypeStruct((size, heads * HEAD), jnp.bfloat16),
            jax.ShapeDtypeStruct((size, heads * HEAD), jnp.float32),
            jax.ShapeDtypeStruct((heads, 1, size), jnp.float32),
            jax.ShapeDtypeStruct((blocks, size, 2 * HEAD), jnp.bfloat16),
        ),
        in_specs=[whole],
        out_specs=(whole, whole, whole, pl.BlockSpec(memory_space=pl.ANY)),
        scratch_shapes=[
            pltpu.VMEM((blocks, size, 2 * HEAD), jnp.bfloat16),
            pltpu.VMEM((size, heads * HEAD), jnp.float32),
            pltpu.VMEM((heads, size, 128), jnp.float32),
            pltpu.SemaphoreType.DMA((blocks // 2,)),
            pltpu.SemaphoreType.DMA((blocks // 2,)),
            pltpu.SemaphoreType.DMA((blocks // 2,)),
            pltpu.SemaphoreType.DMA((blocks // 2,)),
            pltpu.SemaphoreType.DMA,
            pltpu.SemaphoreType.DMA((blocks,)),
        ],
        compiler_params=pltpu.CompilerParams(
            collective_id=0, has_side_effects=True, vmem_limit_bytes=VMEM_BYTES
        ),
        name="attend",
    )(projected)


def attend_back_kernel(
    heads,
    x_ref,
    scaled_ref,
    delta_ref,
    kv_ref,
    out_ref,
    kv,
    part,
    side,
    down,
    dq,
    dk,
    dv,
    load_done,
    side_sent,
    side_landed,
    down_sent,
    down_landed,
):
    at = lax.axis_index("blk")
    blocks = lax.axis_size("blk")
    rows = blocks // 2
    line, column = at // 2, at % 2
    partner = at + 1 - 2 * column
    size = x_ref.shape[0]

    def load(index):
        return pltpu.make_async_copy(kv_ref.at[index], kv.at[index], load_done.at[index])

    @pl.loop(0, blocks)
    def _(index):
        pl.when(index <= at)(lambda: load(index).start())

    greet(at, line, rows)

    def side_copy(target):
        return push(
            part.at[target, 1 - column],
            side.at[target],
            side_sent.at[target],
            side_landed.at[target],
            partner,
        )

    def down_copy(target):
        return push(
            part.at[target, column],
            down.at[target],
            down_sent.at[target],
            down_landed.at[target],
            at - 2,
        )

    dq[...] = jnp.zeros_like(dq)
    ahead = lax.broadcasted_iota(jnp.int32, (size, size), 0) - lax.broadcasted_iota(
        jnp.int32, (size, size), 1
    )

    def compute(target, half):
        index = 2 * target + half
        load(index).wait()
        span = (at - index) * size
        for head in range(heads):
            columns = slice(head * HEAD, (head + 1) * HEAD)
            query = x_ref[:, columns]
            scaled = scaled_ref[:, columns]
            key = kv[index, :, :HEAD]
            raw = lax.dot_general(
                key, query, (((1,), (1,)), ((), ())), preferred_element_type=jnp.float32
            )
            squashed = jnp.tanh(raw * (HEAD ** (-0.5) / CAP_VALUE))
            weights = jnp.exp(CAP_VALUE * squashed)
            weights = jnp.where(ahead <= span, weights, 0.0)
            inner = lax.dot_general(
                kv[index, :, HEAD:],
                scaled,
                (((1,), (1,)), ((), ())),
                preferred_element_type=jnp.float32,
            )
            grad_raw = (
                weights * (inner - delta_ref[head]) * (1.0 - squashed * squashed)
            ).astype(jnp.bfloat16)
            dv_now = jnp.dot(
                weights.astype(jnp.bfloat16), scaled, preferred_element_type=jnp.float32
            )
            dk_now = jnp.dot(grad_raw, query, preferred_element_type=jnp.float32)
            dq[:, columns] += lax.dot_general(
                grad_raw, key, (((0,), (0,)), ((), ())), preferred_element_type=jnp.float32
            )
            if head == 0:
                dv[...] = dv_now
                dk[...] = dk_now
            else:
                dv[...] += dv_now
                dk[...] += dk_now
        part[target, half, :, :HEAD] = (dk[...] * HEAD ** (-0.5)).astype(jnp.bfloat16)
        part[target, half, :, HEAD:] = dv[...].astype(jnp.bfloat16)

    def merge(target):
        last = target == line

        @pl.when(jnp.logical_or(target < line, column == 0))
        def _():
            side_copy(target).wait_recv()
            part[target, column] = (
                part[target, column].astype(jnp.float32) + side[target].astype(jnp.float32)
            ).astype(jnp.bfloat16)

        @pl.when(line < rows - 1)
        def _():
            down_copy(target).wait_recv()
            part[target, column] = (
                part[target, column].astype(jnp.float32) + down[target].astype(jnp.float32)
            ).astype(jnp.bfloat16)

        pl.when(target < line)(lambda: down_copy(target).start())

        @pl.when(last)
        def _():
            out_ref[:, heads * HEAD :] = part[target, column]

    @pl.loop(0, rows)
    def _(target):
        @pl.when(jnp.logical_or(target < line, both(target == line, column == 1)))
        def _():
            compute(target, 1 - column)
            side_copy(target).start()

        pl.when(target <= line)(lambda: compute(target, column))
        pl.when(both(line == rows - 1, target > 0))(lambda: merge(target - 1))

    out_ref[:, : heads * HEAD] = (dq[...] * HEAD ** (-0.5)).astype(jnp.bfloat16)

    @pl.loop(0, rows)
    def _(target):
        pl.when(both(target <= line, jnp.logical_or(line < rows - 1, target == rows - 1)))(
            lambda: merge(target)
        )

    @pl.loop(0, rows)
    def _(target):
        pl.when(jnp.logical_or(target < line, both(target == line, column == 1)))(
            lambda: side_copy(target).wait_send()
        )
        pl.when(target < line)(lambda: down_copy(target).wait_send())


def attend_back(projected, scaled, delta, kv_all):
    size = projected.shape[0]
    blocks = lax.axis_size("blk")
    rows = blocks // 2
    heads = scaled.shape[1] // HEAD
    whole = pl.BlockSpec(memory_space=pltpu.VMEM)
    return pl.pallas_call(
        functools.partial(attend_back_kernel, heads),
        out_shape=jax.ShapeDtypeStruct(projected.shape, jnp.bfloat16),
        in_specs=[whole, whole, whole, pl.BlockSpec(memory_space=pl.ANY)],
        out_specs=whole,
        scratch_shapes=[
            pltpu.VMEM((blocks, size, 2 * HEAD), jnp.bfloat16),
            pltpu.VMEM((rows, 2, size, 2 * HEAD), jnp.bfloat16),
            pltpu.VMEM((rows, size, 2 * HEAD), jnp.bfloat16),
            pltpu.VMEM((rows, size, 2 * HEAD), jnp.bfloat16),
            pltpu.VMEM((size, heads * HEAD), jnp.float32),
            pltpu.VMEM((size, HEAD), jnp.float32),
            pltpu.VMEM((size, HEAD), jnp.float32),
            pltpu.SemaphoreType.DMA((blocks,)),
            pltpu.SemaphoreType.DMA((rows,)),
            pltpu.SemaphoreType.DMA((rows,)),
            pltpu.SemaphoreType.DMA((rows,)),
            pltpu.SemaphoreType.DMA((rows,)),
        ],
        compiler_params=pltpu.CompilerParams(
            collective_id=1, has_side_effects=True, vmem_limit_bytes=VMEM_BYTES
        ),
        name="attend_back",
    )(projected, scaled, delta, kv_all)


def body(tokens, w_qkv, w_out, gains, w_ffn, cotangent):
    row_count = tokens.shape[0]
    groups = lax.axis_size("sp")
    heads_here = HEADS // groups
    kv_here = KV_HEADS // groups
    group_ratio = HEADS // KV_HEADS
    query_width = HEADS * HEAD
    score_scale = HEAD ** (-0.5)
    source = tokens.astype(jnp.float32)
    normed_in, inverse_in = norm_parts(source)
    act_in = (normed_in * gains[0]).astype(jnp.bfloat16)
    act_block = lax.all_gather(act_in, "sp", axis=0, tiled=True)
    group_cols = (group_ratio + 2) * HEAD * kv_here
    sp_at = lax.axis_index("sp")
    w_group = lax.dynamic_slice_in_dim(w_qkv, sp_at * group_cols, group_cols, 0)
    projected = contract_last(act_block, w_group).astype(jnp.bfloat16)
    block_rows = projected.shape[0]
    attended_cols, attended, totals, kv_all = attend(projected, heads_here)
    attended_low = attended_cols.reshape(block_rows, heads_here, HEAD)
    attended_tokens = lax.all_to_all(
        attended_low, "sp", split_axis=0, concat_axis=1, tiled=True
    ).reshape(row_count, query_width)
    attn = jnp.dot(attended_tokens, w_out, preferred_element_type=jnp.float32)
    normed_attn, inverse_attn = norm_parts(attn)
    middle = source + normed_attn * gains[1]
    normed_mid, inverse_mid = norm_parts(middle)
    act_ffn = (normed_mid * gains[2]).astype(jnp.bfloat16)
    w_in = w_ffn[:, :2, :]
    w_down = w_ffn[:, 2, :]
    gate_up = jnp.einsum(
        "td,fkd->tkf",
        lax.all_gather(act_ffn, "blk", axis=0, tiled=True),
        w_in,
        preferred_element_type=jnp.float32,
    )
    hidden = (gelu_value(gate_up[:, 0]) * gate_up[:, 1]).astype(jnp.bfloat16)
    hidden_all = hidden
    part = hidden_all
    ffn_out = lax.psum_scatter(
        jnp.dot(part, w_down, preferred_element_type=jnp.float32).astype(jnp.bfloat16),
        "blk",
        scatter_dimension=0,
        tiled=True,
    ).astype(jnp.float32)
    normed_ffn, inverse_ffn = norm_parts(ffn_out)
    result = middle + normed_ffn * gains[3]
    grad_out = cotangent.astype(jnp.float32)
    grad_ffn_f, gain_grad3 = norm_back(grad_out, normed_ffn, inverse_ffn, gains[3])
    grad_ffn = grad_ffn_f.astype(jnp.bfloat16)
    act_piece = lax.all_gather(act_ffn, "blk", axis=0, tiled=True)
    grad_piece = lax.all_gather(grad_ffn, "blk", axis=0, tiled=True)
    gate_up = jnp.einsum("td,fkd->tkf", act_piece, w_in, preferred_element_type=jnp.float32)
    hidden = (gelu_value(gate_up[:, 0]) * gate_up[:, 1]).astype(jnp.bfloat16)
    grad_hidden = contract_last(grad_piece, w_down)
    grad_gate = grad_hidden * gate_up[:, 1] * gelu_slope(gate_up[:, 0])
    grad_up = grad_hidden * gelu_value(gate_up[:, 0])
    grad_pair = jnp.stack([grad_gate, grad_up], axis=1).astype(jnp.bfloat16)
    in_part = jnp.einsum("tkf,td->fkd", grad_pair, act_piece, preferred_element_type=jnp.float32)
    down_part = jnp.einsum("tf,td->fd", hidden, grad_piece, preferred_element_type=jnp.float32)
    weight_sum = jnp.concatenate([in_part, down_part[:, None, :]], axis=1)
    part = grad_pair
    grad_act_ffn = lax.psum_scatter(
        jnp.einsum("tkf,fkd->td", part, w_in, preferred_element_type=jnp.float32).astype(
            jnp.bfloat16
        ),
        "blk",
        scatter_dimension=0,
        tiled=True,
    ).astype(jnp.float32)
    grad_norm_mid, gain_grad2 = norm_back(grad_act_ffn, normed_mid, inverse_mid, gains[2])
    grad_middle = grad_out + grad_norm_mid
    grad_attn_f, gain_grad1 = norm_back(grad_middle, normed_attn, inverse_attn, gains[1])
    grad_attn = grad_attn_f.astype(jnp.bfloat16)
    grad_block = lax.all_gather(grad_attn, "sp", axis=0, tiled=True)
    out_term = jnp.einsum(
        "tc,td->cd", attended_cols, grad_block, preferred_element_type=jnp.float32
    )
    out_grad = lax.psum_scatter(
        out_term.astype(jnp.bfloat16), "blk", scatter_dimension=0, tiled=True
    ).astype(jnp.float32)
    w_out_group = lax.dynamic_slice_in_dim(w_out, sp_at * heads_here * HEAD, heads_here * HEAD, 0)
    grad_heads = (
        contract_last(grad_block, w_out_group).astype(jnp.bfloat16).astype(jnp.float32)
    ).reshape(block_rows, heads_here, HEAD)
    totals_rows = jnp.transpose(totals.reshape(heads_here, block_rows))
    scaled = (grad_heads / totals_rows[..., None]).astype(jnp.bfloat16)
    row_delta = (
        jnp.sum(grad_heads * attended.reshape(block_rows, heads_here, HEAD), axis=-1) / totals_rows
    )
    grad_cols = attend_back(
        projected,
        scaled.reshape(block_rows, heads_here * HEAD),
        jnp.transpose(row_delta).reshape(heads_here, 1, block_rows),
        kv_all,
    )
    grad_proj_heads = grad_cols.reshape(block_rows, kv_here, group_ratio + 2, HEAD)
    qkv_term = jnp.einsum("tc,td->cd", grad_cols, act_block, preferred_element_type=jnp.float32)
    qkv_grad = lax.psum_scatter(
        qkv_term.astype(jnp.bfloat16), "blk", scatter_dimension=0, tiled=True
    ).astype(jnp.float32)
    grad_proj_tokens = lax.all_to_all(grad_proj_heads, "sp", split_axis=0, concat_axis=1, tiled=True)
    grad_projected = grad_proj_tokens.reshape(row_count, w_qkv.shape[0])
    grad_act_in = jnp.dot(grad_projected, w_qkv, preferred_element_type=jnp.float32)
    grad_source, gain_grad0 = norm_back(grad_act_in, normed_in, inverse_in, gains[0])
    tokens_grad = (grad_middle + grad_source).astype(jnp.bfloat16)
    gains_term = jnp.stack([gain_grad0, gain_grad1, gain_grad2, gain_grad3], axis=0)
    ffn_grad = lax.psum_scatter(
        weight_sum.astype(jnp.bfloat16), "sp", scatter_dimension=0, tiled=True
    ).astype(jnp.float32)
    gains_part = lax.psum_scatter(gains_term, "sp", scatter_dimension=1, tiled=True)
    gains_grad = lax.psum_scatter(gains_part, "blk", scatter_dimension=1, tiled=True)
    return (result.astype(jnp.bfloat16), tokens_grad, qkv_grad, out_grad, gains_grad, ffn_grad)


def solution(mesh):
    return jax.shard_map(
        body,
        mesh=mesh,
        in_specs=(
            P(("blk", "sp"), None),
            P(),
            P(),
            P(),
            P("blk", None, None),
            P(("blk", "sp"), None),
        ),
        out_specs=(
            P(("blk", "sp"), None),
            P(("blk", "sp"), None),
            P(("sp", "blk"), None),
            P(("sp", "blk"), None),
            P(None, ("sp", "blk")),
            P(("blk", "sp"), None, None),
        ),
        check_vma=False,
    )
```

```python
import functools

import jax
import jax.numpy as jnp
from jax import lax
from jax.experimental import pallas as pl
from jax.experimental.pallas import tpu as pltpu
from jax.sharding import PartitionSpec as P

HEADS = 8
KV_HEADS = 4
HEAD = 256


VMEM_BYTES = 62 * 1024 * 1024
NORM_EPSILON = 1e-06
CAP_VALUE = 50.0
GELU_SCALE = 0.7978845608028654
GELU_CUBIC = 0.044715


def norm_parts(values):
    inverse = lax.rsqrt(jnp.mean(values * values, axis=-1, keepdims=True) + NORM_EPSILON)
    return (values * inverse, inverse)


def norm_back(grad_y, normed, inverse, gain):
    grad_n = grad_y * gain
    grad_v = inverse * (grad_n - normed * jnp.mean(grad_n * normed, axis=-1, keepdims=True))
    return (grad_v, jnp.sum(grad_y * normed, axis=0))


def gelu_value(values):
    return (
        0.5
        * values
        * (1.0 + jnp.tanh(GELU_SCALE * (values + GELU_CUBIC * values * values * values)))
    )


def gelu_slope(values):
    bent = jnp.tanh(GELU_SCALE * (values + GELU_CUBIC * values * values * values))
    return 0.5 * (1.0 + bent) + 0.5 * values * (1.0 - bent * bent) * GELU_SCALE * (
        1.0 + 3.0 * GELU_CUBIC * values * values
    )


def contract_last(left, right):
    return lax.dot_general(
        left, right, (((1,), (1,)), ((), ())), preferred_element_type=jnp.float32
    )


def push(source, target, sent, landed, block):
    return pltpu.make_async_remote_copy(
        src_ref=source,
        dst_ref=target,
        send_sem=sent,
        recv_sem=landed,
        device_id={"blk": block},
        device_id_type=pl.DeviceIdType.MESH,
    )


def greet(at, line, rows):
    barrier = pltpu.get_barrier_semaphore()

    def tell(block):
        pl.semaphore_signal(
            barrier, inc=1, device_id={"blk": block}, device_id_type=pl.DeviceIdType.MESH
        )

    tell(at + 1 - 2 * (at % 2))
    pl.when(line > 0)(lambda: tell(at - 2))
    pl.when(line < rows - 1)(lambda: tell(at + 2))
    pl.semaphore_wait(barrier, 1 + jnp.minimum(line, 1) + jnp.minimum(rows - 1 - line, 1))


def both(*terms):
    result = terms[0]
    for term in terms[1:]:
        result = jnp.logical_and(result, term)
    return result


def attend_kernel(
    heads,
    x_ref,
    low_ref,
    att_ref,
    tot_ref,
    kv_ref,
    kv,
    acc,
    part,
    up_sent,
    up_landed,
    side_sent,
    side_landed,
    own_done,
    save_done,
):
    at = lax.axis_index("blk")
    blocks = lax.axis_size("blk")
    rows = blocks // 2
    line, column = at // 2, at % 2
    partner = at + 1 - 2 * column
    size = x_ref.shape[0]
    first = heads * HEAD
    own = x_ref.at[:, pl.ds(first, 2 * HEAD)]
    greet(at, line, rows)

    def up_copy(index, source):
        return push(source, kv.at[index], up_sent.at[index // 2], up_landed.at[index // 2], at + 2)

    def side_copy(index, source):
        return push(
            source, kv.at[index], side_sent.at[index // 2], side_landed.at[index // 2], partner
        )

    def save(index):
        return pltpu.make_async_copy(kv.at[index], kv_ref.at[index], save_done.at[index])

    pl.when(line < rows - 1)(lambda: up_copy(at, own).start())
    pl.when(column == 0)(lambda: side_copy(at, own).start())
    keep = pltpu.make_async_copy(own, kv.at[at], own_done)
    keep.start()
    acc[...] = jnp.zeros_like(acc)
    part[...] = jnp.zeros_like(part)
    keep.wait()
    ahead = lax.broadcasted_iota(jnp.int32, (size, size), 1) - lax.broadcasted_iota(
        jnp.int32, (size, size), 0
    )

    def compute(index):
        save(index).start()
        span = (at - index) * size
        for head in range(heads):
            raw = lax.dot_general(
                x_ref[:, head * HEAD : (head + 1) * HEAD],
                kv[index, :, :HEAD],
                (((1,), (1,)), ((), ())),
                preferred_element_type=jnp.float32,
            )
            weights = jnp.exp(CAP_VALUE * jnp.tanh(raw * (HEAD ** (-0.5) / CAP_VALUE)))
            weights = jnp.where(ahead <= span, weights, 0.0)
            total = weights[:, :128]
            for piece in range(1, size // 128):
                total = total + weights[:, piece * 128 : (piece + 1) * 128]
            part[head] += total
            acc[:, head * HEAD : (head + 1) * HEAD] += jnp.dot(
                weights.astype(jnp.bfloat16),
                kv[index, :, HEAD:],
                preferred_element_type=jnp.float32,
            )

    @pl.loop(0, rows + 1)
    def _(step):
        source = line - step
        index = 2 * source + column

        @pl.when(both(step > 0, source >= 0))
        def _():
            up_copy(index, kv.at[index]).wait_recv()
            pl.when(line < rows - 1)(lambda: up_copy(index, kv.at[index]).start())
            side_copy(index, kv.at[index]).start()

        pl.when(source >= 0)(lambda: compute(index))
        other = 2 * (source + 1) + 1 - column

        @pl.when(both(step > 0, source + 1 >= 0, jnp.logical_or(step > 1, column == 1)))
        def _():
            side_copy(other, kv.at[other]).wait_recv()
            compute(other)

    for head in range(heads):
        columns = slice(head * HEAD, (head + 1) * HEAD)
        total = jnp.sum(part[head], axis=1, keepdims=True)
        value = acc[:, columns] / total
        att_ref[:, columns] = value
        low_ref[:, columns] = value.astype(jnp.bfloat16)
        tot_ref[head] = jnp.sum(part[head].T, axis=0, keepdims=True)

    @pl.loop(0, rows)
    def _(source):
        index = 2 * source + column

        @pl.when(source <= line)
        def _():
            pl.when(line < rows - 1)(lambda: up_copy(index, kv.at[index]).wait_send())
            pl.when(jnp.logical_or(source < line, column == 0))(
                lambda: side_copy(index, kv.at[index]).wait_send()
            )

    @pl.loop(0, blocks)
    def _(index):
        pl.when(index <= at)(lambda: save(index).wait())


def attend(projected, heads):
    size = projected.shape[0]
    blocks = lax.axis_size("blk")
    whole = pl.BlockSpec(memory_space=pltpu.VMEM)
    return pl.pallas_call(
        functools.partial(attend_kernel, heads),
        out_shape=(
            jax.ShapeDtypeStruct((size, heads * HEAD), jnp.bfloat16),
            jax.ShapeDtypeStruct((size, heads * HEAD), jnp.float32),
            jax.ShapeDtypeStruct((heads, 1, size), jnp.float32),
            jax.ShapeDtypeStruct((blocks, size, 2 * HEAD), jnp.bfloat16),
        ),
        in_specs=[whole],
        out_specs=(whole, whole, whole, pl.BlockSpec(memory_space=pl.ANY)),
        scratch_shapes=[
            pltpu.VMEM((blocks, size, 2 * HEAD), jnp.bfloat16),
            pltpu.VMEM((size, heads * HEAD), jnp.float32),
            pltpu.VMEM((heads, size, 128), jnp.float32),
            pltpu.SemaphoreType.DMA((blocks // 2,)),
            pltpu.SemaphoreType.DMA((blocks // 2,)),
            pltpu.SemaphoreType.DMA((blocks // 2,)),
            pltpu.SemaphoreType.DMA((blocks // 2,)),
            pltpu.SemaphoreType.DMA,
            pltpu.SemaphoreType.DMA((blocks,)),
        ],
        compiler_params=pltpu.CompilerParams(
            collective_id=0, has_side_effects=True, vmem_limit_bytes=VMEM_BYTES
        ),
        name="attend",
    )(projected)


def attend_back_kernel(
    heads,
    x_ref,
    scaled_ref,
    delta_ref,
    kv_ref,
    out_ref,
    kv,
    part,
    side,
    down,
    dq,
    dk,
    dv,
    load_done,
    side_sent,
    side_landed,
    down_sent,
    down_landed,
):
    at = lax.axis_index("blk")
    blocks = lax.axis_size("blk")
    rows = blocks // 2
    line, column = at // 2, at % 2
    partner = at + 1 - 2 * column
    size = x_ref.shape[0]

    def load(index):
        return pltpu.make_async_copy(kv_ref.at[index], kv.at[index], load_done.at[index])

    @pl.loop(0, blocks)
    def _(index):
        pl.when(index <= at)(lambda: load(index).start())

    greet(at, line, rows)

    def side_copy(target):
        return push(
            part.at[target, 1 - column],
            side.at[target],
            side_sent.at[target],
            side_landed.at[target],
            partner,
        )

    def down_copy(target):
        return push(
            part.at[target, column],
            down.at[target],
            down_sent.at[target],
            down_landed.at[target],
            at - 2,
        )

    dq[...] = jnp.zeros_like(dq)
    ahead = lax.broadcasted_iota(jnp.int32, (size, size), 0) - lax.broadcasted_iota(
        jnp.int32, (size, size), 1
    )

    def compute(target, half):
        index = 2 * target + half
        load(index).wait()
        span = (at - index) * size
        for head in range(heads):
            columns = slice(head * HEAD, (head + 1) * HEAD)
            query = x_ref[:, columns]
            scaled = scaled_ref[:, columns]
            key = kv[index, :, :HEAD]
            raw = lax.dot_general(
                key, query, (((1,), (1,)), ((), ())), preferred_element_type=jnp.float32
            )
            squashed = jnp.tanh(raw * (HEAD ** (-0.5) / CAP_VALUE))
            weights = jnp.exp(CAP_VALUE * squashed)
            weights = jnp.where(ahead <= span, weights, 0.0)
            inner = lax.dot_general(
                kv[index, :, HEAD:],
                scaled,
                (((1,), (1,)), ((), ())),
                preferred_element_type=jnp.float32,
            )
            grad_raw = (
                weights * (inner - delta_ref[head]) * (1.0 - squashed * squashed)
            ).astype(jnp.bfloat16)
            dv_now = jnp.dot(
                weights.astype(jnp.bfloat16), scaled, preferred_element_type=jnp.float32
            )
            dk_now = jnp.dot(grad_raw, query, preferred_element_type=jnp.float32)
            dq[:, columns] += lax.dot_general(
                grad_raw, key, (((0,), (0,)), ((), ())), preferred_element_type=jnp.float32
            )
            if head == 0:
                dv[...] = dv_now
                dk[...] = dk_now
            else:
                dv[...] += dv_now
                dk[...] += dk_now
        part[target, half, :, :HEAD] = (dk[...] * HEAD ** (-0.5)).astype(jnp.bfloat16)
        part[target, half, :, HEAD:] = dv[...].astype(jnp.bfloat16)

    def merge(target):
        last = target == line

        @pl.when(jnp.logical_or(target < line, column == 0))
        def _():
            side_copy(target).wait_recv()
            part[target, column] = (
                part[target, column].astype(jnp.float32) + side[target].astype(jnp.float32)
            ).astype(jnp.bfloat16)

        @pl.when(line < rows - 1)
        def _():
            down_copy(target).wait_recv()
            part[target, column] = (
                part[target, column].astype(jnp.float32) + down[target].astype(jnp.float32)
            ).astype(jnp.bfloat16)

        pl.when(target < line)(lambda: down_copy(target).start())

        @pl.when(last)
        def _():
            out_ref[:, heads * HEAD :] = part[target, column]

    @pl.loop(0, rows)
    def _(target):
        @pl.when(jnp.logical_or(target < line, both(target == line, column == 1)))
        def _():
            compute(target, 1 - column)
            side_copy(target).start()

        pl.when(target <= line)(lambda: compute(target, column))
        pl.when(both(line == rows - 1, target > 0))(lambda: merge(target - 1))

    out_ref[:, : heads * HEAD] = (dq[...] * HEAD ** (-0.5)).astype(jnp.bfloat16)

    @pl.loop(0, rows)
    def _(target):
        pl.when(both(target <= line, jnp.logical_or(line < rows - 1, target == rows - 1)))(
            lambda: merge(target)
        )

    @pl.loop(0, rows)
    def _(target):
        pl.when(jnp.logical_or(target < line, both(target == line, column == 1)))(
            lambda: side_copy(target).wait_send()
        )
        pl.when(target < line)(lambda: down_copy(target).wait_send())


def attend_back(projected, scaled, delta, kv_all):
    size = projected.shape[0]
    blocks = lax.axis_size("blk")
    rows = blocks // 2
    heads = scaled.shape[1] // HEAD
    whole = pl.BlockSpec(memory_space=pltpu.VMEM)
    return pl.pallas_call(
        functools.partial(attend_back_kernel, heads),
        out_shape=jax.ShapeDtypeStruct(projected.shape, jnp.bfloat16),
        in_specs=[whole, whole, whole, pl.BlockSpec(memory_space=pl.ANY)],
        out_specs=whole,
        scratch_shapes=[
            pltpu.VMEM((blocks, size, 2 * HEAD), jnp.bfloat16),
            pltpu.VMEM((rows, 2, size, 2 * HEAD), jnp.bfloat16),
            pltpu.VMEM((rows, size, 2 * HEAD), jnp.bfloat16),
            pltpu.VMEM((rows, size, 2 * HEAD), jnp.bfloat16),
            pltpu.VMEM((size, heads * HEAD), jnp.float32),
            pltpu.VMEM((size, HEAD), jnp.float32),
            pltpu.VMEM((size, HEAD), jnp.float32),
            pltpu.SemaphoreType.DMA((blocks,)),
            pltpu.SemaphoreType.DMA((rows,)),
            pltpu.SemaphoreType.DMA((rows,)),
            pltpu.SemaphoreType.DMA((rows,)),
            pltpu.SemaphoreType.DMA((rows,)),
        ],
        compiler_params=pltpu.CompilerParams(
            collective_id=1, has_side_effects=True, vmem_limit_bytes=VMEM_BYTES
        ),
        name="attend_back",
    )(projected, scaled, delta, kv_all)


def line_gather(own_ref, full, line_sent, line_landed, side_sent, side_landed, own_done, work):
    at = lax.axis_index("blk")
    rows = lax.axis_size("blk") // 2
    line, column = at // 2, at % 2
    size = own_ref.shape[0]

    def spot(source, side):
        start = pl.multiple_of((2 * source + side) * size, size)
        return full.at[pl.ds(start, size), :]

    def line_copy(source, sign, first=False):
        return push(
            own_ref if first else spot(source, column),
            spot(source, column),
            line_sent.at[(sign + 1) // 2, source],
            line_landed.at[source],
            at + 2 * sign,
        )

    def side_copy(source, side, first=False):
        return push(
            own_ref if first else spot(source, side),
            spot(source, side),
            side_sent.at[source],
            side_landed.at[source],
            at + 1 - 2 * column,
        )

    def inside(row):
        return jnp.logical_and(row >= 0, row < rows)

    pl.when(line < rows - 1)(lambda: line_copy(line, 1, True).start())
    pl.when(line > 0)(lambda: line_copy(line, -1, True).start())
    side_copy(line, column, True).start()
    keep = pltpu.make_async_copy(own_ref, spot(line, column), own_done)
    keep.start()
    keep.wait()

    @pl.loop(0, rows + 1)
    def _(step):
        for sign in (-1, 1):
            source = line - sign * step

            @pl.when(both(step > 0, inside(source)))
            def _():
                line_copy(source, sign).wait_recv()
                pl.when(inside(line + sign))(lambda: line_copy(source, sign).start())
                side_copy(source, column).start()

        for sign in (-1, 1):
            source = line - sign * (step - 1)
            once = step > 0 if sign == -1 else step > 1

            @pl.when(both(once, inside(source)))
            def _():
                side_copy(source, 1 - column).wait_recv()
                work(source)

    @pl.loop(0, rows)
    def _(source):
        pl.when(both(source <= line, line < rows - 1))(lambda: line_copy(source, 1).wait_send())
        pl.when(both(source >= line, line > 0))(lambda: line_copy(source, -1).wait_send())
        side_copy(source, column).wait_send()


def line_scatter(part, side, lane, out_ref, side_sent, side_landed, lane_sent, lane_landed, work, fill):
    at = lax.axis_index("blk")
    rows = lax.axis_size("blk") // 2
    line, column = at // 2, at % 2
    size = out_ref.shape[0]

    def spot(target, half):
        start = pl.multiple_of((2 * target + half) * size, size)
        return pl.ds(start, size)

    def side_copy(target):
        return push(
            part.at[spot(target, 1 - column), :],
            side.at[target],
            side_sent.at[target],
            side_landed.at[target],
            at + 1 - 2 * column,
        )

    def lane_copy(target, sign):
        slot = target if sign == 1 else jnp.where(target == line - 1, rows, target)
        return push(
            part.at[spot(target, column), :],
            lane.at[slot],
            lane_sent.at[target],
            lane_landed.at[slot],
            at + 2 * sign,
        )

    def lane_wait(slot):
        push(
            lane.at[slot], lane.at[slot], lane_sent.at[0], lane_landed.at[slot], at + 1 - 2 * column
        ).wait_recv()

    def inside(row):
        return jnp.logical_and(row >= 0, row < rows)

    @pl.loop(0, rows)
    def _(step):
        for sign in (-1, 1):
            target = line + sign * (rows - 1 - step)
            once = step >= 0 if sign == -1 else step < rows - 1

            @pl.when(both(once, inside(target)))
            def _():
                work(target)
                side_copy(target).start()

    def merge(target):
        mine = spot(target, column)
        side_copy(target).wait_recv()
        part[mine, :] = (
            part[mine, :].astype(jnp.float32) + side[target].astype(jnp.float32)
        ).astype(jnp.bfloat16)

        def pass_on(sign):
            @pl.when(inside(line - sign))
            def _():
                lane_wait(target)
                part[mine, :] = (
                    part[mine, :].astype(jnp.float32) + lane[target].astype(jnp.float32)
                ).astype(jnp.bfloat16)

            lane_copy(target, sign).start()

        pl.when(target > line)(lambda: pass_on(1))
        pl.when(target < line)(lambda: pass_on(-1))

    @pl.loop(0, rows)
    def _(step):
        fill(step)
        for sign in (-1, 1):
            target = line + sign * (rows - 1 - step)
            once = step >= 0 if sign == -1 else step < rows - 1
            pl.when(both(once, inside(target)))(lambda: merge(target))

    mine = spot(line, column)
    out_ref[...] = part[mine, :].astype(jnp.float32)

    @pl.when(line > 0)
    def _():
        lane_wait(line)
        out_ref[...] += lane[line].astype(jnp.float32)

    @pl.when(line < rows - 1)
    def _():
        lane_wait(rows)
        out_ref[...] += lane[rows].astype(jnp.float32)

    @pl.loop(0, rows)
    def _(target):
        side_copy(target).wait_send()
        pl.when(target > line)(lambda: lane_copy(target, 1).wait_send())
        pl.when(target < line)(lambda: lane_copy(target, -1).wait_send())


def line_sems(rows):
    dma = pltpu.SemaphoreType.DMA
    return [dma((2, rows)), dma((rows,)), dma((rows,)), dma((rows,)), dma]


def lane_sems(rows):
    dma = pltpu.SemaphoreType.DMA
    return [dma((rows,)), dma((rows,)), dma((rows,)), dma((rows + 1,))]


def ffn_kernel(
    act_ref,
    w_ref,
    out_ref,
    acts_ref,
    w,
    acts,
    hidden,
    part,
    side,
    lane,
    w_done,
    save_done,
    *sems,
):
    at = lax.axis_index("blk")
    rows = lax.axis_size("blk") // 2
    pair = 2 * act_ref.shape[0]

    def load(which):
        return pltpu.make_async_copy(w_ref.at[which], w.at[which], w_done.at[which])

    def pair_rows(source):
        return pl.ds(pl.multiple_of(source * pair, pair), pair)

    def save(source):
        return pltpu.make_async_copy(
            acts.at[pair_rows(source), :], acts_ref.at[pair_rows(source), :], save_done.at[source]
        )

    for which in range(3):
        load(which).start()
    greet(at, at // 2, rows)
    for which in range(3):
        load(which).wait()

    def expand(source):
        save(source).start()
        rows_now = acts[pair_rows(source), :]
        gate = contract_last(w[0], rows_now)
        up = contract_last(w[1], rows_now)
        hidden[source] = (gelu_value(gate) * up).astype(jnp.bfloat16)

    def reduce(target):
        part[pair_rows(target), :] = lax.dot_general(
            hidden[target], w[2], (((0,), (0,)), ((), ())), preferred_element_type=jnp.float32
        ).astype(jnp.bfloat16)

    line_gather(act_ref, acts, *sems[:5], expand)
    line_scatter(part, side, lane, out_ref, *sems[5:], reduce, lambda step: None)
    pl.loop(0, rows)(lambda source: save(source).wait())


def ffn_forward(act_ffn, w_parts):
    size, width = act_ffn.shape
    units = w_parts.shape[1]
    blocks = lax.axis_size("blk")
    rows = blocks // 2
    whole = pl.BlockSpec(memory_space=pltpu.VMEM)
    far = pl.BlockSpec(memory_space=pl.ANY)
    return pl.pallas_call(
        ffn_kernel,
        out_shape=(
            jax.ShapeDtypeStruct((size, width), jnp.float32),
            jax.ShapeDtypeStruct((blocks * size, width), jnp.bfloat16),
        ),
        in_specs=[whole, far],
        out_specs=(whole, far),
        scratch_shapes=[
            pltpu.VMEM(w_parts.shape, jnp.bfloat16),
            pltpu.VMEM((blocks * size, width), jnp.bfloat16),
            pltpu.VMEM((rows, units, 2 * size), jnp.bfloat16),
            pltpu.VMEM((blocks * size, width), jnp.bfloat16),
            pltpu.VMEM((rows, size, width), jnp.bfloat16),
            pltpu.VMEM((rows + 1, size, width), jnp.bfloat16),
            pltpu.SemaphoreType.DMA((3,)),
            pltpu.SemaphoreType.DMA((rows,)),
            *line_sems(rows),
            *lane_sems(rows),
        ],
        compiler_params=pltpu.CompilerParams(
            collective_id=2, has_side_effects=True, vmem_limit_bytes=VMEM_BYTES
        ),
        name="ffn_forward",
    )(act_ffn, w_parts)


FILL_COLUMNS = 256
FILL_FIRST = 3


def ffn_back_kernel(
    owners,
    grad_ref,
    acts_ref,
    w_ref,
    out_ref,
    sum_ref,
    w,
    rights,
    lefts,
    part,
    side,
    lane,
    stage,
    w_done,
    acts_done,
    stage_done,
    *sems,
):
    at = lax.axis_index("blk")
    rows = lax.axis_size("blk") // 2
    size, width = grad_ref.shape
    pair = 2 * size
    units = w.shape[1]
    acts, grads = rights.at[0], rights.at[1]

    def load(which):
        return pltpu.make_async_copy(w_ref.at[which], w.at[which], w_done.at[which])

    def pair_rows(source):
        return pl.ds(pl.multiple_of(source * pair, pair), pair)

    acts_copy = pltpu.make_async_copy(acts_ref, acts, acts_done)
    acts_copy.start()
    for which in range(3):
        load(which).start()
    greet(at, at // 2, rows)
    acts_copy.wait()
    for which in range(3):
        load(which).wait()

    def expand(source):
        columns = pair_rows(source)
        rows_now = acts[pair_rows(source), :]
        gate = contract_last(w[0], rows_now)
        up = contract_last(w[1], rows_now)
        grad_hidden = contract_last(w[2], grads[pair_rows(source), :])
        bent = jnp.tanh(GELU_SCALE * (gate + GELU_CUBIC * gate * gate * gate))
        value = 0.5 * gate * (1.0 + bent)
        slope = 0.5 * (1.0 + bent) + 0.5 * gate * (1.0 - bent * bent) * GELU_SCALE * (
            1.0 + 3.0 * GELU_CUBIC * gate * gate
        )
        lefts[2, :, columns] = (value * up).astype(jnp.bfloat16)
        lefts[0, :, columns] = (grad_hidden * up * slope).astype(jnp.bfloat16)
        lefts[1, :, columns] = (grad_hidden * value).astype(jnp.bfloat16)

    def reduce(target):
        columns = pair_rows(target)
        dims = (((0,), (0,)), ((), ()))
        total = lax.dot_general(
            lefts[0, :, columns], w[0], dims, preferred_element_type=jnp.float32
        ) + lax.dot_general(lefts[1, :, columns], w[1], dims, preferred_element_type=jnp.float32)
        part[pair_rows(target), :] = total.astype(jnp.bfloat16)

    pieces = width // FILL_COLUMNS
    total_pieces = 3 * pieces

    def piece_columns(item):
        return pl.ds(pl.multiple_of((item % pieces) * FILL_COLUMNS, FILL_COLUMNS), FILL_COLUMNS)

    def stage_copy(item):
        return pltpu.make_async_copy(
            stage.at[item % 2],
            sum_ref.at[:, item // pieces, :, piece_columns(item)],
            stage_done.at[item % 2],
        )

    def fill_one(item):
        which = item // pieces
        total = jnp.dot(
            lefts[which],
            rights[which // 2, :, piece_columns(item)],
            preferred_element_type=jnp.float32,
        )
        pl.when(item > 1)(lambda: stage_copy(item - 2).wait())
        stage[item % 2] = total.astype(jnp.bfloat16).reshape(
            owners, units // owners, FILL_COLUMNS
        )
        stage_copy(item).start()

    each = pl.cdiv(total_pieces - FILL_FIRST, rows - 1)

    def fill(step):
        first = jnp.maximum(FILL_FIRST + (step - 1) * each, 0)
        last = jnp.minimum(FILL_FIRST + step * each, total_pieces)

        @pl.loop(0, each)
        def _(item):
            pl.when(first + item < last)(lambda: fill_one(first + item))

    line_gather(grad_ref, grads, *sems[:5], expand)
    line_scatter(part, side, lane, out_ref, *sems[5:], reduce, fill)
    stage_copy(total_pieces - 2).wait()
    stage_copy(total_pieces - 1).wait()


def ffn_back(grad_ffn, acts, w_parts, owners):
    size, width = grad_ffn.shape
    units = w_parts.shape[1]
    blocks = lax.axis_size("blk")
    rows = blocks // 2
    tokens = blocks * size
    whole = pl.BlockSpec(memory_space=pltpu.VMEM)
    far = pl.BlockSpec(memory_space=pl.ANY)
    return pl.pallas_call(
        functools.partial(ffn_back_kernel, owners),
        out_shape=(
            jax.ShapeDtypeStruct((size, width), jnp.float32),
            jax.ShapeDtypeStruct((owners, 3, units // owners, width), jnp.bfloat16),
        ),
        in_specs=[whole, far, far],
        out_specs=(whole, far),
        scratch_shapes=[
            pltpu.VMEM(w_parts.shape, jnp.bfloat16),
            pltpu.VMEM((2, tokens, width), jnp.bfloat16),
            pltpu.VMEM((3, units, tokens), jnp.bfloat16),
            pltpu.VMEM((tokens, width), jnp.bfloat16),
            pltpu.VMEM((rows, size, width), jnp.bfloat16),
            pltpu.VMEM((rows + 1, size, width), jnp.bfloat16),
            pltpu.VMEM((2, owners, units // owners, FILL_COLUMNS), jnp.bfloat16),
            pltpu.SemaphoreType.DMA((3,)),
            pltpu.SemaphoreType.DMA,
            pltpu.SemaphoreType.DMA((2,)),
            *line_sems(rows),
            *lane_sems(rows),
        ],
        compiler_params=pltpu.CompilerParams(
            collective_id=3, has_side_effects=True, vmem_limit_bytes=VMEM_BYTES
        ),
        name="ffn_back",
    )(grad_ffn, acts, w_parts)


def ffn_hidden(acts, w_parts):
    gate = contract_last(acts, w_parts[0])
    up = contract_last(acts, w_parts[1])
    return (gate, up, (gelu_value(gate) * up).astype(jnp.bfloat16))


def scatter_tokens(partial):
    return lax.psum_scatter(
        partial.astype(jnp.bfloat16), "blk", scatter_dimension=0, tiled=True
    ).astype(jnp.float32)


def ffn_forward_wide(act_ffn, w_parts):
    acts = lax.all_gather(act_ffn, "blk", axis=0, tiled=True)
    hidden = ffn_hidden(acts, w_parts)[2]
    partial = jnp.dot(hidden, w_parts[2], preferred_element_type=jnp.float32)
    return (scatter_tokens(partial), acts)


def ffn_back_wide(grad_ffn, acts, w_parts, owners):
    grads = lax.all_gather(grad_ffn, "blk", axis=0, tiled=True)
    gate, up, hidden = ffn_hidden(acts, w_parts)
    grad_hidden = contract_last(grads, w_parts[2])
    grad_gate = (grad_hidden * up * gelu_slope(gate)).astype(jnp.bfloat16)
    grad_up = (grad_hidden * gelu_value(gate)).astype(jnp.bfloat16)
    partial = jnp.dot(grad_gate, w_parts[0], preferred_element_type=jnp.float32) + jnp.dot(
        grad_up, w_parts[1], preferred_element_type=jnp.float32
    )
    sums = jnp.stack(
        [
            jnp.einsum("tf,td->fd", left, right, preferred_element_type=jnp.float32)
            for left, right in ((grad_gate, acts), (grad_up, acts), (hidden, grads))
        ]
    ).astype(jnp.bfloat16)
    units = w_parts.shape[1]
    owned = sums.reshape(3, owners, units // owners, sums.shape[2])
    return (scatter_tokens(partial), jnp.transpose(owned, (1, 0, 2, 3)))


def body(tokens, w_qkv, w_out, gains, w_ffn, cotangent):
    row_count = tokens.shape[0]
    groups = lax.axis_size("sp")
    heads_here = HEADS // groups
    kv_here = KV_HEADS // groups
    group_ratio = HEADS // KV_HEADS
    query_width = HEADS * HEAD
    score_scale = HEAD ** (-0.5)
    source = tokens.astype(jnp.float32)
    normed_in, inverse_in = norm_parts(source)
    act_in = (normed_in * gains[0]).astype(jnp.bfloat16)
    act_block = lax.all_gather(act_in, "sp", axis=0, tiled=True)
    group_cols = (group_ratio + 2) * HEAD * kv_here
    sp_at = lax.axis_index("sp")
    w_group = lax.dynamic_slice_in_dim(w_qkv, sp_at * group_cols, group_cols, 0)
    projected = contract_last(act_block, w_group).astype(jnp.bfloat16)
    block_rows = projected.shape[0]
    attended_cols, attended, totals, kv_all = attend(projected, heads_here)
    attended_low = attended_cols.reshape(block_rows, heads_here, HEAD)
    attended_tokens = lax.all_to_all(
        attended_low, "sp", split_axis=0, concat_axis=1, tiled=True
    ).reshape(row_count, query_width)
    attn = jnp.dot(attended_tokens, w_out, preferred_element_type=jnp.float32)
    normed_attn, inverse_attn = norm_parts(attn)
    middle = source + normed_attn * gains[1]
    normed_mid, inverse_mid = norm_parts(middle)
    act_ffn = (normed_mid * gains[2]).astype(jnp.bfloat16)
    wide = lax.axis_size("blk") > 8
    w_parts = jnp.transpose(w_ffn, (1, 0, 2))
    ffn_out, act_all = (ffn_forward_wide if wide else ffn_forward)(act_ffn, w_parts)
    normed_ffn, inverse_ffn = norm_parts(ffn_out)
    result = middle + normed_ffn * gains[3]
    grad_out = cotangent.astype(jnp.float32)
    grad_ffn_f, gain_grad3 = norm_back(grad_out, normed_ffn, inverse_ffn, gains[3])
    grad_ffn = grad_ffn_f.astype(jnp.bfloat16)
    grad_act_ffn, ffn_sums = (ffn_back_wide if wide else ffn_back)(
        grad_ffn, act_all, w_parts, groups
    )
    grad_norm_mid, gain_grad2 = norm_back(grad_act_ffn, normed_mid, inverse_mid, gains[2])
    grad_middle = grad_out + grad_norm_mid
    grad_attn_f, gain_grad1 = norm_back(grad_middle, normed_attn, inverse_attn, gains[1])
    grad_attn = grad_attn_f.astype(jnp.bfloat16)
    grad_block = lax.all_gather(grad_attn, "sp", axis=0, tiled=True)
    out_term = jnp.einsum(
        "tc,td->cd", attended_cols, grad_block, preferred_element_type=jnp.float32
    )
    out_grad = lax.psum_scatter(
        out_term.astype(jnp.bfloat16), "blk", scatter_dimension=0, tiled=True
    ).astype(jnp.float32)
    w_out_group = lax.dynamic_slice_in_dim(w_out, sp_at * heads_here * HEAD, heads_here * HEAD, 0)
    grad_heads = (
        contract_last(grad_block, w_out_group).astype(jnp.bfloat16).astype(jnp.float32)
    ).reshape(block_rows, heads_here, HEAD)
    totals_rows = jnp.transpose(totals.reshape(heads_here, block_rows))
    scaled = (grad_heads / totals_rows[..., None]).astype(jnp.bfloat16)
    row_delta = (
        jnp.sum(grad_heads * attended.reshape(block_rows, heads_here, HEAD), axis=-1) / totals_rows
    )
    grad_cols = attend_back(
        projected,
        scaled.reshape(block_rows, heads_here * HEAD),
        jnp.transpose(row_delta).reshape(heads_here, 1, block_rows),
        kv_all,
    )
    grad_proj_heads = grad_cols.reshape(block_rows, kv_here, group_ratio + 2, HEAD)
    qkv_term = jnp.einsum("tc,td->cd", grad_cols, act_block, preferred_element_type=jnp.float32)
    qkv_grad = lax.psum_scatter(
        qkv_term.astype(jnp.bfloat16), "blk", scatter_dimension=0, tiled=True
    ).astype(jnp.float32)
    grad_proj_tokens = lax.all_to_all(grad_proj_heads, "sp", split_axis=0, concat_axis=1, tiled=True)
    grad_projected = grad_proj_tokens.reshape(row_count, w_qkv.shape[0])
    grad_act_in = jnp.dot(grad_projected, w_qkv, preferred_element_type=jnp.float32)
    grad_source, gain_grad0 = norm_back(grad_act_in, normed_in, inverse_in, gains[0])
    tokens_grad = (grad_middle + grad_source).astype(jnp.bfloat16)
    gains_term = jnp.stack([gain_grad0, gain_grad1, gain_grad2, gain_grad3], axis=0)
    ffn_part = lax.psum_scatter(ffn_sums, "sp", scatter_dimension=0, tiled=True)
    ffn_grad = jnp.transpose(ffn_part[0].astype(jnp.float32), (1, 0, 2))
    gains_part = lax.psum_scatter(gains_term, "sp", scatter_dimension=1, tiled=True)
    gains_grad = lax.psum_scatter(gains_part, "blk", scatter_dimension=1, tiled=True)
    return (result.astype(jnp.bfloat16), tokens_grad, qkv_grad, out_grad, gains_grad, ffn_grad)


def solution(mesh):
    return jax.shard_map(
        body,
        mesh=mesh,
        in_specs=(
            P(("blk", "sp"), None),
            P(),
            P(),
            P(),
            P("blk", None, None),
            P(("blk", "sp"), None),
        ),
        out_specs=(
            P(("blk", "sp"), None),
            P(("blk", "sp"), None),
            P(("sp", "blk"), None),
            P(("sp", "blk"), None),
            P(None, ("sp", "blk")),
            P(("blk", "sp"), None, None),
        ),
        check_vma=False,
    )
```

```python
import functools

import jax
import jax.numpy as jnp
from jax import lax
from jax.experimental import pallas as pl
from jax.experimental.pallas import tpu as pltpu
from jax.sharding import PartitionSpec as P

HEADS = 8
KV_HEADS = 4
HEAD = 256


VMEM_BYTES = 62 * 1024 * 1024
NORM_EPSILON = 1e-06
CAP_VALUE = 50.0
GELU_SCALE = 0.7978845608028654
GELU_CUBIC = 0.044715


def norm_parts(values):
    inverse = lax.rsqrt(jnp.mean(values * values, axis=-1, keepdims=True) + NORM_EPSILON)
    return (values * inverse, inverse)


def norm_back(grad_y, normed, inverse, gain):
    grad_n = grad_y * gain
    grad_v = inverse * (grad_n - normed * jnp.mean(grad_n * normed, axis=-1, keepdims=True))
    return (grad_v, jnp.sum(grad_y * normed, axis=0))


def gelu_value(values):
    return (
        0.5
        * values
        * (1.0 + jnp.tanh(GELU_SCALE * (values + GELU_CUBIC * values * values * values)))
    )


def gelu_slope(values):
    bent = jnp.tanh(GELU_SCALE * (values + GELU_CUBIC * values * values * values))
    return 0.5 * (1.0 + bent) + 0.5 * values * (1.0 - bent * bent) * GELU_SCALE * (
        1.0 + 3.0 * GELU_CUBIC * values * values
    )


def contract_last(left, right):
    return lax.dot_general(
        left, right, (((1,), (1,)), ((), ())), preferred_element_type=jnp.float32
    )


def push(source, target, sent, landed, block):
    return pltpu.make_async_remote_copy(
        src_ref=source,
        dst_ref=target,
        send_sem=sent,
        recv_sem=landed,
        device_id={"blk": block},
        device_id_type=pl.DeviceIdType.MESH,
    )


def greet(at, line, rows):
    barrier = pltpu.get_barrier_semaphore()

    def tell(block):
        pl.semaphore_signal(
            barrier, inc=1, device_id={"blk": block}, device_id_type=pl.DeviceIdType.MESH
        )

    tell(at + 1 - 2 * (at % 2))
    pl.when(line > 0)(lambda: tell(at - 2))
    pl.when(line < rows - 1)(lambda: tell(at + 2))
    pl.semaphore_wait(barrier, 1 + jnp.minimum(line, 1) + jnp.minimum(rows - 1 - line, 1))


def both(*terms):
    result = terms[0]
    for term in terms[1:]:
        result = jnp.logical_and(result, term)
    return result


def attend_kernel(
    heads,
    x_ref,
    low_ref,
    att_ref,
    tot_ref,
    kv_ref,
    kv,
    acc,
    part,
    up_sent,
    up_landed,
    side_sent,
    side_landed,
    own_done,
    save_done,
):
    at = lax.axis_index("blk")
    blocks = lax.axis_size("blk")
    rows = blocks // 2
    line, column = at // 2, at % 2
    partner = at + 1 - 2 * column
    size = x_ref.shape[0]
    first = heads * HEAD
    own = x_ref.at[:, pl.ds(first, 2 * HEAD)]
    greet(at, line, rows)

    def up_copy(index, source):
        return push(source, kv.at[index], up_sent.at[index // 2], up_landed.at[index // 2], at + 2)

    def side_copy(index, source):
        return push(
            source, kv.at[index], side_sent.at[index // 2], side_landed.at[index // 2], partner
        )

    def save(index):
        return pltpu.make_async_copy(kv.at[index], kv_ref.at[index], save_done.at[index])

    pl.when(line < rows - 1)(lambda: up_copy(at, own).start())
    pl.when(column == 0)(lambda: side_copy(at, own).start())
    keep = pltpu.make_async_copy(own, kv.at[at], own_done)
    keep.start()
    acc[...] = jnp.zeros_like(acc)
    part[...] = jnp.zeros_like(part)
    keep.wait()
    ahead = lax.broadcasted_iota(jnp.int32, (size, size), 1) - lax.broadcasted_iota(
        jnp.int32, (size, size), 0
    )

    def compute(index):
        save(index).start()
        span = (at - index) * size
        for head in range(heads):
            raw = lax.dot_general(
                x_ref[:, head * HEAD : (head + 1) * HEAD],
                kv[index, :, :HEAD],
                (((1,), (1,)), ((), ())),
                preferred_element_type=jnp.float32,
            )
            weights = jnp.exp(CAP_VALUE * jnp.tanh(raw * (HEAD ** (-0.5) / CAP_VALUE)))
            weights = jnp.where(ahead <= span, weights, 0.0)
            total = weights[:, :128]
            for piece in range(1, size // 128):
                total = total + weights[:, piece * 128 : (piece + 1) * 128]
            part[head] += total
            acc[:, head * HEAD : (head + 1) * HEAD] += jnp.dot(
                weights.astype(jnp.bfloat16),
                kv[index, :, HEAD:],
                preferred_element_type=jnp.float32,
            )

    @pl.loop(0, rows + 1)
    def _(step):
        source = line - step
        index = 2 * source + column

        @pl.when(both(step > 0, source >= 0))
        def _():
            up_copy(index, kv.at[index]).wait_recv()
            pl.when(line < rows - 1)(lambda: up_copy(index, kv.at[index]).start())
            side_copy(index, kv.at[index]).start()

        pl.when(source >= 0)(lambda: compute(index))
        other = 2 * (source + 1) + 1 - column

        @pl.when(both(step > 0, source + 1 >= 0, jnp.logical_or(step > 1, column == 1)))
        def _():
            side_copy(other, kv.at[other]).wait_recv()
            compute(other)

    for head in range(heads):
        columns = slice(head * HEAD, (head + 1) * HEAD)
        total = jnp.sum(part[head], axis=1, keepdims=True)
        value = acc[:, columns] / total
        att_ref[:, columns] = value
        low_ref[:, columns] = value.astype(jnp.bfloat16)
        tot_ref[head] = jnp.sum(part[head].T, axis=0, keepdims=True)

    @pl.loop(0, rows)
    def _(source):
        index = 2 * source + column

        @pl.when(source <= line)
        def _():
            pl.when(line < rows - 1)(lambda: up_copy(index, kv.at[index]).wait_send())
            pl.when(jnp.logical_or(source < line, column == 0))(
                lambda: side_copy(index, kv.at[index]).wait_send()
            )

    @pl.loop(0, blocks)
    def _(index):
        pl.when(index <= at)(lambda: save(index).wait())


def attend(projected, heads):
    size = projected.shape[0]
    blocks = lax.axis_size("blk")
    whole = pl.BlockSpec(memory_space=pltpu.VMEM)
    return pl.pallas_call(
        functools.partial(attend_kernel, heads),
        out_shape=(
            jax.ShapeDtypeStruct((size, heads * HEAD), jnp.bfloat16),
            jax.ShapeDtypeStruct((size, heads * HEAD), jnp.float32),
            jax.ShapeDtypeStruct((heads, 1, size), jnp.float32),
            jax.ShapeDtypeStruct((blocks, size, 2 * HEAD), jnp.bfloat16),
        ),
        in_specs=[whole],
        out_specs=(whole, whole, whole, pl.BlockSpec(memory_space=pl.ANY)),
        scratch_shapes=[
            pltpu.VMEM((blocks, size, 2 * HEAD), jnp.bfloat16),
            pltpu.VMEM((size, heads * HEAD), jnp.float32),
            pltpu.VMEM((heads, size, 128), jnp.float32),
            pltpu.SemaphoreType.DMA((blocks // 2,)),
            pltpu.SemaphoreType.DMA((blocks // 2,)),
            pltpu.SemaphoreType.DMA((blocks // 2,)),
            pltpu.SemaphoreType.DMA((blocks // 2,)),
            pltpu.SemaphoreType.DMA,
            pltpu.SemaphoreType.DMA((blocks,)),
        ],
        compiler_params=pltpu.CompilerParams(
            collective_id=0, has_side_effects=True, vmem_limit_bytes=VMEM_BYTES
        ),
        cost_estimate=cost_of(50),
        name="attend",
    )(projected)


def attend_back_kernel(
    heads,
    x_ref,
    scaled_ref,
    delta_ref,
    kv_ref,
    out_ref,
    kv,
    part,
    side,
    down,
    dq,
    dk,
    dv,
    load_done,
    side_sent,
    side_landed,
    down_sent,
    down_landed,
):
    at = lax.axis_index("blk")
    blocks = lax.axis_size("blk")
    rows = blocks // 2
    line, column = at // 2, at % 2
    partner = at + 1 - 2 * column
    size = x_ref.shape[0]

    def load(index):
        return pltpu.make_async_copy(kv_ref.at[index], kv.at[index], load_done.at[index])

    @pl.loop(0, blocks)
    def _(index):
        pl.when(index <= at)(lambda: load(index).start())

    greet(at, line, rows)

    def side_copy(target):
        return push(
            part.at[target, 1 - column],
            side.at[target],
            side_sent.at[target],
            side_landed.at[target],
            partner,
        )

    def down_copy(target):
        return push(
            part.at[target, column],
            down.at[target],
            down_sent.at[target],
            down_landed.at[target],
            at - 2,
        )

    dq[...] = jnp.zeros_like(dq)
    ahead = lax.broadcasted_iota(jnp.int32, (size, size), 0) - lax.broadcasted_iota(
        jnp.int32, (size, size), 1
    )

    def compute(target, half):
        index = 2 * target + half
        load(index).wait()
        span = (at - index) * size
        for head in range(heads):
            columns = slice(head * HEAD, (head + 1) * HEAD)
            query = x_ref[:, columns]
            scaled = scaled_ref[:, columns]
            key = kv[index, :, :HEAD]
            raw = lax.dot_general(
                key, query, (((1,), (1,)), ((), ())), preferred_element_type=jnp.float32
            )
            squashed = jnp.tanh(raw * (HEAD ** (-0.5) / CAP_VALUE))
            weights = jnp.exp(CAP_VALUE * squashed)
            weights = jnp.where(ahead <= span, weights, 0.0)
            inner = lax.dot_general(
                kv[index, :, HEAD:],
                scaled,
                (((1,), (1,)), ((), ())),
                preferred_element_type=jnp.float32,
            )
            grad_raw = (
                weights * (inner - delta_ref[head]) * (1.0 - squashed * squashed)
            ).astype(jnp.bfloat16)
            dv_now = jnp.dot(
                weights.astype(jnp.bfloat16), scaled, preferred_element_type=jnp.float32
            )
            dk_now = jnp.dot(grad_raw, query, preferred_element_type=jnp.float32)
            dq[:, columns] += lax.dot_general(
                grad_raw, key, (((0,), (0,)), ((), ())), preferred_element_type=jnp.float32
            )
            if head == 0:
                dv[...] = dv_now
                dk[...] = dk_now
            else:
                dv[...] += dv_now
                dk[...] += dk_now
        part[target, half, :, :HEAD] = (dk[...] * HEAD ** (-0.5)).astype(jnp.bfloat16)
        part[target, half, :, HEAD:] = dv[...].astype(jnp.bfloat16)

    def merge(target):
        last = target == line

        @pl.when(jnp.logical_or(target < line, column == 0))
        def _():
            side_copy(target).wait_recv()
            part[target, column] = (
                part[target, column].astype(jnp.float32) + side[target].astype(jnp.float32)
            ).astype(jnp.bfloat16)

        @pl.when(line < rows - 1)
        def _():
            down_copy(target).wait_recv()
            part[target, column] = (
                part[target, column].astype(jnp.float32) + down[target].astype(jnp.float32)
            ).astype(jnp.bfloat16)

        pl.when(target < line)(lambda: down_copy(target).start())

        @pl.when(last)
        def _():
            out_ref[:, heads * HEAD :] = part[target, column]

    @pl.loop(0, rows)
    def _(target):
        @pl.when(jnp.logical_or(target < line, both(target == line, column == 1)))
        def _():
            compute(target, 1 - column)
            side_copy(target).start()

        pl.when(target <= line)(lambda: compute(target, column))
        pl.when(both(line == rows - 1, target > 0))(lambda: merge(target - 1))

    out_ref[:, : heads * HEAD] = (dq[...] * HEAD ** (-0.5)).astype(jnp.bfloat16)

    @pl.loop(0, rows)
    def _(target):
        pl.when(both(target <= line, jnp.logical_or(line < rows - 1, target == rows - 1)))(
            lambda: merge(target)
        )

    @pl.loop(0, rows)
    def _(target):
        pl.when(jnp.logical_or(target < line, both(target == line, column == 1)))(
            lambda: side_copy(target).wait_send()
        )
        pl.when(target < line)(lambda: down_copy(target).wait_send())


def attend_back(projected, scaled, delta, kv_all):
    size = projected.shape[0]
    blocks = lax.axis_size("blk")
    rows = blocks // 2
    heads = scaled.shape[1] // HEAD
    whole = pl.BlockSpec(memory_space=pltpu.VMEM)
    return pl.pallas_call(
        functools.partial(attend_back_kernel, heads),
        out_shape=jax.ShapeDtypeStruct(projected.shape, jnp.bfloat16),
        in_specs=[whole, whole, whole, pl.BlockSpec(memory_space=pl.ANY)],
        out_specs=whole,
        scratch_shapes=[
            pltpu.VMEM((blocks, size, 2 * HEAD), jnp.bfloat16),
            pltpu.VMEM((rows, 2, size, 2 * HEAD), jnp.bfloat16),
            pltpu.VMEM((rows, size, 2 * HEAD), jnp.bfloat16),
            pltpu.VMEM((rows, size, 2 * HEAD), jnp.bfloat16),
            pltpu.VMEM((size, heads * HEAD), jnp.float32),
            pltpu.VMEM((size, HEAD), jnp.float32),
            pltpu.VMEM((size, HEAD), jnp.float32),
            pltpu.SemaphoreType.DMA((blocks,)),
            pltpu.SemaphoreType.DMA((rows,)),
            pltpu.SemaphoreType.DMA((rows,)),
            pltpu.SemaphoreType.DMA((rows,)),
            pltpu.SemaphoreType.DMA((rows,)),
        ],
        compiler_params=pltpu.CompilerParams(
            collective_id=1, has_side_effects=True, vmem_limit_bytes=VMEM_BYTES
        ),
        cost_estimate=cost_of(50),
        name="attend_back",
    )(projected, scaled, delta, kv_all)


def line_gather(own_ref, full, line_sent, line_landed, side_sent, side_landed, own_done, work):
    at = lax.axis_index("blk")
    rows = lax.axis_size("blk") // 2
    line, column = at // 2, at % 2
    size = own_ref.shape[0]

    def spot(source, side):
        start = pl.multiple_of((2 * source + side) * size, size)
        return full.at[pl.ds(start, size), :]

    def line_copy(source, sign, first=False):
        return push(
            own_ref if first else spot(source, column),
            spot(source, column),
            line_sent.at[(sign + 1) // 2, source],
            line_landed.at[source],
            at + 2 * sign,
        )

    def side_copy(source, side, first=False):
        return push(
            own_ref if first else spot(source, side),
            spot(source, side),
            side_sent.at[source],
            side_landed.at[source],
            at + 1 - 2 * column,
        )

    def inside(row):
        return jnp.logical_and(row >= 0, row < rows)

    pl.when(line < rows - 1)(lambda: line_copy(line, 1, True).start())
    pl.when(line > 0)(lambda: line_copy(line, -1, True).start())
    side_copy(line, column, True).start()
    keep = pltpu.make_async_copy(own_ref, spot(line, column), own_done)
    keep.start()
    keep.wait()

    @pl.loop(0, rows + 1)
    def _(step):
        for sign in (-1, 1):
            source = line - sign * step

            @pl.when(both(step > 0, inside(source)))
            def _():
                line_copy(source, sign).wait_recv()
                pl.when(inside(line + sign))(lambda: line_copy(source, sign).start())
                side_copy(source, column).start()

        for sign in (-1, 1):
            source = line - sign * (step - 1)
            once = step > 0 if sign == -1 else step > 1

            @pl.when(both(once, inside(source)))
            def _():
                side_copy(source, 1 - column).wait_recv()
                work(source)

    @pl.loop(0, rows)
    def _(source):
        pl.when(both(source <= line, line < rows - 1))(lambda: line_copy(source, 1).wait_send())
        pl.when(both(source >= line, line > 0))(lambda: line_copy(source, -1).wait_send())
        side_copy(source, column).wait_send()


def line_scatter(part, side, lane, out_ref, side_sent, side_landed, lane_sent, lane_landed, work, fill):
    at = lax.axis_index("blk")
    rows = lax.axis_size("blk") // 2
    line, column = at // 2, at % 2
    size = out_ref.shape[0]

    def spot(target, half):
        start = pl.multiple_of((2 * target + half) * size, size)
        return pl.ds(start, size)

    def side_copy(target):
        return push(
            part.at[spot(target, 1 - column), :],
            side.at[target],
            side_sent.at[target],
            side_landed.at[target],
            at + 1 - 2 * column,
        )

    def lane_copy(target, sign):
        slot = target if sign == 1 else jnp.where(target == line - 1, rows, target)
        return push(
            part.at[spot(target, column), :],
            lane.at[slot],
            lane_sent.at[target],
            lane_landed.at[slot],
            at + 2 * sign,
        )

    def lane_wait(slot):
        push(
            lane.at[slot], lane.at[slot], lane_sent.at[0], lane_landed.at[slot], at + 1 - 2 * column
        ).wait_recv()

    def inside(row):
        return jnp.logical_and(row >= 0, row < rows)

    @pl.loop(0, rows)
    def _(step):
        for sign in (-1, 1):
            target = line + sign * (rows - 1 - step)
            once = step >= 0 if sign == -1 else step < rows - 1

            @pl.when(both(once, inside(target)))
            def _():
                work(target)
                side_copy(target).start()

    def merge(target):
        mine = spot(target, column)
        side_copy(target).wait_recv()
        part[mine, :] = (
            part[mine, :].astype(jnp.float32) + side[target].astype(jnp.float32)
        ).astype(jnp.bfloat16)

        def pass_on(sign):
            @pl.when(inside(line - sign))
            def _():
                lane_wait(target)
                part[mine, :] = (
                    part[mine, :].astype(jnp.float32) + lane[target].astype(jnp.float32)
                ).astype(jnp.bfloat16)

            lane_copy(target, sign).start()

        pl.when(target > line)(lambda: pass_on(1))
        pl.when(target < line)(lambda: pass_on(-1))

    @pl.loop(0, rows)
    def _(step):
        fill(step)
        for sign in (-1, 1):
            target = line + sign * (rows - 1 - step)
            once = step >= 0 if sign == -1 else step < rows - 1
            pl.when(both(once, inside(target)))(lambda: merge(target))

    mine = spot(line, column)
    out_ref[...] = part[mine, :].astype(jnp.float32)

    @pl.when(line > 0)
    def _():
        lane_wait(line)
        out_ref[...] += lane[line].astype(jnp.float32)

    @pl.when(line < rows - 1)
    def _():
        lane_wait(rows)
        out_ref[...] += lane[rows].astype(jnp.float32)

    @pl.loop(0, rows)
    def _(target):
        side_copy(target).wait_send()
        pl.when(target > line)(lambda: lane_copy(target, 1).wait_send())
        pl.when(target < line)(lambda: lane_copy(target, -1).wait_send())


def line_sems(rows):
    dma = pltpu.SemaphoreType.DMA
    return [dma((2, rows)), dma((rows,)), dma((rows,)), dma((rows,)), dma]


def lane_sems(rows):
    dma = pltpu.SemaphoreType.DMA
    return [dma((rows,)), dma((rows,)), dma((rows,)), dma((rows + 1,))]


def ffn_kernel(
    act_ref,
    w_ref,
    out_ref,
    acts_ref,
    w,
    acts,
    hidden,
    part,
    side,
    lane,
    w_done,
    save_done,
    *sems,
):
    at = lax.axis_index("blk")
    rows = lax.axis_size("blk") // 2
    pair = 2 * act_ref.shape[0]

    def load(which):
        return pltpu.make_async_copy(w_ref.at[which], w.at[which], w_done.at[which])

    def pair_rows(source):
        return pl.ds(pl.multiple_of(source * pair, pair), pair)

    def save(source):
        return pltpu.make_async_copy(
            acts.at[pair_rows(source), :], acts_ref.at[pair_rows(source), :], save_done.at[source]
        )

    for which in range(3):
        load(which).start()
    greet(at, at // 2, rows)
    for which in range(3):
        load(which).wait()

    def expand(source):
        save(source).start()
        rows_now = acts[pair_rows(source), :]
        gate = contract_last(w[0], rows_now)
        up = contract_last(w[1], rows_now)
        hidden[source] = (gelu_value(gate) * up).astype(jnp.bfloat16)

    def reduce(target):
        part[pair_rows(target), :] = lax.dot_general(
            hidden[target], w[2], (((0,), (0,)), ((), ())), preferred_element_type=jnp.float32
        ).astype(jnp.bfloat16)

    line_gather(act_ref, acts, *sems[:5], expand)
    line_scatter(part, side, lane, out_ref, *sems[5:], reduce, lambda step: None)
    pl.loop(0, rows)(lambda source: save(source).wait())


def ffn_forward(act_ffn, w_parts):
    size, width = act_ffn.shape
    units = w_parts.shape[1]
    blocks = lax.axis_size("blk")
    rows = blocks // 2
    whole = pl.BlockSpec(memory_space=pltpu.VMEM)
    far = pl.BlockSpec(memory_space=pl.ANY)
    return pl.pallas_call(
        ffn_kernel,
        out_shape=(
            jax.ShapeDtypeStruct((size, width), jnp.float32),
            jax.ShapeDtypeStruct((blocks * size, width), jnp.bfloat16),
        ),
        in_specs=[whole, far],
        out_specs=(whole, far),
        scratch_shapes=[
            pltpu.VMEM(w_parts.shape, jnp.bfloat16),
            pltpu.VMEM((blocks * size, width), jnp.bfloat16),
            pltpu.VMEM((rows, units, 2 * size), jnp.bfloat16),
            pltpu.VMEM((blocks * size, width), jnp.bfloat16),
            pltpu.VMEM((rows, size, width), jnp.bfloat16),
            pltpu.VMEM((rows + 1, size, width), jnp.bfloat16),
            pltpu.SemaphoreType.DMA((3,)),
            pltpu.SemaphoreType.DMA((rows,)),
            *line_sems(rows),
            *lane_sems(rows),
        ],
        compiler_params=pltpu.CompilerParams(
            collective_id=2, has_side_effects=True, vmem_limit_bytes=VMEM_BYTES
        ),
        cost_estimate=cost_of(115),
        name="ffn_forward",
    )(act_ffn, w_parts)


FILL_COLUMNS = 256
FILL_FIRST = 3


def ffn_back_kernel(
    owners,
    grad_ref,
    acts_ref,
    w_ref,
    out_ref,
    sum_ref,
    w,
    rights,
    lefts,
    part,
    side,
    lane,
    stage,
    w_done,
    acts_done,
    stage_done,
    *sems,
):
    at = lax.axis_index("blk")
    rows = lax.axis_size("blk") // 2
    size, width = grad_ref.shape
    pair = 2 * size
    units = w.shape[1]
    acts, grads = rights.at[0], rights.at[1]

    def load(which):
        return pltpu.make_async_copy(w_ref.at[which], w.at[which], w_done.at[which])

    def pair_rows(source):
        return pl.ds(pl.multiple_of(source * pair, pair), pair)

    acts_copy = pltpu.make_async_copy(acts_ref, acts, acts_done)
    acts_copy.start()
    for which in range(3):
        load(which).start()
    greet(at, at // 2, rows)
    acts_copy.wait()
    for which in range(3):
        load(which).wait()

    def expand(source):
        columns = pair_rows(source)
        rows_now = acts[pair_rows(source), :]
        gate = contract_last(w[0], rows_now)
        up = contract_last(w[1], rows_now)
        grad_hidden = contract_last(w[2], grads[pair_rows(source), :])
        bent = jnp.tanh(GELU_SCALE * (gate + GELU_CUBIC * gate * gate * gate))
        value = 0.5 * gate * (1.0 + bent)
        slope = 0.5 * (1.0 + bent) + 0.5 * gate * (1.0 - bent * bent) * GELU_SCALE * (
            1.0 + 3.0 * GELU_CUBIC * gate * gate
        )
        lefts[2, :, columns] = (value * up).astype(jnp.bfloat16)
        lefts[0, :, columns] = (grad_hidden * up * slope).astype(jnp.bfloat16)
        lefts[1, :, columns] = (grad_hidden * value).astype(jnp.bfloat16)

    def reduce(target):
        columns = pair_rows(target)
        dims = (((0,), (0,)), ((), ()))
        total = lax.dot_general(
            lefts[0, :, columns], w[0], dims, preferred_element_type=jnp.float32
        ) + lax.dot_general(lefts[1, :, columns], w[1], dims, preferred_element_type=jnp.float32)
        part[pair_rows(target), :] = total.astype(jnp.bfloat16)

    pieces = width // FILL_COLUMNS
    total_pieces = 3 * pieces

    def piece_columns(item):
        return pl.ds(pl.multiple_of((item % pieces) * FILL_COLUMNS, FILL_COLUMNS), FILL_COLUMNS)

    def stage_copy(item):
        return pltpu.make_async_copy(
            stage.at[item % 2],
            sum_ref.at[:, item // pieces, :, piece_columns(item)],
            stage_done.at[item % 2],
        )

    def fill_one(item):
        which = item // pieces
        total = jnp.dot(
            lefts[which],
            rights[which // 2, :, piece_columns(item)],
            preferred_element_type=jnp.float32,
        )
        pl.when(item > 1)(lambda: stage_copy(item - 2).wait())
        stage[item % 2] = total.astype(jnp.bfloat16).reshape(
            owners, units // owners, FILL_COLUMNS
        )
        stage_copy(item).start()

    each = pl.cdiv(total_pieces - FILL_FIRST, rows - 1)

    def fill(step):
        first = jnp.maximum(FILL_FIRST + (step - 1) * each, 0)
        last = jnp.minimum(FILL_FIRST + step * each, total_pieces)

        @pl.loop(0, each)
        def _(item):
            pl.when(first + item < last)(lambda: fill_one(first + item))

    line_gather(grad_ref, grads, *sems[:5], expand)
    line_scatter(part, side, lane, out_ref, *sems[5:], reduce, fill)
    stage_copy(total_pieces - 2).wait()
    stage_copy(total_pieces - 1).wait()


def ffn_back(grad_ffn, acts, w_parts, owners):
    size, width = grad_ffn.shape
    units = w_parts.shape[1]
    blocks = lax.axis_size("blk")
    rows = blocks // 2
    tokens = blocks * size
    whole = pl.BlockSpec(memory_space=pltpu.VMEM)
    far = pl.BlockSpec(memory_space=pl.ANY)
    return pl.pallas_call(
        functools.partial(ffn_back_kernel, owners),
        out_shape=(
            jax.ShapeDtypeStruct((size, width), jnp.float32),
            jax.ShapeDtypeStruct((owners, 3, units // owners, width), jnp.bfloat16),
        ),
        in_specs=[whole, far, far],
        out_specs=(whole, far),
        scratch_shapes=[
            pltpu.VMEM(w_parts.shape, jnp.bfloat16),
            pltpu.VMEM((2, tokens, width), jnp.bfloat16),
            pltpu.VMEM((3, units, tokens), jnp.bfloat16),
            pltpu.VMEM((tokens, width), jnp.bfloat16),
            pltpu.VMEM((rows, size, width), jnp.bfloat16),
            pltpu.VMEM((rows + 1, size, width), jnp.bfloat16),
            pltpu.VMEM((2, owners, units // owners, FILL_COLUMNS), jnp.bfloat16),
            pltpu.SemaphoreType.DMA((3,)),
            pltpu.SemaphoreType.DMA,
            pltpu.SemaphoreType.DMA((2,)),
            *line_sems(rows),
            *lane_sems(rows),
        ],
        compiler_params=pltpu.CompilerParams(
            collective_id=3, has_side_effects=True, vmem_limit_bytes=VMEM_BYTES
        ),
        cost_estimate=cost_of(115),
        name="ffn_back",
    )(grad_ffn, acts, w_parts)


def ffn_hidden(acts, w_parts):
    gate = contract_last(acts, w_parts[0])
    up = contract_last(acts, w_parts[1])
    return (gate, up, (gelu_value(gate) * up).astype(jnp.bfloat16))


def scatter_tokens(partial):
    return lax.psum_scatter(
        partial.astype(jnp.bfloat16), "blk", scatter_dimension=0, tiled=True
    ).astype(jnp.float32)


def ffn_forward_wide(act_ffn, w_parts):
    acts = lax.all_gather(act_ffn, "blk", axis=0, tiled=True)
    hidden = ffn_hidden(acts, w_parts)[2]
    partial = jnp.dot(hidden, w_parts[2], preferred_element_type=jnp.float32)
    return (scatter_tokens(partial), acts)


def ffn_back_wide(grad_ffn, acts, w_parts, owners):
    grads = lax.all_gather(grad_ffn, "blk", axis=0, tiled=True)
    gate, up, hidden = ffn_hidden(acts, w_parts)
    grad_hidden = contract_last(grads, w_parts[2])
    grad_gate = (grad_hidden * up * gelu_slope(gate)).astype(jnp.bfloat16)
    grad_up = (grad_hidden * gelu_value(gate)).astype(jnp.bfloat16)
    partial = jnp.dot(grad_gate, w_parts[0], preferred_element_type=jnp.float32) + jnp.dot(
        grad_up, w_parts[1], preferred_element_type=jnp.float32
    )
    sums = jnp.stack(
        [
            jnp.einsum("tf,td->fd", left, right, preferred_element_type=jnp.float32)
            for left, right in ((grad_gate, acts), (grad_up, acts), (hidden, grads))
        ]
    ).astype(jnp.bfloat16)
    units = w_parts.shape[1]
    owned = sums.reshape(3, owners, units // owners, sums.shape[2])
    return (scatter_tokens(partial), jnp.transpose(owned, (1, 0, 2, 3)))


def cost_of(microseconds):
    return pl.CostEstimate(
        flops=int(microseconds * 1e9), bytes_accessed=int(microseconds * 3e6), transcendentals=0
    )


def push_sp(source, target, sent, landed, peer):
    return pltpu.make_async_remote_copy(
        src_ref=source,
        dst_ref=target,
        send_sem=sent,
        recv_sem=landed,
        device_id={"sp": peer},
        device_id_type=pl.DeviceIdType.MESH,
    )


def greet_sp(me, groups):
    barrier = pltpu.get_barrier_semaphore()
    for step in range(1, groups):
        pl.semaphore_signal(
            barrier,
            inc=1,
            device_id={"sp": (me + step) % groups},
            device_id_type=pl.DeviceIdType.MESH,
        )
    pl.semaphore_wait(barrier, groups - 1)


def gather_project_kernel(x_ref, w_ref, full_ref, out_ref, w, w_done, own_done, sent, landed):
    me = lax.axis_index("sp")
    size = x_ref.shape[0]
    units = w.shape[0]
    mate = me + 1 - 2 * (me % 2)
    across = (me + 2) % 4

    def spot(member):
        return full_ref.at[pl.ds(pl.multiple_of(member * size, size), size), :]

    load = pltpu.make_async_copy(
        w_ref.at[pl.ds(pl.multiple_of(me * units, units), units), :], w, w_done
    )
    load.start()
    greet_sp(me, 4)
    over = push_sp(x_ref, spot(me), sent.at[0], landed.at[0], across)
    over.start()
    beside = push_sp(x_ref, spot(me), sent.at[1], landed.at[1], mate)
    beside.start()
    keep = pltpu.make_async_copy(x_ref, spot(me), own_done)
    keep.start()
    keep.wait()
    load.wait()

    def project(chip):
        rows = pl.ds(pl.multiple_of(chip * 2 * size, 2 * size), 2 * size)
        out_ref[rows, :] = contract_last(full_ref[rows, :], w[...]).astype(jnp.bfloat16)

    beside.wait_recv()
    project(me // 2)
    over.wait_recv()
    onward = push_sp(spot(across), spot(across), sent.at[2], landed.at[2], mate)
    onward.start()
    onward.wait_recv()
    project(across // 2)
    over.wait_send()
    beside.wait_send()
    onward.wait_send()


def gather_project(rows, weights, identity):
    size, width = rows.shape
    units = weights.shape[0] // 4
    whole = pl.BlockSpec(memory_space=pltpu.VMEM)
    return pl.pallas_call(
        gather_project_kernel,
        out_shape=(
            jax.ShapeDtypeStruct((4 * size, width), jnp.bfloat16),
            jax.ShapeDtypeStruct((4 * size, units), jnp.bfloat16),
        ),
        in_specs=[whole, pl.BlockSpec(memory_space=pl.ANY)],
        out_specs=(whole, whole),
        scratch_shapes=[
            pltpu.VMEM((units, width), jnp.bfloat16),
            pltpu.SemaphoreType.DMA,
            pltpu.SemaphoreType.DMA,
            pltpu.SemaphoreType.DMA((3,)),
            pltpu.SemaphoreType.DMA((3,)),
        ],
        compiler_params=pltpu.CompilerParams(
            collective_id=identity, has_side_effects=True, vmem_limit_bytes=VMEM_BYTES
        ),
        cost_estimate=cost_of(18),
        name="gather_project",
    )(rows, weights)


def exchange_project_kernel(x_ref, w_ref, out_ref, w, got, w_done, own_done, sent, landed):
    me = lax.axis_index("sp")
    size = out_ref.shape[0]
    units = x_ref.shape[1]

    def rows_of(member):
        return x_ref.at[pl.ds(pl.multiple_of(member * size, size), size), :]

    def load(member):
        rows = pl.ds(pl.multiple_of(member * units, units), units)
        return pltpu.make_async_copy(w_ref.at[rows, :], w.at[rows, :], w_done.at[member])

    def send(step):
        peer = (me + step) % 4
        return push_sp(rows_of(peer), got.at[4 - step], sent.at[step], landed.at[4 - step], peer)

    greet_sp(me, 4)
    for step in (2, 1, 3):
        send(step).start()
    keep = pltpu.make_async_copy(rows_of(me), got.at[0], own_done)
    keep.start()
    for step in range(4):
        load((me + step) % 4).start()
    keep.wait()
    for step in (0, 1, 3, 2):
        member = (me + step) % 4
        load(member).wait()
        if step > 0:
            send(4 - step).wait_recv()
        rows = pl.ds(pl.multiple_of(member * units, units), units)
        term = jnp.dot(got[step], w[rows, :], preferred_element_type=jnp.float32)
        if step == 0:
            out_ref[...] = term
        else:
            out_ref[...] += term
    for step in (1, 2, 3):
        send(step).wait_send()


def exchange_project(columns, weights, identity):
    size = columns.shape[0] // 4
    whole = pl.BlockSpec(memory_space=pltpu.VMEM)
    return pl.pallas_call(
        exchange_project_kernel,
        out_shape=jax.ShapeDtypeStruct((size, weights.shape[1]), jnp.float32),
        in_specs=[whole, pl.BlockSpec(memory_space=pl.ANY)],
        out_specs=whole,
        scratch_shapes=[
            pltpu.VMEM(weights.shape, jnp.bfloat16),
            pltpu.VMEM((4, size, columns.shape[1]), jnp.bfloat16),
            pltpu.SemaphoreType.DMA((4,)),
            pltpu.SemaphoreType.DMA,
            pltpu.SemaphoreType.DMA((4,)),
            pltpu.SemaphoreType.DMA((4,)),
        ],
        compiler_params=pltpu.CompilerParams(
            collective_id=identity, has_side_effects=True, vmem_limit_bytes=VMEM_BYTES
        ),
        cost_estimate=cost_of(16),
        name="exchange_project",
    )(columns, weights)


def weight_kernel(left_ref, right_ref, out_ref, part, side, lane, *sems):
    at = lax.axis_index("blk")
    rows = lax.axis_size("blk") // 2
    pair = 2 * out_ref.shape[0]
    greet(at, at // 2, rows)

    def reduce(target):
        span = pl.ds(pl.multiple_of(target * pair, pair), pair)
        part[span, :] = lax.dot_general(
            left_ref[:, span],
            right_ref[...],
            (((0,), (0,)), ((), ())),
            preferred_element_type=jnp.float32,
        ).astype(jnp.bfloat16)

    line_scatter(part, side, lane, out_ref, *sems, reduce, lambda step: None)


def weight_sums(left, right, identity):
    blocks = lax.axis_size("blk")
    rows = blocks // 2
    size, width = left.shape[1] // blocks, right.shape[1]
    whole = pl.BlockSpec(memory_space=pltpu.VMEM)
    return pl.pallas_call(
        weight_kernel,
        out_shape=jax.ShapeDtypeStruct((size, width), jnp.float32),
        in_specs=[whole, whole],
        out_specs=whole,
        scratch_shapes=[
            pltpu.VMEM((blocks * size, width), jnp.bfloat16),
            pltpu.VMEM((rows, size, width), jnp.bfloat16),
            pltpu.VMEM((rows + 1, size, width), jnp.bfloat16),
            *lane_sems(rows),
        ],
        compiler_params=pltpu.CompilerParams(
            collective_id=identity, has_side_effects=True, vmem_limit_bytes=VMEM_BYTES
        ),
        cost_estimate=cost_of(60),
        name="weight_sums",
    )(left, right)


def weight_sums_wide(left, right):
    term = jnp.einsum("tc,td->cd", left, right, preferred_element_type=jnp.float32)
    return scatter_tokens(term)


def body(tokens, w_qkv, w_out, gains, w_ffn, cotangent):
    groups = lax.axis_size("sp")
    heads_here = HEADS // groups
    source = tokens.astype(jnp.float32)
    normed_in, inverse_in = norm_parts(source)
    act_in = (normed_in * gains[0]).astype(jnp.bfloat16)
    act_block, projected = gather_project(act_in, w_qkv, 4)
    block_rows = projected.shape[0]
    attended_cols, attended, totals, kv_all = attend(projected, heads_here)
    attn = exchange_project(attended_cols, w_out, 5)
    normed_attn, inverse_attn = norm_parts(attn)
    middle = source + normed_attn * gains[1]
    normed_mid, inverse_mid = norm_parts(middle)
    act_ffn = (normed_mid * gains[2]).astype(jnp.bfloat16)
    wide = lax.axis_size("blk") > 8
    w_parts = jnp.transpose(w_ffn, (1, 0, 2))
    ffn_out, act_all = (ffn_forward_wide if wide else ffn_forward)(act_ffn, w_parts)
    normed_ffn, inverse_ffn = norm_parts(ffn_out)
    result = middle + normed_ffn * gains[3]
    grad_out = cotangent.astype(jnp.float32)
    grad_ffn_f, gain_grad3 = norm_back(grad_out, normed_ffn, inverse_ffn, gains[3])
    grad_ffn = grad_ffn_f.astype(jnp.bfloat16)
    grad_act_ffn, ffn_sums = (ffn_back_wide if wide else ffn_back)(
        grad_ffn, act_all, w_parts, groups
    )
    grad_norm_mid, gain_grad2 = norm_back(grad_act_ffn, normed_mid, inverse_mid, gains[2])
    grad_middle = grad_out + grad_norm_mid
    grad_attn_f, gain_grad1 = norm_back(grad_middle, normed_attn, inverse_attn, gains[1])
    grad_attn = grad_attn_f.astype(jnp.bfloat16)
    grad_block, grad_attended = gather_project(grad_attn, w_out, 6)
    out_term = jnp.einsum(
        "tc,td->cd", attended_cols, grad_block, preferred_element_type=jnp.float32
    )
    out_grad = lax.psum_scatter(
        out_term.astype(jnp.bfloat16), "blk", scatter_dimension=0, tiled=True
    ).astype(jnp.float32)
    grad_heads = grad_attended.astype(jnp.float32).reshape(block_rows, heads_here, HEAD)
    totals_rows = jnp.transpose(totals.reshape(heads_here, block_rows))
    scaled = (grad_heads / totals_rows[..., None]).astype(jnp.bfloat16)
    row_delta = (
        jnp.sum(grad_heads * attended.reshape(block_rows, heads_here, HEAD), axis=-1) / totals_rows
    )
    grad_cols = attend_back(
        projected,
        scaled.reshape(block_rows, heads_here * HEAD),
        jnp.transpose(row_delta).reshape(heads_here, 1, block_rows),
        kv_all,
    )
    grad_act_in = exchange_project(grad_cols, w_qkv, 7)
    qkv_grad = (
        weight_sums_wide(grad_cols, act_block) if wide else weight_sums(grad_cols, act_block, 8)
    )
    grad_source, gain_grad0 = norm_back(grad_act_in, normed_in, inverse_in, gains[0])
    tokens_grad = (grad_middle + grad_source).astype(jnp.bfloat16)
    gains_term = jnp.stack([gain_grad0, gain_grad1, gain_grad2, gain_grad3], axis=0)
    ffn_part = lax.psum_scatter(ffn_sums, "sp", scatter_dimension=0, tiled=True)
    ffn_grad = jnp.transpose(ffn_part[0].astype(jnp.float32), (1, 0, 2))
    gains_all = lax.psum(gains_term, ("blk", "sp"))
    share = gains_all.shape[1] // (groups * lax.axis_size("blk"))
    place = lax.axis_index("sp") * lax.axis_size("blk") + lax.axis_index("blk")
    gains_grad = lax.dynamic_slice_in_dim(gains_all, place * share, share, 1)
    return (result.astype(jnp.bfloat16), tokens_grad, qkv_grad, out_grad, gains_grad, ffn_grad)


def solution(mesh):
    return jax.shard_map(
        body,
        mesh=mesh,
        in_specs=(
            P(("blk", "sp"), None),
            P(),
            P(),
            P(),
            P("blk", None, None),
            P(("blk", "sp"), None),
        ),
        out_specs=(
            P(("blk", "sp"), None),
            P(("blk", "sp"), None),
            P(("sp", "blk"), None),
            P(("sp", "blk"), None),
            P(None, ("sp", "blk")),
            P(("blk", "sp"), None, None),
        ),
        check_vma=False,
    )
```

```python
import functools

import jax
import jax.numpy as jnp
from jax import lax
from jax.experimental import pallas as pl
from jax.experimental.pallas import tpu as pltpu
from jax.sharding import PartitionSpec as P

HEADS = 8
KV_HEADS = 4
HEAD = 256


VMEM_BYTES = 62 * 1024 * 1024
NORM_EPSILON = 1e-06
CAP_VALUE = 50.0
GELU_SCALE = 0.7978845608028654
GELU_CUBIC = 0.044715


def norm_parts(values):
    inverse = lax.rsqrt(jnp.mean(values * values, axis=-1, keepdims=True) + NORM_EPSILON)
    return (values * inverse, inverse)


def norm_back(grad_y, normed, inverse, gain):
    grad_n = grad_y * gain
    grad_v = inverse * (grad_n - normed * jnp.mean(grad_n * normed, axis=-1, keepdims=True))
    return (grad_v, jnp.sum(grad_y * normed, axis=0))


def gelu_value(values):
    return (
        0.5
        * values
        * (1.0 + jnp.tanh(GELU_SCALE * (values + GELU_CUBIC * values * values * values)))
    )


def gelu_slope(values):
    bent = jnp.tanh(GELU_SCALE * (values + GELU_CUBIC * values * values * values))
    return 0.5 * (1.0 + bent) + 0.5 * values * (1.0 - bent * bent) * GELU_SCALE * (
        1.0 + 3.0 * GELU_CUBIC * values * values
    )


def contract_last(left, right):
    return lax.dot_general(
        left, right, (((1,), (1,)), ((), ())), preferred_element_type=jnp.float32
    )


def push(source, target, sent, landed, block):
    return pltpu.make_async_remote_copy(
        src_ref=source,
        dst_ref=target,
        send_sem=sent,
        recv_sem=landed,
        device_id={"blk": block},
        device_id_type=pl.DeviceIdType.MESH,
    )


def greet(at, line, rows):
    barrier = pltpu.get_barrier_semaphore()

    def tell(block):
        pl.semaphore_signal(
            barrier, inc=1, device_id={"blk": block}, device_id_type=pl.DeviceIdType.MESH
        )

    tell(at + 1 - 2 * (at % 2))
    pl.when(line > 0)(lambda: tell(at - 2))
    pl.when(line < rows - 1)(lambda: tell(at + 2))
    pl.semaphore_wait(barrier, 1 + jnp.minimum(line, 1) + jnp.minimum(rows - 1 - line, 1))


def both(*terms):
    result = terms[0]
    for term in terms[1:]:
        result = jnp.logical_and(result, term)
    return result


def attend_kernel(
    heads,
    x_ref,
    low_ref,
    att_ref,
    tot_ref,
    kv_ref,
    kv,
    acc,
    part,
    up_sent,
    up_landed,
    side_sent,
    side_landed,
    own_done,
    save_done,
):
    at = lax.axis_index("blk")
    blocks = lax.axis_size("blk")
    rows = blocks // 2
    line, column = at // 2, at % 2
    partner = at + 1 - 2 * column
    size = x_ref.shape[0]
    first = heads * HEAD
    own = x_ref.at[:, pl.ds(first, 2 * HEAD)]
    greet(at, line, rows)

    def up_copy(index, source):
        return push(source, kv.at[index], up_sent.at[index // 2], up_landed.at[index // 2], at + 2)

    def side_copy(index, source):
        return push(
            source, kv.at[index], side_sent.at[index // 2], side_landed.at[index // 2], partner
        )

    def save(index):
        return pltpu.make_async_copy(kv.at[index], kv_ref.at[index], save_done.at[index])

    pl.when(line < rows - 1)(lambda: up_copy(at, own).start())
    pl.when(column == 0)(lambda: side_copy(at, own).start())
    keep = pltpu.make_async_copy(own, kv.at[at], own_done)
    keep.start()
    acc[...] = jnp.zeros_like(acc)
    part[...] = jnp.zeros_like(part)
    keep.wait()
    ahead = lax.broadcasted_iota(jnp.int32, (size, size), 1) - lax.broadcasted_iota(
        jnp.int32, (size, size), 0
    )

    def compute(index):
        save(index).start()
        span = (at - index) * size
        for head in range(heads):
            raw = lax.dot_general(
                x_ref[:, head * HEAD : (head + 1) * HEAD],
                kv[index, :, :HEAD],
                (((1,), (1,)), ((), ())),
                preferred_element_type=jnp.float32,
            )
            weights = jnp.exp(CAP_VALUE * jnp.tanh(raw * (HEAD ** (-0.5) / CAP_VALUE)))
            weights = jnp.where(ahead <= span, weights, 0.0)
            total = weights[:, :128]
            for piece in range(1, size // 128):
                total = total + weights[:, piece * 128 : (piece + 1) * 128]
            part[head] += total
            acc[:, head * HEAD : (head + 1) * HEAD] += jnp.dot(
                weights.astype(jnp.bfloat16),
                kv[index, :, HEAD:],
                preferred_element_type=jnp.float32,
            )

    @pl.loop(0, rows + 1)
    def _(step):
        source = line - step
        index = 2 * source + column

        @pl.when(both(step > 0, source >= 0))
        def _():
            up_copy(index, kv.at[index]).wait_recv()
            pl.when(line < rows - 1)(lambda: up_copy(index, kv.at[index]).start())
            side_copy(index, kv.at[index]).start()

        pl.when(source >= 0)(lambda: compute(index))
        other = 2 * (source + 1) + 1 - column

        @pl.when(both(step > 0, source + 1 >= 0, jnp.logical_or(step > 1, column == 1)))
        def _():
            side_copy(other, kv.at[other]).wait_recv()
            compute(other)

    for head in range(heads):
        columns = slice(head * HEAD, (head + 1) * HEAD)
        total = jnp.sum(part[head], axis=1, keepdims=True)
        value = acc[:, columns] / total
        att_ref[:, columns] = value
        low_ref[:, columns] = value.astype(jnp.bfloat16)
        tot_ref[head] = jnp.sum(part[head].T, axis=0, keepdims=True)

    @pl.loop(0, rows)
    def _(source):
        index = 2 * source + column

        @pl.when(source <= line)
        def _():
            pl.when(line < rows - 1)(lambda: up_copy(index, kv.at[index]).wait_send())
            pl.when(jnp.logical_or(source < line, column == 0))(
                lambda: side_copy(index, kv.at[index]).wait_send()
            )

    @pl.loop(0, blocks)
    def _(index):
        pl.when(index <= at)(lambda: save(index).wait())


def attend(projected, heads):
    size = projected.shape[0]
    blocks = lax.axis_size("blk")
    whole = pl.BlockSpec(memory_space=pltpu.VMEM)
    return pl.pallas_call(
        functools.partial(attend_kernel, heads),
        out_shape=(
            jax.ShapeDtypeStruct((size, heads * HEAD), jnp.bfloat16),
            jax.ShapeDtypeStruct((size, heads * HEAD), jnp.float32),
            jax.ShapeDtypeStruct((heads, 1, size), jnp.float32),
            jax.ShapeDtypeStruct((blocks, size, 2 * HEAD), jnp.bfloat16),
        ),
        in_specs=[whole],
        out_specs=(whole, whole, whole, pl.BlockSpec(memory_space=pl.ANY)),
        scratch_shapes=[
            pltpu.VMEM((blocks, size, 2 * HEAD), jnp.bfloat16),
            pltpu.VMEM((size, heads * HEAD), jnp.float32),
            pltpu.VMEM((heads, size, 128), jnp.float32),
            pltpu.SemaphoreType.DMA((blocks // 2,)),
            pltpu.SemaphoreType.DMA((blocks // 2,)),
            pltpu.SemaphoreType.DMA((blocks // 2,)),
            pltpu.SemaphoreType.DMA((blocks // 2,)),
            pltpu.SemaphoreType.DMA,
            pltpu.SemaphoreType.DMA((blocks,)),
        ],
        compiler_params=pltpu.CompilerParams(
            collective_id=0, has_side_effects=True, vmem_limit_bytes=VMEM_BYTES
        ),
        cost_estimate=cost_of(50),
        name="attend",
    )(projected)


def attend_back_kernel(
    heads,
    x_ref,
    scaled_ref,
    delta_ref,
    kv_ref,
    out_ref,
    kv,
    part,
    side,
    down,
    dq,
    dk,
    dv,
    load_done,
    side_sent,
    side_landed,
    down_sent,
    down_landed,
):
    at = lax.axis_index("blk")
    blocks = lax.axis_size("blk")
    rows = blocks // 2
    line, column = at // 2, at % 2
    partner = at + 1 - 2 * column
    size = x_ref.shape[0]

    def load(index):
        return pltpu.make_async_copy(kv_ref.at[index], kv.at[index], load_done.at[index])

    @pl.loop(0, blocks)
    def _(index):
        pl.when(index <= at)(lambda: load(index).start())

    greet(at, line, rows)

    def side_copy(target):
        return push(
            part.at[target, 1 - column],
            side.at[target],
            side_sent.at[target],
            side_landed.at[target],
            partner,
        )

    def down_copy(target):
        return push(
            part.at[target, column],
            down.at[target],
            down_sent.at[target],
            down_landed.at[target],
            at - 2,
        )

    dq[...] = jnp.zeros_like(dq)
    ahead = lax.broadcasted_iota(jnp.int32, (size, size), 0) - lax.broadcasted_iota(
        jnp.int32, (size, size), 1
    )

    def compute(target, half):
        index = 2 * target + half
        load(index).wait()
        span = (at - index) * size
        for head in range(heads):
            columns = slice(head * HEAD, (head + 1) * HEAD)
            query = x_ref[:, columns]
            scaled = scaled_ref[:, columns]
            key = kv[index, :, :HEAD]
            raw = lax.dot_general(
                key, query, (((1,), (1,)), ((), ())), preferred_element_type=jnp.float32
            )
            squashed = jnp.tanh(raw * (HEAD ** (-0.5) / CAP_VALUE))
            weights = jnp.exp(CAP_VALUE * squashed)
            weights = jnp.where(ahead <= span, weights, 0.0)
            inner = lax.dot_general(
                kv[index, :, HEAD:],
                scaled,
                (((1,), (1,)), ((), ())),
                preferred_element_type=jnp.float32,
            )
            grad_raw = (
                weights * (inner - delta_ref[head]) * (1.0 - squashed * squashed)
            ).astype(jnp.bfloat16)
            dv_now = jnp.dot(
                weights.astype(jnp.bfloat16), scaled, preferred_element_type=jnp.float32
            )
            dk_now = jnp.dot(grad_raw, query, preferred_element_type=jnp.float32)
            dq[:, columns] += lax.dot_general(
                grad_raw, key, (((0,), (0,)), ((), ())), preferred_element_type=jnp.float32
            )
            if head == 0:
                dv[...] = dv_now
                dk[...] = dk_now
            else:
                dv[...] += dv_now
                dk[...] += dk_now
        part[target, half, :, :HEAD] = (dk[...] * HEAD ** (-0.5)).astype(jnp.bfloat16)
        part[target, half, :, HEAD:] = dv[...].astype(jnp.bfloat16)

    def merge(target):
        last = target == line

        @pl.when(jnp.logical_or(target < line, column == 0))
        def _():
            side_copy(target).wait_recv()
            part[target, column] = (
                part[target, column].astype(jnp.float32) + side[target].astype(jnp.float32)
            ).astype(jnp.bfloat16)

        @pl.when(line < rows - 1)
        def _():
            down_copy(target).wait_recv()
            part[target, column] = (
                part[target, column].astype(jnp.float32) + down[target].astype(jnp.float32)
            ).astype(jnp.bfloat16)

        pl.when(target < line)(lambda: down_copy(target).start())

        @pl.when(last)
        def _():
            out_ref[:, heads * HEAD :] = part[target, column]

    @pl.loop(0, rows)
    def _(target):
        @pl.when(jnp.logical_or(target < line, both(target == line, column == 1)))
        def _():
            compute(target, 1 - column)
            side_copy(target).start()

        pl.when(target <= line)(lambda: compute(target, column))
        pl.when(both(line == rows - 1, target > 0))(lambda: merge(target - 1))

    out_ref[:, : heads * HEAD] = (dq[...] * HEAD ** (-0.5)).astype(jnp.bfloat16)

    @pl.loop(0, rows)
    def _(target):
        pl.when(both(target <= line, jnp.logical_or(line < rows - 1, target == rows - 1)))(
            lambda: merge(target)
        )

    @pl.loop(0, rows)
    def _(target):
        pl.when(jnp.logical_or(target < line, both(target == line, column == 1)))(
            lambda: side_copy(target).wait_send()
        )
        pl.when(target < line)(lambda: down_copy(target).wait_send())


def attend_back(projected, scaled, delta, kv_all):
    size = projected.shape[0]
    blocks = lax.axis_size("blk")
    rows = blocks // 2
    heads = scaled.shape[1] // HEAD
    whole = pl.BlockSpec(memory_space=pltpu.VMEM)
    return pl.pallas_call(
        functools.partial(attend_back_kernel, heads),
        out_shape=jax.ShapeDtypeStruct(projected.shape, jnp.bfloat16),
        in_specs=[whole, whole, whole, pl.BlockSpec(memory_space=pl.ANY)],
        out_specs=whole,
        scratch_shapes=[
            pltpu.VMEM((blocks, size, 2 * HEAD), jnp.bfloat16),
            pltpu.VMEM((rows, 2, size, 2 * HEAD), jnp.bfloat16),
            pltpu.VMEM((rows, size, 2 * HEAD), jnp.bfloat16),
            pltpu.VMEM((rows, size, 2 * HEAD), jnp.bfloat16),
            pltpu.VMEM((size, heads * HEAD), jnp.float32),
            pltpu.VMEM((size, HEAD), jnp.float32),
            pltpu.VMEM((size, HEAD), jnp.float32),
            pltpu.SemaphoreType.DMA((blocks,)),
            pltpu.SemaphoreType.DMA((rows,)),
            pltpu.SemaphoreType.DMA((rows,)),
            pltpu.SemaphoreType.DMA((rows,)),
            pltpu.SemaphoreType.DMA((rows,)),
        ],
        compiler_params=pltpu.CompilerParams(
            collective_id=1, has_side_effects=True, vmem_limit_bytes=VMEM_BYTES
        ),
        cost_estimate=cost_of(50),
        name="attend_back",
    )(projected, scaled, delta, kv_all)


def line_gather(own_ref, full, line_sent, line_landed, side_sent, side_landed, own_done, work):
    at = lax.axis_index("blk")
    rows = lax.axis_size("blk") // 2
    line, column = at // 2, at % 2
    size = own_ref.shape[0]

    def spot(source, side):
        start = pl.multiple_of((2 * source + side) * size, size)
        return full.at[pl.ds(start, size), :]

    def line_copy(source, sign, first=False):
        return push(
            own_ref if first else spot(source, column),
            spot(source, column),
            line_sent.at[(sign + 1) // 2, source],
            line_landed.at[source],
            at + 2 * sign,
        )

    def side_copy(source, side, first=False):
        return push(
            own_ref if first else spot(source, side),
            spot(source, side),
            side_sent.at[source],
            side_landed.at[source],
            at + 1 - 2 * column,
        )

    def inside(row):
        return jnp.logical_and(row >= 0, row < rows)

    pl.when(line < rows - 1)(lambda: line_copy(line, 1, True).start())
    pl.when(line > 0)(lambda: line_copy(line, -1, True).start())
    side_copy(line, column, True).start()
    keep = pltpu.make_async_copy(own_ref, spot(line, column), own_done)
    keep.start()
    keep.wait()

    @pl.loop(0, rows + 1)
    def _(step):
        for sign in (-1, 1):
            source = line - sign * step

            @pl.when(both(step > 0, inside(source)))
            def _():
                line_copy(source, sign).wait_recv()
                pl.when(inside(line + sign))(lambda: line_copy(source, sign).start())
                side_copy(source, column).start()

        for sign in (-1, 1):
            source = line - sign * (step - 1)
            once = step > 0 if sign == -1 else step > 1

            @pl.when(both(once, inside(source)))
            def _():
                side_copy(source, 1 - column).wait_recv()
                work(source)

    @pl.loop(0, rows)
    def _(source):
        pl.when(both(source <= line, line < rows - 1))(lambda: line_copy(source, 1).wait_send())
        pl.when(both(source >= line, line > 0))(lambda: line_copy(source, -1).wait_send())
        side_copy(source, column).wait_send()


def line_scatter(part, side, lane, out_ref, side_sent, side_landed, lane_sent, lane_landed, work, fill):
    at = lax.axis_index("blk")
    rows = lax.axis_size("blk") // 2
    line, column = at // 2, at % 2
    size = out_ref.shape[0]

    def spot(target, half):
        start = pl.multiple_of((2 * target + half) * size, size)
        return pl.ds(start, size)

    def side_copy(target):
        return push(
            part.at[spot(target, 1 - column), :],
            side.at[target],
            side_sent.at[target],
            side_landed.at[target],
            at + 1 - 2 * column,
        )

    def lane_copy(target, sign):
        slot = target if sign == 1 else jnp.where(target == line - 1, rows, target)
        return push(
            part.at[spot(target, column), :],
            lane.at[slot],
            lane_sent.at[target],
            lane_landed.at[slot],
            at + 2 * sign,
        )

    def lane_wait(slot):
        push(
            lane.at[slot], lane.at[slot], lane_sent.at[0], lane_landed.at[slot], at + 1 - 2 * column
        ).wait_recv()

    def inside(row):
        return jnp.logical_and(row >= 0, row < rows)

    @pl.loop(0, rows)
    def _(step):
        for sign in (-1, 1):
            target = line + sign * (rows - 1 - step)
            once = step >= 0 if sign == -1 else step < rows - 1

            @pl.when(both(once, inside(target)))
            def _():
                work(target)
                side_copy(target).start()

    def merge(target):
        mine = spot(target, column)
        side_copy(target).wait_recv()
        part[mine, :] = (
            part[mine, :].astype(jnp.float32) + side[target].astype(jnp.float32)
        ).astype(jnp.bfloat16)

        def pass_on(sign):
            @pl.when(inside(line - sign))
            def _():
                lane_wait(target)
                part[mine, :] = (
                    part[mine, :].astype(jnp.float32) + lane[target].astype(jnp.float32)
                ).astype(jnp.bfloat16)

            lane_copy(target, sign).start()

        pl.when(target > line)(lambda: pass_on(1))
        pl.when(target < line)(lambda: pass_on(-1))

    @pl.loop(0, rows)
    def _(step):
        fill(step)
        for sign in (-1, 1):
            target = line + sign * (rows - 1 - step)
            once = step >= 0 if sign == -1 else step < rows - 1
            pl.when(both(once, inside(target)))(lambda: merge(target))

    mine = spot(line, column)
    out_ref[...] = part[mine, :].astype(jnp.float32)

    @pl.when(line > 0)
    def _():
        lane_wait(line)
        out_ref[...] += lane[line].astype(jnp.float32)

    @pl.when(line < rows - 1)
    def _():
        lane_wait(rows)
        out_ref[...] += lane[rows].astype(jnp.float32)

    @pl.loop(0, rows)
    def _(target):
        side_copy(target).wait_send()
        pl.when(target > line)(lambda: lane_copy(target, 1).wait_send())
        pl.when(target < line)(lambda: lane_copy(target, -1).wait_send())


def line_sems(rows):
    dma = pltpu.SemaphoreType.DMA
    return [dma((2, rows)), dma((rows,)), dma((rows,)), dma((rows,)), dma]


def lane_sems(rows):
    dma = pltpu.SemaphoreType.DMA
    return [dma((rows,)), dma((rows,)), dma((rows,)), dma((rows + 1,))]


def ffn_kernel(
    act_ref,
    w_ref,
    out_ref,
    acts_ref,
    w,
    acts,
    hidden,
    part,
    side,
    lane,
    w_done,
    save_done,
    *sems,
):
    at = lax.axis_index("blk")
    rows = lax.axis_size("blk") // 2
    pair = 2 * act_ref.shape[0]

    def load(which):
        return pltpu.make_async_copy(w_ref.at[which], w.at[which], w_done.at[which])

    def pair_rows(source):
        return pl.ds(pl.multiple_of(source * pair, pair), pair)

    def save(source):
        return pltpu.make_async_copy(
            acts.at[pair_rows(source), :], acts_ref.at[pair_rows(source), :], save_done.at[source]
        )

    for which in range(3):
        load(which).start()
    greet(at, at // 2, rows)
    for which in range(3):
        load(which).wait()

    def expand(source):
        save(source).start()
        rows_now = acts[pair_rows(source), :]
        gate = contract_last(w[0], rows_now)
        up = contract_last(w[1], rows_now)
        hidden[source] = (gelu_value(gate) * up).astype(jnp.bfloat16)

    def reduce(target):
        part[pair_rows(target), :] = lax.dot_general(
            hidden[target], w[2], (((0,), (0,)), ((), ())), preferred_element_type=jnp.float32
        ).astype(jnp.bfloat16)

    line_gather(act_ref, acts, *sems[:5], expand)
    line_scatter(part, side, lane, out_ref, *sems[5:], reduce, lambda step: None)
    pl.loop(0, rows)(lambda source: save(source).wait())


def ffn_forward(act_ffn, w_parts):
    size, width = act_ffn.shape
    units = w_parts.shape[1]
    blocks = lax.axis_size("blk")
    rows = blocks // 2
    whole = pl.BlockSpec(memory_space=pltpu.VMEM)
    far = pl.BlockSpec(memory_space=pl.ANY)
    return pl.pallas_call(
        ffn_kernel,
        out_shape=(
            jax.ShapeDtypeStruct((size, width), jnp.float32),
            jax.ShapeDtypeStruct((blocks * size, width), jnp.bfloat16),
        ),
        in_specs=[whole, far],
        out_specs=(whole, far),
        scratch_shapes=[
            pltpu.VMEM(w_parts.shape, jnp.bfloat16),
            pltpu.VMEM((blocks * size, width), jnp.bfloat16),
            pltpu.VMEM((rows, units, 2 * size), jnp.bfloat16),
            pltpu.VMEM((blocks * size, width), jnp.bfloat16),
            pltpu.VMEM((rows, size, width), jnp.bfloat16),
            pltpu.VMEM((rows + 1, size, width), jnp.bfloat16),
            pltpu.SemaphoreType.DMA((3,)),
            pltpu.SemaphoreType.DMA((rows,)),
            *line_sems(rows),
            *lane_sems(rows),
        ],
        compiler_params=pltpu.CompilerParams(
            collective_id=2, has_side_effects=True, vmem_limit_bytes=VMEM_BYTES
        ),
        cost_estimate=cost_of(115),
        name="ffn_forward",
    )(act_ffn, w_parts)


FILL_COLUMNS = 256
FILL_FIRST = 3


def ffn_back_kernel(
    owners,
    grad_ref,
    acts_ref,
    w_ref,
    out_ref,
    sum_ref,
    w,
    rights,
    lefts,
    part,
    side,
    lane,
    stage,
    w_done,
    acts_done,
    stage_done,
    *sems,
):
    at = lax.axis_index("blk")
    rows = lax.axis_size("blk") // 2
    size, width = grad_ref.shape
    pair = 2 * size
    units = w.shape[1]
    acts, grads = rights.at[0], rights.at[1]

    def load(which):
        return pltpu.make_async_copy(w_ref.at[which], w.at[which], w_done.at[which])

    def pair_rows(source):
        return pl.ds(pl.multiple_of(source * pair, pair), pair)

    acts_copy = pltpu.make_async_copy(acts_ref, acts, acts_done)
    acts_copy.start()
    for which in range(3):
        load(which).start()
    greet(at, at // 2, rows)
    acts_copy.wait()
    for which in range(3):
        load(which).wait()

    def expand(source):
        columns = pair_rows(source)
        rows_now = acts[pair_rows(source), :]
        gate = contract_last(w[0], rows_now)
        up = contract_last(w[1], rows_now)
        grad_hidden = contract_last(w[2], grads[pair_rows(source), :])
        bent = jnp.tanh(GELU_SCALE * (gate + GELU_CUBIC * gate * gate * gate))
        value = 0.5 * gate * (1.0 + bent)
        slope = 0.5 * (1.0 + bent) + 0.5 * gate * (1.0 - bent * bent) * GELU_SCALE * (
            1.0 + 3.0 * GELU_CUBIC * gate * gate
        )
        lefts[2, :, columns] = (value * up).astype(jnp.bfloat16)
        lefts[0, :, columns] = (grad_hidden * up * slope).astype(jnp.bfloat16)
        lefts[1, :, columns] = (grad_hidden * value).astype(jnp.bfloat16)

    def reduce(target):
        columns = pair_rows(target)
        dims = (((0,), (0,)), ((), ()))
        total = lax.dot_general(
            lefts[0, :, columns], w[0], dims, preferred_element_type=jnp.float32
        ) + lax.dot_general(lefts[1, :, columns], w[1], dims, preferred_element_type=jnp.float32)
        part[pair_rows(target), :] = total.astype(jnp.bfloat16)

    pieces = width // FILL_COLUMNS
    total_pieces = 3 * pieces

    def piece_columns(item):
        return pl.ds(pl.multiple_of((item % pieces) * FILL_COLUMNS, FILL_COLUMNS), FILL_COLUMNS)

    def stage_copy(item):
        return pltpu.make_async_copy(
            stage.at[item % 2],
            sum_ref.at[:, item // pieces, :, piece_columns(item)],
            stage_done.at[item % 2],
        )

    def fill_one(item):
        which = item // pieces
        total = jnp.dot(
            lefts[which],
            rights[which // 2, :, piece_columns(item)],
            preferred_element_type=jnp.float32,
        )
        pl.when(item > 1)(lambda: stage_copy(item - 2).wait())
        stage[item % 2] = total.astype(jnp.bfloat16).reshape(
            owners, units // owners, FILL_COLUMNS
        )
        stage_copy(item).start()

    each = pl.cdiv(total_pieces - FILL_FIRST, rows - 1)

    def fill(step):
        first = jnp.maximum(FILL_FIRST + (step - 1) * each, 0)
        last = jnp.minimum(FILL_FIRST + step * each, total_pieces)

        @pl.loop(0, each)
        def _(item):
            pl.when(first + item < last)(lambda: fill_one(first + item))

    line_gather(grad_ref, grads, *sems[:5], expand)
    line_scatter(part, side, lane, out_ref, *sems[5:], reduce, fill)
    stage_copy(total_pieces - 2).wait()
    stage_copy(total_pieces - 1).wait()


def ffn_back(grad_ffn, acts, w_parts, owners):
    size, width = grad_ffn.shape
    units = w_parts.shape[1]
    blocks = lax.axis_size("blk")
    rows = blocks // 2
    tokens = blocks * size
    whole = pl.BlockSpec(memory_space=pltpu.VMEM)
    far = pl.BlockSpec(memory_space=pl.ANY)
    return pl.pallas_call(
        functools.partial(ffn_back_kernel, owners),
        out_shape=(
            jax.ShapeDtypeStruct((size, width), jnp.float32),
            jax.ShapeDtypeStruct((owners, 3, units // owners, width), jnp.bfloat16),
        ),
        in_specs=[whole, far, far],
        out_specs=(whole, far),
        scratch_shapes=[
            pltpu.VMEM(w_parts.shape, jnp.bfloat16),
            pltpu.VMEM((2, tokens, width), jnp.bfloat16),
            pltpu.VMEM((3, units, tokens), jnp.bfloat16),
            pltpu.VMEM((tokens, width), jnp.bfloat16),
            pltpu.VMEM((rows, size, width), jnp.bfloat16),
            pltpu.VMEM((rows + 1, size, width), jnp.bfloat16),
            pltpu.VMEM((2, owners, units // owners, FILL_COLUMNS), jnp.bfloat16),
            pltpu.SemaphoreType.DMA((3,)),
            pltpu.SemaphoreType.DMA,
            pltpu.SemaphoreType.DMA((2,)),
            *line_sems(rows),
            *lane_sems(rows),
        ],
        compiler_params=pltpu.CompilerParams(
            collective_id=3, has_side_effects=True, vmem_limit_bytes=VMEM_BYTES
        ),
        cost_estimate=cost_of(115),
        name="ffn_back",
    )(grad_ffn, acts, w_parts)


def ffn_hidden(acts, w_parts):
    gate = contract_last(acts, w_parts[0])
    up = contract_last(acts, w_parts[1])
    return (gate, up, (gelu_value(gate) * up).astype(jnp.bfloat16))


def scatter_tokens(partial):
    return lax.psum_scatter(
        partial.astype(jnp.bfloat16), "blk", scatter_dimension=0, tiled=True
    ).astype(jnp.float32)


def ffn_forward_wide(act_ffn, w_parts):
    acts = lax.all_gather(act_ffn, "blk", axis=0, tiled=True)
    hidden = ffn_hidden(acts, w_parts)[2]
    partial = jnp.dot(hidden, w_parts[2], preferred_element_type=jnp.float32)
    return (scatter_tokens(partial), acts)


def ffn_back_wide(grad_ffn, acts, w_parts, owners):
    grads = lax.all_gather(grad_ffn, "blk", axis=0, tiled=True)
    gate, up, hidden = ffn_hidden(acts, w_parts)
    grad_hidden = contract_last(grads, w_parts[2])
    grad_gate = (grad_hidden * up * gelu_slope(gate)).astype(jnp.bfloat16)
    grad_up = (grad_hidden * gelu_value(gate)).astype(jnp.bfloat16)
    partial = jnp.dot(grad_gate, w_parts[0], preferred_element_type=jnp.float32) + jnp.dot(
        grad_up, w_parts[1], preferred_element_type=jnp.float32
    )
    sums = jnp.stack(
        [
            jnp.einsum("tf,td->fd", left, right, preferred_element_type=jnp.float32)
            for left, right in ((grad_gate, acts), (grad_up, acts), (hidden, grads))
        ]
    ).astype(jnp.bfloat16)
    units = w_parts.shape[1]
    owned = sums.reshape(3, owners, units // owners, sums.shape[2])
    return (scatter_tokens(partial), jnp.transpose(owned, (1, 0, 2, 3)))


def cost_of(microseconds):
    return pl.CostEstimate(
        flops=int(microseconds * 1e9), bytes_accessed=int(microseconds * 3e6), transcendentals=0
    )


def push_sp(source, target, sent, landed, peer):
    return pltpu.make_async_remote_copy(
        src_ref=source,
        dst_ref=target,
        send_sem=sent,
        recv_sem=landed,
        device_id={"sp": peer},
        device_id_type=pl.DeviceIdType.MESH,
    )


def greet_sp(me, groups):
    barrier = pltpu.get_barrier_semaphore()
    for step in range(1, groups):
        pl.semaphore_signal(
            barrier,
            inc=1,
            device_id={"sp": (me + step) % groups},
            device_id_type=pl.DeviceIdType.MESH,
        )
    pl.semaphore_wait(barrier, groups - 1)


def gather_project_kernel(x_ref, w_ref, full_ref, out_ref, w, w_done, own_done, sent, landed):
    me = lax.axis_index("sp")
    size = x_ref.shape[0]
    units = w.shape[0]
    mate = me + 1 - 2 * (me % 2)
    across = (me + 2) % 4

    def spot(member):
        return full_ref.at[pl.ds(pl.multiple_of(member * size, size), size), :]

    load = pltpu.make_async_copy(
        w_ref.at[pl.ds(pl.multiple_of(me * units, units), units), :], w, w_done
    )
    load.start()
    greet_sp(me, 4)
    over = push_sp(x_ref, spot(me), sent.at[0], landed.at[0], across)
    over.start()
    beside = push_sp(x_ref, spot(me), sent.at[1], landed.at[1], mate)
    beside.start()
    keep = pltpu.make_async_copy(x_ref, spot(me), own_done)
    keep.start()
    keep.wait()
    load.wait()

    def project(chip):
        rows = pl.ds(pl.multiple_of(chip * 2 * size, 2 * size), 2 * size)
        out_ref[rows, :] = contract_last(full_ref[rows, :], w[...]).astype(jnp.bfloat16)

    beside.wait_recv()
    project(me // 2)
    over.wait_recv()
    onward = push_sp(spot(across), spot(across), sent.at[2], landed.at[2], mate)
    onward.start()
    onward.wait_recv()
    project(across // 2)
    over.wait_send()
    beside.wait_send()
    onward.wait_send()


def gather_project(rows, weights, identity):
    size, width = rows.shape
    units = weights.shape[0] // 4
    whole = pl.BlockSpec(memory_space=pltpu.VMEM)
    return pl.pallas_call(
        gather_project_kernel,
        out_shape=(
            jax.ShapeDtypeStruct((4 * size, width), jnp.bfloat16),
            jax.ShapeDtypeStruct((4 * size, units), jnp.bfloat16),
        ),
        in_specs=[whole, pl.BlockSpec(memory_space=pl.ANY)],
        out_specs=(whole, whole),
        scratch_shapes=[
            pltpu.VMEM((units, width), jnp.bfloat16),
            pltpu.SemaphoreType.DMA,
            pltpu.SemaphoreType.DMA,
            pltpu.SemaphoreType.DMA((3,)),
            pltpu.SemaphoreType.DMA((3,)),
        ],
        compiler_params=pltpu.CompilerParams(
            collective_id=identity, has_side_effects=True, vmem_limit_bytes=VMEM_BYTES
        ),
        cost_estimate=cost_of(18),
        name="gather_project",
    )(rows, weights)


def exchange_project_kernel(x_ref, w_ref, out_ref, w, got, w_done, own_done, sent, landed):
    me = lax.axis_index("sp")
    size = out_ref.shape[0]
    units = x_ref.shape[1]

    def rows_of(member):
        return x_ref.at[pl.ds(pl.multiple_of(member * size, size), size), :]

    def load(member):
        rows = pl.ds(pl.multiple_of(member * units, units), units)
        return pltpu.make_async_copy(w_ref.at[rows, :], w.at[rows, :], w_done.at[member])

    def send(step):
        peer = (me + step) % 4
        return push_sp(rows_of(peer), got.at[4 - step], sent.at[step], landed.at[4 - step], peer)

    greet_sp(me, 4)
    for step in (2, 1, 3):
        send(step).start()
    keep = pltpu.make_async_copy(rows_of(me), got.at[0], own_done)
    keep.start()
    for step in range(4):
        load((me + step) % 4).start()
    keep.wait()
    for step in (0, 1, 3, 2):
        member = (me + step) % 4
        load(member).wait()
        if step > 0:
            send(4 - step).wait_recv()
        rows = pl.ds(pl.multiple_of(member * units, units), units)
        term = jnp.dot(got[step], w[rows, :], preferred_element_type=jnp.float32)
        if step == 0:
            out_ref[...] = term
        else:
            out_ref[...] += term
    for step in (1, 2, 3):
        send(step).wait_send()


def exchange_project(columns, weights, identity):
    size = columns.shape[0] // 4
    whole = pl.BlockSpec(memory_space=pltpu.VMEM)
    return pl.pallas_call(
        exchange_project_kernel,
        out_shape=jax.ShapeDtypeStruct((size, weights.shape[1]), jnp.float32),
        in_specs=[whole, pl.BlockSpec(memory_space=pl.ANY)],
        out_specs=whole,
        scratch_shapes=[
            pltpu.VMEM(weights.shape, jnp.bfloat16),
            pltpu.VMEM((4, size, columns.shape[1]), jnp.bfloat16),
            pltpu.SemaphoreType.DMA((4,)),
            pltpu.SemaphoreType.DMA,
            pltpu.SemaphoreType.DMA((4,)),
            pltpu.SemaphoreType.DMA((4,)),
        ],
        compiler_params=pltpu.CompilerParams(
            collective_id=identity, has_side_effects=True, vmem_limit_bytes=VMEM_BYTES
        ),
        cost_estimate=cost_of(16),
        name="exchange_project",
    )(columns, weights)


def finish_kernel(
    cols_ref,
    act_ref,
    att_ref,
    grad_ref,
    w_ref,
    tokens_ref,
    middle_ref,
    gain_ref,
    rows_ref,
    sum_ref,
    tokens_grad_ref,
    gains_ref,
    w,
    got,
    grad_in,
    part,
    side,
    lane,
    mine,
    from_sp,
    from_side,
    from_line,
    w_done,
    own_done,
    swap_sent,
    swap_landed,
    sp_sent,
    sp_landed,
    gain_side,
    line_sent,
    line_landed,
    *sems,
):
    at = lax.axis_index("blk")
    me = lax.axis_index("sp")
    rows = lax.axis_size("blk") // 2
    line, column = at // 2, at % 2
    partner = at + 1 - 2 * column
    block = sum_ref.shape[0]
    size = tokens_ref.shape[0]
    units = cols_ref.shape[1]
    extra = block - size

    barrier = pltpu.get_barrier_semaphore()
    for step in range(1, 4):
        pl.semaphore_signal(
            barrier, inc=1, device_id={"sp": (me + step) % 4}, device_id_type=pl.DeviceIdType.MESH
        )

    def line_peer(step):
        return 2 * ((line + step) % rows) + column

    for peer in [partner] + [line_peer(step) for step in range(1, rows)]:
        pl.semaphore_signal(
            barrier, inc=1, device_id={"blk": peer}, device_id_type=pl.DeviceIdType.MESH
        )

    def load(member):
        span = pl.ds(pl.multiple_of(member * units, units), units)
        return pltpu.make_async_copy(w_ref.at[span, :], w.at[span, :], w_done.at[member])

    def rows_of(member):
        return cols_ref.at[pl.ds(pl.multiple_of(member * size, size), size), :]

    def swap(step):
        peer = (me + step) % 4
        return push_sp(
            rows_of(peer), got.at[4 - step], swap_sent.at[step], swap_landed.at[4 - step], peer
        )

    for step in range(4):
        load((me + step) % 4).start()
    keep = pltpu.make_async_copy(rows_of(me), got.at[0], own_done)
    keep.start()
    pl.semaphore_wait(barrier, 3 + rows)
    for step in (2, 1, 3):
        swap(step).start()
    keep.wait()

    def sp_gains(step):
        return push_sp(
            mine, from_sp.at[4 - step], sp_sent.at[step], sp_landed.at[4 - step], (me + step) % 4
        )

    def side_gains():
        return push(from_sp.at[0], from_side, gain_side.at[0], gain_side.at[1], partner)

    def line_gains(step):
        return push(
            from_line.at[0],
            from_line.at[rows - step],
            line_sent.at[step],
            line_landed.at[rows - step],
            line_peer(step),
        )

    def reduce(target):
        dims = (((0,), (0,)), ((), ()))
        wide_columns = pl.ds(pl.multiple_of(target * 2 * size, 2 * size), 2 * size)
        term = lax.dot_general(
            cols_ref[:, wide_columns], act_ref[...], dims, preferred_element_type=jnp.float32
        ).astype(jnp.bfloat16)
        columns = pl.ds(pl.multiple_of(target * 2 * extra, 2 * extra), 2 * extra)
        more = lax.dot_general(
            att_ref[:, columns], grad_ref[...], dims, preferred_element_type=jnp.float32
        ).astype(jnp.bfloat16)
        for half in range(2):
            start = pl.multiple_of((2 * target + half) * block, block)
            part[pl.ds(start, size), :] = term[half * size : (half + 1) * size]
            start = pl.multiple_of((2 * target + half) * block + size, extra)
            part[pl.ds(start, extra), :] = more[half * extra : (half + 1) * extra]

    def inputs_back():
        for step in (0, 1, 3, 2):
            member = (me + step) % 4
            load(member).wait()
            if step > 0:
                swap(4 - step).wait_recv()
            span = pl.ds(pl.multiple_of(member * units, units), units)
            term = jnp.dot(got[step], w[span, :], preferred_element_type=jnp.float32)
            if step == 0:
                grad_in[...] = term
            else:
                grad_in[...] += term
        normed, inverse = norm_parts(tokens_ref[...].astype(jnp.float32))
        grad_v, gain_row = norm_back(grad_in[...], normed, inverse, gain_ref[...])
        tokens_grad_ref[...] = (middle_ref[...] + grad_v).astype(jnp.bfloat16)
        mine[...] = rows_ref[...]
        mine[0:1, :] = gain_row[None, :]
        for step in range(1, 4):
            sp_gains(step).start()

    def fill(step):
        pl.when(step == 0)(inputs_back)

        @pl.when(step == 1)
        def _():
            total = mine[...]
            for other in range(1, 4):
                sp_gains(4 - other).wait_recv()
                total = total + from_sp[other]
            from_sp[0] = total
            side_gains().start()

        @pl.when(step == 2)
        def _():
            side_gains().wait_recv()
            from_line[0] = from_sp[0] + from_side[...]
            for other in range(1, rows):
                line_gains(other).start()

    line_scatter(part, side, lane, sum_ref, *sems, reduce, fill)
    total = from_line[0]
    for other in range(1, rows):
        line_gains(rows - other).wait_recv()
        total = total + from_line[other]
    gains_ref[...] = total
    for step in (1, 2, 3):
        swap(step).wait_send()
        sp_gains(step).wait_send()
    side_gains().wait_send()
    for step in range(1, rows):
        line_gains(step).wait_send()


def finish(cols, act_block, attended, grad_block, w_qkv, tokens, grad_middle, gain, gain_rows):
    blocks = lax.axis_size("blk")
    rows = blocks // 2
    size, width = tokens.shape
    block = (cols.shape[1] + attended.shape[1]) // blocks
    whole = pl.BlockSpec(memory_space=pltpu.VMEM)
    dma = pltpu.SemaphoreType.DMA
    small = gain_rows.shape
    total, tokens_grad, gains_all = pl.pallas_call(
        finish_kernel,
        out_shape=(
            jax.ShapeDtypeStruct((block, width), jnp.float32),
            jax.ShapeDtypeStruct((size, width), jnp.bfloat16),
            jax.ShapeDtypeStruct(small, jnp.float32),
        ),
        in_specs=[whole] * 4 + [pl.BlockSpec(memory_space=pl.ANY)] + [whole] * 4,
        out_specs=(whole,) * 3,
        scratch_shapes=[
            pltpu.VMEM(w_qkv.shape, jnp.bfloat16),
            pltpu.VMEM((4, size, cols.shape[1]), jnp.bfloat16),
            pltpu.VMEM((size, width), jnp.float32),
            pltpu.VMEM((blocks * block, width), jnp.bfloat16),
            pltpu.VMEM((rows, block, width), jnp.bfloat16),
            pltpu.VMEM((rows + 1, block, width), jnp.bfloat16),
            pltpu.VMEM(small, jnp.float32),
            pltpu.VMEM((4, *small), jnp.float32),
            pltpu.VMEM(small, jnp.float32),
            pltpu.VMEM((rows, *small), jnp.float32),
            dma((4,)),
            dma,
            dma((4,)),
            dma((4,)),
            dma((4,)),
            dma((4,)),
            dma((2,)),
            dma((rows,)),
            dma((rows,)),
            *lane_sems(rows),
        ],
        compiler_params=pltpu.CompilerParams(
            collective_id=8, has_side_effects=True, vmem_limit_bytes=VMEM_BYTES
        ),
        cost_estimate=cost_of(85),
        name="finish",
    )(cols, act_block, attended, grad_block, w_qkv, tokens, grad_middle, gain, gain_rows)
    shared = cols.shape[1] // blocks
    return (total[:shared], total[shared:], tokens_grad, gains_all)


def weight_sums_wide(left, right):
    term = jnp.einsum("tc,td->cd", left, right, preferred_element_type=jnp.float32)
    return scatter_tokens(term)


def finish_wide(cols, act_block, attended, grad_block, w_qkv, tokens, grad_middle, gain, gain_rows):
    grad_act_in = exchange_project(cols, w_qkv, 7)
    normed, inverse = norm_parts(tokens.astype(jnp.float32))
    grad_v, gain_row = norm_back(grad_act_in, normed, inverse, gain)
    gains_all = lax.psum(jnp.concatenate([gain_row[None], gain_rows[1:]]), ("blk", "sp"))
    return (
        weight_sums_wide(cols, act_block),
        weight_sums_wide(attended, grad_block),
        (grad_middle + grad_v).astype(jnp.bfloat16),
        gains_all,
    )


def body(tokens, w_qkv, w_out, gains, w_ffn, cotangent):
    groups = lax.axis_size("sp")
    heads_here = HEADS // groups
    source = tokens.astype(jnp.float32)
    normed_in, inverse_in = norm_parts(source)
    act_in = (normed_in * gains[0]).astype(jnp.bfloat16)
    act_block, projected = gather_project(act_in, w_qkv, 4)
    block_rows = projected.shape[0]
    attended_cols, attended, totals, kv_all = attend(projected, heads_here)
    attn = exchange_project(attended_cols, w_out, 5)
    normed_attn, inverse_attn = norm_parts(attn)
    middle = source + normed_attn * gains[1]
    normed_mid, inverse_mid = norm_parts(middle)
    act_ffn = (normed_mid * gains[2]).astype(jnp.bfloat16)
    wide = lax.axis_size("blk") > 8
    w_parts = jnp.transpose(w_ffn, (1, 0, 2))
    ffn_out, act_all = (ffn_forward_wide if wide else ffn_forward)(act_ffn, w_parts)
    normed_ffn, inverse_ffn = norm_parts(ffn_out)
    result = middle + normed_ffn * gains[3]
    grad_out = cotangent.astype(jnp.float32)
    grad_ffn_f, gain_grad3 = norm_back(grad_out, normed_ffn, inverse_ffn, gains[3])
    grad_ffn = grad_ffn_f.astype(jnp.bfloat16)
    grad_act_ffn, ffn_sums = (ffn_back_wide if wide else ffn_back)(
        grad_ffn, act_all, w_parts, groups
    )
    grad_norm_mid, gain_grad2 = norm_back(grad_act_ffn, normed_mid, inverse_mid, gains[2])
    grad_middle = grad_out + grad_norm_mid
    grad_attn_f, gain_grad1 = norm_back(grad_middle, normed_attn, inverse_attn, gains[1])
    grad_attn = grad_attn_f.astype(jnp.bfloat16)
    grad_block, grad_attended = gather_project(grad_attn, w_out, 6)
    grad_heads = grad_attended.astype(jnp.float32).reshape(block_rows, heads_here, HEAD)
    totals_rows = jnp.transpose(totals.reshape(heads_here, block_rows))
    scaled = (grad_heads / totals_rows[..., None]).astype(jnp.bfloat16)
    row_delta = (
        jnp.sum(grad_heads * attended.reshape(block_rows, heads_here, HEAD), axis=-1) / totals_rows
    )
    grad_cols = attend_back(
        projected,
        scaled.reshape(block_rows, heads_here * HEAD),
        jnp.transpose(row_delta).reshape(heads_here, 1, block_rows),
        kv_all,
    )
    gain_rows = jnp.stack(
        [jnp.zeros_like(gain_grad1), gain_grad1, gain_grad2, gain_grad3]
        + [jnp.zeros_like(gain_grad1)] * 4
    )
    qkv_grad, out_grad, tokens_grad, gains_all = (finish_wide if wide else finish)(
        grad_cols,
        act_block,
        attended_cols,
        grad_block,
        w_qkv,
        tokens,
        grad_middle,
        gains[0][None],
        gain_rows,
    )
    ffn_part = lax.psum_scatter(ffn_sums, "sp", scatter_dimension=0, tiled=True)
    ffn_grad = jnp.transpose(ffn_part[0].astype(jnp.float32), (1, 0, 2))
    share = gains_all.shape[1] // (groups * lax.axis_size("blk"))
    place = lax.axis_index("sp") * lax.axis_size("blk") + lax.axis_index("blk")
    gains_grad = lax.dynamic_slice_in_dim(gains_all[:4], place * share, share, 1)
    return (result.astype(jnp.bfloat16), tokens_grad, qkv_grad, out_grad, gains_grad, ffn_grad)


def solution(mesh):
    return jax.shard_map(
        body,
        mesh=mesh,
        in_specs=(
            P(("blk", "sp"), None),
            P(),
            P(),
            P(),
            P("blk", None, None),
            P(("blk", "sp"), None),
        ),
        out_specs=(
            P(("blk", "sp"), None),
            P(("blk", "sp"), None),
            P(("sp", "blk"), None),
            P(("sp", "blk"), None),
            P(None, ("sp", "blk")),
            P(("blk", "sp"), None, None),
        ),
        check_vma=False,
    )
```

```python
import functools

import jax
import jax.numpy as jnp
from jax import lax
from jax.experimental import pallas as pl
from jax.experimental.pallas import tpu as pltpu
from jax.sharding import PartitionSpec as P

HEADS = 8
KV_HEADS = 4
HEAD = 256


VMEM_BYTES = 62 * 1024 * 1024
NORM_EPSILON = 1e-06
CAP_VALUE = 50.0
GELU_SCALE = 0.7978845608028654
GELU_CUBIC = 0.044715


def norm_parts(values):
    inverse = lax.rsqrt(jnp.mean(values * values, axis=-1, keepdims=True) + NORM_EPSILON)
    return (values * inverse, inverse)


def norm_back(grad_y, normed, inverse, gain):
    grad_n = grad_y * gain
    grad_v = inverse * (grad_n - normed * jnp.mean(grad_n * normed, axis=-1, keepdims=True))
    return (grad_v, jnp.sum(grad_y * normed, axis=0))


def gelu_value(values):
    return (
        0.5
        * values
        * (1.0 + jnp.tanh(GELU_SCALE * (values + GELU_CUBIC * values * values * values)))
    )


def gelu_slope(values):
    bent = jnp.tanh(GELU_SCALE * (values + GELU_CUBIC * values * values * values))
    return 0.5 * (1.0 + bent) + 0.5 * values * (1.0 - bent * bent) * GELU_SCALE * (
        1.0 + 3.0 * GELU_CUBIC * values * values
    )


def contract_last(left, right):
    return lax.dot_general(
        left, right, (((1,), (1,)), ((), ())), preferred_element_type=jnp.float32
    )


def push(source, target, sent, landed, block):
    return pltpu.make_async_remote_copy(
        src_ref=source,
        dst_ref=target,
        send_sem=sent,
        recv_sem=landed,
        device_id={"blk": block},
        device_id_type=pl.DeviceIdType.MESH,
    )


def greet(at, line, rows, sp_peer=None):
    barrier = pltpu.get_barrier_semaphore()
    others = 1
    if sp_peer is not None:
        others = 2
        pl.semaphore_signal(
            barrier, inc=1, device_id={"sp": sp_peer}, device_id_type=pl.DeviceIdType.MESH
        )

    def tell(block):
        pl.semaphore_signal(
            barrier, inc=1, device_id={"blk": block}, device_id_type=pl.DeviceIdType.MESH
        )

    tell(at + 1 - 2 * (at % 2))
    pl.when(line > 0)(lambda: tell(at - 2))
    pl.when(line < rows - 1)(lambda: tell(at + 2))
    pl.semaphore_wait(barrier, others + jnp.minimum(line, 1) + jnp.minimum(rows - 1 - line, 1))


def both(*terms):
    result = terms[0]
    for term in terms[1:]:
        result = jnp.logical_and(result, term)
    return result


def attend_kernel(
    heads,
    x_ref,
    low_ref,
    att_ref,
    tot_ref,
    kv_ref,
    kv,
    acc,
    part,
    up_sent,
    up_landed,
    side_sent,
    side_landed,
    own_done,
    save_done,
):
    at = lax.axis_index("blk")
    blocks = lax.axis_size("blk")
    rows = blocks // 2
    line, column = at // 2, at % 2
    partner = at + 1 - 2 * column
    size = x_ref.shape[0]
    first = heads * HEAD
    own = x_ref.at[:, pl.ds(first, 2 * HEAD)]
    greet(at, line, rows)

    def up_copy(index, source):
        return push(source, kv.at[index], up_sent.at[index // 2], up_landed.at[index // 2], at + 2)

    def side_copy(index, source):
        return push(
            source, kv.at[index], side_sent.at[index // 2], side_landed.at[index // 2], partner
        )

    def save(index):
        return pltpu.make_async_copy(kv.at[index], kv_ref.at[index], save_done.at[index])

    pl.when(line < rows - 1)(lambda: up_copy(at, own).start())
    pl.when(column == 0)(lambda: side_copy(at, own).start())
    keep = pltpu.make_async_copy(own, kv.at[at], own_done)
    keep.start()
    acc[...] = jnp.zeros_like(acc)
    part[...] = jnp.zeros_like(part)
    keep.wait()
    ahead = lax.broadcasted_iota(jnp.int32, (size, size), 1) - lax.broadcasted_iota(
        jnp.int32, (size, size), 0
    )

    def compute(index):
        save(index).start()
        span = (at - index) * size
        for head in range(heads):
            raw = lax.dot_general(
                x_ref[:, head * HEAD : (head + 1) * HEAD],
                kv[index, :, :HEAD],
                (((1,), (1,)), ((), ())),
                preferred_element_type=jnp.float32,
            )
            weights = jnp.exp(CAP_VALUE * jnp.tanh(raw * (HEAD ** (-0.5) / CAP_VALUE)))
            weights = jnp.where(ahead <= span, weights, 0.0)
            total = weights[:, :128]
            for piece in range(1, size // 128):
                total = total + weights[:, piece * 128 : (piece + 1) * 128]
            part[head] += total
            acc[:, head * HEAD : (head + 1) * HEAD] += jnp.dot(
                weights.astype(jnp.bfloat16),
                kv[index, :, HEAD:],
                preferred_element_type=jnp.float32,
            )

    @pl.loop(0, rows + 1)
    def _(step):
        source = line - step
        index = 2 * source + column

        @pl.when(both(step > 0, source >= 0))
        def _():
            up_copy(index, kv.at[index]).wait_recv()
            pl.when(line < rows - 1)(lambda: up_copy(index, kv.at[index]).start())
            side_copy(index, kv.at[index]).start()

        pl.when(source >= 0)(lambda: compute(index))
        other = 2 * (source + 1) + 1 - column

        @pl.when(both(step > 0, source + 1 >= 0, jnp.logical_or(step > 1, column == 1)))
        def _():
            side_copy(other, kv.at[other]).wait_recv()
            compute(other)

    for head in range(heads):
        columns = slice(head * HEAD, (head + 1) * HEAD)
        total = jnp.sum(part[head], axis=1, keepdims=True)
        value = acc[:, columns] / total
        att_ref[:, columns] = value
        low_ref[:, columns] = value.astype(jnp.bfloat16)
        tot_ref[head] = jnp.sum(part[head].T, axis=0, keepdims=True)

    @pl.loop(0, rows)
    def _(source):
        index = 2 * source + column

        @pl.when(source <= line)
        def _():
            pl.when(line < rows - 1)(lambda: up_copy(index, kv.at[index]).wait_send())
            pl.when(jnp.logical_or(source < line, column == 0))(
                lambda: side_copy(index, kv.at[index]).wait_send()
            )

    @pl.loop(0, blocks)
    def _(index):
        pl.when(index <= at)(lambda: save(index).wait())


def attend(projected, heads):
    size = projected.shape[0]
    blocks = lax.axis_size("blk")
    whole = pl.BlockSpec(memory_space=pltpu.VMEM)
    return pl.pallas_call(
        functools.partial(attend_kernel, heads),
        out_shape=(
            jax.ShapeDtypeStruct((size, heads * HEAD), jnp.bfloat16),
            jax.ShapeDtypeStruct((size, heads * HEAD), jnp.float32),
            jax.ShapeDtypeStruct((heads, 1, size), jnp.float32),
            jax.ShapeDtypeStruct((blocks, size, 2 * HEAD), jnp.bfloat16),
        ),
        in_specs=[whole],
        out_specs=(whole, whole, whole, pl.BlockSpec(memory_space=pl.ANY)),
        scratch_shapes=[
            pltpu.VMEM((blocks, size, 2 * HEAD), jnp.bfloat16),
            pltpu.VMEM((size, heads * HEAD), jnp.float32),
            pltpu.VMEM((heads, size, 128), jnp.float32),
            pltpu.SemaphoreType.DMA((blocks // 2,)),
            pltpu.SemaphoreType.DMA((blocks // 2,)),
            pltpu.SemaphoreType.DMA((blocks // 2,)),
            pltpu.SemaphoreType.DMA((blocks // 2,)),
            pltpu.SemaphoreType.DMA,
            pltpu.SemaphoreType.DMA((blocks,)),
        ],
        compiler_params=pltpu.CompilerParams(
            collective_id=0, has_side_effects=True, vmem_limit_bytes=VMEM_BYTES
        ),
        cost_estimate=cost_of(50),
        name="attend",
    )(projected)


def carry(cross_ref, far_ref, first, sent, landed, across):
    return push_sp(
        cross_ref.at[:, pl.ds(first, far_ref.shape[1]), :], far_ref, sent, landed, across
    )


def attend_back_kernel(heads, carried, *refs):
    if carried:
        x_ref, scaled_ref, delta_ref, kv_ref, cross_ref, out_ref, far_ref, *scratch = refs
        *scratch, cross_sent, cross_landed = scratch
        across = (lax.axis_index("sp") + 2) % 4
        over = carry(cross_ref, far_ref, 0, cross_sent, cross_landed, across)
        after = over.start
    else:
        x_ref, scaled_ref, delta_ref, kv_ref, out_ref, *scratch = refs
        across, after = None, lambda: None
    attend_back_steps(
        heads, across, after, x_ref, scaled_ref, delta_ref, kv_ref, out_ref, *scratch
    )
    if carried:
        over.wait()


def attend_back_steps(
    heads,
    across,
    after_greeting,
    x_ref,
    scaled_ref,
    delta_ref,
    kv_ref,
    out_ref,
    kv,
    part,
    side,
    down,
    dq,
    dk,
    dv,
    load_done,
    side_sent,
    side_landed,
    down_sent,
    down_landed,
):
    at = lax.axis_index("blk")
    blocks = lax.axis_size("blk")
    rows = blocks // 2
    line, column = at // 2, at % 2
    partner = at + 1 - 2 * column
    size = x_ref.shape[0]

    def load(index):
        return pltpu.make_async_copy(kv_ref.at[index], kv.at[index], load_done.at[index])

    @pl.loop(0, blocks)
    def _(index):
        pl.when(index <= at)(lambda: load(index).start())

    greet(at, line, rows, across)
    after_greeting()

    def side_copy(target):
        return push(
            part.at[target, 1 - column],
            side.at[target],
            side_sent.at[target],
            side_landed.at[target],
            partner,
        )

    def down_copy(target):
        return push(
            part.at[target, column],
            down.at[target],
            down_sent.at[target],
            down_landed.at[target],
            at - 2,
        )

    dq[...] = jnp.zeros_like(dq)
    ahead = lax.broadcasted_iota(jnp.int32, (size, size), 0) - lax.broadcasted_iota(
        jnp.int32, (size, size), 1
    )

    def compute(target, half):
        index = 2 * target + half
        load(index).wait()
        span = (at - index) * size
        for head in range(heads):
            columns = slice(head * HEAD, (head + 1) * HEAD)
            query = x_ref[:, columns]
            scaled = scaled_ref[:, columns]
            key = kv[index, :, :HEAD]
            raw = lax.dot_general(
                key, query, (((1,), (1,)), ((), ())), preferred_element_type=jnp.float32
            )
            squashed = jnp.tanh(raw * (HEAD ** (-0.5) / CAP_VALUE))
            weights = jnp.exp(CAP_VALUE * squashed)
            weights = jnp.where(ahead <= span, weights, 0.0)
            inner = lax.dot_general(
                kv[index, :, HEAD:],
                scaled,
                (((1,), (1,)), ((), ())),
                preferred_element_type=jnp.float32,
            )
            grad_raw = (
                weights * (inner - delta_ref[head]) * (1.0 - squashed * squashed)
            ).astype(jnp.bfloat16)
            dv_now = jnp.dot(
                weights.astype(jnp.bfloat16), scaled, preferred_element_type=jnp.float32
            )
            dk_now = jnp.dot(grad_raw, query, preferred_element_type=jnp.float32)
            dq[:, columns] += lax.dot_general(
                grad_raw, key, (((0,), (0,)), ((), ())), preferred_element_type=jnp.float32
            )
            if head == 0:
                dv[...] = dv_now
                dk[...] = dk_now
            else:
                dv[...] += dv_now
                dk[...] += dk_now
        part[target, half, :, :HEAD] = (dk[...] * HEAD ** (-0.5)).astype(jnp.bfloat16)
        part[target, half, :, HEAD:] = dv[...].astype(jnp.bfloat16)

    def merge(target):
        last = target == line

        @pl.when(jnp.logical_or(target < line, column == 0))
        def _():
            side_copy(target).wait_recv()
            part[target, column] = (
                part[target, column].astype(jnp.float32) + side[target].astype(jnp.float32)
            ).astype(jnp.bfloat16)

        @pl.when(line < rows - 1)
        def _():
            down_copy(target).wait_recv()
            part[target, column] = (
                part[target, column].astype(jnp.float32) + down[target].astype(jnp.float32)
            ).astype(jnp.bfloat16)

        pl.when(target < line)(lambda: down_copy(target).start())

        @pl.when(last)
        def _():
            out_ref[:, heads * HEAD :] = part[target, column]

    @pl.loop(0, rows)
    def _(target):
        @pl.when(jnp.logical_or(target < line, both(target == line, column == 1)))
        def _():
            compute(target, 1 - column)
            side_copy(target).start()

        pl.when(target <= line)(lambda: compute(target, column))
        pl.when(both(line == rows - 1, target > 0))(lambda: merge(target - 1))

    out_ref[:, : heads * HEAD] = (dq[...] * HEAD ** (-0.5)).astype(jnp.bfloat16)

    @pl.loop(0, rows)
    def _(target):
        pl.when(both(target <= line, jnp.logical_or(line < rows - 1, target == rows - 1)))(
            lambda: merge(target)
        )

    @pl.loop(0, rows)
    def _(target):
        pl.when(jnp.logical_or(target < line, both(target == line, column == 1)))(
            lambda: side_copy(target).wait_send()
        )
        pl.when(target < line)(lambda: down_copy(target).wait_send())


def half_of(cross):
    kinds, units, width = cross.shape
    return jax.ShapeDtypeStruct((kinds, units // 2, width), cross.dtype)


def attend_back(projected, scaled, delta, kv_all, cross=None):
    size = projected.shape[0]
    blocks = lax.axis_size("blk")
    rows = blocks // 2
    heads = scaled.shape[1] // HEAD
    whole = pl.BlockSpec(memory_space=pltpu.VMEM)
    far = pl.BlockSpec(memory_space=pl.ANY)
    carried = cross is not None
    far_shape, operands = [], [projected, scaled, delta, kv_all]
    if carried:
        far_shape = [half_of(cross)]
        operands.append(cross)
    return pl.pallas_call(
        functools.partial(attend_back_kernel, heads, carried),
        out_shape=[jax.ShapeDtypeStruct(projected.shape, jnp.bfloat16)] + far_shape,
        in_specs=[whole, whole, whole, far] + [far] * carried,
        out_specs=[whole] + [far] * carried,
        scratch_shapes=[
            pltpu.VMEM((blocks, size, 2 * HEAD), jnp.bfloat16),
            pltpu.VMEM((rows, 2, size, 2 * HEAD), jnp.bfloat16),
            pltpu.VMEM((rows, size, 2 * HEAD), jnp.bfloat16),
            pltpu.VMEM((rows, size, 2 * HEAD), jnp.bfloat16),
            pltpu.VMEM((size, heads * HEAD), jnp.float32),
            pltpu.VMEM((size, HEAD), jnp.float32),
            pltpu.VMEM((size, HEAD), jnp.float32),
            pltpu.SemaphoreType.DMA((blocks,)),
            pltpu.SemaphoreType.DMA((rows,)),
            pltpu.SemaphoreType.DMA((rows,)),
            pltpu.SemaphoreType.DMA((rows,)),
            pltpu.SemaphoreType.DMA((rows,)),
        ]
        + [pltpu.SemaphoreType.DMA, pltpu.SemaphoreType.DMA] * carried,
        compiler_params=pltpu.CompilerParams(
            collective_id=1, has_side_effects=True, vmem_limit_bytes=VMEM_BYTES
        ),
        cost_estimate=cost_of(50),
        name="attend_back",
    )(*operands)


def line_gather(own_ref, full, line_sent, line_landed, side_sent, side_landed, own_done, work):
    at = lax.axis_index("blk")
    rows = lax.axis_size("blk") // 2
    line, column = at // 2, at % 2
    size = own_ref.shape[0]

    def spot(source, side):
        start = pl.multiple_of((2 * source + side) * size, size)
        return full.at[pl.ds(start, size), :]

    def line_copy(source, sign, first=False):
        return push(
            own_ref if first else spot(source, column),
            spot(source, column),
            line_sent.at[(sign + 1) // 2, source],
            line_landed.at[source],
            at + 2 * sign,
        )

    def side_copy(source, side, first=False):
        return push(
            own_ref if first else spot(source, side),
            spot(source, side),
            side_sent.at[source],
            side_landed.at[source],
            at + 1 - 2 * column,
        )

    def inside(row):
        return jnp.logical_and(row >= 0, row < rows)

    pl.when(line < rows - 1)(lambda: line_copy(line, 1, True).start())
    pl.when(line > 0)(lambda: line_copy(line, -1, True).start())
    side_copy(line, column, True).start()
    keep = pltpu.make_async_copy(own_ref, spot(line, column), own_done)
    keep.start()
    keep.wait()

    @pl.loop(0, rows + 1)
    def _(step):
        for sign in (-1, 1):
            source = line - sign * step

            @pl.when(both(step > 0, inside(source)))
            def _():
                line_copy(source, sign).wait_recv()
                pl.when(inside(line + sign))(lambda: line_copy(source, sign).start())
                side_copy(source, column).start()

        for sign in (-1, 1):
            source = line - sign * (step - 1)
            once = step > 0 if sign == -1 else step > 1

            @pl.when(both(once, inside(source)))
            def _():
                side_copy(source, 1 - column).wait_recv()
                work(source)

    @pl.loop(0, rows)
    def _(source):
        pl.when(both(source <= line, line < rows - 1))(lambda: line_copy(source, 1).wait_send())
        pl.when(both(source >= line, line > 0))(lambda: line_copy(source, -1).wait_send())
        side_copy(source, column).wait_send()


def line_scatter(part, side, lane, out_ref, side_sent, side_landed, lane_sent, lane_landed, work, fill):
    at = lax.axis_index("blk")
    rows = lax.axis_size("blk") // 2
    line, column = at // 2, at % 2
    size = out_ref.shape[0]

    def spot(target, half):
        start = pl.multiple_of((2 * target + half) * size, size)
        return pl.ds(start, size)

    def side_copy(target):
        return push(
            part.at[spot(target, 1 - column), :],
            side.at[target],
            side_sent.at[target],
            side_landed.at[target],
            at + 1 - 2 * column,
        )

    def lane_copy(target, sign):
        slot = target if sign == 1 else jnp.where(target == line - 1, rows, target)
        return push(
            part.at[spot(target, column), :],
            lane.at[slot],
            lane_sent.at[target],
            lane_landed.at[slot],
            at + 2 * sign,
        )

    def lane_wait(slot):
        push(
            lane.at[slot], lane.at[slot], lane_sent.at[0], lane_landed.at[slot], at + 1 - 2 * column
        ).wait_recv()

    def inside(row):
        return jnp.logical_and(row >= 0, row < rows)

    @pl.loop(0, rows)
    def _(step):
        for sign in (-1, 1):
            target = line + sign * (rows - 1 - step)
            once = step >= 0 if sign == -1 else step < rows - 1

            @pl.when(both(once, inside(target)))
            def _():
                work(target)
                side_copy(target).start()

    def merge(target):
        mine = spot(target, column)
        side_copy(target).wait_recv()
        part[mine, :] = (
            part[mine, :].astype(jnp.float32) + side[target].astype(jnp.float32)
        ).astype(jnp.bfloat16)

        def pass_on(sign):
            @pl.when(inside(line - sign))
            def _():
                lane_wait(target)
                part[mine, :] = (
                    part[mine, :].astype(jnp.float32) + lane[target].astype(jnp.float32)
                ).astype(jnp.bfloat16)

            lane_copy(target, sign).start()

        pl.when(target > line)(lambda: pass_on(1))
        pl.when(target < line)(lambda: pass_on(-1))

    @pl.loop(0, rows)
    def _(step):
        fill(step)
        for sign in (-1, 1):
            target = line + sign * (rows - 1 - step)
            once = step >= 0 if sign == -1 else step < rows - 1
            pl.when(both(once, inside(target)))(lambda: merge(target))

    mine = spot(line, column)
    out_ref[...] = part[mine, :].astype(jnp.float32)

    @pl.when(line > 0)
    def _():
        lane_wait(line)
        out_ref[...] += lane[line].astype(jnp.float32)

    @pl.when(line < rows - 1)
    def _():
        lane_wait(rows)
        out_ref[...] += lane[rows].astype(jnp.float32)

    @pl.loop(0, rows)
    def _(target):
        side_copy(target).wait_send()
        pl.when(target > line)(lambda: lane_copy(target, 1).wait_send())
        pl.when(target < line)(lambda: lane_copy(target, -1).wait_send())


def line_sems(rows):
    dma = pltpu.SemaphoreType.DMA
    return [dma((2, rows)), dma((rows,)), dma((rows,)), dma((rows,)), dma]


def lane_sems(rows):
    dma = pltpu.SemaphoreType.DMA
    return [dma((rows,)), dma((rows,)), dma((rows,)), dma((rows + 1,))]


def ffn_kernel(
    act_ref,
    w_ref,
    out_ref,
    acts_ref,
    w,
    acts,
    hidden,
    part,
    side,
    lane,
    w_done,
    save_done,
    *sems,
):
    at = lax.axis_index("blk")
    rows = lax.axis_size("blk") // 2
    pair = 2 * act_ref.shape[0]

    def load(which):
        return pltpu.make_async_copy(w_ref.at[which], w.at[which], w_done.at[which])

    def pair_rows(source):
        return pl.ds(pl.multiple_of(source * pair, pair), pair)

    def save(source):
        return pltpu.make_async_copy(
            acts.at[pair_rows(source), :], acts_ref.at[pair_rows(source), :], save_done.at[source]
        )

    for which in range(3):
        load(which).start()
    greet(at, at // 2, rows)
    for which in range(3):
        load(which).wait()

    def expand(source):
        save(source).start()
        rows_now = acts[pair_rows(source), :]
        gate = contract_last(w[0], rows_now)
        up = contract_last(w[1], rows_now)
        hidden[source] = (gelu_value(gate) * up).astype(jnp.bfloat16)

    def reduce(target):
        part[pair_rows(target), :] = lax.dot_general(
            hidden[target], w[2], (((0,), (0,)), ((), ())), preferred_element_type=jnp.float32
        ).astype(jnp.bfloat16)

    line_gather(act_ref, acts, *sems[:5], expand)
    line_scatter(part, side, lane, out_ref, *sems[5:], reduce, lambda step: None)
    pl.loop(0, rows)(lambda source: save(source).wait())


def ffn_forward(act_ffn, w_parts):
    size, width = act_ffn.shape
    units = w_parts.shape[1]
    blocks = lax.axis_size("blk")
    rows = blocks // 2
    whole = pl.BlockSpec(memory_space=pltpu.VMEM)
    far = pl.BlockSpec(memory_space=pl.ANY)
    return pl.pallas_call(
        ffn_kernel,
        out_shape=(
            jax.ShapeDtypeStruct((size, width), jnp.float32),
            jax.ShapeDtypeStruct((blocks * size, width), jnp.bfloat16),
        ),
        in_specs=[whole, far],
        out_specs=(whole, far),
        scratch_shapes=[
            pltpu.VMEM(w_parts.shape, jnp.bfloat16),
            pltpu.VMEM((blocks * size, width), jnp.bfloat16),
            pltpu.VMEM((rows, units, 2 * size), jnp.bfloat16),
            pltpu.VMEM((blocks * size, width), jnp.bfloat16),
            pltpu.VMEM((rows, size, width), jnp.bfloat16),
            pltpu.VMEM((rows + 1, size, width), jnp.bfloat16),
            pltpu.SemaphoreType.DMA((3,)),
            pltpu.SemaphoreType.DMA((rows,)),
            *line_sems(rows),
            *lane_sems(rows),
        ],
        compiler_params=pltpu.CompilerParams(
            collective_id=2, has_side_effects=True, vmem_limit_bytes=VMEM_BYTES
        ),
        cost_estimate=cost_of(115),
        name="ffn_forward",
    )(act_ffn, w_parts)


FILL_COLUMNS = 256
FILL_FIRST = 3


def ffn_back_kernel(
    owners,
    grad_ref,
    acts_ref,
    w_ref,
    out_ref,
    keep_ref,
    cross_ref,
    w,
    rights,
    lefts,
    part,
    side,
    lane,
    stage,
    mate_part,
    summed,
    w_done,
    acts_done,
    mate_sent,
    mate_landed,
    summed_done,
    *sems,
):
    at = lax.axis_index("blk")
    me = lax.axis_index("sp")
    chip, core = me // 2, me % 2
    mate = me + 1 - 2 * core
    rows = lax.axis_size("blk") // 2
    size, width = grad_ref.shape
    pair = 2 * size
    units = w.shape[1]
    acts, grads = rights.at[0], rights.at[1]

    def load(which):
        return pltpu.make_async_copy(w_ref.at[which], w.at[which], w_done.at[which])

    def pair_rows(source):
        return pl.ds(pl.multiple_of(source * pair, pair), pair)

    acts_copy = pltpu.make_async_copy(acts_ref, acts, acts_done)
    acts_copy.start()
    for which in range(3):
        load(which).start()
    greet(at, at // 2, rows, mate)
    acts_copy.wait()
    for which in range(3):
        load(which).wait()

    def expand(source):
        columns = pair_rows(source)
        rows_now = acts[pair_rows(source), :]
        gate = contract_last(w[0], rows_now)
        up = contract_last(w[1], rows_now)
        grad_hidden = contract_last(w[2], grads[pair_rows(source), :])
        bent = jnp.tanh(GELU_SCALE * (gate + GELU_CUBIC * gate * gate * gate))
        value = 0.5 * gate * (1.0 + bent)
        slope = 0.5 * (1.0 + bent) + 0.5 * gate * (1.0 - bent * bent) * GELU_SCALE * (
            1.0 + 3.0 * GELU_CUBIC * gate * gate
        )
        lefts[2, :, columns] = (value * up).astype(jnp.bfloat16)
        lefts[0, :, columns] = (grad_hidden * up * slope).astype(jnp.bfloat16)
        lefts[1, :, columns] = (grad_hidden * value).astype(jnp.bfloat16)

    def reduce(target):
        columns = pair_rows(target)
        dims = (((0,), (0,)), ((), ()))
        total = lax.dot_general(
            lefts[0, :, columns], w[0], dims, preferred_element_type=jnp.float32
        ) + lax.dot_general(lefts[1, :, columns], w[1], dims, preferred_element_type=jnp.float32)
        part[pair_rows(target), :] = total.astype(jnp.bfloat16)

    pieces = width // FILL_COLUMNS
    total_pieces = 3 * pieces

    def piece_columns(item):
        return pl.ds(pl.multiple_of((item % pieces) * FILL_COLUMNS, FILL_COLUMNS), FILL_COLUMNS)

    def mate_copy(item):
        return push_sp(
            stage.at[item % 3, :, 1 - core],
            mate_part.at[item],
            mate_sent.at[item % 3],
            mate_landed.at[item],
            mate,
        )

    def put(item, side_chip, target):
        return pltpu.make_async_copy(
            summed.at[item % 2, side_chip],
            target.at[item // pieces, :, piece_columns(item)],
            summed_done.at[item % 2, side_chip],
        )

    def put_wait(item):
        put(item, chip, keep_ref).wait()
        put(item, 1 - chip, cross_ref).wait()

    def sum_one(item):
        pl.when(item > 1)(lambda: put_wait(item - 2))
        mate_copy(item).wait_recv()
        summed[item % 2] = (
            stage[item % 3, :, core].astype(jnp.float32) + mate_part[item].astype(jnp.float32)
        ).astype(jnp.bfloat16)
        put(item, chip, keep_ref).start()
        put(item, 1 - chip, cross_ref).start()

    def fill_one(item):
        which = item // pieces
        total = jnp.dot(
            lefts[which],
            rights[which // 2, :, piece_columns(item)],
            preferred_element_type=jnp.float32,
        )
        pl.when(item > 2)(lambda: mate_copy(item - 3).wait_send())
        stage[item % 3] = total.astype(jnp.bfloat16).reshape(
            2, 2, units // owners, FILL_COLUMNS
        )
        mate_copy(item).start()
        pl.when(item > 0)(lambda: sum_one(item - 1))

    each = pl.cdiv(total_pieces - FILL_FIRST, rows - 1)

    def fill(step):
        first = jnp.maximum(FILL_FIRST + (step - 1) * each, 0)
        last = jnp.minimum(FILL_FIRST + step * each, total_pieces)

        @pl.loop(0, each)
        def _(item):
            pl.when(first + item < last)(lambda: fill_one(first + item))

    line_gather(grad_ref, grads, *sems[:5], expand)
    line_scatter(part, side, lane, out_ref, *sems[5:], reduce, fill)
    sum_one(total_pieces - 1)
    put_wait(total_pieces - 2)
    put_wait(total_pieces - 1)
    for item in range(total_pieces - 3, total_pieces):
        mate_copy(item).wait_send()


def ffn_back(grad_ffn, acts, w_parts, owners):
    size, width = grad_ffn.shape
    units = w_parts.shape[1]
    blocks = lax.axis_size("blk")
    rows = blocks // 2
    tokens = blocks * size
    items = 3 * width // FILL_COLUMNS
    whole = pl.BlockSpec(memory_space=pltpu.VMEM)
    far = pl.BlockSpec(memory_space=pl.ANY)
    return pl.pallas_call(
        functools.partial(ffn_back_kernel, owners),
        out_shape=(
            jax.ShapeDtypeStruct((size, width), jnp.float32),
            jax.ShapeDtypeStruct((3, units // owners, width), jnp.bfloat16),
            jax.ShapeDtypeStruct((3, units // owners, width), jnp.bfloat16),
        ),
        in_specs=[whole, far, far],
        out_specs=(whole, far, far),
        scratch_shapes=[
            pltpu.VMEM(w_parts.shape, jnp.bfloat16),
            pltpu.VMEM((2, tokens, width), jnp.bfloat16),
            pltpu.VMEM((3, units, tokens), jnp.bfloat16),
            pltpu.VMEM((tokens, width), jnp.bfloat16),
            pltpu.VMEM((rows, size, width), jnp.bfloat16),
            pltpu.VMEM((rows + 1, size, width), jnp.bfloat16),
            pltpu.VMEM((3, 2, 2, units // owners, FILL_COLUMNS), jnp.bfloat16),
            pltpu.VMEM((items, 2, units // owners, FILL_COLUMNS), jnp.bfloat16),
            pltpu.VMEM((2, 2, units // owners, FILL_COLUMNS), jnp.bfloat16),
            pltpu.SemaphoreType.DMA((3,)),
            pltpu.SemaphoreType.DMA,
            pltpu.SemaphoreType.DMA((3,)),
            pltpu.SemaphoreType.DMA((items,)),
            pltpu.SemaphoreType.DMA((2, 2)),
            *line_sems(rows),
            *lane_sems(rows),
        ],
        compiler_params=pltpu.CompilerParams(
            collective_id=3, has_side_effects=True, vmem_limit_bytes=VMEM_BYTES
        ),
        cost_estimate=cost_of(115),
        name="ffn_back",
    )(grad_ffn, acts, w_parts)


def ffn_hidden(acts, w_parts):
    gate = contract_last(acts, w_parts[0])
    up = contract_last(acts, w_parts[1])
    return (gate, up, (gelu_value(gate) * up).astype(jnp.bfloat16))


def scatter_tokens(partial):
    return lax.psum_scatter(
        partial.astype(jnp.bfloat16), "blk", scatter_dimension=0, tiled=True
    ).astype(jnp.float32)


def ffn_forward_wide(act_ffn, w_parts):
    acts = lax.all_gather(act_ffn, "blk", axis=0, tiled=True)
    hidden = ffn_hidden(acts, w_parts)[2]
    partial = jnp.dot(hidden, w_parts[2], preferred_element_type=jnp.float32)
    return (scatter_tokens(partial), acts)


def ffn_back_wide(grad_ffn, acts, w_parts, owners):
    grads = lax.all_gather(grad_ffn, "blk", axis=0, tiled=True)
    gate, up, hidden = ffn_hidden(acts, w_parts)
    grad_hidden = contract_last(grads, w_parts[2])
    grad_gate = (grad_hidden * up * gelu_slope(gate)).astype(jnp.bfloat16)
    grad_up = (grad_hidden * gelu_value(gate)).astype(jnp.bfloat16)
    partial = jnp.dot(grad_gate, w_parts[0], preferred_element_type=jnp.float32) + jnp.dot(
        grad_up, w_parts[1], preferred_element_type=jnp.float32
    )
    sums = jnp.stack(
        [
            jnp.einsum("tf,td->fd", left, right, preferred_element_type=jnp.float32)
            for left, right in ((grad_gate, acts), (grad_up, acts), (hidden, grads))
        ]
    ).astype(jnp.bfloat16)
    units = w_parts.shape[1]
    owned = sums.reshape(3, owners, units // owners, sums.shape[2])
    mine = lax.psum_scatter(
        jnp.transpose(owned, (1, 0, 2, 3)), "sp", scatter_dimension=0, tiled=True
    )
    return (scatter_tokens(partial), mine[0], None)


def cost_of(microseconds):
    return pl.CostEstimate(
        flops=int(microseconds * 1e9), bytes_accessed=int(microseconds * 3e6), transcendentals=0
    )


def push_sp(source, target, sent, landed, peer):
    return pltpu.make_async_remote_copy(
        src_ref=source,
        dst_ref=target,
        send_sem=sent,
        recv_sem=landed,
        device_id={"sp": peer},
        device_id_type=pl.DeviceIdType.MESH,
    )


def greet_sp(me, groups):
    barrier = pltpu.get_barrier_semaphore()
    for step in range(1, groups):
        pl.semaphore_signal(
            barrier,
            inc=1,
            device_id={"sp": (me + step) % groups},
            device_id_type=pl.DeviceIdType.MESH,
        )
    pl.semaphore_wait(barrier, groups - 1)


def gather_project_kernel(x_ref, w_ref, full_ref, out_ref, w, w_done, own_done, sent, landed):
    me = lax.axis_index("sp")
    size = x_ref.shape[0]
    units = w.shape[0]
    mate = me + 1 - 2 * (me % 2)
    across = (me + 2) % 4

    def spot(member):
        return full_ref.at[pl.ds(pl.multiple_of(member * size, size), size), :]

    load = pltpu.make_async_copy(
        w_ref.at[pl.ds(pl.multiple_of(me * units, units), units), :], w, w_done
    )
    load.start()
    greet_sp(me, 4)
    over = push_sp(x_ref, spot(me), sent.at[0], landed.at[0], across)
    over.start()
    beside = push_sp(x_ref, spot(me), sent.at[1], landed.at[1], mate)
    beside.start()
    keep = pltpu.make_async_copy(x_ref, spot(me), own_done)
    keep.start()
    keep.wait()
    load.wait()

    def project(chip):
        rows = pl.ds(pl.multiple_of(chip * 2 * size, 2 * size), 2 * size)
        out_ref[rows, :] = contract_last(full_ref[rows, :], w[...]).astype(jnp.bfloat16)

    beside.wait_recv()
    project(me // 2)
    over.wait_recv()
    onward = push_sp(spot(across), spot(across), sent.at[2], landed.at[2], mate)
    onward.start()
    onward.wait_recv()
    project(across // 2)
    over.wait_send()
    beside.wait_send()
    onward.wait_send()


def gather_project(rows, weights, identity):
    size, width = rows.shape
    units = weights.shape[0] // 4
    whole = pl.BlockSpec(memory_space=pltpu.VMEM)
    return pl.pallas_call(
        gather_project_kernel,
        out_shape=(
            jax.ShapeDtypeStruct((4 * size, width), jnp.bfloat16),
            jax.ShapeDtypeStruct((4 * size, units), jnp.bfloat16),
        ),
        in_specs=[whole, pl.BlockSpec(memory_space=pl.ANY)],
        out_specs=(whole, whole),
        scratch_shapes=[
            pltpu.VMEM((units, width), jnp.bfloat16),
            pltpu.SemaphoreType.DMA,
            pltpu.SemaphoreType.DMA,
            pltpu.SemaphoreType.DMA((3,)),
            pltpu.SemaphoreType.DMA((3,)),
        ],
        compiler_params=pltpu.CompilerParams(
            collective_id=identity, has_side_effects=True, vmem_limit_bytes=VMEM_BYTES
        ),
        cost_estimate=cost_of(18),
        name="gather_project",
    )(rows, weights)


def exchange_project_kernel(x_ref, w_ref, out_ref, w, got, w_done, own_done, sent, landed):
    me = lax.axis_index("sp")
    size = out_ref.shape[0]
    units = x_ref.shape[1]

    def rows_of(member):
        return x_ref.at[pl.ds(pl.multiple_of(member * size, size), size), :]

    def load(member):
        rows = pl.ds(pl.multiple_of(member * units, units), units)
        return pltpu.make_async_copy(w_ref.at[rows, :], w.at[rows, :], w_done.at[member])

    def send(step):
        peer = (me + step) % 4
        return push_sp(rows_of(peer), got.at[4 - step], sent.at[step], landed.at[4 - step], peer)

    greet_sp(me, 4)
    for step in (2, 1, 3):
        send(step).start()
    keep = pltpu.make_async_copy(rows_of(me), got.at[0], own_done)
    keep.start()
    for step in range(4):
        load((me + step) % 4).start()
    keep.wait()
    for step in (0, 1, 3, 2):
        member = (me + step) % 4
        load(member).wait()
        if step > 0:
            send(4 - step).wait_recv()
        rows = pl.ds(pl.multiple_of(member * units, units), units)
        term = jnp.dot(got[step], w[rows, :], preferred_element_type=jnp.float32)
        if step == 0:
            out_ref[...] = term
        else:
            out_ref[...] += term
    for step in (1, 2, 3):
        send(step).wait_send()


def exchange_project(columns, weights, identity):
    size = columns.shape[0] // 4
    whole = pl.BlockSpec(memory_space=pltpu.VMEM)
    return pl.pallas_call(
        exchange_project_kernel,
        out_shape=jax.ShapeDtypeStruct((size, weights.shape[1]), jnp.float32),
        in_specs=[whole, pl.BlockSpec(memory_space=pl.ANY)],
        out_specs=whole,
        scratch_shapes=[
            pltpu.VMEM(weights.shape, jnp.bfloat16),
            pltpu.VMEM((4, size, columns.shape[1]), jnp.bfloat16),
            pltpu.SemaphoreType.DMA((4,)),
            pltpu.SemaphoreType.DMA,
            pltpu.SemaphoreType.DMA((4,)),
            pltpu.SemaphoreType.DMA((4,)),
        ],
        compiler_params=pltpu.CompilerParams(
            collective_id=identity, has_side_effects=True, vmem_limit_bytes=VMEM_BYTES
        ),
        cost_estimate=cost_of(16),
        name="exchange_project",
    )(columns, weights)


def finish_kernel(
    cols_ref,
    act_ref,
    att_ref,
    grad_ref,
    w_ref,
    tokens_ref,
    middle_ref,
    gain_ref,
    rows_ref,
    cross_ref,
    sum_ref,
    tokens_grad_ref,
    gains_ref,
    far_ref,
    w,
    got,
    grad_in,
    part,
    side,
    lane,
    mine,
    from_sp,
    from_side,
    from_line,
    w_done,
    own_done,
    swap_sent,
    swap_landed,
    sp_sent,
    sp_landed,
    gain_side,
    line_sent,
    line_landed,
    cross_sent,
    cross_landed,
    *sems,
):
    at = lax.axis_index("blk")
    me = lax.axis_index("sp")
    rows = lax.axis_size("blk") // 2
    line, column = at // 2, at % 2
    partner = at + 1 - 2 * column
    block = sum_ref.shape[0]
    size = tokens_ref.shape[0]
    units = cols_ref.shape[1]
    extra = block - size

    barrier = pltpu.get_barrier_semaphore()
    for step in range(1, 4):
        pl.semaphore_signal(
            barrier, inc=1, device_id={"sp": (me + step) % 4}, device_id_type=pl.DeviceIdType.MESH
        )

    def line_peer(step):
        return 2 * ((line + step) % rows) + column

    for peer in [partner] + [line_peer(step) for step in range(1, rows)]:
        pl.semaphore_signal(
            barrier, inc=1, device_id={"blk": peer}, device_id_type=pl.DeviceIdType.MESH
        )

    def load(member):
        span = pl.ds(pl.multiple_of(member * units, units), units)
        return pltpu.make_async_copy(w_ref.at[span, :], w.at[span, :], w_done.at[member])

    def rows_of(member):
        return cols_ref.at[pl.ds(pl.multiple_of(member * size, size), size), :]

    def swap(step):
        peer = (me + step) % 4
        return push_sp(
            rows_of(peer), got.at[4 - step], swap_sent.at[step], swap_landed.at[4 - step], peer
        )

    for step in range(4):
        load((me + step) % 4).start()
    keep = pltpu.make_async_copy(rows_of(me), got.at[0], own_done)
    keep.start()
    pl.semaphore_wait(barrier, 3 + rows)
    for step in (2, 1, 3):
        swap(step).start()
    over = carry(
        cross_ref, far_ref, far_ref.shape[1], cross_sent, cross_landed, (me + 2) % 4
    )
    over.start()
    keep.wait()

    def sp_gains(step):
        return push_sp(
            mine, from_sp.at[4 - step], sp_sent.at[step], sp_landed.at[4 - step], (me + step) % 4
        )

    def side_gains():
        return push(from_sp.at[0], from_side, gain_side.at[0], gain_side.at[1], partner)

    def line_gains(step):
        return push(
            from_line.at[0],
            from_line.at[rows - step],
            line_sent.at[step],
            line_landed.at[rows - step],
            line_peer(step),
        )

    def reduce(target):
        dims = (((0,), (0,)), ((), ()))
        wide_columns = pl.ds(pl.multiple_of(target * 2 * size, 2 * size), 2 * size)
        term = lax.dot_general(
            cols_ref[:, wide_columns], act_ref[...], dims, preferred_element_type=jnp.float32
        ).astype(jnp.bfloat16)
        columns = pl.ds(pl.multiple_of(target * 2 * extra, 2 * extra), 2 * extra)
        more = lax.dot_general(
            att_ref[:, columns], grad_ref[...], dims, preferred_element_type=jnp.float32
        ).astype(jnp.bfloat16)
        for half in range(2):
            start = pl.multiple_of((2 * target + half) * block, block)
            part[pl.ds(start, size), :] = term[half * size : (half + 1) * size]
            start = pl.multiple_of((2 * target + half) * block + size, extra)
            part[pl.ds(start, extra), :] = more[half * extra : (half + 1) * extra]

    def inputs_back():
        for step in (0, 1, 3, 2):
            member = (me + step) % 4
            load(member).wait()
            if step > 0:
                swap(4 - step).wait_recv()
            span = pl.ds(pl.multiple_of(member * units, units), units)
            term = jnp.dot(got[step], w[span, :], preferred_element_type=jnp.float32)
            if step == 0:
                grad_in[...] = term
            else:
                grad_in[...] += term
        normed, inverse = norm_parts(tokens_ref[...].astype(jnp.float32))
        grad_v, gain_row = norm_back(grad_in[...], normed, inverse, gain_ref[...])
        tokens_grad_ref[...] = (middle_ref[...] + grad_v).astype(jnp.bfloat16)
        mine[...] = rows_ref[...]
        mine[0:1, :] = gain_row[None, :]
        for step in range(1, 4):
            sp_gains(step).start()

    def fill(step):
        pl.when(step == 0)(inputs_back)

        @pl.when(step == 1)
        def _():
            total = mine[...]
            for other in range(1, 4):
                sp_gains(4 - other).wait_recv()
                total = total + from_sp[other]
            from_sp[0] = total
            side_gains().start()

        @pl.when(step == 2)
        def _():
            side_gains().wait_recv()
            from_line[0] = from_sp[0] + from_side[...]
            for other in range(1, rows):
                line_gains(other).start()

    line_scatter(part, side, lane, sum_ref, *sems, reduce, fill)
    total = from_line[0]
    for other in range(1, rows):
        line_gains(rows - other).wait_recv()
        total = total + from_line[other]
    gains_ref[...] = total
    for step in (1, 2, 3):
        swap(step).wait_send()
        sp_gains(step).wait_send()
    over.wait()
    side_gains().wait_send()
    for step in range(1, rows):
        line_gains(step).wait_send()


def finish(
    cols, act_block, attended, grad_block, w_qkv, tokens, grad_middle, gain, gain_rows, cross
):
    blocks = lax.axis_size("blk")
    rows = blocks // 2
    size, width = tokens.shape
    block = (cols.shape[1] + attended.shape[1]) // blocks
    whole = pl.BlockSpec(memory_space=pltpu.VMEM)
    any_space = pl.BlockSpec(memory_space=pl.ANY)
    dma = pltpu.SemaphoreType.DMA
    small = gain_rows.shape
    total, tokens_grad, gains_all, far = pl.pallas_call(
        finish_kernel,
        out_shape=(
            jax.ShapeDtypeStruct((block, width), jnp.float32),
            jax.ShapeDtypeStruct((size, width), jnp.bfloat16),
            jax.ShapeDtypeStruct(small, jnp.float32),
            half_of(cross),
        ),
        in_specs=[whole] * 4 + [any_space] + [whole] * 4 + [any_space],
        out_specs=(whole, whole, whole, any_space),
        scratch_shapes=[
            pltpu.VMEM(w_qkv.shape, jnp.bfloat16),
            pltpu.VMEM((4, size, cols.shape[1]), jnp.bfloat16),
            pltpu.VMEM((size, width), jnp.float32),
            pltpu.VMEM((blocks * block, width), jnp.bfloat16),
            pltpu.VMEM((rows, block, width), jnp.bfloat16),
            pltpu.VMEM((rows + 1, block, width), jnp.bfloat16),
            pltpu.VMEM(small, jnp.float32),
            pltpu.VMEM((4, *small), jnp.float32),
            pltpu.VMEM(small, jnp.float32),
            pltpu.VMEM((rows, *small), jnp.float32),
            dma((4,)),
            dma,
            dma((4,)),
            dma((4,)),
            dma((4,)),
            dma((4,)),
            dma((2,)),
            dma((rows,)),
            dma((rows,)),
            dma,
            dma,
            *lane_sems(rows),
        ],
        compiler_params=pltpu.CompilerParams(
            collective_id=8, has_side_effects=True, vmem_limit_bytes=VMEM_BYTES
        ),
        cost_estimate=cost_of(85),
        name="finish",
    )(cols, act_block, attended, grad_block, w_qkv, tokens, grad_middle, gain, gain_rows, cross)
    shared = cols.shape[1] // blocks
    return (total[:shared], total[shared:], tokens_grad, gains_all, far)


def weight_sums_wide(left, right):
    term = jnp.einsum("tc,td->cd", left, right, preferred_element_type=jnp.float32)
    return scatter_tokens(term)


def finish_wide(
    cols, act_block, attended, grad_block, w_qkv, tokens, grad_middle, gain, gain_rows, cross
):
    grad_act_in = exchange_project(cols, w_qkv, 7)
    normed, inverse = norm_parts(tokens.astype(jnp.float32))
    grad_v, gain_row = norm_back(grad_act_in, normed, inverse, gain)
    gains_all = lax.psum(jnp.concatenate([gain_row[None], gain_rows[1:]]), ("blk", "sp"))
    return (
        weight_sums_wide(cols, act_block),
        weight_sums_wide(attended, grad_block),
        (grad_middle + grad_v).astype(jnp.bfloat16),
        gains_all,
        None,
    )


def body(tokens, w_qkv, w_out, gains, w_ffn, cotangent):
    groups = lax.axis_size("sp")
    heads_here = HEADS // groups
    source = tokens.astype(jnp.float32)
    normed_in, inverse_in = norm_parts(source)
    act_in = (normed_in * gains[0]).astype(jnp.bfloat16)
    act_block, projected = gather_project(act_in, w_qkv, 4)
    block_rows = projected.shape[0]
    attended_cols, attended, totals, kv_all = attend(projected, heads_here)
    attn = exchange_project(attended_cols, w_out, 5)
    normed_attn, inverse_attn = norm_parts(attn)
    middle = source + normed_attn * gains[1]
    normed_mid, inverse_mid = norm_parts(middle)
    act_ffn = (normed_mid * gains[2]).astype(jnp.bfloat16)
    wide = lax.axis_size("blk") > 8
    w_parts = jnp.transpose(w_ffn, (1, 0, 2))
    ffn_out, act_all = (ffn_forward_wide if wide else ffn_forward)(act_ffn, w_parts)
    normed_ffn, inverse_ffn = norm_parts(ffn_out)
    result = middle + normed_ffn * gains[3]
    grad_out = cotangent.astype(jnp.float32)
    grad_ffn_f, gain_grad3 = norm_back(grad_out, normed_ffn, inverse_ffn, gains[3])
    grad_ffn = grad_ffn_f.astype(jnp.bfloat16)
    grad_act_ffn, ffn_part, cross = (ffn_back_wide if wide else ffn_back)(
        grad_ffn, act_all, w_parts, groups
    )
    grad_norm_mid, gain_grad2 = norm_back(grad_act_ffn, normed_mid, inverse_mid, gains[2])
    grad_middle = grad_out + grad_norm_mid
    grad_attn_f, gain_grad1 = norm_back(grad_middle, normed_attn, inverse_attn, gains[1])
    grad_attn = grad_attn_f.astype(jnp.bfloat16)
    grad_block, grad_attended = gather_project(grad_attn, w_out, 6)
    grad_heads = grad_attended.astype(jnp.float32).reshape(block_rows, heads_here, HEAD)
    totals_rows = jnp.transpose(totals.reshape(heads_here, block_rows))
    scaled = (grad_heads / totals_rows[..., None]).astype(jnp.bfloat16)
    row_delta = (
        jnp.sum(grad_heads * attended.reshape(block_rows, heads_here, HEAD), axis=-1) / totals_rows
    )
    grad_cols, *far_first = attend_back(
        projected,
        scaled.reshape(block_rows, heads_here * HEAD),
        jnp.transpose(row_delta).reshape(heads_here, 1, block_rows),
        kv_all,
        cross,
    )
    gain_rows = jnp.stack(
        [jnp.zeros_like(gain_grad1), gain_grad1, gain_grad2, gain_grad3]
        + [jnp.zeros_like(gain_grad1)] * 4
    )
    qkv_grad, out_grad, tokens_grad, gains_all, far_last = (finish_wide if wide else finish)(
        grad_cols,
        act_block,
        attended_cols,
        grad_block,
        w_qkv,
        tokens,
        grad_middle,
        gains[0][None],
        gain_rows,
        cross,
    )
    ffn_sum = ffn_part.astype(jnp.float32)
    if not wide:
        ffn_sum = ffn_sum + jnp.concatenate([*far_first, far_last], axis=1).astype(jnp.float32)
    ffn_grad = jnp.transpose(ffn_sum, (1, 0, 2))
    share = gains_all.shape[1] // (groups * lax.axis_size("blk"))
    place = lax.axis_index("sp") * lax.axis_size("blk") + lax.axis_index("blk")
    gains_grad = lax.dynamic_slice_in_dim(gains_all[:4], place * share, share, 1)
    return (result.astype(jnp.bfloat16), tokens_grad, qkv_grad, out_grad, gains_grad, ffn_grad)


def solution(mesh):
    return jax.shard_map(
        body,
        mesh=mesh,
        in_specs=(
            P(("blk", "sp"), None),
            P(),
            P(),
            P(),
            P("blk", None, None),
            P(("blk", "sp"), None),
        ),
        out_specs=(
            P(("blk", "sp"), None),
            P(("blk", "sp"), None),
            P(("sp", "blk"), None),
            P(("sp", "blk"), None),
            P(None, ("sp", "blk")),
            P(("blk", "sp"), None, None),
        ),
        check_vma=False,
    )
```

```python
import functools

import jax
import jax.numpy as jnp
from jax import lax
from jax.experimental import pallas as pl
from jax.experimental.pallas import tpu as pltpu
from jax.sharding import PartitionSpec as P

HEADS = 8
KV_HEADS = 4
HEAD = 256


VMEM_BYTES = 62 * 1024 * 1024
NORM_EPSILON = 1e-06
CAP_VALUE = 50.0
GELU_SCALE = 0.7978845608028654
GELU_CUBIC = 0.044715


def norm_parts(values):
    inverse = lax.rsqrt(jnp.mean(values * values, axis=-1, keepdims=True) + NORM_EPSILON)
    return (values * inverse, inverse)


def norm_back(grad_y, normed, inverse, gain):
    grad_n = grad_y * gain
    grad_v = inverse * (grad_n - normed * jnp.mean(grad_n * normed, axis=-1, keepdims=True))
    return (grad_v, jnp.sum(grad_y * normed, axis=0))


def gelu_value(values):
    return (
        0.5
        * values
        * (1.0 + jnp.tanh(GELU_SCALE * (values + GELU_CUBIC * values * values * values)))
    )


def gelu_slope(values):
    bent = jnp.tanh(GELU_SCALE * (values + GELU_CUBIC * values * values * values))
    return 0.5 * (1.0 + bent) + 0.5 * values * (1.0 - bent * bent) * GELU_SCALE * (
        1.0 + 3.0 * GELU_CUBIC * values * values
    )


def contract_last(left, right):
    return lax.dot_general(
        left, right, (((1,), (1,)), ((), ())), preferred_element_type=jnp.float32
    )


def push(source, target, sent, landed, block):
    return pltpu.make_async_remote_copy(
        src_ref=source,
        dst_ref=target,
        send_sem=sent,
        recv_sem=landed,
        device_id={"blk": block},
        device_id_type=pl.DeviceIdType.MESH,
    )


def greet(at, line, rows, sp_peer=None):
    barrier = pltpu.get_barrier_semaphore()
    others = 1
    if sp_peer is not None:
        others = 2
        pl.semaphore_signal(
            barrier, inc=1, device_id={"sp": sp_peer}, device_id_type=pl.DeviceIdType.MESH
        )

    def tell(block):
        pl.semaphore_signal(
            barrier, inc=1, device_id={"blk": block}, device_id_type=pl.DeviceIdType.MESH
        )

    tell(at + 1 - 2 * (at % 2))
    pl.when(line > 0)(lambda: tell(at - 2))
    pl.when(line < rows - 1)(lambda: tell(at + 2))
    pl.semaphore_wait(barrier, others + jnp.minimum(line, 1) + jnp.minimum(rows - 1 - line, 1))


def both(*terms):
    result = terms[0]
    for term in terms[1:]:
        result = jnp.logical_and(result, term)
    return result


def attend_kernel(
    heads,
    x_ref,
    low_ref,
    att_ref,
    tot_ref,
    kv_ref,
    kv,
    acc,
    part,
    up_sent,
    up_landed,
    side_sent,
    side_landed,
    own_done,
    save_done,
):
    at = lax.axis_index("blk")
    blocks = lax.axis_size("blk")
    rows = blocks // 2
    line, column = at // 2, at % 2
    partner = at + 1 - 2 * column
    size = x_ref.shape[0]
    first = heads * HEAD
    own = x_ref.at[:, pl.ds(first, 2 * HEAD)]
    greet(at, line, rows)

    def up_copy(index, source):
        return push(source, kv.at[index], up_sent.at[index // 2], up_landed.at[index // 2], at + 2)

    def side_copy(index, source):
        return push(
            source, kv.at[index], side_sent.at[index // 2], side_landed.at[index // 2], partner
        )

    def save(index):
        return pltpu.make_async_copy(kv.at[index], kv_ref.at[index], save_done.at[index])

    pl.when(line < rows - 1)(lambda: up_copy(at, own).start())
    pl.when(column == 0)(lambda: side_copy(at, own).start())
    keep = pltpu.make_async_copy(own, kv.at[at], own_done)
    keep.start()
    acc[...] = jnp.zeros_like(acc)
    part[...] = jnp.zeros_like(part)
    keep.wait()
    ahead = lax.broadcasted_iota(jnp.int32, (size, size), 1) - lax.broadcasted_iota(
        jnp.int32, (size, size), 0
    )

    def compute(index):
        save(index).start()
        span = (at - index) * size
        for head in range(heads):
            raw = lax.dot_general(
                x_ref[:, head * HEAD : (head + 1) * HEAD],
                kv[index, :, :HEAD],
                (((1,), (1,)), ((), ())),
                preferred_element_type=jnp.float32,
            )
            weights = jnp.exp(CAP_VALUE * jnp.tanh(raw * (HEAD ** (-0.5) / CAP_VALUE)))
            weights = jnp.where(ahead <= span, weights, 0.0)
            total = weights[:, :128]
            for piece in range(1, size // 128):
                total = total + weights[:, piece * 128 : (piece + 1) * 128]
            part[head] += total
            acc[:, head * HEAD : (head + 1) * HEAD] += jnp.dot(
                weights.astype(jnp.bfloat16),
                kv[index, :, HEAD:],
                preferred_element_type=jnp.float32,
            )

    @pl.loop(0, rows + 1)
    def _(step):
        source = line - step
        index = 2 * source + column

        @pl.when(both(step > 0, source >= 0))
        def _():
            up_copy(index, kv.at[index]).wait_recv()
            pl.when(line < rows - 1)(lambda: up_copy(index, kv.at[index]).start())
            side_copy(index, kv.at[index]).start()

        @pl.loop(0, 2)
        def _(way):
            found = source + way
            here = 2 * found + jnp.where(way == 0, column, 1 - column)
            due = jnp.logical_or(way == 0, both(step > 0, jnp.logical_or(step > 1, column == 1)))

            @pl.when(both(found >= 0, due))
            def _():
                pl.when(way == 1)(lambda: side_copy(here, kv.at[here]).wait_recv())
                compute(here)

    for head in range(heads):
        columns = slice(head * HEAD, (head + 1) * HEAD)
        total = jnp.sum(part[head], axis=1, keepdims=True)
        value = acc[:, columns] / total
        att_ref[:, columns] = value
        low_ref[:, columns] = value.astype(jnp.bfloat16)
        tot_ref[head] = jnp.sum(part[head].T, axis=0, keepdims=True)

    @pl.loop(0, rows)
    def _(source):
        index = 2 * source + column

        @pl.when(source <= line)
        def _():
            pl.when(line < rows - 1)(lambda: up_copy(index, kv.at[index]).wait_send())
            pl.when(jnp.logical_or(source < line, column == 0))(
                lambda: side_copy(index, kv.at[index]).wait_send()
            )

    @pl.loop(0, blocks)
    def _(index):
        pl.when(index <= at)(lambda: save(index).wait())


def attend(projected, heads):
    size = projected.shape[0]
    blocks = lax.axis_size("blk")
    whole = pl.BlockSpec(memory_space=pltpu.VMEM)
    return pl.pallas_call(
        functools.partial(attend_kernel, heads),
        out_shape=(
            jax.ShapeDtypeStruct((size, heads * HEAD), jnp.bfloat16),
            jax.ShapeDtypeStruct((size, heads * HEAD), jnp.float32),
            jax.ShapeDtypeStruct((heads, 1, size), jnp.float32),
            jax.ShapeDtypeStruct((blocks, size, 2 * HEAD), jnp.bfloat16),
        ),
        in_specs=[whole],
        out_specs=(whole, whole, whole, pl.BlockSpec(memory_space=pl.ANY)),
        scratch_shapes=[
            pltpu.VMEM((blocks, size, 2 * HEAD), jnp.bfloat16),
            pltpu.VMEM((size, heads * HEAD), jnp.float32),
            pltpu.VMEM((heads, size, 128), jnp.float32),
            pltpu.SemaphoreType.DMA((blocks // 2,)),
            pltpu.SemaphoreType.DMA((blocks // 2,)),
            pltpu.SemaphoreType.DMA((blocks // 2,)),
            pltpu.SemaphoreType.DMA((blocks // 2,)),
            pltpu.SemaphoreType.DMA,
            pltpu.SemaphoreType.DMA((blocks,)),
        ],
        compiler_params=pltpu.CompilerParams(
            collective_id=0, has_side_effects=True, vmem_limit_bytes=VMEM_BYTES
        ),
        cost_estimate=cost_of(50),
        name="attend",
    )(projected)


def carry(cross_ref, far_ref, first, sent, landed, across):
    return push_sp(
        cross_ref.at[:, pl.ds(first, far_ref.shape[1]), :], far_ref, sent, landed, across
    )


def attend_back_kernel(heads, carried, *refs):
    if carried:
        x_ref, scaled_ref, delta_ref, kv_ref, cross_ref, out_ref, far_ref, *scratch = refs
        *scratch, cross_sent, cross_landed = scratch
        across = (lax.axis_index("sp") + 2) % 4
        over = carry(cross_ref, far_ref, 0, cross_sent, cross_landed, across)
        after = over.start
    else:
        x_ref, scaled_ref, delta_ref, kv_ref, out_ref, *scratch = refs
        across, after = None, lambda: None
    attend_back_steps(
        heads, across, after, x_ref, scaled_ref, delta_ref, kv_ref, out_ref, *scratch
    )
    if carried:
        over.wait()


def attend_back_steps(
    heads,
    across,
    after_greeting,
    x_ref,
    scaled_ref,
    delta_ref,
    kv_ref,
    out_ref,
    kv,
    part,
    side,
    down,
    dq,
    dk,
    dv,
    load_done,
    side_sent,
    side_landed,
    down_sent,
    down_landed,
):
    at = lax.axis_index("blk")
    blocks = lax.axis_size("blk")
    rows = blocks // 2
    line, column = at // 2, at % 2
    partner = at + 1 - 2 * column
    size = x_ref.shape[0]

    def load(index):
        return pltpu.make_async_copy(kv_ref.at[index], kv.at[index], load_done.at[index])

    @pl.loop(0, blocks)
    def _(index):
        pl.when(index <= at)(lambda: load(index).start())

    greet(at, line, rows, across)
    after_greeting()

    def side_copy(target):
        return push(
            part.at[target, 1 - column],
            side.at[target],
            side_sent.at[target],
            side_landed.at[target],
            partner,
        )

    def down_copy(target):
        return push(
            part.at[target, column],
            down.at[target],
            down_sent.at[target],
            down_landed.at[target],
            at - 2,
        )

    dq[...] = jnp.zeros_like(dq)
    ahead = lax.broadcasted_iota(jnp.int32, (size, size), 0) - lax.broadcasted_iota(
        jnp.int32, (size, size), 1
    )

    def compute(target, half):
        index = 2 * target + half
        load(index).wait()
        span = (at - index) * size
        for head in range(heads):
            columns = slice(head * HEAD, (head + 1) * HEAD)
            query = x_ref[:, columns]
            scaled = scaled_ref[:, columns]
            key = kv[index, :, :HEAD]
            raw = lax.dot_general(
                key, query, (((1,), (1,)), ((), ())), preferred_element_type=jnp.float32
            )
            squashed = jnp.tanh(raw * (HEAD ** (-0.5) / CAP_VALUE))
            weights = jnp.exp(CAP_VALUE * squashed)
            weights = jnp.where(ahead <= span, weights, 0.0)
            inner = lax.dot_general(
                kv[index, :, HEAD:],
                scaled,
                (((1,), (1,)), ((), ())),
                preferred_element_type=jnp.float32,
            )
            grad_raw = (
                weights * (inner - delta_ref[head]) * (1.0 - squashed * squashed)
            ).astype(jnp.bfloat16)
            dv_now = jnp.dot(
                weights.astype(jnp.bfloat16), scaled, preferred_element_type=jnp.float32
            )
            dk_now = jnp.dot(grad_raw, query, preferred_element_type=jnp.float32)
            dq[:, columns] += lax.dot_general(
                grad_raw, key, (((0,), (0,)), ((), ())), preferred_element_type=jnp.float32
            )
            if head == 0:
                dv[...] = dv_now
                dk[...] = dk_now
            else:
                dv[...] += dv_now
                dk[...] += dk_now
        part[target, half, :, :HEAD] = (dk[...] * HEAD ** (-0.5)).astype(jnp.bfloat16)
        part[target, half, :, HEAD:] = dv[...].astype(jnp.bfloat16)

    def merge(target):
        last = target == line

        @pl.when(jnp.logical_or(target < line, column == 0))
        def _():
            side_copy(target).wait_recv()
            part[target, column] = (
                part[target, column].astype(jnp.float32) + side[target].astype(jnp.float32)
            ).astype(jnp.bfloat16)

        @pl.when(line < rows - 1)
        def _():
            down_copy(target).wait_recv()
            part[target, column] = (
                part[target, column].astype(jnp.float32) + down[target].astype(jnp.float32)
            ).astype(jnp.bfloat16)

        pl.when(target < line)(lambda: down_copy(target).start())

        @pl.when(last)
        def _():
            out_ref[:, heads * HEAD :] = part[target, column]

    @pl.loop(0, rows)
    def _(target):
        away = jnp.logical_or(target < line, both(target == line, column == 1))

        @pl.loop(0, 2)
        def _(way):
            @pl.when(jnp.logical_or(both(way == 0, away), both(way == 1, target <= line)))
            def _():
                compute(target, jnp.where(way == 0, 1 - column, column))
                pl.when(way == 0)(lambda: side_copy(target).start())

        pl.when(both(line == rows - 1, target > 0))(lambda: merge(target - 1))

    out_ref[:, : heads * HEAD] = (dq[...] * HEAD ** (-0.5)).astype(jnp.bfloat16)

    @pl.loop(0, rows)
    def _(target):
        pl.when(both(target <= line, jnp.logical_or(line < rows - 1, target == rows - 1)))(
            lambda: merge(target)
        )

    @pl.loop(0, rows)
    def _(target):
        pl.when(jnp.logical_or(target < line, both(target == line, column == 1)))(
            lambda: side_copy(target).wait_send()
        )
        pl.when(target < line)(lambda: down_copy(target).wait_send())


def half_of(cross):
    kinds, units, width = cross.shape
    return jax.ShapeDtypeStruct((kinds, units // 2, width), cross.dtype)


def attend_back(projected, scaled, delta, kv_all, cross=None):
    size = projected.shape[0]
    blocks = lax.axis_size("blk")
    rows = blocks // 2
    heads = scaled.shape[1] // HEAD
    whole = pl.BlockSpec(memory_space=pltpu.VMEM)
    far = pl.BlockSpec(memory_space=pl.ANY)
    carried = cross is not None
    far_shape, operands = [], [projected, scaled, delta, kv_all]
    if carried:
        far_shape = [half_of(cross)]
        operands.append(cross)
    return pl.pallas_call(
        functools.partial(attend_back_kernel, heads, carried),
        out_shape=[jax.ShapeDtypeStruct(projected.shape, jnp.bfloat16)] + far_shape,
        in_specs=[whole, whole, whole, far] + [far] * carried,
        out_specs=[whole] + [far] * carried,
        scratch_shapes=[
            pltpu.VMEM((blocks, size, 2 * HEAD), jnp.bfloat16),
            pltpu.VMEM((rows, 2, size, 2 * HEAD), jnp.bfloat16),
            pltpu.VMEM((rows, size, 2 * HEAD), jnp.bfloat16),
            pltpu.VMEM((rows, size, 2 * HEAD), jnp.bfloat16),
            pltpu.VMEM((size, heads * HEAD), jnp.float32),
            pltpu.VMEM((size, HEAD), jnp.float32),
            pltpu.VMEM((size, HEAD), jnp.float32),
            pltpu.SemaphoreType.DMA((blocks,)),
            pltpu.SemaphoreType.DMA((rows,)),
            pltpu.SemaphoreType.DMA((rows,)),
            pltpu.SemaphoreType.DMA((rows,)),
            pltpu.SemaphoreType.DMA((rows,)),
        ]
        + [pltpu.SemaphoreType.DMA, pltpu.SemaphoreType.DMA] * carried,
        compiler_params=pltpu.CompilerParams(
            collective_id=1, has_side_effects=True, vmem_limit_bytes=VMEM_BYTES
        ),
        cost_estimate=cost_of(50),
        name="attend_back",
    )(*operands)


def line_gather(own_ref, full, line_sent, line_landed, side_sent, side_landed, own_done, ready, work):
    at = lax.axis_index("blk")
    rows = lax.axis_size("blk") // 2
    line, column = at // 2, at % 2
    size = own_ref.shape[0]

    def spot(source, side):
        start = pl.multiple_of((2 * source + side) * size, size)
        return full.at[pl.ds(start, size), :]

    def line_copy(source, sign, first=False):
        return push(
            own_ref if first else spot(source, column),
            spot(source, column),
            line_sent.at[(sign + 1) // 2, source],
            line_landed.at[source],
            at + 2 * sign,
        )

    def side_copy(source, side, first=False):
        return push(
            own_ref if first else spot(source, side),
            spot(source, side),
            side_sent.at[source],
            side_landed.at[source],
            at + 1 - 2 * column,
        )

    def inside(row):
        return jnp.logical_and(row >= 0, row < rows)

    pl.when(line < rows - 1)(lambda: line_copy(line, 1, True).start())
    pl.when(line > 0)(lambda: line_copy(line, -1, True).start())
    side_copy(line, column, True).start()
    keep = pltpu.make_async_copy(own_ref, spot(line, column), own_done)
    keep.start()
    keep.wait()
    ready()

    @pl.loop(0, rows + 1)
    def _(step):
        @pl.loop(0, 2)
        def _(way):
            sign = 2 * way - 1
            source = line - sign * step

            @pl.when(both(step > 0, inside(source)))
            def _():
                line_copy(source, sign).wait_recv()
                pl.when(inside(line + sign))(lambda: line_copy(source, sign).start())
                side_copy(source, column).start()

        @pl.loop(0, 2)
        def _(way):
            sign = 2 * way - 1
            source = line - sign * (step - 1)
            once = step > way

            @pl.when(both(once, inside(source)))
            def _():
                side_copy(source, 1 - column).wait_recv()
                work(source)

    @pl.loop(0, rows)
    def _(source):
        pl.when(both(source <= line, line < rows - 1))(lambda: line_copy(source, 1).wait_send())
        pl.when(both(source >= line, line > 0))(lambda: line_copy(source, -1).wait_send())
        side_copy(source, column).wait_send()


def line_scatter(part, side, lane, out_ref, side_sent, side_landed, lane_sent, lane_landed, work, fill):
    at = lax.axis_index("blk")
    rows = lax.axis_size("blk") // 2
    line, column = at // 2, at % 2
    size = out_ref.shape[0]

    def spot(target, half):
        start = pl.multiple_of((2 * target + half) * size, size)
        return pl.ds(start, size)

    def side_copy(target):
        return push(
            part.at[spot(target, 1 - column), :],
            side.at[target],
            side_sent.at[target],
            side_landed.at[target],
            at + 1 - 2 * column,
        )

    def lane_copy(target, sign):
        slot = target if sign == 1 else jnp.where(target == line - 1, rows, target)
        return push(
            part.at[spot(target, column), :],
            lane.at[slot],
            lane_sent.at[target],
            lane_landed.at[slot],
            at + 2 * sign,
        )

    def lane_wait(slot):
        push(
            lane.at[slot], lane.at[slot], lane_sent.at[0], lane_landed.at[slot], at + 1 - 2 * column
        ).wait_recv()

    def inside(row):
        return jnp.logical_and(row >= 0, row < rows)

    @pl.loop(0, rows)
    def _(step):
        @pl.loop(0, 2)
        def _(way):
            target = line + (2 * way - 1) * (rows - 1 - step)
            once = step < rows - way

            @pl.when(both(once, inside(target)))
            def _():
                work(target)
                side_copy(target).start()

    def merge(target):
        mine = spot(target, column)
        side_copy(target).wait_recv()
        part[mine, :] = (
            part[mine, :].astype(jnp.float32) + side[target].astype(jnp.float32)
        ).astype(jnp.bfloat16)

        def pass_on(sign):
            @pl.when(inside(line - sign))
            def _():
                lane_wait(target)
                part[mine, :] = (
                    part[mine, :].astype(jnp.float32) + lane[target].astype(jnp.float32)
                ).astype(jnp.bfloat16)

            lane_copy(target, sign).start()

        pl.when(target > line)(lambda: pass_on(1))
        pl.when(target < line)(lambda: pass_on(-1))

    @pl.loop(0, rows)
    def _(step):
        fill(step)
        @pl.loop(0, 2)
        def _(way):
            target = line + (2 * way - 1) * (rows - 1 - step)
            once = step < rows - way
            pl.when(both(once, inside(target)))(lambda: merge(target))

    mine = spot(line, column)
    out_ref[...] = part[mine, :].astype(jnp.float32)

    @pl.when(line > 0)
    def _():
        lane_wait(line)
        out_ref[...] += lane[line].astype(jnp.float32)

    @pl.when(line < rows - 1)
    def _():
        lane_wait(rows)
        out_ref[...] += lane[rows].astype(jnp.float32)

    @pl.loop(0, rows)
    def _(target):
        side_copy(target).wait_send()
        pl.when(target > line)(lambda: lane_copy(target, 1).wait_send())
        pl.when(target < line)(lambda: lane_copy(target, -1).wait_send())


def line_sems(rows):
    dma = pltpu.SemaphoreType.DMA
    return [dma((2, rows)), dma((rows,)), dma((rows,)), dma((rows,)), dma]


def lane_sems(rows):
    dma = pltpu.SemaphoreType.DMA
    return [dma((rows,)), dma((rows,)), dma((rows,)), dma((rows + 1,))]


def ffn_kernel(
    act_ref,
    w_ref,
    out_ref,
    acts_ref,
    w,
    acts,
    hidden,
    part,
    side,
    lane,
    w_done,
    save_done,
    *sems,
):
    at = lax.axis_index("blk")
    rows = lax.axis_size("blk") // 2
    pair = 2 * act_ref.shape[0]

    def load(which):
        return pltpu.make_async_copy(w_ref.at[which], w.at[which], w_done.at[which])

    def pair_rows(source):
        return pl.ds(pl.multiple_of(source * pair, pair), pair)

    def save(source):
        return pltpu.make_async_copy(
            acts.at[pair_rows(source), :], acts_ref.at[pair_rows(source), :], save_done.at[source]
        )

    for which in range(3):
        load(which).start()
    greet(at, at // 2, rows)

    def ready():
        for which in range(3):
            load(which).wait()

    def expand(source):
        save(source).start()
        rows_now = acts[pair_rows(source), :]
        gate = contract_last(w[0], rows_now)
        up = contract_last(w[1], rows_now)
        hidden[source] = (gelu_value(gate) * up).astype(jnp.bfloat16)

    def reduce(target):
        part[pair_rows(target), :] = lax.dot_general(
            hidden[target], w[2], (((0,), (0,)), ((), ())), preferred_element_type=jnp.float32
        ).astype(jnp.bfloat16)

    line_gather(act_ref, acts, *sems[:5], ready, expand)
    line_scatter(part, side, lane, out_ref, *sems[5:], reduce, lambda step: None)
    pl.loop(0, rows)(lambda source: save(source).wait())


def ffn_forward(act_ffn, w_parts):
    size, width = act_ffn.shape
    units = w_parts.shape[1]
    blocks = lax.axis_size("blk")
    rows = blocks // 2
    whole = pl.BlockSpec(memory_space=pltpu.VMEM)
    far = pl.BlockSpec(memory_space=pl.ANY)
    return pl.pallas_call(
        ffn_kernel,
        out_shape=(
            jax.ShapeDtypeStruct((size, width), jnp.float32),
            jax.ShapeDtypeStruct((blocks * size, width), jnp.bfloat16),
        ),
        in_specs=[whole, far],
        out_specs=(whole, far),
        scratch_shapes=[
            pltpu.VMEM(w_parts.shape, jnp.bfloat16),
            pltpu.VMEM((blocks * size, width), jnp.bfloat16),
            pltpu.VMEM((rows, units, 2 * size), jnp.bfloat16),
            pltpu.VMEM((blocks * size, width), jnp.bfloat16),
            pltpu.VMEM((rows, size, width), jnp.bfloat16),
            pltpu.VMEM((rows + 1, size, width), jnp.bfloat16),
            pltpu.SemaphoreType.DMA((3,)),
            pltpu.SemaphoreType.DMA((rows,)),
            *line_sems(rows),
            *lane_sems(rows),
        ],
        compiler_params=pltpu.CompilerParams(
            collective_id=2, has_side_effects=True, vmem_limit_bytes=VMEM_BYTES
        ),
        cost_estimate=cost_of(115),
        name="ffn_forward",
    )(act_ffn, w_parts)


FILL_COLUMNS = 256
FILL_FIRST = 3


def ffn_back_kernel(
    owners,
    grad_ref,
    acts_ref,
    w_ref,
    out_ref,
    keep_ref,
    cross_ref,
    w,
    rights,
    lefts,
    part,
    side,
    lane,
    stage,
    mate_part,
    summed,
    w_done,
    acts_done,
    mate_sent,
    mate_landed,
    summed_done,
    *sems,
):
    at = lax.axis_index("blk")
    me = lax.axis_index("sp")
    chip, core = me // 2, me % 2
    mate = me + 1 - 2 * core
    rows = lax.axis_size("blk") // 2
    size, width = grad_ref.shape
    pair = 2 * size
    units = w.shape[1]
    acts, grads = rights.at[0], rights.at[1]

    def load(which):
        return pltpu.make_async_copy(w_ref.at[which], w.at[which], w_done.at[which])

    def pair_rows(source):
        return pl.ds(pl.multiple_of(source * pair, pair), pair)

    acts_copy = pltpu.make_async_copy(acts_ref, acts, acts_done)
    acts_copy.start()
    for which in range(3):
        load(which).start()
    greet(at, at // 2, rows, mate)

    def ready():
        acts_copy.wait()
        for which in range(3):
            load(which).wait()

    def expand(source):
        columns = pair_rows(source)
        rows_now = acts[pair_rows(source), :]
        gate = contract_last(w[0], rows_now)
        up = contract_last(w[1], rows_now)
        grad_hidden = contract_last(w[2], grads[pair_rows(source), :])
        bent = jnp.tanh(GELU_SCALE * (gate + GELU_CUBIC * gate * gate * gate))
        value = 0.5 * gate * (1.0 + bent)
        slope = 0.5 * (1.0 + bent) + 0.5 * gate * (1.0 - bent * bent) * GELU_SCALE * (
            1.0 + 3.0 * GELU_CUBIC * gate * gate
        )
        lefts[2, :, columns] = (value * up).astype(jnp.bfloat16)
        lefts[0, :, columns] = (grad_hidden * up * slope).astype(jnp.bfloat16)
        lefts[1, :, columns] = (grad_hidden * value).astype(jnp.bfloat16)

    def reduce(target):
        columns = pair_rows(target)
        dims = (((0,), (0,)), ((), ()))
        total = lax.dot_general(
            lefts[0, :, columns], w[0], dims, preferred_element_type=jnp.float32
        ) + lax.dot_general(lefts[1, :, columns], w[1], dims, preferred_element_type=jnp.float32)
        part[pair_rows(target), :] = total.astype(jnp.bfloat16)

    pieces = width // FILL_COLUMNS
    total_pieces = 3 * pieces

    def piece_columns(item):
        return pl.ds(pl.multiple_of((item % pieces) * FILL_COLUMNS, FILL_COLUMNS), FILL_COLUMNS)

    def mate_copy(item):
        return push_sp(
            stage.at[item % 3, :, 1 - core],
            mate_part.at[item],
            mate_sent.at[item % 3],
            mate_landed.at[item],
            mate,
        )

    def put(item, side_chip, target):
        return pltpu.make_async_copy(
            summed.at[item % 2, side_chip],
            target.at[item // pieces, :, piece_columns(item)],
            summed_done.at[item % 2, side_chip],
        )

    def put_wait(item):
        put(item, chip, keep_ref).wait()
        put(item, 1 - chip, cross_ref).wait()

    def sum_one(item):
        pl.when(item > 1)(lambda: put_wait(item - 2))
        mate_copy(item).wait_recv()
        summed[item % 2] = (
            stage[item % 3, :, core].astype(jnp.float32) + mate_part[item].astype(jnp.float32)
        ).astype(jnp.bfloat16)
        put(item, chip, keep_ref).start()
        put(item, 1 - chip, cross_ref).start()

    def fill_one(item):
        which = item // pieces
        total = jnp.dot(
            lefts[which],
            rights[which // 2, :, piece_columns(item)],
            preferred_element_type=jnp.float32,
        )
        pl.when(item > 2)(lambda: mate_copy(item - 3).wait_send())
        stage[item % 3] = total.astype(jnp.bfloat16).reshape(
            2, 2, units // owners, FILL_COLUMNS
        )
        mate_copy(item).start()
        pl.when(item > 0)(lambda: sum_one(item - 1))

    each = pl.cdiv(total_pieces - FILL_FIRST, rows - 1)

    def fill(step):
        first = jnp.maximum(FILL_FIRST + (step - 1) * each, 0)
        last = jnp.minimum(FILL_FIRST + step * each, total_pieces)

        @pl.loop(0, each)
        def _(item):
            pl.when(first + item < last)(lambda: fill_one(first + item))

    line_gather(grad_ref, grads, *sems[:5], ready, expand)
    line_scatter(part, side, lane, out_ref, *sems[5:], reduce, fill)
    sum_one(total_pieces - 1)
    put_wait(total_pieces - 2)
    put_wait(total_pieces - 1)
    for item in range(total_pieces - 3, total_pieces):
        mate_copy(item).wait_send()


def ffn_back(grad_ffn, acts, w_parts, owners):
    size, width = grad_ffn.shape
    units = w_parts.shape[1]
    blocks = lax.axis_size("blk")
    rows = blocks // 2
    tokens = blocks * size
    items = 3 * width // FILL_COLUMNS
    whole = pl.BlockSpec(memory_space=pltpu.VMEM)
    far = pl.BlockSpec(memory_space=pl.ANY)
    return pl.pallas_call(
        functools.partial(ffn_back_kernel, owners),
        out_shape=(
            jax.ShapeDtypeStruct((size, width), jnp.float32),
            jax.ShapeDtypeStruct((3, units // owners, width), jnp.bfloat16),
            jax.ShapeDtypeStruct((3, units // owners, width), jnp.bfloat16),
        ),
        in_specs=[whole, far, far],
        out_specs=(whole, far, far),
        scratch_shapes=[
            pltpu.VMEM(w_parts.shape, jnp.bfloat16),
            pltpu.VMEM((2, tokens, width), jnp.bfloat16),
            pltpu.VMEM((3, units, tokens), jnp.bfloat16),
            pltpu.VMEM((tokens, width), jnp.bfloat16),
            pltpu.VMEM((rows, size, width), jnp.bfloat16),
            pltpu.VMEM((rows + 1, size, width), jnp.bfloat16),
            pltpu.VMEM((3, 2, 2, units // owners, FILL_COLUMNS), jnp.bfloat16),
            pltpu.VMEM((items, 2, units // owners, FILL_COLUMNS), jnp.bfloat16),
            pltpu.VMEM((2, 2, units // owners, FILL_COLUMNS), jnp.bfloat16),
            pltpu.SemaphoreType.DMA((3,)),
            pltpu.SemaphoreType.DMA,
            pltpu.SemaphoreType.DMA((3,)),
            pltpu.SemaphoreType.DMA((items,)),
            pltpu.SemaphoreType.DMA((2, 2)),
            *line_sems(rows),
            *lane_sems(rows),
        ],
        compiler_params=pltpu.CompilerParams(
            collective_id=3, has_side_effects=True, vmem_limit_bytes=VMEM_BYTES
        ),
        cost_estimate=cost_of(115),
        name="ffn_back",
    )(grad_ffn, acts, w_parts)


def ffn_hidden(acts, w_parts):
    gate = contract_last(acts, w_parts[0])
    up = contract_last(acts, w_parts[1])
    return (gate, up, (gelu_value(gate) * up).astype(jnp.bfloat16))


def scatter_tokens(partial):
    return lax.psum_scatter(
        partial.astype(jnp.bfloat16), "blk", scatter_dimension=0, tiled=True
    ).astype(jnp.float32)


def ffn_forward_wide(act_ffn, w_parts):
    acts = lax.all_gather(act_ffn, "blk", axis=0, tiled=True)
    hidden = ffn_hidden(acts, w_parts)[2]
    partial = jnp.dot(hidden, w_parts[2], preferred_element_type=jnp.float32)
    return (scatter_tokens(partial), acts)


def ffn_back_wide(grad_ffn, acts, w_parts, owners):
    grads = lax.all_gather(grad_ffn, "blk", axis=0, tiled=True)
    gate, up, hidden = ffn_hidden(acts, w_parts)
    grad_hidden = contract_last(grads, w_parts[2])
    grad_gate = (grad_hidden * up * gelu_slope(gate)).astype(jnp.bfloat16)
    grad_up = (grad_hidden * gelu_value(gate)).astype(jnp.bfloat16)
    partial = jnp.dot(grad_gate, w_parts[0], preferred_element_type=jnp.float32) + jnp.dot(
        grad_up, w_parts[1], preferred_element_type=jnp.float32
    )
    sums = jnp.stack(
        [
            jnp.einsum("tf,td->fd", left, right, preferred_element_type=jnp.float32)
            for left, right in ((grad_gate, acts), (grad_up, acts), (hidden, grads))
        ]
    ).astype(jnp.bfloat16)
    units = w_parts.shape[1]
    owned = sums.reshape(3, owners, units // owners, sums.shape[2])
    mine = lax.psum_scatter(
        jnp.transpose(owned, (1, 0, 2, 3)), "sp", scatter_dimension=0, tiled=True
    )
    return (scatter_tokens(partial), mine[0], None)


def cost_of(microseconds):
    return pl.CostEstimate(
        flops=int(microseconds * 1e9), bytes_accessed=int(microseconds * 3e6), transcendentals=0
    )


def push_sp(source, target, sent, landed, peer):
    return pltpu.make_async_remote_copy(
        src_ref=source,
        dst_ref=target,
        send_sem=sent,
        recv_sem=landed,
        device_id={"sp": peer},
        device_id_type=pl.DeviceIdType.MESH,
    )


def greet_sp(me, groups):
    barrier = pltpu.get_barrier_semaphore()
    for step in range(1, groups):
        pl.semaphore_signal(
            barrier,
            inc=1,
            device_id={"sp": (me + step) % groups},
            device_id_type=pl.DeviceIdType.MESH,
        )
    pl.semaphore_wait(barrier, groups - 1)


def gather_project_kernel(x_ref, w_ref, full_ref, out_ref, w, w_done, own_done, sent, landed):
    me = lax.axis_index("sp")
    size = x_ref.shape[0]
    units = w.shape[0]
    mate = me + 1 - 2 * (me % 2)
    across = (me + 2) % 4

    def spot(member):
        return full_ref.at[pl.ds(pl.multiple_of(member * size, size), size), :]

    load = pltpu.make_async_copy(
        w_ref.at[pl.ds(pl.multiple_of(me * units, units), units), :], w, w_done
    )
    load.start()
    greet_sp(me, 4)
    over = push_sp(x_ref, spot(me), sent.at[0], landed.at[0], across)
    over.start()
    beside = push_sp(x_ref, spot(me), sent.at[1], landed.at[1], mate)
    beside.start()
    keep = pltpu.make_async_copy(x_ref, spot(me), own_done)
    keep.start()
    keep.wait()
    load.wait()

    def project(chip):
        rows = pl.ds(pl.multiple_of(chip * 2 * size, 2 * size), 2 * size)
        out_ref[rows, :] = contract_last(full_ref[rows, :], w[...]).astype(jnp.bfloat16)

    beside.wait_recv()
    project(me // 2)
    over.wait_recv()
    onward = push_sp(spot(across), spot(across), sent.at[2], landed.at[2], mate)
    onward.start()
    onward.wait_recv()
    project(across // 2)
    over.wait_send()
    beside.wait_send()
    onward.wait_send()


def gather_project(rows, weights, identity):
    size, width = rows.shape
    units = weights.shape[0] // 4
    whole = pl.BlockSpec(memory_space=pltpu.VMEM)
    return pl.pallas_call(
        gather_project_kernel,
        out_shape=(
            jax.ShapeDtypeStruct((4 * size, width), jnp.bfloat16),
            jax.ShapeDtypeStruct((4 * size, units), jnp.bfloat16),
        ),
        in_specs=[whole, pl.BlockSpec(memory_space=pl.ANY)],
        out_specs=(whole, whole),
        scratch_shapes=[
            pltpu.VMEM((units, width), jnp.bfloat16),
            pltpu.SemaphoreType.DMA,
            pltpu.SemaphoreType.DMA,
            pltpu.SemaphoreType.DMA((3,)),
            pltpu.SemaphoreType.DMA((3,)),
        ],
        compiler_params=pltpu.CompilerParams(
            collective_id=identity, has_side_effects=True, vmem_limit_bytes=VMEM_BYTES
        ),
        cost_estimate=cost_of(18),
        name="gather_project",
    )(rows, weights)


def exchange_project_kernel(x_ref, w_ref, out_ref, w, got, w_done, own_done, sent, landed):
    me = lax.axis_index("sp")
    size = out_ref.shape[0]
    units = x_ref.shape[1]

    def rows_of(member):
        return x_ref.at[pl.ds(pl.multiple_of(member * size, size), size), :]

    def load(member):
        rows = pl.ds(pl.multiple_of(member * units, units), units)
        return pltpu.make_async_copy(w_ref.at[rows, :], w.at[rows, :], w_done.at[member])

    def send(step):
        peer = (me + step) % 4
        return push_sp(rows_of(peer), got.at[4 - step], sent.at[step], landed.at[4 - step], peer)

    greet_sp(me, 4)
    for step in (2, 1, 3):
        send(step).start()
    keep = pltpu.make_async_copy(rows_of(me), got.at[0], own_done)
    keep.start()
    for step in range(4):
        load((me + step) % 4).start()
    keep.wait()
    for step in (0, 1, 3, 2):
        member = (me + step) % 4
        load(member).wait()
        if step > 0:
            send(4 - step).wait_recv()
        rows = pl.ds(pl.multiple_of(member * units, units), units)
        term = jnp.dot(got[step], w[rows, :], preferred_element_type=jnp.float32)
        if step == 0:
            out_ref[...] = term
        else:
            out_ref[...] += term
    for step in (1, 2, 3):
        send(step).wait_send()


def exchange_project(columns, weights, identity):
    size = columns.shape[0] // 4
    whole = pl.BlockSpec(memory_space=pltpu.VMEM)
    return pl.pallas_call(
        exchange_project_kernel,
        out_shape=jax.ShapeDtypeStruct((size, weights.shape[1]), jnp.float32),
        in_specs=[whole, pl.BlockSpec(memory_space=pl.ANY)],
        out_specs=whole,
        scratch_shapes=[
            pltpu.VMEM(weights.shape, jnp.bfloat16),
            pltpu.VMEM((4, size, columns.shape[1]), jnp.bfloat16),
            pltpu.SemaphoreType.DMA((4,)),
            pltpu.SemaphoreType.DMA,
            pltpu.SemaphoreType.DMA((4,)),
            pltpu.SemaphoreType.DMA((4,)),
        ],
        compiler_params=pltpu.CompilerParams(
            collective_id=identity, has_side_effects=True, vmem_limit_bytes=VMEM_BYTES
        ),
        cost_estimate=cost_of(16),
        name="exchange_project",
    )(columns, weights)


def finish_kernel(
    cols_ref,
    act_ref,
    att_ref,
    grad_ref,
    w_ref,
    tokens_ref,
    middle_ref,
    gain_ref,
    rows_ref,
    cross_ref,
    qkv_ref,
    out_ref,
    tokens_grad_ref,
    gains_ref,
    far_ref,
    w,
    got,
    grad_in,
    total,
    part,
    side,
    lane,
    mine,
    from_sp,
    from_side,
    from_line,
    w_done,
    own_done,
    swap_sent,
    swap_landed,
    sp_sent,
    sp_landed,
    gain_side,
    line_sent,
    line_landed,
    cross_sent,
    cross_landed,
    *sems,
):
    at = lax.axis_index("blk")
    me = lax.axis_index("sp")
    rows = lax.axis_size("blk") // 2
    line, column = at // 2, at % 2
    partner = at + 1 - 2 * column
    block = total.shape[0]
    size = tokens_ref.shape[0]
    units = cols_ref.shape[1]
    extra = block - size

    barrier = pltpu.get_barrier_semaphore()
    for step in range(1, 4):
        pl.semaphore_signal(
            barrier, inc=1, device_id={"sp": (me + step) % 4}, device_id_type=pl.DeviceIdType.MESH
        )

    def line_peer(step):
        return 2 * ((line + step) % rows) + column

    for peer in [partner] + [line_peer(step) for step in range(1, rows)]:
        pl.semaphore_signal(
            barrier, inc=1, device_id={"blk": peer}, device_id_type=pl.DeviceIdType.MESH
        )

    def load(member):
        span = pl.ds(pl.multiple_of(member * units, units), units)
        return pltpu.make_async_copy(w_ref.at[span, :], w.at[span, :], w_done.at[member])

    def rows_of(member):
        return cols_ref.at[pl.ds(pl.multiple_of(member * size, size), size), :]

    def swap(step):
        peer = (me + step) % 4
        return push_sp(
            rows_of(peer), got.at[4 - step], swap_sent.at[step], swap_landed.at[4 - step], peer
        )

    for step in range(4):
        load((me + step) % 4).start()
    keep = pltpu.make_async_copy(rows_of(me), got.at[0], own_done)
    keep.start()
    pl.semaphore_wait(barrier, 3 + rows)
    for step in (2, 1, 3):
        swap(step).start()
    over = carry(
        cross_ref, far_ref, far_ref.shape[1], cross_sent, cross_landed, (me + 2) % 4
    )
    over.start()
    keep.wait()

    def sp_gains(step):
        return push_sp(
            mine, from_sp.at[4 - step], sp_sent.at[step], sp_landed.at[4 - step], (me + step) % 4
        )

    def side_gains():
        return push(from_sp.at[0], from_side, gain_side.at[0], gain_side.at[1], partner)

    def line_gains(step):
        return push(
            from_line.at[0],
            from_line.at[rows - step],
            line_sent.at[step],
            line_landed.at[rows - step],
            line_peer(step),
        )

    def reduce(target):
        dims = (((0,), (0,)), ((), ()))
        wide_columns = pl.ds(pl.multiple_of(target * 2 * size, 2 * size), 2 * size)
        term = lax.dot_general(
            cols_ref[:, wide_columns], act_ref[...], dims, preferred_element_type=jnp.float32
        ).astype(jnp.bfloat16)
        columns = pl.ds(pl.multiple_of(target * 2 * extra, 2 * extra), 2 * extra)
        more = lax.dot_general(
            att_ref[:, columns], grad_ref[...], dims, preferred_element_type=jnp.float32
        ).astype(jnp.bfloat16)
        for half in range(2):
            start = pl.multiple_of((2 * target + half) * block, block)
            part[pl.ds(start, size), :] = term[half * size : (half + 1) * size]
            start = pl.multiple_of((2 * target + half) * block + size, extra)
            part[pl.ds(start, extra), :] = more[half * extra : (half + 1) * extra]

    def inputs_back():
        for step in (0, 1, 3, 2):
            member = (me + step) % 4
            load(member).wait()
            if step > 0:
                swap(4 - step).wait_recv()
            span = pl.ds(pl.multiple_of(member * units, units), units)
            term = jnp.dot(got[step], w[span, :], preferred_element_type=jnp.float32)
            if step == 0:
                grad_in[...] = term
            else:
                grad_in[...] += term
        normed, inverse = norm_parts(tokens_ref[...].astype(jnp.float32))
        grad_v, gain_row = norm_back(grad_in[...], normed, inverse, gain_ref[...])
        tokens_grad_ref[...] = (middle_ref[...] + grad_v).astype(jnp.bfloat16)
        mine[...] = rows_ref[...]
        mine[0:1, :] = gain_row[None, :]
        for step in range(1, 4):
            sp_gains(step).start()

    def fill(step):
        pl.when(step == 1)(inputs_back)

        @pl.when(step == 2)
        def _():
            gains = mine[...]
            for other in range(1, 4):
                sp_gains(4 - other).wait_recv()
                gains = gains + from_sp[other]
            from_sp[0] = gains
            side_gains().start()

        @pl.when(step == 3)
        def _():
            side_gains().wait_recv()
            from_line[0] = from_sp[0] + from_side[...]
            for other in range(1, rows):
                line_gains(other).start()

    line_scatter(part, side, lane, total, *sems, reduce, fill)
    qkv_ref[...] = total[:size]
    out_ref[...] = total[size:]
    gains = from_line[0]
    for other in range(1, rows):
        line_gains(rows - other).wait_recv()
        gains = gains + from_line[other]
    gains_ref[...] = gains
    for step in (1, 2, 3):
        swap(step).wait_send()
        sp_gains(step).wait_send()
    over.wait()
    side_gains().wait_send()
    for step in range(1, rows):
        line_gains(step).wait_send()


def finish(
    cols, act_block, attended, grad_block, w_qkv, tokens, grad_middle, gain, gain_rows, cross
):
    blocks = lax.axis_size("blk")
    rows = blocks // 2
    size, width = tokens.shape
    block = (cols.shape[1] + attended.shape[1]) // blocks
    whole = pl.BlockSpec(memory_space=pltpu.VMEM)
    any_space = pl.BlockSpec(memory_space=pl.ANY)
    dma = pltpu.SemaphoreType.DMA
    small = gain_rows.shape
    return pl.pallas_call(
        finish_kernel,
        out_shape=(
            jax.ShapeDtypeStruct((cols.shape[1] // blocks, width), jnp.float32),
            jax.ShapeDtypeStruct((attended.shape[1] // blocks, width), jnp.float32),
            jax.ShapeDtypeStruct((size, width), jnp.bfloat16),
            jax.ShapeDtypeStruct(small, jnp.float32),
            half_of(cross),
        ),
        in_specs=[whole] * 4 + [any_space] + [whole] * 4 + [any_space],
        out_specs=(whole, whole, whole, whole, any_space),
        scratch_shapes=[
            pltpu.VMEM(w_qkv.shape, jnp.bfloat16),
            pltpu.VMEM((4, size, cols.shape[1]), jnp.bfloat16),
            pltpu.VMEM((size, width), jnp.float32),
            pltpu.VMEM((block, width), jnp.float32),
            pltpu.VMEM((blocks * block, width), jnp.bfloat16),
            pltpu.VMEM((rows, block, width), jnp.bfloat16),
            pltpu.VMEM((rows + 1, block, width), jnp.bfloat16),
            pltpu.VMEM(small, jnp.float32),
            pltpu.VMEM((4, *small), jnp.float32),
            pltpu.VMEM(small, jnp.float32),
            pltpu.VMEM((rows, *small), jnp.float32),
            dma((4,)),
            dma,
            dma((4,)),
            dma((4,)),
            dma((4,)),
            dma((4,)),
            dma((2,)),
            dma((rows,)),
            dma((rows,)),
            dma,
            dma,
            *lane_sems(rows),
        ],
        compiler_params=pltpu.CompilerParams(
            collective_id=8, has_side_effects=True, vmem_limit_bytes=VMEM_BYTES
        ),
        cost_estimate=cost_of(85),
        name="finish",
    )(cols, act_block, attended, grad_block, w_qkv, tokens, grad_middle, gain, gain_rows, cross)


def weight_sums_wide(left, right):
    term = jnp.einsum("tc,td->cd", left, right, preferred_element_type=jnp.float32)
    return scatter_tokens(term)


def finish_wide(
    cols, act_block, attended, grad_block, w_qkv, tokens, grad_middle, gain, gain_rows, cross
):
    grad_act_in = exchange_project(cols, w_qkv, 7)
    normed, inverse = norm_parts(tokens.astype(jnp.float32))
    grad_v, gain_row = norm_back(grad_act_in, normed, inverse, gain)
    gains_all = lax.psum(jnp.concatenate([gain_row[None], gain_rows[1:]]), ("blk", "sp"))
    return (
        weight_sums_wide(cols, act_block),
        weight_sums_wide(attended, grad_block),
        (grad_middle + grad_v).astype(jnp.bfloat16),
        gains_all,
        None,
    )


def body(tokens, w_qkv, w_out, gains, w_ffn, cotangent):
    groups = lax.axis_size("sp")
    heads_here = HEADS // groups
    source = tokens.astype(jnp.float32)
    normed_in, inverse_in = norm_parts(source)
    act_in = (normed_in * gains[0]).astype(jnp.bfloat16)
    act_block, projected = gather_project(act_in, w_qkv, 4)
    block_rows = projected.shape[0]
    attended_cols, attended, totals, kv_all = attend(projected, heads_here)
    attn = exchange_project(attended_cols, w_out, 5)
    normed_attn, inverse_attn = norm_parts(attn)
    middle = source + normed_attn * gains[1]
    normed_mid, inverse_mid = norm_parts(middle)
    act_ffn = (normed_mid * gains[2]).astype(jnp.bfloat16)
    wide = lax.axis_size("blk") > 8
    w_parts = jnp.transpose(w_ffn, (1, 0, 2))
    ffn_out, act_all = (ffn_forward_wide if wide else ffn_forward)(act_ffn, w_parts)
    normed_ffn, inverse_ffn = norm_parts(ffn_out)
    result = middle + normed_ffn * gains[3]
    grad_out = cotangent.astype(jnp.float32)
    grad_ffn_f, gain_grad3 = norm_back(grad_out, normed_ffn, inverse_ffn, gains[3])
    grad_ffn = grad_ffn_f.astype(jnp.bfloat16)
    grad_act_ffn, ffn_part, cross = (ffn_back_wide if wide else ffn_back)(
        grad_ffn, act_all, w_parts, groups
    )
    grad_norm_mid, gain_grad2 = norm_back(grad_act_ffn, normed_mid, inverse_mid, gains[2])
    grad_middle = grad_out + grad_norm_mid
    grad_attn_f, gain_grad1 = norm_back(grad_middle, normed_attn, inverse_attn, gains[1])
    grad_attn = grad_attn_f.astype(jnp.bfloat16)
    grad_block, grad_attended = gather_project(grad_attn, w_out, 6)
    grad_heads = grad_attended.astype(jnp.float32).reshape(block_rows, heads_here, HEAD)
    totals_rows = jnp.transpose(totals.reshape(heads_here, block_rows))
    scaled = (grad_heads / totals_rows[..., None]).astype(jnp.bfloat16)
    row_delta = (
        jnp.sum(grad_heads * attended.reshape(block_rows, heads_here, HEAD), axis=-1) / totals_rows
    )
    grad_cols, *far_first = attend_back(
        projected,
        scaled.reshape(block_rows, heads_here * HEAD),
        jnp.transpose(row_delta).reshape(heads_here, 1, block_rows),
        kv_all,
        cross,
    )
    gain_rows = jnp.stack(
        [jnp.zeros_like(gain_grad1), gain_grad1, gain_grad2, gain_grad3]
        + [jnp.zeros_like(gain_grad1)] * 4
    )
    qkv_grad, out_grad, tokens_grad, gains_all, far_last = (finish_wide if wide else finish)(
        grad_cols,
        act_block,
        attended_cols,
        grad_block,
        w_qkv,
        tokens,
        grad_middle,
        gains[0][None],
        gain_rows,
        cross,
    )
    ffn_sum = ffn_part.astype(jnp.float32)
    if not wide:
        ffn_sum = ffn_sum + jnp.concatenate([*far_first, far_last], axis=1).astype(jnp.float32)
    ffn_grad = jnp.transpose(ffn_sum, (1, 0, 2))
    share = gains_all.shape[1] // (groups * lax.axis_size("blk"))
    place = lax.axis_index("sp") * lax.axis_size("blk") + lax.axis_index("blk")
    gains_grad = lax.dynamic_slice_in_dim(gains_all[:4], place * share, share, 1)
    return (result.astype(jnp.bfloat16), tokens_grad, qkv_grad, out_grad, gains_grad, ffn_grad)


def solution(mesh):
    return jax.shard_map(
        body,
        mesh=mesh,
        in_specs=(
            P(("blk", "sp"), None),
            P(),
            P(),
            P(),
            P("blk", None, None),
            P(("blk", "sp"), None),
        ),
        out_specs=(
            P(("blk", "sp"), None),
            P(("blk", "sp"), None),
            P(("sp", "blk"), None),
            P(("sp", "blk"), None),
            P(None, ("sp", "blk")),
            P(("blk", "sp"), None, None),
        ),
        check_vma=False,
    )
```

```python
import functools

import jax
import jax.numpy as jnp
from jax import lax
from jax.experimental import pallas as pl
from jax.experimental.pallas import tpu as pltpu
from jax.sharding import PartitionSpec as P

HEADS = 8
KV_HEADS = 4
HEAD = 256


VMEM_BYTES = 62 * 1024 * 1024
NORM_EPSILON = 1e-06
CAP_VALUE = 50.0
GELU_SCALE = 0.7978845608028654
GELU_CUBIC = 0.044715


def norm_parts(values):
    inverse = lax.rsqrt(jnp.mean(values * values, axis=-1, keepdims=True) + NORM_EPSILON)
    return (values * inverse, inverse)


def norm_back(grad_y, normed, inverse, gain):
    grad_n = grad_y * gain
    grad_v = inverse * (grad_n - normed * jnp.mean(grad_n * normed, axis=-1, keepdims=True))
    return (grad_v, jnp.sum(grad_y * normed, axis=0))


def gelu_value(values):
    return (
        0.5
        * values
        * (1.0 + jnp.tanh(GELU_SCALE * (values + GELU_CUBIC * values * values * values)))
    )


def gelu_slope(values):
    bent = jnp.tanh(GELU_SCALE * (values + GELU_CUBIC * values * values * values))
    return 0.5 * (1.0 + bent) + 0.5 * values * (1.0 - bent * bent) * GELU_SCALE * (
        1.0 + 3.0 * GELU_CUBIC * values * values
    )


def contract_last(left, right):
    return lax.dot_general(
        left, right, (((1,), (1,)), ((), ())), preferred_element_type=jnp.float32
    )


def push(source, target, sent, landed, block):
    return pltpu.make_async_remote_copy(
        src_ref=source,
        dst_ref=target,
        send_sem=sent,
        recv_sem=landed,
        device_id={"blk": block},
        device_id_type=pl.DeviceIdType.MESH,
    )


def greet(at, line, rows, sp_peer=None):
    barrier = pltpu.get_barrier_semaphore()
    others = 1
    if sp_peer is not None:
        others = 2
        pl.semaphore_signal(
            barrier, inc=1, device_id={"sp": sp_peer}, device_id_type=pl.DeviceIdType.MESH
        )

    def tell(block):
        pl.semaphore_signal(
            barrier, inc=1, device_id={"blk": block}, device_id_type=pl.DeviceIdType.MESH
        )

    tell(at + 1 - 2 * (at % 2))
    pl.when(line > 0)(lambda: tell(at - 2))
    pl.when(line < rows - 1)(lambda: tell(at + 2))
    pl.semaphore_wait(barrier, others + jnp.minimum(line, 1) + jnp.minimum(rows - 1 - line, 1))


def both(*terms):
    result = terms[0]
    for term in terms[1:]:
        result = jnp.logical_and(result, term)
    return result


def attend_kernel(
    heads,
    x_ref,
    low_ref,
    att_ref,
    tot_ref,
    kv_ref,
    kv,
    acc,
    part,
    up_sent,
    up_landed,
    side_sent,
    side_landed,
    own_done,
    save_done,
):
    at = lax.axis_index("blk")
    blocks = lax.axis_size("blk")
    rows = blocks // 2
    line, column = at // 2, at % 2
    partner = at + 1 - 2 * column
    size = x_ref.shape[0]
    first = heads * HEAD
    own = x_ref.at[:, pl.ds(first, 2 * HEAD)]
    greet(at, line, rows)

    def up_copy(index, source):
        return push(source, kv.at[index], up_sent.at[index // 2], up_landed.at[index // 2], at + 2)

    def side_copy(index, source):
        return push(
            source, kv.at[index], side_sent.at[index // 2], side_landed.at[index // 2], partner
        )

    def save(index):
        return pltpu.make_async_copy(kv.at[index], kv_ref.at[index], save_done.at[index])

    pl.when(line < rows - 1)(lambda: up_copy(at, own).start())
    pl.when(column == 0)(lambda: side_copy(at, own).start())
    keep = pltpu.make_async_copy(own, kv.at[at], own_done)
    keep.start()
    acc[...] = jnp.zeros_like(acc)
    part[...] = jnp.zeros_like(part)
    keep.wait()
    ahead = lax.broadcasted_iota(jnp.int32, (size, size), 1) - lax.broadcasted_iota(
        jnp.int32, (size, size), 0
    )

    def compute(index):
        save(index).start()
        span = (at - index) * size
        for head in range(heads):
            raw = lax.dot_general(
                x_ref[:, head * HEAD : (head + 1) * HEAD],
                kv[index, :, :HEAD],
                (((1,), (1,)), ((), ())),
                preferred_element_type=jnp.float32,
            )
            weights = jnp.exp(CAP_VALUE * jnp.tanh(raw * (HEAD ** (-0.5) / CAP_VALUE)))
            weights = jnp.where(ahead <= span, weights, 0.0)
            total = weights[:, :128]
            for piece in range(1, size // 128):
                total = total + weights[:, piece * 128 : (piece + 1) * 128]
            part[head] += total
            acc[:, head * HEAD : (head + 1) * HEAD] += jnp.dot(
                weights.astype(jnp.bfloat16),
                kv[index, :, HEAD:],
                preferred_element_type=jnp.float32,
            )

    @pl.loop(0, rows + 1)
    def _(step):
        source = line - step
        index = 2 * source + column

        @pl.when(both(step > 0, source >= 0))
        def _():
            up_copy(index, kv.at[index]).wait_recv()
            pl.when(line < rows - 1)(lambda: up_copy(index, kv.at[index]).start())
            side_copy(index, kv.at[index]).start()

        @pl.loop(0, 2)
        def _(way):
            found = source + way
            here = 2 * found + jnp.where(way == 0, column, 1 - column)
            due = jnp.logical_or(way == 0, both(step > 0, jnp.logical_or(step > 1, column == 1)))

            @pl.when(both(found >= 0, due))
            def _():
                pl.when(way == 1)(lambda: side_copy(here, kv.at[here]).wait_recv())
                compute(here)

    for head in range(heads):
        columns = slice(head * HEAD, (head + 1) * HEAD)
        total = jnp.sum(part[head], axis=1, keepdims=True)
        value = acc[:, columns] / total
        att_ref[:, columns] = value
        low_ref[:, columns] = value.astype(jnp.bfloat16)
        tot_ref[head] = jnp.sum(part[head].T, axis=0, keepdims=True)

    @pl.loop(0, rows)
    def _(source):
        index = 2 * source + column

        @pl.when(source <= line)
        def _():
            pl.when(line < rows - 1)(lambda: up_copy(index, kv.at[index]).wait_send())
            pl.when(jnp.logical_or(source < line, column == 0))(
                lambda: side_copy(index, kv.at[index]).wait_send()
            )

    @pl.loop(0, blocks)
    def _(index):
        pl.when(index <= at)(lambda: save(index).wait())


def attend(projected, heads):
    size = projected.shape[0]
    blocks = lax.axis_size("blk")
    whole = pl.BlockSpec(memory_space=pltpu.VMEM)
    return pl.pallas_call(
        functools.partial(attend_kernel, heads),
        out_shape=(
            jax.ShapeDtypeStruct((size, heads * HEAD), jnp.bfloat16),
            jax.ShapeDtypeStruct((size, heads * HEAD), jnp.float32),
            jax.ShapeDtypeStruct((heads, 1, size), jnp.float32),
            jax.ShapeDtypeStruct((blocks, size, 2 * HEAD), jnp.bfloat16),
        ),
        in_specs=[whole],
        out_specs=(whole, whole, whole, pl.BlockSpec(memory_space=pl.ANY)),
        scratch_shapes=[
            pltpu.VMEM((blocks, size, 2 * HEAD), jnp.bfloat16),
            pltpu.VMEM((size, heads * HEAD), jnp.float32),
            pltpu.VMEM((heads, size, 128), jnp.float32),
            pltpu.SemaphoreType.DMA((blocks // 2,)),
            pltpu.SemaphoreType.DMA((blocks // 2,)),
            pltpu.SemaphoreType.DMA((blocks // 2,)),
            pltpu.SemaphoreType.DMA((blocks // 2,)),
            pltpu.SemaphoreType.DMA,
            pltpu.SemaphoreType.DMA((blocks,)),
        ],
        compiler_params=pltpu.CompilerParams(
            collective_id=0, has_side_effects=True, vmem_limit_bytes=VMEM_BYTES
        ),
        cost_estimate=cost_of(50),
        name="attend",
    )(projected)


def carry(cross_ref, far_ref, first, sent, landed, across):
    return push_sp(
        cross_ref.at[:, pl.ds(first, far_ref.shape[1]), :], far_ref, sent, landed, across
    )


def attend_back_kernel(heads, carried, *refs):
    if carried:
        x_ref, scaled_ref, delta_ref, kv_ref, cross_ref, out_ref, far_ref, *scratch = refs
        *scratch, cross_sent, cross_landed = scratch
        across = (lax.axis_index("sp") + 2) % 4
        over = carry(cross_ref, far_ref, 0, cross_sent, cross_landed, across)
        after = over.start
    else:
        x_ref, scaled_ref, delta_ref, kv_ref, out_ref, *scratch = refs
        across, after = None, lambda: None
    attend_back_steps(
        heads, across, after, x_ref, scaled_ref, delta_ref, kv_ref, out_ref, *scratch
    )
    if carried:
        over.wait()


def attend_back_steps(
    heads,
    across,
    after_greeting,
    x_ref,
    scaled_ref,
    delta_ref,
    kv_ref,
    out_ref,
    kv,
    part,
    side,
    down,
    dq,
    dk,
    dv,
    load_done,
    side_sent,
    side_landed,
    down_sent,
    down_landed,
):
    at = lax.axis_index("blk")
    blocks = lax.axis_size("blk")
    rows = blocks // 2
    line, column = at // 2, at % 2
    partner = at + 1 - 2 * column
    size = x_ref.shape[0]

    def load(index):
        return pltpu.make_async_copy(kv_ref.at[index], kv.at[index], load_done.at[index])

    @pl.loop(0, blocks)
    def _(index):
        pl.when(index <= at)(lambda: load(index).start())

    greet(at, line, rows, across)
    after_greeting()

    def side_copy(target):
        return push(
            part.at[target, 1 - column],
            side.at[target],
            side_sent.at[target],
            side_landed.at[target],
            partner,
        )

    def down_copy(target):
        return push(
            part.at[target, column],
            down.at[target],
            down_sent.at[target],
            down_landed.at[target],
            at - 2,
        )

    dq[...] = jnp.zeros_like(dq)
    ahead = lax.broadcasted_iota(jnp.int32, (size, size), 0) - lax.broadcasted_iota(
        jnp.int32, (size, size), 1
    )

    def compute(target, half):
        index = 2 * target + half
        load(index).wait()
        span = (at - index) * size
        for head in range(heads):
            columns = slice(head * HEAD, (head + 1) * HEAD)
            query = x_ref[:, columns]
            scaled = scaled_ref[:, columns]
            key = kv[index, :, :HEAD]
            raw = lax.dot_general(
                key, query, (((1,), (1,)), ((), ())), preferred_element_type=jnp.float32
            )
            squashed = jnp.tanh(raw * (HEAD ** (-0.5) / CAP_VALUE))
            weights = jnp.exp(CAP_VALUE * squashed)
            weights = jnp.where(ahead <= span, weights, 0.0)
            inner = lax.dot_general(
                kv[index, :, HEAD:],
                scaled,
                (((1,), (1,)), ((), ())),
                preferred_element_type=jnp.float32,
            )
            grad_raw = (
                weights * (inner - delta_ref[head]) * (1.0 - squashed * squashed)
            ).astype(jnp.bfloat16)
            dv_now = jnp.dot(
                weights.astype(jnp.bfloat16), scaled, preferred_element_type=jnp.float32
            )
            dk_now = jnp.dot(grad_raw, query, preferred_element_type=jnp.float32)
            dq[:, columns] += lax.dot_general(
                grad_raw, key, (((0,), (0,)), ((), ())), preferred_element_type=jnp.float32
            )
            if head == 0:
                dv[...] = dv_now
                dk[...] = dk_now
            else:
                dv[...] += dv_now
                dk[...] += dk_now
        part[target, half, :, :HEAD] = (dk[...] * HEAD ** (-0.5)).astype(jnp.bfloat16)
        part[target, half, :, HEAD:] = dv[...].astype(jnp.bfloat16)

    def merge(target):
        last = target == line

        @pl.when(jnp.logical_or(target < line, column == 0))
        def _():
            side_copy(target).wait_recv()
            part[target, column] = (
                part[target, column].astype(jnp.float32) + side[target].astype(jnp.float32)
            ).astype(jnp.bfloat16)

        @pl.when(line < rows - 1)
        def _():
            down_copy(target).wait_recv()
            part[target, column] = (
                part[target, column].astype(jnp.float32) + down[target].astype(jnp.float32)
            ).astype(jnp.bfloat16)

        pl.when(target < line)(lambda: down_copy(target).start())

        @pl.when(last)
        def _():
            out_ref[:, heads * HEAD :] = part[target, column]

    @pl.loop(0, rows)
    def _(target):
        away = jnp.logical_or(target < line, both(target == line, column == 1))

        @pl.loop(0, 2)
        def _(way):
            @pl.when(jnp.logical_or(both(way == 0, away), both(way == 1, target <= line)))
            def _():
                compute(target, jnp.where(way == 0, 1 - column, column))
                pl.when(way == 0)(lambda: side_copy(target).start())

        pl.when(both(line == rows - 1, target > 0))(lambda: merge(target - 1))

    out_ref[:, : heads * HEAD] = (dq[...] * HEAD ** (-0.5)).astype(jnp.bfloat16)

    @pl.loop(0, rows)
    def _(target):
        pl.when(both(target <= line, jnp.logical_or(line < rows - 1, target == rows - 1)))(
            lambda: merge(target)
        )

    @pl.loop(0, rows)
    def _(target):
        pl.when(jnp.logical_or(target < line, both(target == line, column == 1)))(
            lambda: side_copy(target).wait_send()
        )
        pl.when(target < line)(lambda: down_copy(target).wait_send())


def half_of(cross):
    kinds, units, width = cross.shape
    return jax.ShapeDtypeStruct((kinds, units // 2, width), cross.dtype)


def attend_back(projected, scaled, delta, kv_all, cross=None):
    size = projected.shape[0]
    blocks = lax.axis_size("blk")
    rows = blocks // 2
    heads = scaled.shape[1] // HEAD
    whole = pl.BlockSpec(memory_space=pltpu.VMEM)
    far = pl.BlockSpec(memory_space=pl.ANY)
    carried = cross is not None
    far_shape, operands = [], [projected, scaled, delta, kv_all]
    if carried:
        far_shape = [half_of(cross)]
        operands.append(cross)
    return pl.pallas_call(
        functools.partial(attend_back_kernel, heads, carried),
        out_shape=[jax.ShapeDtypeStruct(projected.shape, jnp.bfloat16)] + far_shape,
        in_specs=[whole, whole, whole, far] + [far] * carried,
        out_specs=[whole] + [far] * carried,
        scratch_shapes=[
            pltpu.VMEM((blocks, size, 2 * HEAD), jnp.bfloat16),
            pltpu.VMEM((rows, 2, size, 2 * HEAD), jnp.bfloat16),
            pltpu.VMEM((rows, size, 2 * HEAD), jnp.bfloat16),
            pltpu.VMEM((rows, size, 2 * HEAD), jnp.bfloat16),
            pltpu.VMEM((size, heads * HEAD), jnp.float32),
            pltpu.VMEM((size, HEAD), jnp.float32),
            pltpu.VMEM((size, HEAD), jnp.float32),
            pltpu.SemaphoreType.DMA((blocks,)),
            pltpu.SemaphoreType.DMA((rows,)),
            pltpu.SemaphoreType.DMA((rows,)),
            pltpu.SemaphoreType.DMA((rows,)),
            pltpu.SemaphoreType.DMA((rows,)),
        ]
        + [pltpu.SemaphoreType.DMA, pltpu.SemaphoreType.DMA] * carried,
        compiler_params=pltpu.CompilerParams(
            collective_id=1, has_side_effects=True, vmem_limit_bytes=VMEM_BYTES
        ),
        cost_estimate=cost_of(50),
        name="attend_back",
    )(*operands)


def line_gather(
    own_ref,
    full,
    line_sent,
    line_landed,
    extra_sent,
    extra_landed,
    side_sent,
    side_landed,
    first_done,
    own_done,
    ready,
    work,
):
    at = lax.axis_index("blk")
    rows = lax.axis_size("blk") // 2
    line, column = at // 2, at % 2
    partner = at + 1 - 2 * column
    size = own_ref.shape[0]
    half = size // 2

    def span(source, start, count):
        return full.at[pl.ds(pl.multiple_of(2 * source * size + start, half), count), :]

    def line_copy(source, sign, first=False):
        target = span(source, column * size, size)
        return push(
            own_ref if first else target,
            target,
            line_sent.at[(sign + 1) // 2, source],
            line_landed.at[source],
            at + 2 * sign,
        )

    def extra_copy(source, sign):
        target = span(source, (1 - column) * size + half, half)
        return push(
            target,
            target,
            extra_sent.at[(sign + 1) // 2, source],
            extra_landed.at[source],
            at + 2 * sign,
        )

    def side_copy(source, member, count, first=False):
        target = span(source, member * size, count)
        return push(
            own_ref.at[:count] if first else target,
            target,
            side_sent.at[source],
            side_landed.at[source],
            partner,
        )

    def first_copy(member):
        return push(
            own_ref.at[half:],
            span(line, member * size + half, half),
            first_done.at[0],
            first_done.at[1],
            partner,
        )

    def inside(row):
        return jnp.logical_and(row >= 0, row < rows)

    def end(row):
        return jnp.logical_or(row == 0, row == rows - 1)

    def by_end(source, act):
        pl.when(end(source))(lambda: act(half))
        pl.when(jnp.logical_not(end(source)))(lambda: act(size))

    pl.when(end(line))(lambda: first_copy(column).start())
    pl.when(line < rows - 1)(lambda: line_copy(line, 1, True).start())
    pl.when(line > 0)(lambda: line_copy(line, -1, True).start())
    by_end(line, lambda count: side_copy(line, column, count, True).start())
    keep = pltpu.make_async_copy(own_ref, span(line, column * size, size), own_done)
    keep.start()

    @pl.when(end(line))
    def _():
        first_copy(1 - column).wait_recv()
        pl.when(line < rows - 1)(lambda: extra_copy(line, 1).start())
        pl.when(line > 0)(lambda: extra_copy(line, -1).start())

    keep.wait()
    ready()

    @pl.loop(0, rows + 1)
    def _(step):
        @pl.loop(0, 2)
        def _(way):
            sign = 2 * way - 1
            source = line - sign * step

            @pl.when(both(step > 0, inside(source)))
            def _():
                line_copy(source, sign).wait_recv()
                pl.when(inside(line + sign))(lambda: line_copy(source, sign).start())
                by_end(source, lambda count: side_copy(source, column, count).start())

        @pl.loop(0, 2)
        def _(way):
            sign = 2 * way - 1
            source = line - sign * step

            @pl.when(both(step > 0, inside(source), end(source)))
            def _():
                extra_copy(source, sign).wait_recv()
                pl.when(inside(line + sign))(lambda: extra_copy(source, sign).start())

        @pl.loop(0, 2)
        def _(way):
            source = line - (2 * way - 1) * (step - 1)

            @pl.when(both(step > way, inside(source)))
            def _():
                by_end(source, lambda count: side_copy(source, 1 - column, count).wait_recv())
                work(source)

    @pl.loop(0, rows)
    def _(source):
        @pl.when(both(source <= line, line < rows - 1))
        def _():
            line_copy(source, 1).wait_send()
            pl.when(end(source))(lambda: extra_copy(source, 1).wait_send())

        @pl.when(both(source >= line, line > 0))
        def _():
            line_copy(source, -1).wait_send()
            pl.when(end(source))(lambda: extra_copy(source, -1).wait_send())

        by_end(source, lambda count: side_copy(source, column, count).wait_send())

    pl.when(end(line))(lambda: first_copy(column).wait_send())


def line_scatter(
    part,
    side,
    lane,
    tail,
    out_ref,
    side_sent,
    side_landed,
    lane_sent,
    lane_landed,
    tail_done,
    work,
    fill,
):
    at = lax.axis_index("blk")
    rows = lax.axis_size("blk") // 2
    line, column = at // 2, at % 2
    partner = at + 1 - 2 * column
    size = out_ref.shape[0]
    half = size // 2

    def span(target, start, count):
        return pl.ds(pl.multiple_of(2 * target * size + start, half), count)

    def piece(target, which):
        start = ((0, 0), (0, half), (size, half))[which]
        return span(target, column * (size - 2 * start[0]) + start[0] + start[1], half)

    def side_copy(target, count):
        return push(
            part.at[span(target, (1 - column) * size, count), :],
            side.at[target, :count],
            side_sent.at[target],
            side_landed.at[target],
            partner,
        )

    def lane_copy(target, which, sign):
        slot = target if sign == 1 else jnp.where(target == line - 1, rows, target)
        return push(
            part.at[piece(target, which), :],
            lane.at[slot, which],
            lane_sent.at[target, which],
            lane_landed.at[slot, which],
            at + 2 * sign,
        )

    def lane_wait(slot, which):
        push(
            lane.at[slot, which],
            lane.at[slot, which],
            lane_sent.at[0, which],
            lane_landed.at[slot, which],
            partner,
        ).wait_recv()

    def tail_copy():
        return push(
            part.at[piece(line, 2), :], tail, tail_done.at[0], tail_done.at[1], partner
        )

    def inside(row):
        return jnp.logical_and(row >= 0, row < rows)

    def end(row):
        return jnp.logical_or(row == 0, row == rows - 1)

    def by_end(target, act):
        pl.when(end(target))(lambda: act(half))
        pl.when(jnp.logical_not(end(target)))(lambda: act(size))

    def add(where, more):
        part[where, :] = (
            part[where, :].astype(jnp.float32) + more.astype(jnp.float32)
        ).astype(jnp.bfloat16)

    def hop(target, which):
        for sign in (1, -1):

            @pl.when(target > line if sign == 1 else target < line)
            def _():
                @pl.when(inside(line - sign))
                def _():
                    lane_wait(target, which)
                    add(piece(target, which), lane[target, which])

                lane_copy(target, which, sign).start()

    def early(target):
        return both(end(target), end(line), target != line)

    @pl.loop(0, rows)
    def _(step):
        @pl.loop(0, 2)
        def _(way):
            target = line + (2 * way - 1) * (rows - 1 - step)

            @pl.when(both(step < rows - way, inside(target)))
            def _():
                work(target)
                by_end(target, lambda count: side_copy(target, count).start())

                @pl.when(early(target))
                def _():
                    hop(target, 1)
                    hop(target, 2)

    def gather_lanes(which):
        for slot, present in ((line, line > 0), (rows, line < rows - 1)):

            @pl.when(present)
            def _():
                lane_wait(slot, which)
                add(piece(line, which), lane[slot, which])

    def merge(target):
        @pl.when(both(end(target), target != line, jnp.logical_not(early(target))))
        def _():
            hop(target, 1)
            hop(target, 2)

        @pl.when(both(end(line), target == line))
        def _():
            gather_lanes(2)
            tail_copy().start()

        def add_side(count):
            side_copy(target, count).wait_recv()
            add(span(target, column * size, count), side[target, :count])

        by_end(target, add_side)

        @pl.when(target != line)
        def _():
            hop(target, 0)
            pl.when(jnp.logical_not(end(target)))(lambda: hop(target, 1))

    @pl.loop(0, rows)
    def _(step):
        fill(step)

        @pl.loop(0, 2)
        def _(way):
            target = line + (2 * way - 1) * (rows - 1 - step)
            pl.when(both(step < rows - way, inside(target)))(lambda: merge(target))

    gather_lanes(1)
    gather_lanes(0)
    out_ref[...] = part[span(line, column * size, size), :].astype(jnp.float32)

    @pl.when(end(line))
    def _():
        tail_copy().wait_recv()
        out_ref[half:, :] += tail[...].astype(jnp.float32)
        tail_copy().wait_send()

    @pl.loop(0, rows)
    def _(target):
        by_end(target, lambda count: side_copy(target, count).wait_send())

        def sent(sign):
            for which in (0, 1):
                lane_copy(target, which, sign).wait_send()
            pl.when(end(target))(lambda: lane_copy(target, 2, sign).wait_send())

        pl.when(target > line)(lambda: sent(1))
        pl.when(target < line)(lambda: sent(-1))


def line_sems(rows):
    dma = pltpu.SemaphoreType.DMA
    ways, each = dma((2, rows)), dma((rows,))
    return [ways, each, ways, each, each, each, dma((2,)), dma]


def lane_sems(rows):
    dma = pltpu.SemaphoreType.DMA
    return [dma((rows,)), dma((rows,)), dma((rows, 3)), dma((rows + 1, 3)), dma((2,))]


def lane_buffers(rows, size, width):
    return [
        pltpu.VMEM((2 * rows * size, width), jnp.bfloat16),
        pltpu.VMEM((rows, size, width), jnp.bfloat16),
        pltpu.VMEM((rows + 1, 3, size // 2, width), jnp.bfloat16),
        pltpu.VMEM((size // 2, width), jnp.bfloat16),
    ]


def ffn_kernel(
    act_ref,
    w_ref,
    out_ref,
    acts_ref,
    factors_ref,
    w,
    acts,
    hidden,
    factors,
    part,
    side,
    lane,
    tail,
    w_done,
    save_done,
    factors_done,
    *sems,
):
    at = lax.axis_index("blk")
    rows = lax.axis_size("blk") // 2
    pair = 2 * act_ref.shape[0]

    def load(which):
        return pltpu.make_async_copy(w_ref.at[which], w.at[which], w_done.at[which])

    def pair_rows(source):
        return pl.ds(pl.multiple_of(source * pair, pair), pair)

    def save(source):
        return pltpu.make_async_copy(
            acts.at[pair_rows(source), :], acts_ref.at[pair_rows(source), :], save_done.at[source]
        )

    for which in range(3):
        load(which).start()
    greet(at, at // 2, rows)

    def ready():
        for which in range(3):
            load(which).wait()

    def expand(source):
        save(source).start()
        rows_now = acts[pair_rows(source), :]
        gate = contract_last(w[0], rows_now)
        up = contract_last(w[1], rows_now)
        hidden[source] = (gelu_value(gate) * up).astype(jnp.bfloat16)

    def reduce(target):
        part[pair_rows(target), :] = lax.dot_general(
            hidden[target], w[2], (((0,), (0,)), ((), ())), preferred_element_type=jnp.float32
        ).astype(jnp.bfloat16)

    line_gather(act_ref, acts, *sems[:8], ready, expand)
    def factors_copy(source):
        return pltpu.make_async_copy(
            factors.at[source % 2],
            factors_ref.at[:, :, pair_rows(source)],
            factors_done.at[source % 2],
        )

    def fill(source):
        rows_now = acts[pair_rows(source), :]
        gate = contract_last(w[0], rows_now)
        up = contract_last(w[1], rows_now)
        bent = jnp.tanh(GELU_SCALE * (gate + GELU_CUBIC * gate * gate * gate))
        slope = 0.5 * (1.0 + bent) + 0.5 * gate * (1.0 - bent * bent) * GELU_SCALE * (
            1.0 + 3.0 * GELU_CUBIC * gate * gate
        )
        pl.when(source > 1)(lambda: factors_copy(source - 2).wait())
        slot = source % 2
        factors[slot, 0] = (up * slope).astype(jnp.bfloat16)
        factors[slot, 1] = (0.5 * gate * (1.0 + bent)).astype(jnp.bfloat16)
        factors[slot, 2] = hidden[source]
        factors_copy(source).start()

    line_scatter(part, side, lane, tail, out_ref, *sems[8:], reduce, fill)
    factors_copy(rows - 2).wait()
    factors_copy(rows - 1).wait()
    pl.loop(0, rows)(lambda source: save(source).wait())


def ffn_forward(act_ffn, w_parts):
    size, width = act_ffn.shape
    units = w_parts.shape[1]
    blocks = lax.axis_size("blk")
    rows = blocks // 2
    whole = pl.BlockSpec(memory_space=pltpu.VMEM)
    far = pl.BlockSpec(memory_space=pl.ANY)
    return pl.pallas_call(
        ffn_kernel,
        out_shape=(
            jax.ShapeDtypeStruct((size, width), jnp.float32),
            jax.ShapeDtypeStruct((blocks * size, width), jnp.bfloat16),
            jax.ShapeDtypeStruct((3, units, blocks * size), jnp.bfloat16),
        ),
        in_specs=[whole, far],
        out_specs=(whole, far, far),
        scratch_shapes=[
            pltpu.VMEM(w_parts.shape, jnp.bfloat16),
            pltpu.VMEM((blocks * size, width), jnp.bfloat16),
            pltpu.VMEM((rows, units, 2 * size), jnp.bfloat16),
            pltpu.VMEM((2, 3, units, 2 * size), jnp.bfloat16),
            *lane_buffers(rows, size, width),
            pltpu.SemaphoreType.DMA((3,)),
            pltpu.SemaphoreType.DMA((rows,)),
            pltpu.SemaphoreType.DMA((2,)),
            *line_sems(rows),
            *lane_sems(rows),
        ],
        compiler_params=pltpu.CompilerParams(
            collective_id=2, has_side_effects=True, vmem_limit_bytes=VMEM_BYTES
        ),
        cost_estimate=cost_of(115),
        name="ffn_forward",
    )(act_ffn, w_parts)


FILL_COLUMNS = 256
FILL_FIRST = 0


def ffn_back_kernel(
    owners,
    grad_ref,
    acts_ref,
    factors_ref,
    w_ref,
    out_ref,
    keep_ref,
    cross_ref,
    w,
    rights,
    lefts,
    part,
    side,
    lane,
    tail,
    stage,
    mate_part,
    summed,
    w_done,
    acts_done,
    factors_done,
    mate_sent,
    mate_landed,
    summed_done,
    *sems,
):
    at = lax.axis_index("blk")
    me = lax.axis_index("sp")
    chip, core = me // 2, me % 2
    mate = me + 1 - 2 * core
    rows = lax.axis_size("blk") // 2
    size, width = grad_ref.shape
    pair = 2 * size
    units = w.shape[1]
    acts, grads = rights.at[0], rights.at[1]

    def load(which):
        return pltpu.make_async_copy(w_ref.at[which], w.at[which], w_done.at[which])

    def pair_rows(source):
        return pl.ds(pl.multiple_of(source * pair, pair), pair)

    acts_copy = pltpu.make_async_copy(acts_ref, acts, acts_done)
    factors_copy = pltpu.make_async_copy(factors_ref, lefts, factors_done)
    load(2).start()
    factors_copy.start()
    load(0).start()
    load(1).start()
    acts_copy.start()
    greet(at, at // 2, rows, mate)

    def ready():
        load(2).wait()
        factors_copy.wait()

    def expand(source):
        columns = pair_rows(source)
        grad_hidden = contract_last(w[2], grads[columns, :])
        for which in range(2):
            lefts[which, :, columns] = (
                lefts[which, :, columns].astype(jnp.float32) * grad_hidden
            ).astype(jnp.bfloat16)

    def reduce(target):
        columns = pair_rows(target)
        dims = (((0,), (0,)), ((), ()))
        total = lax.dot_general(
            lefts[0, :, columns], w[0], dims, preferred_element_type=jnp.float32
        ) + lax.dot_general(lefts[1, :, columns], w[1], dims, preferred_element_type=jnp.float32)
        part[pair_rows(target), :] = total.astype(jnp.bfloat16)

    pieces = width // FILL_COLUMNS
    total_pieces = 3 * pieces

    def piece_columns(item):
        return pl.ds(pl.multiple_of((item % pieces) * FILL_COLUMNS, FILL_COLUMNS), FILL_COLUMNS)

    def mate_copy(item):
        return push_sp(
            stage.at[item % 3, :, 1 - core],
            mate_part.at[item],
            mate_sent.at[item % 3],
            mate_landed.at[item],
            mate,
        )

    def put(item, side_chip, target):
        return pltpu.make_async_copy(
            summed.at[item % 2, side_chip],
            target.at[item // pieces, :, piece_columns(item)],
            summed_done.at[item % 2, side_chip],
        )

    def put_wait(item):
        put(item, chip, keep_ref).wait()
        put(item, 1 - chip, cross_ref).wait()

    def sum_one(item):
        pl.when(item > 1)(lambda: put_wait(item - 2))
        mate_copy(item).wait_recv()
        summed[item % 2] = (
            stage[item % 3, :, core].astype(jnp.float32) + mate_part[item].astype(jnp.float32)
        ).astype(jnp.bfloat16)
        put(item, chip, keep_ref).start()
        put(item, 1 - chip, cross_ref).start()

    def fill_one(item):
        which = item // pieces
        total = jnp.dot(
            lefts[which],
            rights[which // 2, :, piece_columns(item)],
            preferred_element_type=jnp.float32,
        )
        pl.when(item > 2)(lambda: mate_copy(item - 3).wait_send())
        stage[item % 3] = total.astype(jnp.bfloat16).reshape(
            2, 2, units // owners, FILL_COLUMNS
        )
        mate_copy(item).start()
        pl.when(item > 0)(lambda: sum_one(item - 1))

    each = pl.cdiv(total_pieces - FILL_FIRST, rows - 1)

    def fill(step):
        first = jnp.maximum(FILL_FIRST + (step - 1) * each, 0)
        last = jnp.minimum(FILL_FIRST + step * each, total_pieces)

        @pl.loop(0, each)
        def _(item):
            pl.when(first + item < last)(lambda: fill_one(first + item))

    line_gather(grad_ref, grads, *sems[:8], ready, expand)
    load(0).wait()
    load(1).wait()
    acts_copy.wait()
    line_scatter(part, side, lane, tail, out_ref, *sems[8:], reduce, fill)
    sum_one(total_pieces - 1)
    put_wait(total_pieces - 2)
    put_wait(total_pieces - 1)
    for item in range(total_pieces - 3, total_pieces):
        mate_copy(item).wait_send()


def ffn_back(grad_ffn, kept, w_parts, owners):
    size, width = grad_ffn.shape
    units = w_parts.shape[1]
    blocks = lax.axis_size("blk")
    rows = blocks // 2
    tokens = blocks * size
    items = 3 * width // FILL_COLUMNS
    whole = pl.BlockSpec(memory_space=pltpu.VMEM)
    far = pl.BlockSpec(memory_space=pl.ANY)
    return pl.pallas_call(
        functools.partial(ffn_back_kernel, owners),
        out_shape=(
            jax.ShapeDtypeStruct((size, width), jnp.float32),
            jax.ShapeDtypeStruct((3, units // owners, width), jnp.bfloat16),
            jax.ShapeDtypeStruct((3, units // owners, width), jnp.bfloat16),
        ),
        in_specs=[whole, far, far, far],
        out_specs=(whole, far, far),
        scratch_shapes=[
            pltpu.VMEM(w_parts.shape, jnp.bfloat16),
            pltpu.VMEM((2, tokens, width), jnp.bfloat16),
            pltpu.VMEM((3, units, tokens), jnp.bfloat16),
            *lane_buffers(rows, size, width),
            pltpu.VMEM((3, 2, 2, units // owners, FILL_COLUMNS), jnp.bfloat16),
            pltpu.VMEM((items, 2, units // owners, FILL_COLUMNS), jnp.bfloat16),
            pltpu.VMEM((2, 2, units // owners, FILL_COLUMNS), jnp.bfloat16),
            pltpu.SemaphoreType.DMA((3,)),
            pltpu.SemaphoreType.DMA,
            pltpu.SemaphoreType.DMA,
            pltpu.SemaphoreType.DMA((3,)),
            pltpu.SemaphoreType.DMA((items,)),
            pltpu.SemaphoreType.DMA((2, 2)),
            *line_sems(rows),
            *lane_sems(rows),
        ],
        compiler_params=pltpu.CompilerParams(
            collective_id=3, has_side_effects=True, vmem_limit_bytes=VMEM_BYTES
        ),
        cost_estimate=cost_of(115),
        name="ffn_back",
    )(grad_ffn, *kept, w_parts)


def ffn_hidden(acts, w_parts):
    gate = contract_last(acts, w_parts[0])
    up = contract_last(acts, w_parts[1])
    return (gate, up, (gelu_value(gate) * up).astype(jnp.bfloat16))


def scatter_tokens(partial):
    return lax.psum_scatter(
        partial.astype(jnp.bfloat16), "blk", scatter_dimension=0, tiled=True
    ).astype(jnp.float32)


def ffn_forward_wide(act_ffn, w_parts):
    acts = lax.all_gather(act_ffn, "blk", axis=0, tiled=True)
    hidden = ffn_hidden(acts, w_parts)[2]
    partial = jnp.dot(hidden, w_parts[2], preferred_element_type=jnp.float32)
    return (scatter_tokens(partial), acts)


def ffn_back_wide(grad_ffn, kept, w_parts, owners):
    (acts,) = kept
    grads = lax.all_gather(grad_ffn, "blk", axis=0, tiled=True)
    gate, up, hidden = ffn_hidden(acts, w_parts)
    grad_hidden = contract_last(grads, w_parts[2])
    grad_gate = (grad_hidden * up * gelu_slope(gate)).astype(jnp.bfloat16)
    grad_up = (grad_hidden * gelu_value(gate)).astype(jnp.bfloat16)
    partial = jnp.dot(grad_gate, w_parts[0], preferred_element_type=jnp.float32) + jnp.dot(
        grad_up, w_parts[1], preferred_element_type=jnp.float32
    )
    sums = jnp.stack(
        [
            jnp.einsum("tf,td->fd", left, right, preferred_element_type=jnp.float32)
            for left, right in ((grad_gate, acts), (grad_up, acts), (hidden, grads))
        ]
    ).astype(jnp.bfloat16)
    units = w_parts.shape[1]
    owned = sums.reshape(3, owners, units // owners, sums.shape[2])
    mine = lax.psum_scatter(
        jnp.transpose(owned, (1, 0, 2, 3)), "sp", scatter_dimension=0, tiled=True
    )
    return (scatter_tokens(partial), mine[0], None)


def cost_of(microseconds):
    return pl.CostEstimate(
        flops=int(microseconds * 1e9), bytes_accessed=int(microseconds * 3e6), transcendentals=0
    )


def push_sp(source, target, sent, landed, peer):
    return pltpu.make_async_remote_copy(
        src_ref=source,
        dst_ref=target,
        send_sem=sent,
        recv_sem=landed,
        device_id={"sp": peer},
        device_id_type=pl.DeviceIdType.MESH,
    )


def greet_sp(me, groups):
    barrier = pltpu.get_barrier_semaphore()
    for step in range(1, groups):
        pl.semaphore_signal(
            barrier,
            inc=1,
            device_id={"sp": (me + step) % groups},
            device_id_type=pl.DeviceIdType.MESH,
        )
    pl.semaphore_wait(barrier, groups - 1)


def gather_project_kernel(x_ref, w_ref, full_ref, out_ref, w, w_done, own_done, sent, landed):
    me = lax.axis_index("sp")
    size = x_ref.shape[0]
    units = w.shape[0]
    mate = me + 1 - 2 * (me % 2)
    across = (me + 2) % 4

    def spot(member):
        return full_ref.at[pl.ds(pl.multiple_of(member * size, size), size), :]

    load = pltpu.make_async_copy(
        w_ref.at[pl.ds(pl.multiple_of(me * units, units), units), :], w, w_done
    )
    load.start()
    greet_sp(me, 4)
    over = push_sp(x_ref, spot(me), sent.at[0], landed.at[0], across)
    over.start()
    beside = push_sp(x_ref, spot(me), sent.at[1], landed.at[1], mate)
    beside.start()
    keep = pltpu.make_async_copy(x_ref, spot(me), own_done)
    keep.start()
    keep.wait()
    load.wait()

    def project(chip):
        rows = pl.ds(pl.multiple_of(chip * 2 * size, 2 * size), 2 * size)
        out_ref[rows, :] = contract_last(full_ref[rows, :], w[...]).astype(jnp.bfloat16)

    beside.wait_recv()
    project(me // 2)
    over.wait_recv()
    onward = push_sp(spot(across), spot(across), sent.at[2], landed.at[2], mate)
    onward.start()
    onward.wait_recv()
    project(across // 2)
    over.wait_send()
    beside.wait_send()
    onward.wait_send()


def gather_project(rows, weights, identity):
    size, width = rows.shape
    units = weights.shape[0] // 4
    whole = pl.BlockSpec(memory_space=pltpu.VMEM)
    return pl.pallas_call(
        gather_project_kernel,
        out_shape=(
            jax.ShapeDtypeStruct((4 * size, width), jnp.bfloat16),
            jax.ShapeDtypeStruct((4 * size, units), jnp.bfloat16),
        ),
        in_specs=[whole, pl.BlockSpec(memory_space=pl.ANY)],
        out_specs=(whole, whole),
        scratch_shapes=[
            pltpu.VMEM((units, width), jnp.bfloat16),
            pltpu.SemaphoreType.DMA,
            pltpu.SemaphoreType.DMA,
            pltpu.SemaphoreType.DMA((3,)),
            pltpu.SemaphoreType.DMA((3,)),
        ],
        compiler_params=pltpu.CompilerParams(
            collective_id=identity, has_side_effects=True, vmem_limit_bytes=VMEM_BYTES
        ),
        cost_estimate=cost_of(18),
        name="gather_project",
    )(rows, weights)


def exchange_project_kernel(x_ref, w_ref, out_ref, w, got, w_done, own_done, sent, landed):
    me = lax.axis_index("sp")
    size = out_ref.shape[0]
    units = x_ref.shape[1]

    def rows_of(member):
        return x_ref.at[pl.ds(pl.multiple_of(member * size, size), size), :]

    def load(member):
        rows = pl.ds(pl.multiple_of(member * units, units), units)
        return pltpu.make_async_copy(w_ref.at[rows, :], w.at[rows, :], w_done.at[member])

    def send(step):
        peer = (me + step) % 4
        return push_sp(rows_of(peer), got.at[4 - step], sent.at[step], landed.at[4 - step], peer)

    greet_sp(me, 4)
    for step in (2, 1, 3):
        send(step).start()
    keep = pltpu.make_async_copy(rows_of(me), got.at[0], own_done)
    keep.start()
    for step in range(4):
        load((me + step) % 4).start()
    keep.wait()
    for step in (0, 1, 3, 2):
        member = (me + step) % 4
        load(member).wait()
        if step > 0:
            send(4 - step).wait_recv()
        rows = pl.ds(pl.multiple_of(member * units, units), units)
        term = jnp.dot(got[step], w[rows, :], preferred_element_type=jnp.float32)
        if step == 0:
            out_ref[...] = term
        else:
            out_ref[...] += term
    for step in (1, 2, 3):
        send(step).wait_send()


def exchange_project(columns, weights, identity):
    size = columns.shape[0] // 4
    whole = pl.BlockSpec(memory_space=pltpu.VMEM)
    return pl.pallas_call(
        exchange_project_kernel,
        out_shape=jax.ShapeDtypeStruct((size, weights.shape[1]), jnp.float32),
        in_specs=[whole, pl.BlockSpec(memory_space=pl.ANY)],
        out_specs=whole,
        scratch_shapes=[
            pltpu.VMEM(weights.shape, jnp.bfloat16),
            pltpu.VMEM((4, size, columns.shape[1]), jnp.bfloat16),
            pltpu.SemaphoreType.DMA((4,)),
            pltpu.SemaphoreType.DMA,
            pltpu.SemaphoreType.DMA((4,)),
            pltpu.SemaphoreType.DMA((4,)),
        ],
        compiler_params=pltpu.CompilerParams(
            collective_id=identity, has_side_effects=True, vmem_limit_bytes=VMEM_BYTES
        ),
        cost_estimate=cost_of(16),
        name="exchange_project",
    )(columns, weights)


def finish_kernel(
    cols_ref,
    act_ref,
    att_ref,
    grad_ref,
    w_ref,
    tokens_ref,
    middle_ref,
    gain_ref,
    rows_ref,
    cross_ref,
    qkv_ref,
    out_ref,
    tokens_grad_ref,
    gains_ref,
    far_ref,
    w,
    got,
    grad_in,
    total,
    part,
    side,
    lane,
    tail,
    mine,
    from_sp,
    from_side,
    from_line,
    w_done,
    own_done,
    swap_sent,
    swap_landed,
    sp_sent,
    sp_landed,
    gain_side,
    line_sent,
    line_landed,
    cross_sent,
    cross_landed,
    *sems,
):
    at = lax.axis_index("blk")
    me = lax.axis_index("sp")
    rows = lax.axis_size("blk") // 2
    line, column = at // 2, at % 2
    partner = at + 1 - 2 * column
    block = total.shape[0]
    size = tokens_ref.shape[0]
    units = cols_ref.shape[1]
    extra = block - size

    barrier = pltpu.get_barrier_semaphore()
    for step in range(1, 4):
        pl.semaphore_signal(
            barrier, inc=1, device_id={"sp": (me + step) % 4}, device_id_type=pl.DeviceIdType.MESH
        )

    def line_peer(step):
        return 2 * ((line + step) % rows) + column

    for peer in [partner] + [line_peer(step) for step in range(1, rows)]:
        pl.semaphore_signal(
            barrier, inc=1, device_id={"blk": peer}, device_id_type=pl.DeviceIdType.MESH
        )

    def load(member):
        span = pl.ds(pl.multiple_of(member * units, units), units)
        return pltpu.make_async_copy(w_ref.at[span, :], w.at[span, :], w_done.at[member])

    def rows_of(member):
        return cols_ref.at[pl.ds(pl.multiple_of(member * size, size), size), :]

    def swap(step):
        peer = (me + step) % 4
        return push_sp(
            rows_of(peer), got.at[4 - step], swap_sent.at[step], swap_landed.at[4 - step], peer
        )

    for step in range(4):
        load((me + step) % 4).start()
    keep = pltpu.make_async_copy(rows_of(me), got.at[0], own_done)
    keep.start()
    pl.semaphore_wait(barrier, 3 + rows)
    for step in (2, 1, 3):
        swap(step).start()
    over = carry(
        cross_ref, far_ref, far_ref.shape[1], cross_sent, cross_landed, (me + 2) % 4
    )
    over.start()
    keep.wait()

    def sp_gains(step):
        return push_sp(
            mine, from_sp.at[4 - step], sp_sent.at[step], sp_landed.at[4 - step], (me + step) % 4
        )

    def side_gains():
        return push(from_sp.at[0], from_side, gain_side.at[0], gain_side.at[1], partner)

    def line_gains(step):
        return push(
            from_line.at[0],
            from_line.at[rows - step],
            line_sent.at[step],
            line_landed.at[rows - step],
            line_peer(step),
        )

    def reduce(target):
        dims = (((0,), (0,)), ((), ()))
        wide_columns = pl.ds(pl.multiple_of(target * 2 * size, 2 * size), 2 * size)
        term = lax.dot_general(
            cols_ref[:, wide_columns], act_ref[...], dims, preferred_element_type=jnp.float32
        ).astype(jnp.bfloat16)
        columns = pl.ds(pl.multiple_of(target * 2 * extra, 2 * extra), 2 * extra)
        more = lax.dot_general(
            att_ref[:, columns], grad_ref[...], dims, preferred_element_type=jnp.float32
        ).astype(jnp.bfloat16)
        for half in range(2):
            start = pl.multiple_of((2 * target + half) * block, block)
            part[pl.ds(start, size), :] = term[half * size : (half + 1) * size]
            start = pl.multiple_of((2 * target + half) * block + size, extra)
            part[pl.ds(start, extra), :] = more[half * extra : (half + 1) * extra]

    def inputs_back():
        for step in (0, 1, 3, 2):
            member = (me + step) % 4
            load(member).wait()
            if step > 0:
                swap(4 - step).wait_recv()
            span = pl.ds(pl.multiple_of(member * units, units), units)
            term = jnp.dot(got[step], w[span, :], preferred_element_type=jnp.float32)
            if step == 0:
                grad_in[...] = term
            else:
                grad_in[...] += term
        normed, inverse = norm_parts(tokens_ref[...].astype(jnp.float32))
        grad_v, gain_row = norm_back(grad_in[...], normed, inverse, gain_ref[...])
        tokens_grad_ref[...] = (middle_ref[...] + grad_v).astype(jnp.bfloat16)
        mine[...] = rows_ref[...]
        mine[0:1, :] = gain_row[None, :]
        for step in range(1, 4):
            sp_gains(step).start()

    def fill(step):
        pl.when(step == 2)(inputs_back)

        @pl.when(step == 3)
        def _():
            gains = mine[...]
            for other in range(1, 4):
                sp_gains(4 - other).wait_recv()
                gains = gains + from_sp[other]
            from_sp[0] = gains
            side_gains().start()

        @pl.when(step == 3)
        def _():
            side_gains().wait_recv()
            from_line[0] = from_sp[0] + from_side[...]
            for other in range(1, rows):
                line_gains(other).start()

    line_scatter(part, side, lane, tail, total, *sems, reduce, fill)
    qkv_ref[...] = total[:size]
    out_ref[...] = total[size:]
    gains = from_line[0]
    for other in range(1, rows):
        line_gains(rows - other).wait_recv()
        gains = gains + from_line[other]
    gains_ref[...] = gains
    for step in (1, 2, 3):
        swap(step).wait_send()
        sp_gains(step).wait_send()
    over.wait()
    side_gains().wait_send()
    for step in range(1, rows):
        line_gains(step).wait_send()


def finish(
    cols, act_block, attended, grad_block, w_qkv, tokens, grad_middle, gain, gain_rows, cross
):
    blocks = lax.axis_size("blk")
    rows = blocks // 2
    size, width = tokens.shape
    block = (cols.shape[1] + attended.shape[1]) // blocks
    whole = pl.BlockSpec(memory_space=pltpu.VMEM)
    any_space = pl.BlockSpec(memory_space=pl.ANY)
    dma = pltpu.SemaphoreType.DMA
    small = gain_rows.shape
    return pl.pallas_call(
        finish_kernel,
        out_shape=(
            jax.ShapeDtypeStruct((cols.shape[1] // blocks, width), jnp.float32),
            jax.ShapeDtypeStruct((attended.shape[1] // blocks, width), jnp.float32),
            jax.ShapeDtypeStruct((size, width), jnp.bfloat16),
            jax.ShapeDtypeStruct(small, jnp.float32),
            half_of(cross),
        ),
        in_specs=[whole] * 4 + [any_space] + [whole] * 4 + [any_space],
        out_specs=(whole, whole, whole, whole, any_space),
        scratch_shapes=[
            pltpu.VMEM(w_qkv.shape, jnp.bfloat16),
            pltpu.VMEM((4, size, cols.shape[1]), jnp.bfloat16),
            pltpu.VMEM((size, width), jnp.float32),
            pltpu.VMEM((block, width), jnp.float32),
            *lane_buffers(rows, block, width),
            pltpu.VMEM(small, jnp.float32),
            pltpu.VMEM((4, *small), jnp.float32),
            pltpu.VMEM(small, jnp.float32),
            pltpu.VMEM((rows, *small), jnp.float32),
            dma((4,)),
            dma,
            dma((4,)),
            dma((4,)),
            dma((4,)),
            dma((4,)),
            dma((2,)),
            dma((rows,)),
            dma((rows,)),
            dma,
            dma,
            *lane_sems(rows),
        ],
        compiler_params=pltpu.CompilerParams(
            collective_id=8, has_side_effects=True, vmem_limit_bytes=VMEM_BYTES
        ),
        cost_estimate=cost_of(85),
        name="finish",
    )(cols, act_block, attended, grad_block, w_qkv, tokens, grad_middle, gain, gain_rows, cross)


def weight_sums_wide(left, right):
    term = jnp.einsum("tc,td->cd", left, right, preferred_element_type=jnp.float32)
    return scatter_tokens(term)


def finish_wide(
    cols, act_block, attended, grad_block, w_qkv, tokens, grad_middle, gain, gain_rows, cross
):
    grad_act_in = exchange_project(cols, w_qkv, 7)
    normed, inverse = norm_parts(tokens.astype(jnp.float32))
    grad_v, gain_row = norm_back(grad_act_in, normed, inverse, gain)
    gains_all = lax.psum(jnp.concatenate([gain_row[None], gain_rows[1:]]), ("blk", "sp"))
    return (
        weight_sums_wide(cols, act_block),
        weight_sums_wide(attended, grad_block),
        (grad_middle + grad_v).astype(jnp.bfloat16),
        gains_all,
        None,
    )


def body(tokens, w_qkv, w_out, gains, w_ffn, cotangent):
    groups = lax.axis_size("sp")
    heads_here = HEADS // groups
    source = tokens.astype(jnp.float32)
    normed_in, inverse_in = norm_parts(source)
    act_in = (normed_in * gains[0]).astype(jnp.bfloat16)
    act_block, projected = gather_project(act_in, w_qkv, 4)
    block_rows = projected.shape[0]
    attended_cols, attended, totals, kv_all = attend(projected, heads_here)
    attn = exchange_project(attended_cols, w_out, 5)
    normed_attn, inverse_attn = norm_parts(attn)
    middle = source + normed_attn * gains[1]
    normed_mid, inverse_mid = norm_parts(middle)
    act_ffn = (normed_mid * gains[2]).astype(jnp.bfloat16)
    wide = lax.axis_size("blk") > 8
    w_parts = jnp.transpose(w_ffn, (1, 0, 2))
    ffn_out, *kept = (ffn_forward_wide if wide else ffn_forward)(act_ffn, w_parts)
    normed_ffn, inverse_ffn = norm_parts(ffn_out)
    result = middle + normed_ffn * gains[3]
    grad_out = cotangent.astype(jnp.float32)
    grad_ffn_f, gain_grad3 = norm_back(grad_out, normed_ffn, inverse_ffn, gains[3])
    grad_ffn = grad_ffn_f.astype(jnp.bfloat16)
    grad_act_ffn, ffn_part, cross = (ffn_back_wide if wide else ffn_back)(
        grad_ffn, kept, w_parts, groups
    )
    grad_norm_mid, gain_grad2 = norm_back(grad_act_ffn, normed_mid, inverse_mid, gains[2])
    grad_middle = grad_out + grad_norm_mid
    grad_attn_f, gain_grad1 = norm_back(grad_middle, normed_attn, inverse_attn, gains[1])
    grad_attn = grad_attn_f.astype(jnp.bfloat16)
    grad_block, grad_attended = gather_project(grad_attn, w_out, 6)
    grad_heads = grad_attended.astype(jnp.float32).reshape(block_rows, heads_here, HEAD)
    totals_rows = jnp.transpose(totals.reshape(heads_here, block_rows))
    scaled = (grad_heads / totals_rows[..., None]).astype(jnp.bfloat16)
    row_delta = (
        jnp.sum(grad_heads * attended.reshape(block_rows, heads_here, HEAD), axis=-1) / totals_rows
    )
    grad_cols, *far_first = attend_back(
        projected,
        scaled.reshape(block_rows, heads_here * HEAD),
        jnp.transpose(row_delta).reshape(heads_here, 1, block_rows),
        kv_all,
        cross,
    )
    gain_rows = jnp.stack(
        [jnp.zeros_like(gain_grad1), gain_grad1, gain_grad2, gain_grad3]
        + [jnp.zeros_like(gain_grad1)] * 4
    )
    qkv_grad, out_grad, tokens_grad, gains_all, far_last = (finish_wide if wide else finish)(
        grad_cols,
        act_block,
        attended_cols,
        grad_block,
        w_qkv,
        tokens,
        grad_middle,
        gains[0][None],
        gain_rows,
        cross,
    )
    ffn_sum = ffn_part.astype(jnp.float32)
    if not wide:
        ffn_sum = ffn_sum + jnp.concatenate([*far_first, far_last], axis=1).astype(jnp.float32)
    ffn_grad = jnp.transpose(ffn_sum, (1, 0, 2))
    share = gains_all.shape[1] // (groups * lax.axis_size("blk"))
    place = lax.axis_index("sp") * lax.axis_size("blk") + lax.axis_index("blk")
    gains_grad = lax.dynamic_slice_in_dim(gains_all[:4], place * share, share, 1)
    return (result.astype(jnp.bfloat16), tokens_grad, qkv_grad, out_grad, gains_grad, ffn_grad)


def solution(mesh):
    return jax.shard_map(
        body,
        mesh=mesh,
        in_specs=(
            P(("blk", "sp"), None),
            P(),
            P(),
            P(),
            P("blk", None, None),
            P(("blk", "sp"), None),
        ),
        out_specs=(
            P(("blk", "sp"), None),
            P(("blk", "sp"), None),
            P(("sp", "blk"), None),
            P(("sp", "blk"), None),
            P(None, ("sp", "blk")),
            P(("blk", "sp"), None, None),
        ),
        check_vma=False,
    )
```

```python
import functools

import jax
import jax.numpy as jnp
from jax import lax
from jax.experimental import pallas as pl
from jax.experimental.pallas import tpu as pltpu
from jax.sharding import PartitionSpec as P

HEADS = 8
KV_HEADS = 4
HEAD = 256


VMEM_BYTES = 62 * 1024 * 1024
NORM_EPSILON = 1e-06
CAP_VALUE = 50.0
GELU_SCALE = 0.7978845608028654
GELU_CUBIC = 0.044715


def norm_parts(values):
    inverse = lax.rsqrt(jnp.mean(values * values, axis=-1, keepdims=True) + NORM_EPSILON)
    return (values * inverse, inverse)


def norm_back(grad_y, normed, inverse, gain):
    grad_n = grad_y * gain
    grad_v = inverse * (grad_n - normed * jnp.mean(grad_n * normed, axis=-1, keepdims=True))
    return (grad_v, jnp.sum(grad_y * normed, axis=0))


def gelu_value(values):
    return (
        0.5
        * values
        * (1.0 + jnp.tanh(GELU_SCALE * (values + GELU_CUBIC * values * values * values)))
    )


def gelu_slope(values):
    bent = jnp.tanh(GELU_SCALE * (values + GELU_CUBIC * values * values * values))
    return 0.5 * (1.0 + bent) + 0.5 * values * (1.0 - bent * bent) * GELU_SCALE * (
        1.0 + 3.0 * GELU_CUBIC * values * values
    )


def contract_last(left, right):
    return lax.dot_general(
        left, right, (((1,), (1,)), ((), ())), preferred_element_type=jnp.float32
    )


def push(source, target, sent, landed, block):
    return pltpu.make_async_remote_copy(
        src_ref=source,
        dst_ref=target,
        send_sem=sent,
        recv_sem=landed,
        device_id={"blk": block},
        device_id_type=pl.DeviceIdType.MESH,
    )


def greet(at, line, rows, sp_peer=None):
    barrier = pltpu.get_barrier_semaphore()
    others = 1
    if sp_peer is not None:
        others = 2
        pl.semaphore_signal(
            barrier, inc=1, device_id={"sp": sp_peer}, device_id_type=pl.DeviceIdType.MESH
        )

    def tell(block):
        pl.semaphore_signal(
            barrier, inc=1, device_id={"blk": block}, device_id_type=pl.DeviceIdType.MESH
        )

    tell(at + 1 - 2 * (at % 2))
    pl.when(line > 0)(lambda: tell(at - 2))
    pl.when(line < rows - 1)(lambda: tell(at + 2))
    pl.semaphore_wait(barrier, others + jnp.minimum(line, 1) + jnp.minimum(rows - 1 - line, 1))


def both(*terms):
    result = terms[0]
    for term in terms[1:]:
        result = jnp.logical_and(result, term)
    return result


def attend_kernel(
    heads,
    x_ref,
    low_ref,
    att_ref,
    tot_ref,
    by_row_ref,
    kv_ref,
    kv,
    acc,
    part,
    up_sent,
    up_landed,
    side_sent,
    side_landed,
    own_done,
    save_done,
):
    at = lax.axis_index("blk")
    blocks = lax.axis_size("blk")
    rows = blocks // 2
    line, column = at // 2, at % 2
    partner = at + 1 - 2 * column
    size = x_ref.shape[0]
    first = heads * HEAD
    own = x_ref.at[:, pl.ds(first, 2 * HEAD)]
    greet(at, line, rows)

    def up_copy(index, source):
        return push(source, kv.at[index], up_sent.at[index // 2], up_landed.at[index // 2], at + 2)

    def side_copy(index, source):
        return push(
            source, kv.at[index], side_sent.at[index // 2], side_landed.at[index // 2], partner
        )

    def save(index):
        return pltpu.make_async_copy(kv.at[index], kv_ref.at[index], save_done.at[index])

    pl.when(line < rows - 1)(lambda: up_copy(at, own).start())
    pl.when(column == 0)(lambda: side_copy(at, own).start())
    keep = pltpu.make_async_copy(own, kv.at[at], own_done)
    keep.start()
    acc[...] = jnp.zeros_like(acc)
    part[...] = jnp.zeros_like(part)
    keep.wait()
    ahead = lax.broadcasted_iota(jnp.int32, (size, size), 1) - lax.broadcasted_iota(
        jnp.int32, (size, size), 0
    )

    def compute(index):
        save(index).start()
        span = (at - index) * size
        for head in range(heads):
            raw = lax.dot_general(
                x_ref[:, head * HEAD : (head + 1) * HEAD],
                kv[index, :, :HEAD],
                (((1,), (1,)), ((), ())),
                preferred_element_type=jnp.float32,
            )
            weights = jnp.exp(CAP_VALUE * jnp.tanh(raw * (HEAD ** (-0.5) / CAP_VALUE)))
            weights = jnp.where(ahead <= span, weights, 0.0)
            total = weights[:, :128]
            for piece in range(1, size // 128):
                total = total + weights[:, piece * 128 : (piece + 1) * 128]
            part[head] += total
            acc[:, head * HEAD : (head + 1) * HEAD] += jnp.dot(
                weights.astype(jnp.bfloat16),
                kv[index, :, HEAD:],
                preferred_element_type=jnp.float32,
            )

    @pl.loop(0, rows + 1)
    def _(step):
        source = line - step
        index = 2 * source + column

        @pl.when(both(step > 0, source >= 0))
        def _():
            up_copy(index, kv.at[index]).wait_recv()
            pl.when(line < rows - 1)(lambda: up_copy(index, kv.at[index]).start())
            side_copy(index, kv.at[index]).start()

        @pl.loop(0, 2)
        def _(way):
            found = source + way
            here = 2 * found + jnp.where(way == 0, column, 1 - column)
            due = jnp.logical_or(way == 0, both(step > 0, jnp.logical_or(step > 1, column == 1)))

            @pl.when(both(found >= 0, due))
            def _():
                pl.when(way == 1)(lambda: side_copy(here, kv.at[here]).wait_recv())
                compute(here)

    for head in range(heads):
        columns = slice(head * HEAD, (head + 1) * HEAD)
        total = jnp.sum(part[head], axis=1, keepdims=True)
        by_row_ref[head] = jnp.broadcast_to(total, by_row_ref.shape[1:])
        value = acc[:, columns] / total
        att_ref[:, columns] = value
        low_ref[:, columns] = value.astype(jnp.bfloat16)
        tot_ref[head] = jnp.sum(part[head].T, axis=0, keepdims=True)

    @pl.loop(0, rows)
    def _(source):
        index = 2 * source + column

        @pl.when(source <= line)
        def _():
            pl.when(line < rows - 1)(lambda: up_copy(index, kv.at[index]).wait_send())
            pl.when(jnp.logical_or(source < line, column == 0))(
                lambda: side_copy(index, kv.at[index]).wait_send()
            )

    @pl.loop(0, blocks)
    def _(index):
        pl.when(index <= at)(lambda: save(index).wait())


def attend(projected, heads):
    size = projected.shape[0]
    blocks = lax.axis_size("blk")
    whole = pl.BlockSpec(memory_space=pltpu.VMEM)
    return pl.pallas_call(
        functools.partial(attend_kernel, heads),
        out_shape=(
            jax.ShapeDtypeStruct((size, heads * HEAD), jnp.bfloat16),
            jax.ShapeDtypeStruct((size, heads * HEAD), jnp.float32),
            jax.ShapeDtypeStruct((heads, 1, size), jnp.float32),
            jax.ShapeDtypeStruct((heads, size, 128), jnp.float32),
            jax.ShapeDtypeStruct((blocks, size, 2 * HEAD), jnp.bfloat16),
        ),
        in_specs=[whole],
        out_specs=(whole, whole, whole, whole, pl.BlockSpec(memory_space=pl.ANY)),
        scratch_shapes=[
            pltpu.VMEM((blocks, size, 2 * HEAD), jnp.bfloat16),
            pltpu.VMEM((size, heads * HEAD), jnp.float32),
            pltpu.VMEM((heads, size, 128), jnp.float32),
            pltpu.SemaphoreType.DMA((blocks // 2,)),
            pltpu.SemaphoreType.DMA((blocks // 2,)),
            pltpu.SemaphoreType.DMA((blocks // 2,)),
            pltpu.SemaphoreType.DMA((blocks // 2,)),
            pltpu.SemaphoreType.DMA,
            pltpu.SemaphoreType.DMA((blocks,)),
        ],
        compiler_params=pltpu.CompilerParams(
            collective_id=0, has_side_effects=True, vmem_limit_bytes=VMEM_BYTES
        ),
        cost_estimate=cost_of(50),
        name="attend",
    )(projected)


def carry(cross_ref, far_ref, first, sent, landed, across):
    return push_sp(
        cross_ref.at[:, pl.ds(first, far_ref.shape[1]), :], far_ref, sent, landed, across
    )


def attend_back_kernel(heads, carried, *refs):
    if carried:
        x_ref, scaled_ref, delta_ref, kv_ref, cross_ref, out_ref, far_ref, *scratch = refs
        *scratch, cross_sent, cross_landed = scratch
        across = (lax.axis_index("sp") + 2) % 4
        over = carry(cross_ref, far_ref, 0, cross_sent, cross_landed, across)
        after = over.start
    else:
        x_ref, scaled_ref, delta_ref, kv_ref, out_ref, *scratch = refs
        across, after = None, lambda: None
    attend_back_steps(
        heads, across, after, x_ref, scaled_ref, delta_ref, kv_ref, out_ref, *scratch
    )
    if carried:
        over.wait()


def attend_back_steps(
    heads,
    across,
    after_greeting,
    x_ref,
    scaled_ref,
    delta_ref,
    kv_ref,
    out_ref,
    kv,
    part,
    side,
    down,
    dq,
    dk,
    dv,
    load_done,
    side_sent,
    side_landed,
    down_sent,
    down_landed,
):
    at = lax.axis_index("blk")
    blocks = lax.axis_size("blk")
    rows = blocks // 2
    line, column = at // 2, at % 2
    partner = at + 1 - 2 * column
    size = x_ref.shape[0]

    def load(index):
        return pltpu.make_async_copy(kv_ref.at[index], kv.at[index], load_done.at[index])

    @pl.loop(0, blocks)
    def _(index):
        pl.when(index <= at)(lambda: load(index).start())

    greet(at, line, rows, across)
    after_greeting()

    def side_copy(target):
        return push(
            part.at[target, 1 - column],
            side.at[target],
            side_sent.at[target],
            side_landed.at[target],
            partner,
        )

    def down_copy(target):
        return push(
            part.at[target, column],
            down.at[target],
            down_sent.at[target],
            down_landed.at[target],
            at - 2,
        )

    dq[...] = jnp.zeros_like(dq)
    ahead = lax.broadcasted_iota(jnp.int32, (size, size), 0) - lax.broadcasted_iota(
        jnp.int32, (size, size), 1
    )

    def compute(target, half):
        index = 2 * target + half
        load(index).wait()
        span = (at - index) * size
        for head in range(heads):
            columns = slice(head * HEAD, (head + 1) * HEAD)
            query = x_ref[:, columns]
            scaled = scaled_ref[:, columns]
            key = kv[index, :, :HEAD]
            raw = lax.dot_general(
                key, query, (((1,), (1,)), ((), ())), preferred_element_type=jnp.float32
            )
            squashed = jnp.tanh(raw * (HEAD ** (-0.5) / CAP_VALUE))
            weights = jnp.exp(CAP_VALUE * squashed)
            weights = jnp.where(ahead <= span, weights, 0.0)
            inner = lax.dot_general(
                kv[index, :, HEAD:],
                scaled,
                (((1,), (1,)), ((), ())),
                preferred_element_type=jnp.float32,
            )
            grad_raw = (
                weights * (inner - delta_ref[head]) * (1.0 - squashed * squashed)
            ).astype(jnp.bfloat16)
            dv_now = jnp.dot(
                weights.astype(jnp.bfloat16), scaled, preferred_element_type=jnp.float32
            )
            dk_now = jnp.dot(grad_raw, query, preferred_element_type=jnp.float32)
            dq[:, columns] += lax.dot_general(
                grad_raw, key, (((0,), (0,)), ((), ())), preferred_element_type=jnp.float32
            )
            if head == 0:
                dv[...] = dv_now
                dk[...] = dk_now
            else:
                dv[...] += dv_now
                dk[...] += dk_now
        part[target, half, :, :HEAD] = (dk[...] * HEAD ** (-0.5)).astype(jnp.bfloat16)
        part[target, half, :, HEAD:] = dv[...].astype(jnp.bfloat16)

    def merge(target):
        last = target == line

        @pl.when(jnp.logical_or(target < line, column == 0))
        def _():
            side_copy(target).wait_recv()
            part[target, column] = (
                part[target, column].astype(jnp.float32) + side[target].astype(jnp.float32)
            ).astype(jnp.bfloat16)

        @pl.when(line < rows - 1)
        def _():
            down_copy(target).wait_recv()
            part[target, column] = (
                part[target, column].astype(jnp.float32) + down[target].astype(jnp.float32)
            ).astype(jnp.bfloat16)

        pl.when(target < line)(lambda: down_copy(target).start())

        @pl.when(last)
        def _():
            out_ref[:, heads * HEAD :] = part[target, column]

    @pl.loop(0, rows)
    def _(target):
        away = jnp.logical_or(target < line, both(target == line, column == 1))

        @pl.loop(0, 2)
        def _(way):
            @pl.when(jnp.logical_or(both(way == 0, away), both(way == 1, target <= line)))
            def _():
                compute(target, jnp.where(way == 0, 1 - column, column))
                pl.when(way == 0)(lambda: side_copy(target).start())

        pl.when(both(line == rows - 1, target > 0))(lambda: merge(target - 1))

    out_ref[:, : heads * HEAD] = (dq[...] * HEAD ** (-0.5)).astype(jnp.bfloat16)

    @pl.loop(0, rows)
    def _(target):
        pl.when(both(target <= line, jnp.logical_or(line < rows - 1, target == rows - 1)))(
            lambda: merge(target)
        )

    @pl.loop(0, rows)
    def _(target):
        pl.when(jnp.logical_or(target < line, both(target == line, column == 1)))(
            lambda: side_copy(target).wait_send()
        )
        pl.when(target < line)(lambda: down_copy(target).wait_send())


def half_of(cross):
    kinds, units, width = cross.shape
    return jax.ShapeDtypeStruct((kinds, units // 2, width), cross.dtype)


def attend_back(projected, scaled, delta, kv_all, cross=None):
    size = projected.shape[0]
    blocks = lax.axis_size("blk")
    rows = blocks // 2
    heads = scaled.shape[1] // HEAD
    whole = pl.BlockSpec(memory_space=pltpu.VMEM)
    far = pl.BlockSpec(memory_space=pl.ANY)
    carried = cross is not None
    far_shape, operands = [], [projected, scaled, delta, kv_all]
    if carried:
        far_shape = [half_of(cross)]
        operands.append(cross)
    return pl.pallas_call(
        functools.partial(attend_back_kernel, heads, carried),
        out_shape=[jax.ShapeDtypeStruct(projected.shape, jnp.bfloat16)] + far_shape,
        in_specs=[whole, whole, whole, far] + [far] * carried,
        out_specs=[whole] + [far] * carried,
        scratch_shapes=[
            pltpu.VMEM((blocks, size, 2 * HEAD), jnp.bfloat16),
            pltpu.VMEM((rows, 2, size, 2 * HEAD), jnp.bfloat16),
            pltpu.VMEM((rows, size, 2 * HEAD), jnp.bfloat16),
            pltpu.VMEM((rows, size, 2 * HEAD), jnp.bfloat16),
            pltpu.VMEM((size, heads * HEAD), jnp.float32),
            pltpu.VMEM((size, HEAD), jnp.float32),
            pltpu.VMEM((size, HEAD), jnp.float32),
            pltpu.SemaphoreType.DMA((blocks,)),
            pltpu.SemaphoreType.DMA((rows,)),
            pltpu.SemaphoreType.DMA((rows,)),
            pltpu.SemaphoreType.DMA((rows,)),
            pltpu.SemaphoreType.DMA((rows,)),
        ]
        + [pltpu.SemaphoreType.DMA, pltpu.SemaphoreType.DMA] * carried,
        compiler_params=pltpu.CompilerParams(
            collective_id=1, has_side_effects=True, vmem_limit_bytes=VMEM_BYTES
        ),
        cost_estimate=cost_of(50),
        name="attend_back",
    )(*operands)


def line_gather(
    own_ref,
    full,
    line_sent,
    line_landed,
    extra_sent,
    extra_landed,
    side_sent,
    side_landed,
    first_done,
    own_done,
    ready,
    work,
):
    at = lax.axis_index("blk")
    rows = lax.axis_size("blk") // 2
    line, column = at // 2, at % 2
    partner = at + 1 - 2 * column
    size = own_ref.shape[0]
    half = size // 2

    def span(source, start, count):
        return full.at[pl.ds(pl.multiple_of(2 * source * size + start, half), count), :]

    def line_copy(source, sign, first=False):
        target = span(source, column * size, size)
        return push(
            own_ref if first else target,
            target,
            line_sent.at[(sign + 1) // 2, source],
            line_landed.at[source],
            at + 2 * sign,
        )

    def extra_copy(source, sign):
        target = span(source, (1 - column) * size + half, half)
        return push(
            target,
            target,
            extra_sent.at[(sign + 1) // 2, source],
            extra_landed.at[source],
            at + 2 * sign,
        )

    def side_copy(source, member, count, first=False):
        target = span(source, member * size, count)
        return push(
            own_ref.at[:count] if first else target,
            target,
            side_sent.at[source],
            side_landed.at[source],
            partner,
        )

    def first_copy(member):
        return push(
            own_ref.at[half:],
            span(line, member * size + half, half),
            first_done.at[0],
            first_done.at[1],
            partner,
        )

    def inside(row):
        return jnp.logical_and(row >= 0, row < rows)

    def end(row):
        return jnp.logical_or(row == 0, row == rows - 1)

    def by_end(source, act):
        pl.when(end(source))(lambda: act(half))
        pl.when(jnp.logical_not(end(source)))(lambda: act(size))

    pl.when(end(line))(lambda: first_copy(column).start())
    pl.when(line < rows - 1)(lambda: line_copy(line, 1, True).start())
    pl.when(line > 0)(lambda: line_copy(line, -1, True).start())
    by_end(line, lambda count: side_copy(line, column, count, True).start())
    keep = pltpu.make_async_copy(own_ref, span(line, column * size, size), own_done)
    keep.start()

    @pl.when(end(line))
    def _():
        first_copy(1 - column).wait_recv()
        pl.when(line < rows - 1)(lambda: extra_copy(line, 1).start())
        pl.when(line > 0)(lambda: extra_copy(line, -1).start())

    keep.wait()
    ready()

    @pl.loop(0, rows + 1)
    def _(step):
        @pl.loop(0, 2)
        def _(way):
            sign = 2 * way - 1
            source = line - sign * step

            @pl.when(both(step > 0, inside(source)))
            def _():
                line_copy(source, sign).wait_recv()
                pl.when(inside(line + sign))(lambda: line_copy(source, sign).start())
                by_end(source, lambda count: side_copy(source, column, count).start())

        @pl.loop(0, 2)
        def _(way):
            sign = 2 * way - 1
            source = line - sign * step

            @pl.when(both(step > 0, inside(source), end(source)))
            def _():
                extra_copy(source, sign).wait_recv()
                pl.when(inside(line + sign))(lambda: extra_copy(source, sign).start())

        @pl.loop(0, 2)
        def _(way):
            source = line - (2 * way - 1) * (step - 1)

            @pl.when(both(step > way, inside(source)))
            def _():
                by_end(source, lambda count: side_copy(source, 1 - column, count).wait_recv())
                work(source)

    @pl.loop(0, rows)
    def _(source):
        @pl.when(both(source <= line, line < rows - 1))
        def _():
            line_copy(source, 1).wait_send()
            pl.when(end(source))(lambda: extra_copy(source, 1).wait_send())

        @pl.when(both(source >= line, line > 0))
        def _():
            line_copy(source, -1).wait_send()
            pl.when(end(source))(lambda: extra_copy(source, -1).wait_send())

        by_end(source, lambda count: side_copy(source, column, count).wait_send())

    pl.when(end(line))(lambda: first_copy(column).wait_send())


def line_scatter(
    part,
    side,
    lane,
    tail,
    out_ref,
    side_sent,
    side_landed,
    lane_sent,
    lane_landed,
    tail_done,
    work,
    fill,
):
    at = lax.axis_index("blk")
    rows = lax.axis_size("blk") // 2
    line, column = at // 2, at % 2
    partner = at + 1 - 2 * column
    size = out_ref.shape[0]
    half = size // 2

    def span(target, start, count):
        return pl.ds(pl.multiple_of(2 * target * size + start, half), count)

    def piece(target, which):
        member = jnp.where(which == 2, 1 - column, column)
        return span(target, member * size + jnp.where(which == 0, 0, half), half)

    def side_copy(target, count):
        return push(
            part.at[span(target, (1 - column) * size, count), :],
            side.at[target, :count],
            side_sent.at[target],
            side_landed.at[target],
            partner,
        )

    def lane_copy(target, which, sign):
        slot = target if sign == 1 else jnp.where(target == line - 1, rows, target)
        return push(
            part.at[piece(target, which), :],
            lane.at[slot, which],
            lane_sent.at[target, which],
            lane_landed.at[slot, which],
            at + 2 * sign,
        )

    def lane_wait(slot, which):
        push(
            lane.at[slot, which],
            lane.at[slot, which],
            lane_sent.at[0, which],
            lane_landed.at[slot, which],
            partner,
        ).wait_recv()

    def tail_copy():
        return push(
            part.at[piece(line, 2), :], tail, tail_done.at[0], tail_done.at[1], partner
        )

    def inside(row):
        return jnp.logical_and(row >= 0, row < rows)

    def end(row):
        return jnp.logical_or(row == 0, row == rows - 1)

    def by_end(target, act):
        pl.when(end(target))(lambda: act(half))
        pl.when(jnp.logical_not(end(target)))(lambda: act(size))

    def add(where, more):
        part[where, :] = (
            part[where, :].astype(jnp.float32) + more.astype(jnp.float32)
        ).astype(jnp.bfloat16)

    def hop(target, which):
        sign = jnp.where(target > line, 1, -1)

        @pl.when(inside(line - sign))
        def _():
            lane_wait(target, which)
            add(piece(target, which), lane[target, which])

        pl.when(target > line)(lambda: lane_copy(target, which, 1).start())
        pl.when(target < line)(lambda: lane_copy(target, which, -1).start())

    def early(target):
        return both(end(target), end(line), target != line)

    @pl.loop(0, rows)
    def _(step):
        @pl.loop(0, 2)
        def _(way):
            target = line + (2 * way - 1) * (rows - 1 - step)

            @pl.when(both(step < rows - way, inside(target)))
            def _():
                work(target)
                by_end(target, lambda count: side_copy(target, count).start())

                pl.when(early(target))(lambda: pl.loop(1, 3)(lambda which: hop(target, which)))

    def gather_lanes(which):
        @pl.loop(0, 2)
        def _(above):
            slot = jnp.where(above == 0, line, rows)

            @pl.when(jnp.where(above == 0, line > 0, line < rows - 1))
            def _():
                lane_wait(slot, which)
                add(piece(line, which), lane[slot, which])

    def merge(target):
        @pl.when(both(end(target), target != line, jnp.logical_not(early(target))))
        def _():
            pl.loop(1, 3)(lambda which: hop(target, which))

        @pl.when(both(end(line), target == line))
        def _():
            gather_lanes(2)
            tail_copy().start()

        by_end(target, lambda count: side_copy(target, count).wait_recv())

        @pl.loop(0, 2)
        def _(which):
            @pl.when(jnp.logical_or(which == 0, jnp.logical_not(end(target))))
            def _():
                add(piece(target, which), side[target, pl.ds(which * half, half)])
                pl.when(target != line)(lambda: hop(target, which))

    @pl.loop(0, rows)
    def _(step):
        fill(step)

        @pl.loop(0, 2)
        def _(way):
            target = line + (2 * way - 1) * (rows - 1 - step)
            pl.when(both(step < rows - way, inside(target)))(lambda: merge(target))

    pl.loop(0, 2)(lambda which: gather_lanes(1 - which))
    out_ref[...] = part[span(line, column * size, size), :].astype(jnp.float32)

    @pl.when(end(line))
    def _():
        tail_copy().wait_recv()
        out_ref[half:, :] += tail[...].astype(jnp.float32)
        tail_copy().wait_send()

    @pl.loop(0, rows)
    def _(target):
        by_end(target, lambda count: side_copy(target, count).wait_send())

        def sent(sign):
            pl.loop(0, jnp.where(end(target), 3, 2))(
                lambda which: lane_copy(target, which, sign).wait_send()
            )

        pl.when(target > line)(lambda: sent(1))
        pl.when(target < line)(lambda: sent(-1))


def line_sems(rows):
    dma = pltpu.SemaphoreType.DMA
    ways, each = dma((2, rows)), dma((rows,))
    return [ways, each, ways, each, each, each, dma((2,)), dma]


def lane_sems(rows):
    dma = pltpu.SemaphoreType.DMA
    return [dma((rows,)), dma((rows,)), dma((rows, 3)), dma((rows + 1, 3)), dma((2,))]


def lane_buffers(rows, size, width):
    return [
        pltpu.VMEM((2 * rows * size, width), jnp.bfloat16),
        pltpu.VMEM((rows, size, width), jnp.bfloat16),
        pltpu.VMEM((rows + 1, 3, size // 2, width), jnp.bfloat16),
        pltpu.VMEM((size // 2, width), jnp.bfloat16),
    ]


def ffn_kernel(
    act_ref,
    w_ref,
    middle_ref,
    cotangent_ref,
    gains_ref,
    result_ref,
    grad_ref,
    row_ref,
    acts_ref,
    factors_ref,
    out_ref,
    w,
    acts,
    hidden,
    factors,
    part,
    side,
    lane,
    tail,
    w_done,
    save_done,
    factors_done,
    *sems,
):
    at = lax.axis_index("blk")
    rows = lax.axis_size("blk") // 2
    pair = 2 * act_ref.shape[0]

    def load(which):
        return pltpu.make_async_copy(w_ref.at[which], w.at[which], w_done.at[which])

    def pair_rows(source):
        return pl.ds(pl.multiple_of(source * pair, pair), pair)

    def save(source):
        return pltpu.make_async_copy(
            acts.at[pair_rows(source), :], acts_ref.at[pair_rows(source), :], save_done.at[source]
        )

    for which in range(3):
        load(which).start()
    greet(at, at // 2, rows)

    def ready():
        for which in range(3):
            load(which).wait()

    def expand(source):
        save(source).start()
        rows_now = acts[pair_rows(source), :]
        gate = contract_last(w[0], rows_now)
        up = contract_last(w[1], rows_now)
        hidden[source] = (gelu_value(gate) * up).astype(jnp.bfloat16)

    def reduce(target):
        part[pair_rows(target), :] = lax.dot_general(
            hidden[target], w[2], (((0,), (0,)), ((), ())), preferred_element_type=jnp.float32
        ).astype(jnp.bfloat16)

    line_gather(act_ref, acts, *sems[:8], ready, expand)
    def factors_copy(source):
        return pltpu.make_async_copy(
            factors.at[source % 2],
            factors_ref.at[:, :, pair_rows(source)],
            factors_done.at[source % 2],
        )

    def fill(source):
        rows_now = acts[pair_rows(source), :]
        gate = contract_last(w[0], rows_now)
        up = contract_last(w[1], rows_now)
        bent = jnp.tanh(GELU_SCALE * (gate + GELU_CUBIC * gate * gate * gate))
        slope = 0.5 * (1.0 + bent) + 0.5 * gate * (1.0 - bent * bent) * GELU_SCALE * (
            1.0 + 3.0 * GELU_CUBIC * gate * gate
        )
        pl.when(source > 1)(lambda: factors_copy(source - 2).wait())
        slot = source % 2
        factors[slot, 0] = (up * slope).astype(jnp.bfloat16)
        factors[slot, 1] = (0.5 * gate * (1.0 + bent)).astype(jnp.bfloat16)
        factors[slot, 2] = hidden[source]
        factors_copy(source).start()

    line_scatter(part, side, lane, tail, out_ref, *sems[8:], reduce, fill)
    normed, inverse = norm_parts(out_ref[...])
    result_ref[...] = (middle_ref[...] + normed * gains_ref[3:4, :]).astype(jnp.bfloat16)
    grad_v, gain_row = norm_back(
        cotangent_ref[...].astype(jnp.float32), normed, inverse, gains_ref[3:4, :]
    )
    grad_ref[...] = grad_v.astype(jnp.bfloat16)
    row_ref[...] = gain_row[None, :]
    factors_copy(rows - 2).wait()
    factors_copy(rows - 1).wait()
    pl.loop(0, rows)(lambda source: save(source).wait())


def ffn_forward(act_ffn, w_parts, middle, cotangent, gains):
    size, width = act_ffn.shape
    units = w_parts.shape[1]
    blocks = lax.axis_size("blk")
    rows = blocks // 2
    whole = pl.BlockSpec(memory_space=pltpu.VMEM)
    far = pl.BlockSpec(memory_space=pl.ANY)
    return pl.pallas_call(
        ffn_kernel,
        out_shape=(
            jax.ShapeDtypeStruct((size, width), jnp.bfloat16),
            jax.ShapeDtypeStruct((size, width), jnp.bfloat16),
            jax.ShapeDtypeStruct((1, width), jnp.float32),
            jax.ShapeDtypeStruct((blocks * size, width), jnp.bfloat16),
            jax.ShapeDtypeStruct((3, units, blocks * size), jnp.bfloat16),
        ),
        in_specs=[whole, far, whole, whole, whole],
        out_specs=(whole, whole, whole, far, far),
        scratch_shapes=[
            pltpu.VMEM((size, width), jnp.float32),
            pltpu.VMEM(w_parts.shape, jnp.bfloat16),
            pltpu.VMEM((blocks * size, width), jnp.bfloat16),
            pltpu.VMEM((rows, units, 2 * size), jnp.bfloat16),
            pltpu.VMEM((2, 3, units, 2 * size), jnp.bfloat16),
            *lane_buffers(rows, size, width),
            pltpu.SemaphoreType.DMA((3,)),
            pltpu.SemaphoreType.DMA((rows,)),
            pltpu.SemaphoreType.DMA((2,)),
            *line_sems(rows),
            *lane_sems(rows),
        ],
        compiler_params=pltpu.CompilerParams(
            collective_id=2, has_side_effects=True, vmem_limit_bytes=VMEM_BYTES
        ),
        cost_estimate=cost_of(115),
        name="ffn_forward",
    )(act_ffn, w_parts, middle, cotangent, gains)


FILL_COLUMNS = 256
FILL_FIRST = 0


def ffn_back_kernel(
    owners,
    grad_ref,
    acts_ref,
    factors_ref,
    w_ref,
    out_ref,
    keep_ref,
    cross_ref,
    w,
    rights,
    lefts,
    part,
    side,
    lane,
    tail,
    stage,
    mate_part,
    summed,
    w_done,
    acts_done,
    factors_done,
    mate_sent,
    mate_landed,
    summed_done,
    *sems,
):
    at = lax.axis_index("blk")
    me = lax.axis_index("sp")
    chip, core = me // 2, me % 2
    mate = me + 1 - 2 * core
    rows = lax.axis_size("blk") // 2
    size, width = grad_ref.shape
    pair = 2 * size
    units = w.shape[1]
    acts, grads = rights.at[0], rights.at[1]

    def load(which):
        return pltpu.make_async_copy(w_ref.at[which], w.at[which], w_done.at[which])

    def pair_rows(source):
        return pl.ds(pl.multiple_of(source * pair, pair), pair)

    acts_copy = pltpu.make_async_copy(acts_ref, acts, acts_done)
    factors_copy = pltpu.make_async_copy(factors_ref, lefts, factors_done)
    load(2).start()
    factors_copy.start()
    load(0).start()
    load(1).start()
    acts_copy.start()
    greet(at, at // 2, rows, mate)

    def ready():
        load(2).wait()
        factors_copy.wait()

    def expand(source):
        columns = pair_rows(source)
        grad_hidden = contract_last(w[2], grads[columns, :])
        for which in range(2):
            lefts[which, :, columns] = (
                lefts[which, :, columns].astype(jnp.float32) * grad_hidden
            ).astype(jnp.bfloat16)

    def reduce(target):
        columns = pair_rows(target)
        dims = (((0,), (0,)), ((), ()))
        total = lax.dot_general(
            lefts[0, :, columns], w[0], dims, preferred_element_type=jnp.float32
        ) + lax.dot_general(lefts[1, :, columns], w[1], dims, preferred_element_type=jnp.float32)
        part[pair_rows(target), :] = total.astype(jnp.bfloat16)

    pieces = width // FILL_COLUMNS
    total_pieces = 3 * pieces

    def piece_columns(item):
        return pl.ds(pl.multiple_of((item % pieces) * FILL_COLUMNS, FILL_COLUMNS), FILL_COLUMNS)

    def mate_copy(item):
        return push_sp(
            stage.at[item % 3, :, 1 - core],
            mate_part.at[item],
            mate_sent.at[item % 3],
            mate_landed.at[item],
            mate,
        )

    def put(item, side_chip, target):
        return pltpu.make_async_copy(
            summed.at[item % 2, side_chip],
            target.at[item // pieces, :, piece_columns(item)],
            summed_done.at[item % 2, side_chip],
        )

    def put_wait(item):
        put(item, chip, keep_ref).wait()
        put(item, 1 - chip, cross_ref).wait()

    def sum_one(item):
        pl.when(item > 1)(lambda: put_wait(item - 2))
        mate_copy(item).wait_recv()
        summed[item % 2] = (
            stage[item % 3, :, core].astype(jnp.float32) + mate_part[item].astype(jnp.float32)
        ).astype(jnp.bfloat16)
        put(item, chip, keep_ref).start()
        put(item, 1 - chip, cross_ref).start()

    def fill_one(item):
        which = item // pieces
        total = jnp.dot(
            lefts[which],
            rights[which // 2, :, piece_columns(item)],
            preferred_element_type=jnp.float32,
        )
        pl.when(item > 2)(lambda: mate_copy(item - 3).wait_send())
        stage[item % 3] = total.astype(jnp.bfloat16).reshape(
            2, 2, units // owners, FILL_COLUMNS
        )
        mate_copy(item).start()
        pl.when(item > 0)(lambda: sum_one(item - 1))

    each = pl.cdiv(total_pieces - FILL_FIRST, rows - 1)

    def fill(step):
        first = jnp.maximum(FILL_FIRST + (step - 1) * each, 0)
        last = jnp.minimum(FILL_FIRST + step * each, total_pieces)

        @pl.loop(0, each)
        def _(item):
            pl.when(first + item < last)(lambda: fill_one(first + item))

    line_gather(grad_ref, grads, *sems[:8], ready, expand)
    load(0).wait()
    load(1).wait()
    acts_copy.wait()
    line_scatter(part, side, lane, tail, out_ref, *sems[8:], reduce, fill)
    sum_one(total_pieces - 1)
    put_wait(total_pieces - 2)
    put_wait(total_pieces - 1)
    for item in range(total_pieces - 3, total_pieces):
        mate_copy(item).wait_send()


def ffn_back(grad_ffn, kept, w_parts, owners):
    size, width = grad_ffn.shape
    units = w_parts.shape[1]
    blocks = lax.axis_size("blk")
    rows = blocks // 2
    tokens = blocks * size
    items = 3 * width // FILL_COLUMNS
    whole = pl.BlockSpec(memory_space=pltpu.VMEM)
    far = pl.BlockSpec(memory_space=pl.ANY)
    return pl.pallas_call(
        functools.partial(ffn_back_kernel, owners),
        out_shape=(
            jax.ShapeDtypeStruct((size, width), jnp.float32),
            jax.ShapeDtypeStruct((3, units // owners, width), jnp.bfloat16),
            jax.ShapeDtypeStruct((3, units // owners, width), jnp.bfloat16),
        ),
        in_specs=[whole, far, far, far],
        out_specs=(whole, far, far),
        scratch_shapes=[
            pltpu.VMEM(w_parts.shape, jnp.bfloat16),
            pltpu.VMEM((2, tokens, width), jnp.bfloat16),
            pltpu.VMEM((3, units, tokens), jnp.bfloat16),
            *lane_buffers(rows, size, width),
            pltpu.VMEM((3, 2, 2, units // owners, FILL_COLUMNS), jnp.bfloat16),
            pltpu.VMEM((items, 2, units // owners, FILL_COLUMNS), jnp.bfloat16),
            pltpu.VMEM((2, 2, units // owners, FILL_COLUMNS), jnp.bfloat16),
            pltpu.SemaphoreType.DMA((3,)),
            pltpu.SemaphoreType.DMA,
            pltpu.SemaphoreType.DMA,
            pltpu.SemaphoreType.DMA((3,)),
            pltpu.SemaphoreType.DMA((items,)),
            pltpu.SemaphoreType.DMA((2, 2)),
            *line_sems(rows),
            *lane_sems(rows),
        ],
        compiler_params=pltpu.CompilerParams(
            collective_id=3, has_side_effects=True, vmem_limit_bytes=VMEM_BYTES
        ),
        cost_estimate=cost_of(115),
        name="ffn_back",
    )(grad_ffn, *kept, w_parts)


def ffn_hidden(acts, w_parts):
    gate = contract_last(acts, w_parts[0])
    up = contract_last(acts, w_parts[1])
    return (gate, up, (gelu_value(gate) * up).astype(jnp.bfloat16))


def scatter_tokens(partial):
    return lax.psum_scatter(
        partial.astype(jnp.bfloat16), "blk", scatter_dimension=0, tiled=True
    ).astype(jnp.float32)


def ffn_forward_wide(act_ffn, w_parts, middle, cotangent, gains):
    acts = lax.all_gather(act_ffn, "blk", axis=0, tiled=True)
    hidden = ffn_hidden(acts, w_parts)[2]
    partial = jnp.dot(hidden, w_parts[2], preferred_element_type=jnp.float32)
    normed, inverse = norm_parts(scatter_tokens(partial))
    result = (middle + normed * gains[3]).astype(jnp.bfloat16)
    grad_v, gain_row = norm_back(cotangent.astype(jnp.float32), normed, inverse, gains[3])
    return (result, grad_v.astype(jnp.bfloat16), gain_row[None], acts)


def ffn_back_wide(grad_ffn, kept, w_parts, owners):
    (acts,) = kept
    grads = lax.all_gather(grad_ffn, "blk", axis=0, tiled=True)
    gate, up, hidden = ffn_hidden(acts, w_parts)
    grad_hidden = contract_last(grads, w_parts[2])
    grad_gate = (grad_hidden * up * gelu_slope(gate)).astype(jnp.bfloat16)
    grad_up = (grad_hidden * gelu_value(gate)).astype(jnp.bfloat16)
    partial = jnp.dot(grad_gate, w_parts[0], preferred_element_type=jnp.float32) + jnp.dot(
        grad_up, w_parts[1], preferred_element_type=jnp.float32
    )
    sums = jnp.stack(
        [
            jnp.einsum("tf,td->fd", left, right, preferred_element_type=jnp.float32)
            for left, right in ((grad_gate, acts), (grad_up, acts), (hidden, grads))
        ]
    ).astype(jnp.bfloat16)
    units = w_parts.shape[1]
    owned = sums.reshape(3, owners, units // owners, sums.shape[2])
    mine = lax.psum_scatter(
        jnp.transpose(owned, (1, 0, 2, 3)), "sp", scatter_dimension=0, tiled=True
    )
    return (scatter_tokens(partial), mine[0], None)


def cost_of(microseconds):
    return pl.CostEstimate(
        flops=int(microseconds * 1e9), bytes_accessed=int(microseconds * 3e6), transcendentals=0
    )


def push_sp(source, target, sent, landed, peer):
    return pltpu.make_async_remote_copy(
        src_ref=source,
        dst_ref=target,
        send_sem=sent,
        recv_sem=landed,
        device_id={"sp": peer},
        device_id_type=pl.DeviceIdType.MESH,
    )


def greet_sp(me, groups):
    barrier = pltpu.get_barrier_semaphore()
    for step in range(1, groups):
        pl.semaphore_signal(
            barrier,
            inc=1,
            device_id={"sp": (me + step) % groups},
            device_id_type=pl.DeviceIdType.MESH,
        )
    pl.semaphore_wait(barrier, groups - 1)


def gather_rows(x, w_ref, full_ref, w, w_done, own_done, sent, landed, prepare, project):
    me = lax.axis_index("sp")
    size = x.shape[0]
    units = w.shape[0]
    mate = me + 1 - 2 * (me % 2)
    across = (me + 2) % 4

    def spot(member):
        return full_ref.at[pl.ds(pl.multiple_of(member * size, size), size), :]

    load = pltpu.make_async_copy(
        w_ref.at[pl.ds(pl.multiple_of(me * units, units), units), :], w, w_done
    )
    load.start()
    prepare()
    greet_sp(me, 4)
    over = push_sp(x, spot(me), sent.at[0], landed.at[0], across)
    over.start()
    beside = push_sp(x, spot(me), sent.at[1], landed.at[1], mate)
    beside.start()
    keep = pltpu.make_async_copy(x, spot(me), own_done)
    keep.start()
    keep.wait()
    load.wait()

    def project_chip(chip):
        rows = pl.ds(pl.multiple_of(chip * 2 * size, 2 * size), 2 * size)
        project(rows, contract_last(full_ref[rows, :], w[...]).astype(jnp.bfloat16))

    beside.wait_recv()
    project_chip(me // 2)
    over.wait_recv()
    onward = push_sp(spot(across), spot(across), sent.at[2], landed.at[2], mate)
    onward.start()
    onward.wait_recv()
    project_chip(across // 2)
    over.wait_send()
    beside.wait_send()
    onward.wait_send()


def project_in_kernel(tokens_ref, gains_ref, w_ref, full_ref, out_ref, x, *scratch):
    def prepare():
        normed = norm_parts(tokens_ref[...].astype(jnp.float32))[0]
        x[...] = (normed * gains_ref[0:1, :]).astype(jnp.bfloat16)

    def project(rows, value):
        out_ref[rows, :] = value

    gather_rows(x, w_ref, full_ref, *scratch, prepare, project)


def gather_scratch(size, width, units):
    dma = pltpu.SemaphoreType.DMA
    return [
        pltpu.VMEM((size, width), jnp.bfloat16),
        pltpu.VMEM((units, width), jnp.bfloat16),
        dma,
        dma,
        dma((3,)),
        dma((3,)),
    ]


def project_in(tokens, gains, weights):
    size, width = tokens.shape
    units = weights.shape[0] // 4
    whole = pl.BlockSpec(memory_space=pltpu.VMEM)
    return pl.pallas_call(
        project_in_kernel,
        out_shape=(
            jax.ShapeDtypeStruct((4 * size, width), jnp.bfloat16),
            jax.ShapeDtypeStruct((4 * size, units), jnp.bfloat16),
        ),
        in_specs=[whole, whole, pl.BlockSpec(memory_space=pl.ANY)],
        out_specs=(whole, whole),
        scratch_shapes=gather_scratch(size, width, units),
        compiler_params=pltpu.CompilerParams(
            collective_id=4, has_side_effects=True, vmem_limit_bytes=VMEM_BYTES
        ),
        cost_estimate=cost_of(18),
        name="project_in",
    )(tokens, gains, weights)


def project_back_kernel(
    grad_ref,
    middle_ref,
    attn_ref,
    cotangent_ref,
    gains_ref,
    attended_ref,
    by_row_ref,
    totals_ref,
    w_ref,
    full_ref,
    scaled_ref,
    delta_ref,
    grad_middle_ref,
    rows_ref,
    x,
    *scratch,
):
    def prepare():
        grad_v, row_two = norm_back(
            grad_ref[...], *norm_parts(middle_ref[...]), gains_ref[2:3, :]
        )
        grad_middle = cotangent_ref[...].astype(jnp.float32) + grad_v
        grad_middle_ref[...] = grad_middle
        grad_v, row_one = norm_back(grad_middle, *norm_parts(attn_ref[...]), gains_ref[1:2, :])
        x[...] = grad_v.astype(jnp.bfloat16)
        rows_ref[...] = jnp.zeros_like(rows_ref)
        rows_ref[1:2, :] = row_one[None, :]
        rows_ref[2:3, :] = row_two[None, :]

    def project(rows, value):
        for head in range(value.shape[1] // HEAD):
            columns = slice(head * HEAD, (head + 1) * HEAD)
            grad = value[:, columns].astype(jnp.float32)
            scaled_ref[rows, columns] = (grad / by_row_ref[head, rows, :1]).astype(jnp.bfloat16)
            product = grad * attended_ref[rows, columns]
            delta_ref[head, :, rows] = (
                jnp.sum(product.T, axis=0, keepdims=True) / totals_ref[head, :, rows]
            )

    gather_rows(x, w_ref, full_ref, *scratch, prepare, project)


def project_back(
    grad_act, middle, attn, cotangent, gains, attended, by_row, totals, weights
):
    size, width = attn.shape
    units = weights.shape[0] // 4
    whole = pl.BlockSpec(memory_space=pltpu.VMEM)
    return pl.pallas_call(
        project_back_kernel,
        out_shape=(
            jax.ShapeDtypeStruct((4 * size, width), jnp.bfloat16),
            jax.ShapeDtypeStruct((4 * size, units), jnp.bfloat16),
            jax.ShapeDtypeStruct(totals.shape, jnp.float32),
            jax.ShapeDtypeStruct((size, width), jnp.float32),
            jax.ShapeDtypeStruct((8, width), jnp.float32),
        ),
        in_specs=[whole] * 8 + [pl.BlockSpec(memory_space=pl.ANY)],
        out_specs=(whole,) * 5,
        scratch_shapes=gather_scratch(size, width, units),
        compiler_params=pltpu.CompilerParams(
            collective_id=6, has_side_effects=True, vmem_limit_bytes=VMEM_BYTES
        ),
        cost_estimate=cost_of(20),
        name="project_back",
    )(grad_act, middle, attn, cotangent, gains, attended, by_row, totals, weights)


def exchange_norm_kernel(x_ref, w_ref, tokens_ref, gains_ref, out_ref, middle_ref, act_ref, *scratch):
    exchange_project_kernel(x_ref, w_ref, out_ref, *scratch)
    normed = norm_parts(out_ref[...])[0]
    middle = tokens_ref[...].astype(jnp.float32) + normed * gains_ref[1:2, :]
    middle_ref[...] = middle
    act_ref[...] = (norm_parts(middle)[0] * gains_ref[2:3, :]).astype(jnp.bfloat16)


def exchange_project_kernel(x_ref, w_ref, out_ref, w, got, w_done, own_done, sent, landed):
    me = lax.axis_index("sp")
    size = out_ref.shape[0]
    units = x_ref.shape[1]

    def rows_of(member):
        return x_ref.at[pl.ds(pl.multiple_of(member * size, size), size), :]

    def load(member):
        rows = pl.ds(pl.multiple_of(member * units, units), units)
        return pltpu.make_async_copy(w_ref.at[rows, :], w.at[rows, :], w_done.at[member])

    def send(step):
        peer = (me + step) % 4
        return push_sp(rows_of(peer), got.at[4 - step], sent.at[step], landed.at[4 - step], peer)

    greet_sp(me, 4)
    for step in (2, 1, 3):
        send(step).start()
    keep = pltpu.make_async_copy(rows_of(me), got.at[0], own_done)
    keep.start()
    for step in range(4):
        load((me + step) % 4).start()
    keep.wait()
    for step in (0, 1, 3, 2):
        member = (me + step) % 4
        load(member).wait()
        if step > 0:
            send(4 - step).wait_recv()
        rows = pl.ds(pl.multiple_of(member * units, units), units)
        term = jnp.dot(got[step], w[rows, :], preferred_element_type=jnp.float32)
        if step == 0:
            out_ref[...] = term
        else:
            out_ref[...] += term
    for step in (1, 2, 3):
        send(step).wait_send()


def exchange_project(columns, weights, identity, norm_inputs=()):
    size = columns.shape[0] // 4
    whole = pl.BlockSpec(memory_space=pltpu.VMEM)
    total = jax.ShapeDtypeStruct((size, weights.shape[1]), jnp.float32)
    low = jax.ShapeDtypeStruct(total.shape, jnp.bfloat16)
    shapes = [total, total, low] if norm_inputs else [total]
    return pl.pallas_call(
        exchange_norm_kernel if norm_inputs else exchange_project_kernel,
        out_shape=shapes,
        in_specs=[whole, pl.BlockSpec(memory_space=pl.ANY)] + [whole] * len(norm_inputs),
        out_specs=[whole] * len(shapes),
        scratch_shapes=[
            pltpu.VMEM(weights.shape, jnp.bfloat16),
            pltpu.VMEM((4, size, columns.shape[1]), jnp.bfloat16),
            pltpu.SemaphoreType.DMA((4,)),
            pltpu.SemaphoreType.DMA,
            pltpu.SemaphoreType.DMA((4,)),
            pltpu.SemaphoreType.DMA((4,)),
        ],
        compiler_params=pltpu.CompilerParams(
            collective_id=identity, has_side_effects=True, vmem_limit_bytes=VMEM_BYTES
        ),
        cost_estimate=cost_of(16),
        name="exchange_project",
    )(columns, weights, *norm_inputs)


def finish_kernel(
    cols_ref,
    act_ref,
    att_ref,
    grad_ref,
    w_ref,
    tokens_ref,
    middle_ref,
    gains_in_ref,
    rows_ref,
    row_three_ref,
    cross_ref,
    qkv_ref,
    out_ref,
    tokens_grad_ref,
    gains_ref,
    far_ref,
    w,
    got,
    grad_in,
    total,
    part,
    side,
    lane,
    tail,
    mine,
    from_sp,
    from_side,
    from_line,
    w_done,
    own_done,
    swap_sent,
    swap_landed,
    sp_sent,
    sp_landed,
    gain_side,
    line_sent,
    line_landed,
    cross_sent,
    cross_landed,
    *sems,
):
    at = lax.axis_index("blk")
    me = lax.axis_index("sp")
    rows = lax.axis_size("blk") // 2
    line, column = at // 2, at % 2
    partner = at + 1 - 2 * column
    block = total.shape[0]
    size = tokens_ref.shape[0]
    units = cols_ref.shape[1]
    extra = block - size

    barrier = pltpu.get_barrier_semaphore()
    for step in range(1, 4):
        pl.semaphore_signal(
            barrier, inc=1, device_id={"sp": (me + step) % 4}, device_id_type=pl.DeviceIdType.MESH
        )

    def line_peer(step):
        return 2 * ((line + step) % rows) + column

    for peer in [partner] + [line_peer(step) for step in range(1, rows)]:
        pl.semaphore_signal(
            barrier, inc=1, device_id={"blk": peer}, device_id_type=pl.DeviceIdType.MESH
        )

    def load(member):
        span = pl.ds(pl.multiple_of(member * units, units), units)
        return pltpu.make_async_copy(w_ref.at[span, :], w.at[span, :], w_done.at[member])

    def rows_of(member):
        return cols_ref.at[pl.ds(pl.multiple_of(member * size, size), size), :]

    def swap(step):
        peer = (me + step) % 4
        return push_sp(
            rows_of(peer), got.at[4 - step], swap_sent.at[step], swap_landed.at[4 - step], peer
        )

    for step in range(4):
        load((me + step) % 4).start()
    keep = pltpu.make_async_copy(rows_of(me), got.at[0], own_done)
    keep.start()
    pl.semaphore_wait(barrier, 3 + rows)
    for step in (2, 1, 3):
        swap(step).start()
    over = carry(
        cross_ref, far_ref, far_ref.shape[1], cross_sent, cross_landed, (me + 2) % 4
    )
    over.start()
    keep.wait()

    def sp_gains(step):
        return push_sp(
            mine, from_sp.at[4 - step], sp_sent.at[step], sp_landed.at[4 - step], (me + step) % 4
        )

    def side_gains():
        return push(from_sp.at[0], from_side, gain_side.at[0], gain_side.at[1], partner)

    def line_gains(step):
        return push(
            from_line.at[0],
            from_line.at[rows - step],
            line_sent.at[step],
            line_landed.at[rows - step],
            line_peer(step),
        )

    def reduce(target):
        dims = (((0,), (0,)), ((), ()))
        wide_columns = pl.ds(pl.multiple_of(target * 2 * size, 2 * size), 2 * size)
        term = lax.dot_general(
            cols_ref[:, wide_columns], act_ref[...], dims, preferred_element_type=jnp.float32
        ).astype(jnp.bfloat16)
        columns = pl.ds(pl.multiple_of(target * 2 * extra, 2 * extra), 2 * extra)
        more = lax.dot_general(
            att_ref[:, columns], grad_ref[...], dims, preferred_element_type=jnp.float32
        ).astype(jnp.bfloat16)
        for half in range(2):
            start = pl.multiple_of((2 * target + half) * block, block)
            part[pl.ds(start, size), :] = term[half * size : (half + 1) * size]
            start = pl.multiple_of((2 * target + half) * block + size, extra)
            part[pl.ds(start, extra), :] = more[half * extra : (half + 1) * extra]

    def inputs_back():
        for step in (0, 1, 3, 2):
            member = (me + step) % 4
            load(member).wait()
            if step > 0:
                swap(4 - step).wait_recv()
            span = pl.ds(pl.multiple_of(member * units, units), units)
            term = jnp.dot(got[step], w[span, :], preferred_element_type=jnp.float32)
            if step == 0:
                grad_in[...] = term
            else:
                grad_in[...] += term
        normed, inverse = norm_parts(tokens_ref[...].astype(jnp.float32))
        grad_v, gain_row = norm_back(grad_in[...], normed, inverse, gains_in_ref[0:1, :])
        tokens_grad_ref[...] = (middle_ref[...] + grad_v).astype(jnp.bfloat16)
        mine[...] = rows_ref[...]
        mine[0:1, :] = gain_row[None, :]
        mine[3:4, :] = row_three_ref[...]
        for step in range(1, 4):
            sp_gains(step).start()

    def fill(step):
        pl.when(step == 2)(inputs_back)

        @pl.when(step == 3)
        def _():
            gains = mine[...]
            for other in range(1, 4):
                sp_gains(4 - other).wait_recv()
                gains = gains + from_sp[other]
            from_sp[0] = gains
            side_gains().start()

        @pl.when(step == 3)
        def _():
            side_gains().wait_recv()
            from_line[0] = from_sp[0] + from_side[...]
            for other in range(1, rows):
                line_gains(other).start()

    line_scatter(part, side, lane, tail, total, *sems, reduce, fill)
    qkv_ref[...] = total[:size]
    out_ref[...] = total[size:]
    gains = from_line[0]
    for other in range(1, rows):
        line_gains(rows - other).wait_recv()
        gains = gains + from_line[other]
    gains_ref[...] = gains
    for step in (1, 2, 3):
        swap(step).wait_send()
        sp_gains(step).wait_send()
    over.wait()
    side_gains().wait_send()
    for step in range(1, rows):
        line_gains(step).wait_send()


def finish(
    cols, act_block, attended, grad_block, w_qkv, tokens, grad_middle, gains, rows, row_three, cross
):
    blocks = lax.axis_size("blk")
    lines = blocks // 2
    size, width = tokens.shape
    block = (cols.shape[1] + attended.shape[1]) // blocks
    whole = pl.BlockSpec(memory_space=pltpu.VMEM)
    any_space = pl.BlockSpec(memory_space=pl.ANY)
    dma = pltpu.SemaphoreType.DMA
    small = rows.shape
    return pl.pallas_call(
        finish_kernel,
        out_shape=(
            jax.ShapeDtypeStruct((cols.shape[1] // blocks, width), jnp.float32),
            jax.ShapeDtypeStruct((attended.shape[1] // blocks, width), jnp.float32),
            jax.ShapeDtypeStruct((size, width), jnp.bfloat16),
            jax.ShapeDtypeStruct(small, jnp.float32),
            half_of(cross),
        ),
        in_specs=[whole] * 4 + [any_space] + [whole] * 5 + [any_space],
        out_specs=(whole, whole, whole, whole, any_space),
        scratch_shapes=[
            pltpu.VMEM(w_qkv.shape, jnp.bfloat16),
            pltpu.VMEM((4, size, cols.shape[1]), jnp.bfloat16),
            pltpu.VMEM((size, width), jnp.float32),
            pltpu.VMEM((block, width), jnp.float32),
            *lane_buffers(lines, block, width),
            pltpu.VMEM(small, jnp.float32),
            pltpu.VMEM((4, *small), jnp.float32),
            pltpu.VMEM(small, jnp.float32),
            pltpu.VMEM((lines, *small), jnp.float32),
            dma((4,)),
            dma,
            dma((4,)),
            dma((4,)),
            dma((4,)),
            dma((4,)),
            dma((2,)),
            dma((lines,)),
            dma((lines,)),
            dma,
            dma,
            *lane_sems(lines),
        ],
        compiler_params=pltpu.CompilerParams(
            collective_id=8, has_side_effects=True, vmem_limit_bytes=VMEM_BYTES
        ),
        cost_estimate=cost_of(85),
        name="finish",
    )(
        cols,
        act_block,
        attended,
        grad_block,
        w_qkv,
        tokens,
        grad_middle,
        gains,
        rows,
        row_three,
        cross,
    )


def weight_sums_wide(left, right):
    term = jnp.einsum("tc,td->cd", left, right, preferred_element_type=jnp.float32)
    return scatter_tokens(term)


def finish_wide(
    cols, act_block, attended, grad_block, w_qkv, tokens, grad_middle, gains, rows, row_three, cross
):
    (grad_act_in,) = exchange_project(cols, w_qkv, 7)
    normed, inverse = norm_parts(tokens.astype(jnp.float32))
    grad_v, gain_row = norm_back(grad_act_in, normed, inverse, gains[0])
    gains_all = lax.psum(
        jnp.concatenate([gain_row[None], rows[1:3], row_three, rows[4:]]), ("blk", "sp")
    )
    return (
        weight_sums_wide(cols, act_block),
        weight_sums_wide(attended, grad_block),
        (grad_middle + grad_v).astype(jnp.bfloat16),
        gains_all,
        None,
    )


def body(tokens, w_qkv, w_out, gains, w_ffn, cotangent):
    groups = lax.axis_size("sp")
    wide = lax.axis_size("blk") > 8
    act_block, projected = project_in(tokens, gains, w_qkv)
    attended_low, attended, totals, by_row, kv_all = attend(projected, HEADS // groups)
    attn, middle, act_ffn = exchange_project(attended_low, w_out, 5, (tokens, gains))
    w_parts = jnp.transpose(w_ffn, (1, 0, 2))
    result, grad_ffn, row_three, *kept = (ffn_forward_wide if wide else ffn_forward)(
        act_ffn, w_parts, middle, cotangent, gains
    )
    grad_act_ffn, ffn_part, cross = (ffn_back_wide if wide else ffn_back)(
        grad_ffn, kept, w_parts, groups
    )
    grad_block, scaled, delta, grad_middle, rows = project_back(
        grad_act_ffn, middle, attn, cotangent, gains, attended, by_row, totals, w_out
    )
    grad_cols, *far_first = attend_back(projected, scaled, delta, kv_all, cross)
    qkv_grad, out_grad, tokens_grad, gains_all, far_last = (finish_wide if wide else finish)(
        grad_cols,
        act_block,
        attended_low,
        grad_block,
        w_qkv,
        tokens,
        grad_middle,
        gains,
        rows,
        row_three,
        cross,
    )
    ffn_sum = ffn_part.astype(jnp.float32)
    if not wide:
        ffn_sum = ffn_sum + jnp.concatenate([*far_first, far_last], axis=1).astype(jnp.float32)
    ffn_grad = jnp.transpose(ffn_sum, (1, 0, 2))
    share = gains_all.shape[1] // (groups * lax.axis_size("blk"))
    place = lax.axis_index("sp") * lax.axis_size("blk") + lax.axis_index("blk")
    gains_grad = lax.dynamic_slice_in_dim(gains_all[:4], place * share, share, 1)
    return (result, tokens_grad, qkv_grad, out_grad, gains_grad, ffn_grad)


def solution(mesh):
    return jax.shard_map(
        body,
        mesh=mesh,
        in_specs=(
            P(("blk", "sp"), None),
            P(),
            P(),
            P(),
            P("blk", None, None),
            P(("blk", "sp"), None),
        ),
        out_specs=(
            P(("blk", "sp"), None),
            P(("blk", "sp"), None),
            P(("sp", "blk"), None),
            P(("sp", "blk"), None),
            P(None, ("sp", "blk")),
            P(("blk", "sp"), None, None),
        ),
        check_vma=False,
    )
```

```python
import functools

import jax
import jax.numpy as jnp
from jax import lax
from jax.experimental import pallas as pl
from jax.experimental.pallas import tpu as pltpu
from jax.sharding import PartitionSpec as P

HEADS = 8
KV_HEADS = 4
HEAD = 256


VMEM_BYTES = 62 * 1024 * 1024
PIECES = 2
NORM_EPSILON = 1e-06
CAP_VALUE = 50.0
GELU_SCALE = 0.7978845608028654
GELU_CUBIC = 0.044715


def norm_parts(values):
    inverse = lax.rsqrt(jnp.mean(values * values, axis=-1, keepdims=True) + NORM_EPSILON)
    return (values * inverse, inverse)


def norm_back(grad_y, normed, inverse, gain):
    grad_n = grad_y * gain
    grad_v = inverse * (grad_n - normed * jnp.mean(grad_n * normed, axis=-1, keepdims=True))
    return (grad_v, jnp.sum(grad_y * normed, axis=0))


def gelu_value(values):
    return (
        0.5
        * values
        * (1.0 + jnp.tanh(GELU_SCALE * (values + GELU_CUBIC * values * values * values)))
    )


def gelu_slope(values):
    bent = jnp.tanh(GELU_SCALE * (values + GELU_CUBIC * values * values * values))
    return 0.5 * (1.0 + bent) + 0.5 * values * (1.0 - bent * bent) * GELU_SCALE * (
        1.0 + 3.0 * GELU_CUBIC * values * values
    )


def contract_last(left, right):
    return lax.dot_general(
        left, right, (((1,), (1,)), ((), ())), preferred_element_type=jnp.float32
    )


def push(source, target, sent, landed, block):
    return pltpu.make_async_remote_copy(
        src_ref=source,
        dst_ref=target,
        send_sem=sent,
        recv_sem=landed,
        device_id={"blk": block},
        device_id_type=pl.DeviceIdType.MESH,
    )


def greet(at, line, rows, sp_peer=None):
    barrier = pltpu.get_barrier_semaphore()
    others = 1
    if sp_peer is not None:
        others = 2
        pl.semaphore_signal(
            barrier, inc=1, device_id={"sp": sp_peer}, device_id_type=pl.DeviceIdType.MESH
        )

    def tell(block):
        pl.semaphore_signal(
            barrier, inc=1, device_id={"blk": block}, device_id_type=pl.DeviceIdType.MESH
        )

    tell(at + 1 - 2 * (at % 2))
    pl.when(line > 0)(lambda: tell(at - 2))
    pl.when(line < rows - 1)(lambda: tell(at + 2))
    pl.semaphore_wait(barrier, others + jnp.minimum(line, 1) + jnp.minimum(rows - 1 - line, 1))


def both(*terms):
    result = terms[0]
    for term in terms[1:]:
        result = jnp.logical_and(result, term)
    return result


def attend_kernel(
    heads,
    x_ref,
    low_ref,
    att_ref,
    tot_ref,
    by_row_ref,
    kv_ref,
    kv,
    acc,
    part,
    up_sent,
    up_landed,
    side_sent,
    side_landed,
    extra_sent,
    extra_landed,
    own_done,
    save_done,
):
    at = lax.axis_index("blk")
    blocks = lax.axis_size("blk")
    rows = blocks // 2
    line, column = at // 2, at % 2
    partner = at + 1 - 2 * column
    size = x_ref.shape[0]
    first = heads * HEAD
    own = x_ref.at[:, pl.ds(first, 2 * HEAD)]
    greet(at, line, rows)

    def halves(act):
        pl.loop(0, PIECES)(act)

    def span(piece):
        count = size // PIECES
        return pl.ds(pl.multiple_of(piece * count, count), count)

    def source_of(index, piece, is_own):
        if is_own:
            return x_ref.at[span(piece), pl.ds(first, 2 * HEAD)]
        return kv.at[index, span(piece)]

    def up_copy(index, piece, is_own=False):
        return push(
            source_of(index, piece, is_own),
            kv.at[index, span(piece)],
            up_sent.at[index // 2, piece],
            up_landed.at[index // 2, piece],
            at + 2,
        )

    def side_copy(index, piece, is_own=False):
        return push(
            source_of(index, piece, is_own),
            kv.at[index, span(piece)],
            side_sent.at[index // 2, piece],
            side_landed.at[index // 2, piece],
            partner,
        )

    def extra_copy():
        rows_now = kv.at[0, span(PIECES - 1)]
        return push(rows_now, rows_now, extra_sent.at[0], extra_landed.at[0], at + 2)

    def crossing(index):
        return jnp.where(both(index == 0, at > 0), PIECES - 1, PIECES)

    def save(index):
        return pltpu.make_async_copy(kv.at[index], kv_ref.at[index], save_done.at[index])

    @pl.loop(0, PIECES)
    def _(piece):
        pl.when(line < rows - 1)(lambda: up_copy(at, piece, True).start())
        pl.when(column == 0)(lambda: side_copy(at, PIECES - 1 - piece, True).start())

    keep = pltpu.make_async_copy(own, kv.at[at], own_done)
    keep.start()
    acc[...] = jnp.zeros_like(acc)
    part[...] = jnp.zeros_like(part)
    keep.wait()

    @pl.when(at == 1)
    def _():
        side_copy(0, PIECES - 1).wait_recv()
        extra_copy().start()

    ahead = lax.broadcasted_iota(jnp.int32, (size, size), 1) - lax.broadcasted_iota(
        jnp.int32, (size, size), 0
    )

    def compute(index):
        save(index).start()
        span = (at - index) * size
        for head in range(heads):
            raw = lax.dot_general(
                x_ref[:, head * HEAD : (head + 1) * HEAD],
                kv[index, :, :HEAD],
                (((1,), (1,)), ((), ())),
                preferred_element_type=jnp.float32,
            )
            weights = jnp.exp(CAP_VALUE * jnp.tanh(raw * (HEAD ** (-0.5) / CAP_VALUE)))
            weights = jnp.where(ahead <= span, weights, 0.0)
            total = weights[:, :128]
            for piece in range(1, size // 128):
                total = total + weights[:, piece * 128 : (piece + 1) * 128]
            part[head] += total
            acc[:, head * HEAD : (head + 1) * HEAD] += jnp.dot(
                weights.astype(jnp.bfloat16),
                kv[index, :, HEAD:],
                preferred_element_type=jnp.float32,
            )

    @pl.loop(0, rows + 1)
    def _(step):
        source = line - step
        index = 2 * source + column

        @pl.when(both(step > 0, source >= 0))
        def _():
            @pl.loop(0, PIECES)
            def _(piece):
                up_copy(index, piece).wait_recv()
                pl.when(line < rows - 1)(lambda: up_copy(index, piece).start())
                pl.when(piece < crossing(index))(lambda: side_copy(index, piece).start())

        @pl.when(both(step > 0, source == 0, column == 1))
        def _():
            extra_copy().wait_recv()
            pl.when(line < rows - 1)(lambda: extra_copy().start())

        @pl.loop(0, 2)
        def _(way):
            found = source + way
            here = 2 * found + jnp.where(way == 0, column, 1 - column)
            due = jnp.logical_or(way == 0, both(step > 0, jnp.logical_or(step > 1, column == 1)))

            @pl.when(both(found >= 0, due))
            def _():
                pl.when(way == 1)(
                    lambda: pl.loop(0, crossing(here))(
                        lambda piece: side_copy(here, piece).wait_recv()
                    )
                )
                compute(here)

    for head in range(heads):
        columns = slice(head * HEAD, (head + 1) * HEAD)
        total = jnp.sum(part[head], axis=1, keepdims=True)
        by_row_ref[head] = jnp.broadcast_to(total, by_row_ref.shape[1:])
        value = acc[:, columns] / total
        att_ref[:, columns] = value
        low_ref[:, columns] = value.astype(jnp.bfloat16)
        tot_ref[head] = jnp.sum(part[head].T, axis=0, keepdims=True)

    @pl.loop(0, rows)
    def _(source):
        index = 2 * source + column

        @pl.when(source <= line)
        def _():
            pl.when(line < rows - 1)(
                lambda: halves(lambda piece: up_copy(index, piece).wait_send())
            )
            pl.when(jnp.logical_or(source < line, column == 0))(
                lambda: pl.loop(0, crossing(index))(
                    lambda piece: side_copy(index, piece).wait_send()
                )
            )

    pl.when(both(column == 1, line < rows - 1))(lambda: extra_copy().wait_send())

    @pl.loop(0, blocks)
    def _(index):
        pl.when(index <= at)(lambda: save(index).wait())


def attend(projected, heads):
    size = projected.shape[0]
    blocks = lax.axis_size("blk")
    whole = pl.BlockSpec(memory_space=pltpu.VMEM)
    return pl.pallas_call(
        functools.partial(attend_kernel, heads),
        out_shape=(
            jax.ShapeDtypeStruct((size, heads * HEAD), jnp.bfloat16),
            jax.ShapeDtypeStruct((size, heads * HEAD), jnp.float32),
            jax.ShapeDtypeStruct((heads, 1, size), jnp.float32),
            jax.ShapeDtypeStruct((heads, size, 128), jnp.float32),
            jax.ShapeDtypeStruct((blocks, size, 2 * HEAD), jnp.bfloat16),
        ),
        in_specs=[whole],
        out_specs=(whole, whole, whole, whole, pl.BlockSpec(memory_space=pl.ANY)),
        scratch_shapes=[
            pltpu.VMEM((blocks, size, 2 * HEAD), jnp.bfloat16),
            pltpu.VMEM((size, heads * HEAD), jnp.float32),
            pltpu.VMEM((heads, size, 128), jnp.float32),
            pltpu.SemaphoreType.DMA((blocks // 2, PIECES)),
            pltpu.SemaphoreType.DMA((blocks // 2, PIECES)),
            pltpu.SemaphoreType.DMA((blocks // 2, PIECES)),
            pltpu.SemaphoreType.DMA((blocks // 2, PIECES)),
            pltpu.SemaphoreType.DMA((1,)),
            pltpu.SemaphoreType.DMA((1,)),
            pltpu.SemaphoreType.DMA,
            pltpu.SemaphoreType.DMA((blocks,)),
        ],
        compiler_params=pltpu.CompilerParams(
            collective_id=0, has_side_effects=True, vmem_limit_bytes=VMEM_BYTES
        ),
        cost_estimate=cost_of(50),
        name="attend",
    )(projected)


def carry(cross_ref, far_ref, first, sent, landed, across):
    return push_sp(
        cross_ref.at[:, pl.ds(first, far_ref.shape[1]), :], far_ref, sent, landed, across
    )


def attend_back_kernel(heads, carried, *refs):
    if carried:
        x_ref, scaled_ref, delta_ref, kv_ref, cross_ref, out_ref, far_ref, *scratch = refs
        *scratch, cross_sent, cross_landed = scratch
        across = (lax.axis_index("sp") + 2) % 4
        over = carry(cross_ref, far_ref, 0, cross_sent, cross_landed, across)
        after = over.start
    else:
        x_ref, scaled_ref, delta_ref, kv_ref, out_ref, *scratch = refs
        across, after = None, lambda: None
    attend_back_steps(
        heads, across, after, x_ref, scaled_ref, delta_ref, kv_ref, out_ref, *scratch
    )
    if carried:
        over.wait()


def attend_back_steps(
    heads,
    across,
    after_greeting,
    x_ref,
    scaled_ref,
    delta_ref,
    kv_ref,
    out_ref,
    kv,
    part,
    side,
    down,
    dq,
    dk,
    dv,
    load_done,
    side_sent,
    side_landed,
    down_sent,
    down_landed,
):
    at = lax.axis_index("blk")
    blocks = lax.axis_size("blk")
    rows = blocks // 2
    line, column = at // 2, at % 2
    partner = at + 1 - 2 * column
    size = x_ref.shape[0]

    def load(index):
        return pltpu.make_async_copy(kv_ref.at[index], kv.at[index], load_done.at[index])

    @pl.loop(0, blocks)
    def _(index):
        pl.when(index <= at)(lambda: load(index).start())

    greet(at, line, rows, across)
    after_greeting()

    def halves(act):
        pl.loop(0, PIECES)(act)

    def span(piece):
        count = size // PIECES
        return pl.ds(pl.multiple_of(piece * count, count), count)

    def side_copy(target, piece):
        return push(
            part.at[target, 1 - column, span(piece)],
            side.at[target, span(piece)],
            side_sent.at[target, piece],
            side_landed.at[target, piece],
            partner,
        )

    def down_copy(target, piece):
        return push(
            part.at[target, column, span(piece)],
            down.at[target, span(piece)],
            down_sent.at[target, piece],
            down_landed.at[target, piece],
            at - 2,
        )

    dq[...] = jnp.zeros_like(dq)
    ahead = lax.broadcasted_iota(jnp.int32, (size, size), 0) - lax.broadcasted_iota(
        jnp.int32, (size, size), 1
    )

    def compute(target, half):
        index = 2 * target + half
        load(index).wait()
        span = (at - index) * size
        for head in range(heads):
            columns = slice(head * HEAD, (head + 1) * HEAD)
            query = x_ref[:, columns]
            scaled = scaled_ref[:, columns]
            key = kv[index, :, :HEAD]
            raw = lax.dot_general(
                key, query, (((1,), (1,)), ((), ())), preferred_element_type=jnp.float32
            )
            squashed = jnp.tanh(raw * (HEAD ** (-0.5) / CAP_VALUE))
            weights = jnp.exp(CAP_VALUE * squashed)
            weights = jnp.where(ahead <= span, weights, 0.0)
            inner = lax.dot_general(
                kv[index, :, HEAD:],
                scaled,
                (((1,), (1,)), ((), ())),
                preferred_element_type=jnp.float32,
            )
            grad_raw = (
                weights * (inner - delta_ref[head]) * (1.0 - squashed * squashed)
            ).astype(jnp.bfloat16)
            dv_now = jnp.dot(
                weights.astype(jnp.bfloat16), scaled, preferred_element_type=jnp.float32
            )
            dk_now = jnp.dot(grad_raw, query, preferred_element_type=jnp.float32)
            dq[:, columns] += lax.dot_general(
                grad_raw, key, (((0,), (0,)), ((), ())), preferred_element_type=jnp.float32
            )
            if head == 0:
                dv[...] = dv_now
                dk[...] = dk_now
            else:
                dv[...] += dv_now
                dk[...] += dk_now
        part[target, half, :, :HEAD] = (dk[...] * HEAD ** (-0.5)).astype(jnp.bfloat16)
        part[target, half, :, HEAD:] = dv[...].astype(jnp.bfloat16)

    def merge(target):
        def add(piece, more):
            part[target, column, span(piece)] = (
                part[target, column, span(piece)].astype(jnp.float32) + more.astype(jnp.float32)
            ).astype(jnp.bfloat16)

        def merge_piece(piece):
            @pl.when(jnp.logical_or(target < line, column == 0))
            def _():
                side_copy(target, piece).wait_recv()
                add(piece, side[target, span(piece)])

            @pl.when(line < rows - 1)
            def _():
                down_copy(target, piece).wait_recv()
                add(piece, down[target, span(piece)])

            pl.when(target < line)(lambda: down_copy(target, piece).start())

        halves(merge_piece)

        @pl.when(target == line)
        def _():
            out_ref[:, heads * HEAD :] = part[target, column]

    @pl.loop(0, rows)
    def _(target):
        away = jnp.logical_or(target < line, both(target == line, column == 1))

        @pl.loop(0, 2)
        def _(way):
            @pl.when(jnp.logical_or(both(way == 0, away), both(way == 1, target <= line)))
            def _():
                compute(target, jnp.where(way == 0, 1 - column, column))
                pl.when(way == 0)(lambda: halves(lambda piece: side_copy(target, piece).start()))

            pl.when(both(way == 0, line == rows - 1, target > 0))(lambda: merge(target - 1))


    out_ref[:, : heads * HEAD] = (dq[...] * HEAD ** (-0.5)).astype(jnp.bfloat16)

    @pl.loop(0, rows)
    def _(target):
        pl.when(both(target <= line, jnp.logical_or(line < rows - 1, target == rows - 1)))(
            lambda: merge(target)
        )

    @pl.loop(0, rows)
    def _(target):
        pl.when(jnp.logical_or(target < line, both(target == line, column == 1)))(
            lambda: halves(lambda piece: side_copy(target, piece).wait_send())
        )
        pl.when(target < line)(lambda: halves(lambda piece: down_copy(target, piece).wait_send()))


def half_of(cross):
    kinds, units, width = cross.shape
    return jax.ShapeDtypeStruct((kinds, units // 2, width), cross.dtype)


def attend_back(projected, scaled, delta, kv_all, cross=None):
    size = projected.shape[0]
    blocks = lax.axis_size("blk")
    rows = blocks // 2
    heads = scaled.shape[1] // HEAD
    whole = pl.BlockSpec(memory_space=pltpu.VMEM)
    far = pl.BlockSpec(memory_space=pl.ANY)
    carried = cross is not None
    far_shape, operands = [], [projected, scaled, delta, kv_all]
    if carried:
        far_shape = [half_of(cross)]
        operands.append(cross)
    return pl.pallas_call(
        functools.partial(attend_back_kernel, heads, carried),
        out_shape=[jax.ShapeDtypeStruct(projected.shape, jnp.bfloat16)] + far_shape,
        in_specs=[whole, whole, whole, far] + [far] * carried,
        out_specs=[whole] + [far] * carried,
        scratch_shapes=[
            pltpu.VMEM((blocks, size, 2 * HEAD), jnp.bfloat16),
            pltpu.VMEM((rows, 2, size, 2 * HEAD), jnp.bfloat16),
            pltpu.VMEM((rows, size, 2 * HEAD), jnp.bfloat16),
            pltpu.VMEM((rows, size, 2 * HEAD), jnp.bfloat16),
            pltpu.VMEM((size, heads * HEAD), jnp.float32),
            pltpu.VMEM((size, HEAD), jnp.float32),
            pltpu.VMEM((size, HEAD), jnp.float32),
            pltpu.SemaphoreType.DMA((blocks,)),
            pltpu.SemaphoreType.DMA((rows, PIECES)),
            pltpu.SemaphoreType.DMA((rows, PIECES)),
            pltpu.SemaphoreType.DMA((rows, PIECES)),
            pltpu.SemaphoreType.DMA((rows, PIECES)),
        ]
        + [pltpu.SemaphoreType.DMA, pltpu.SemaphoreType.DMA] * carried,
        compiler_params=pltpu.CompilerParams(
            collective_id=1, has_side_effects=True, vmem_limit_bytes=VMEM_BYTES
        ),
        cost_estimate=cost_of(50),
        name="attend_back",
    )(*operands)


def line_gather(
    own_ref,
    full,
    line_sent,
    line_landed,
    extra_sent,
    extra_landed,
    side_sent,
    side_landed,
    first_done,
    own_done,
    ready,
    work,
):
    at = lax.axis_index("blk")
    rows = lax.axis_size("blk") // 2
    line, column = at // 2, at % 2
    partner = at + 1 - 2 * column
    size = own_ref.shape[0]
    half = size // 2

    def span(source, start, count):
        return full.at[pl.ds(pl.multiple_of(2 * source * size + start, half), count), :]

    def line_copy(source, sign, first=False):
        target = span(source, column * size, size)
        return push(
            own_ref if first else target,
            target,
            line_sent.at[(sign + 1) // 2, source],
            line_landed.at[source],
            at + 2 * sign,
        )

    def extra_copy(source, sign):
        target = span(source, (1 - column) * size + half, half)
        return push(
            target,
            target,
            extra_sent.at[(sign + 1) // 2, source],
            extra_landed.at[source],
            at + 2 * sign,
        )

    def side_copy(source, member, count, first=False):
        target = span(source, member * size, count)
        return push(
            own_ref.at[:count] if first else target,
            target,
            side_sent.at[source],
            side_landed.at[source],
            partner,
        )

    def first_copy(member):
        return push(
            own_ref.at[half:],
            span(line, member * size + half, half),
            first_done.at[0],
            first_done.at[1],
            partner,
        )

    def inside(row):
        return jnp.logical_and(row >= 0, row < rows)

    def end(row):
        return jnp.logical_or(row == 0, row == rows - 1)

    def by_end(source, act):
        pl.when(end(source))(lambda: act(half))
        pl.when(jnp.logical_not(end(source)))(lambda: act(size))

    pl.when(end(line))(lambda: first_copy(column).start())
    pl.when(line < rows - 1)(lambda: line_copy(line, 1, True).start())
    pl.when(line > 0)(lambda: line_copy(line, -1, True).start())
    by_end(line, lambda count: side_copy(line, column, count, True).start())
    keep = pltpu.make_async_copy(own_ref, span(line, column * size, size), own_done)
    keep.start()

    @pl.when(end(line))
    def _():
        first_copy(1 - column).wait_recv()
        pl.when(line < rows - 1)(lambda: extra_copy(line, 1).start())
        pl.when(line > 0)(lambda: extra_copy(line, -1).start())

    keep.wait()
    ready()

    @pl.loop(0, rows + 1)
    def _(step):
        @pl.loop(0, 2)
        def _(way):
            sign = 2 * way - 1
            source = line - sign * step

            @pl.when(both(step > 0, inside(source)))
            def _():
                line_copy(source, sign).wait_recv()
                pl.when(inside(line + sign))(lambda: line_copy(source, sign).start())
                by_end(source, lambda count: side_copy(source, column, count).start())

        @pl.loop(0, 2)
        def _(way):
            sign = 2 * way - 1
            source = line - sign * step

            @pl.when(both(step > 0, inside(source), end(source)))
            def _():
                extra_copy(source, sign).wait_recv()
                pl.when(inside(line + sign))(lambda: extra_copy(source, sign).start())

        @pl.loop(0, 2)
        def _(way):
            source = line - (2 * way - 1) * (step - 1)

            @pl.when(both(step > way, inside(source)))
            def _():
                by_end(source, lambda count: side_copy(source, 1 - column, count).wait_recv())
                work(source)

    @pl.loop(0, rows)
    def _(source):
        @pl.when(both(source <= line, line < rows - 1))
        def _():
            line_copy(source, 1).wait_send()
            pl.when(end(source))(lambda: extra_copy(source, 1).wait_send())

        @pl.when(both(source >= line, line > 0))
        def _():
            line_copy(source, -1).wait_send()
            pl.when(end(source))(lambda: extra_copy(source, -1).wait_send())

        by_end(source, lambda count: side_copy(source, column, count).wait_send())

    pl.when(end(line))(lambda: first_copy(column).wait_send())


def line_scatter(
    part,
    side,
    lane,
    tail,
    out_ref,
    side_sent,
    side_landed,
    lane_sent,
    lane_landed,
    tail_done,
    work,
    fill,
):
    at = lax.axis_index("blk")
    rows = lax.axis_size("blk") // 2
    line, column = at // 2, at % 2
    partner = at + 1 - 2 * column
    size = out_ref.shape[0]
    half = size // 2

    def span(target, start, count):
        return pl.ds(pl.multiple_of(2 * target * size + start, half), count)

    def piece(target, which):
        member = jnp.where(which == 2, 1 - column, column)
        return span(target, member * size + jnp.where(which == 0, 0, half), half)

    def side_copy(target, count):
        return push(
            part.at[span(target, (1 - column) * size, count), :],
            side.at[target, :count],
            side_sent.at[target],
            side_landed.at[target],
            partner,
        )

    def lane_copy(target, which, sign):
        slot = target if sign == 1 else jnp.where(target == line - 1, rows, target)
        return push(
            part.at[piece(target, which), :],
            lane.at[slot, which],
            lane_sent.at[target, which],
            lane_landed.at[slot, which],
            at + 2 * sign,
        )

    def lane_wait(slot, which):
        push(
            lane.at[slot, which],
            lane.at[slot, which],
            lane_sent.at[0, which],
            lane_landed.at[slot, which],
            partner,
        ).wait_recv()

    def tail_copy():
        return push(
            part.at[piece(line, 2), :], tail, tail_done.at[0], tail_done.at[1], partner
        )

    def inside(row):
        return jnp.logical_and(row >= 0, row < rows)

    def end(row):
        return jnp.logical_or(row == 0, row == rows - 1)

    def by_end(target, act):
        pl.when(end(target))(lambda: act(half))
        pl.when(jnp.logical_not(end(target)))(lambda: act(size))

    def add(where, more):
        part[where, :] = (
            part[where, :].astype(jnp.float32) + more.astype(jnp.float32)
        ).astype(jnp.bfloat16)

    def hop(target, which):
        sign = jnp.where(target > line, 1, -1)

        @pl.when(inside(line - sign))
        def _():
            lane_wait(target, which)
            add(piece(target, which), lane[target, which])

        pl.when(target > line)(lambda: lane_copy(target, which, 1).start())
        pl.when(target < line)(lambda: lane_copy(target, which, -1).start())

    def early(target):
        return both(end(target), end(line), target != line)

    @pl.loop(0, rows)
    def _(step):
        @pl.loop(0, 2)
        def _(way):
            target = line + (2 * way - 1) * (rows - 1 - step)

            @pl.when(both(step < rows - way, inside(target)))
            def _():
                work(target)
                by_end(target, lambda count: side_copy(target, count).start())

                pl.when(early(target))(lambda: pl.loop(1, 3)(lambda which: hop(target, which)))

    def gather_lanes(which):
        @pl.loop(0, 2)
        def _(above):
            slot = jnp.where(above == 0, line, rows)

            @pl.when(jnp.where(above == 0, line > 0, line < rows - 1))
            def _():
                lane_wait(slot, which)
                add(piece(line, which), lane[slot, which])

    def merge(target):
        @pl.when(both(end(target), target != line, jnp.logical_not(early(target))))
        def _():
            pl.loop(1, 3)(lambda which: hop(target, which))

        @pl.when(both(end(line), target == line))
        def _():
            gather_lanes(2)
            tail_copy().start()

        by_end(target, lambda count: side_copy(target, count).wait_recv())

        @pl.loop(0, 2)
        def _(which):
            @pl.when(jnp.logical_or(which == 0, jnp.logical_not(end(target))))
            def _():
                add(piece(target, which), side[target, pl.ds(which * half, half)])
                pl.when(target != line)(lambda: hop(target, which))

    @pl.loop(0, rows)
    def _(step):
        fill(step)

        @pl.loop(0, 2)
        def _(way):
            target = line + (2 * way - 1) * (rows - 1 - step)
            pl.when(both(step < rows - way, inside(target)))(lambda: merge(target))

    pl.loop(0, 2)(lambda which: gather_lanes(1 - which))
    out_ref[...] = part[span(line, column * size, size), :].astype(jnp.float32)

    @pl.when(end(line))
    def _():
        tail_copy().wait_recv()
        out_ref[half:, :] += tail[...].astype(jnp.float32)
        tail_copy().wait_send()

    @pl.loop(0, rows)
    def _(target):
        by_end(target, lambda count: side_copy(target, count).wait_send())

        def sent(sign):
            pl.loop(0, jnp.where(end(target), 3, 2))(
                lambda which: lane_copy(target, which, sign).wait_send()
            )

        pl.when(target > line)(lambda: sent(1))
        pl.when(target < line)(lambda: sent(-1))


def line_sems(rows):
    dma = pltpu.SemaphoreType.DMA
    ways, each = dma((2, rows)), dma((rows,))
    return [ways, each, ways, each, each, each, dma((2,)), dma]


def lane_sems(rows):
    dma = pltpu.SemaphoreType.DMA
    return [dma((rows,)), dma((rows,)), dma((rows, 3)), dma((rows + 1, 3)), dma((2,))]


def lane_buffers(rows, size, width):
    return [
        pltpu.VMEM((2 * rows * size, width), jnp.bfloat16),
        pltpu.VMEM((rows, size, width), jnp.bfloat16),
        pltpu.VMEM((rows + 1, 3, size // 2, width), jnp.bfloat16),
        pltpu.VMEM((size // 2, width), jnp.bfloat16),
    ]


def ffn_kernel(
    act_ref,
    w_ref,
    middle_ref,
    cotangent_ref,
    gains_ref,
    result_ref,
    grad_ref,
    row_ref,
    acts_ref,
    factors_ref,
    out_ref,
    w,
    acts,
    hidden,
    factors,
    part,
    side,
    lane,
    tail,
    w_done,
    save_done,
    factors_done,
    *sems,
):
    at = lax.axis_index("blk")
    rows = lax.axis_size("blk") // 2
    pair = 2 * act_ref.shape[0]

    def load(which):
        return pltpu.make_async_copy(w_ref.at[which], w.at[which], w_done.at[which])

    def pair_rows(source):
        return pl.ds(pl.multiple_of(source * pair, pair), pair)

    def save(source):
        return pltpu.make_async_copy(
            acts.at[pair_rows(source), :], acts_ref.at[pair_rows(source), :], save_done.at[source]
        )

    for which in range(3):
        load(which).start()
    greet(at, at // 2, rows)

    def ready():
        for which in range(3):
            load(which).wait()

    def expand(source):
        save(source).start()
        rows_now = acts[pair_rows(source), :]
        gate = contract_last(w[0], rows_now)
        up = contract_last(w[1], rows_now)
        hidden[source] = (gelu_value(gate) * up).astype(jnp.bfloat16)

    def reduce(target):
        part[pair_rows(target), :] = lax.dot_general(
            hidden[target], w[2], (((0,), (0,)), ((), ())), preferred_element_type=jnp.float32
        ).astype(jnp.bfloat16)

    line_gather(act_ref, acts, *sems[:8], ready, expand)
    def factors_copy(source):
        return pltpu.make_async_copy(
            factors.at[source % 2],
            factors_ref.at[:, :, pair_rows(source)],
            factors_done.at[source % 2],
        )

    def fill(source):
        rows_now = acts[pair_rows(source), :]
        gate = contract_last(w[0], rows_now)
        up = contract_last(w[1], rows_now)
        bent = jnp.tanh(GELU_SCALE * (gate + GELU_CUBIC * gate * gate * gate))
        slope = 0.5 * (1.0 + bent) + 0.5 * gate * (1.0 - bent * bent) * GELU_SCALE * (
            1.0 + 3.0 * GELU_CUBIC * gate * gate
        )
        pl.when(source > 1)(lambda: factors_copy(source - 2).wait())
        slot = source % 2
        factors[slot, 0] = (up * slope).astype(jnp.bfloat16)
        factors[slot, 1] = (0.5 * gate * (1.0 + bent)).astype(jnp.bfloat16)
        factors[slot, 2] = hidden[source]
        factors_copy(source).start()

    line_scatter(part, side, lane, tail, out_ref, *sems[8:], reduce, fill)
    normed, inverse = norm_parts(out_ref[...])
    result_ref[...] = (middle_ref[...] + normed * gains_ref[3:4, :]).astype(jnp.bfloat16)
    grad_v, gain_row = norm_back(
        cotangent_ref[...].astype(jnp.float32), normed, inverse, gains_ref[3:4, :]
    )
    grad_ref[...] = grad_v.astype(jnp.bfloat16)
    row_ref[...] = gain_row[None, :]
    factors_copy(rows - 2).wait()
    factors_copy(rows - 1).wait()
    pl.loop(0, rows)(lambda source: save(source).wait())


def ffn_forward(act_ffn, w_parts, middle, cotangent, gains):
    size, width = act_ffn.shape
    units = w_parts.shape[1]
    blocks = lax.axis_size("blk")
    rows = blocks // 2
    whole = pl.BlockSpec(memory_space=pltpu.VMEM)
    far = pl.BlockSpec(memory_space=pl.ANY)
    return pl.pallas_call(
        ffn_kernel,
        out_shape=(
            jax.ShapeDtypeStruct((size, width), jnp.bfloat16),
            jax.ShapeDtypeStruct((size, width), jnp.bfloat16),
            jax.ShapeDtypeStruct((1, width), jnp.float32),
            jax.ShapeDtypeStruct((blocks * size, width), jnp.bfloat16),
            jax.ShapeDtypeStruct((3, units, blocks * size), jnp.bfloat16),
        ),
        in_specs=[whole, far, whole, whole, whole],
        out_specs=(whole, whole, whole, far, far),
        scratch_shapes=[
            pltpu.VMEM((size, width), jnp.float32),
            pltpu.VMEM(w_parts.shape, jnp.bfloat16),
            pltpu.VMEM((blocks * size, width), jnp.bfloat16),
            pltpu.VMEM((rows, units, 2 * size), jnp.bfloat16),
            pltpu.VMEM((2, 3, units, 2 * size), jnp.bfloat16),
            *lane_buffers(rows, size, width),
            pltpu.SemaphoreType.DMA((3,)),
            pltpu.SemaphoreType.DMA((rows,)),
            pltpu.SemaphoreType.DMA((2,)),
            *line_sems(rows),
            *lane_sems(rows),
        ],
        compiler_params=pltpu.CompilerParams(
            collective_id=2, has_side_effects=True, vmem_limit_bytes=VMEM_BYTES
        ),
        cost_estimate=cost_of(115),
        name="ffn_forward",
    )(act_ffn, w_parts, middle, cotangent, gains)


FILL_COLUMNS = 768
FILL_FIRST = 0


def ffn_back_kernel(
    owners,
    grad_ref,
    acts_ref,
    factors_ref,
    w_ref,
    out_ref,
    keep_ref,
    cross_ref,
    w,
    rights,
    lefts,
    part,
    side,
    lane,
    tail,
    stage,
    mate_part,
    w_done,
    acts_done,
    factors_done,
    mate_sent,
    mate_landed,
    summed_done,
    *sems,
):
    at = lax.axis_index("blk")
    me = lax.axis_index("sp")
    chip, core = me // 2, me % 2
    mate = me + 1 - 2 * core
    rows = lax.axis_size("blk") // 2
    size, width = grad_ref.shape
    pair = 2 * size
    units = w.shape[1]
    acts, grads = rights.at[0], rights.at[1]

    def load(which):
        return pltpu.make_async_copy(w_ref.at[which], w.at[which], w_done.at[which])

    def pair_rows(source):
        return pl.ds(pl.multiple_of(source * pair, pair), pair)

    acts_copy = pltpu.make_async_copy(acts_ref, acts, acts_done)
    factors_copy = pltpu.make_async_copy(factors_ref, lefts, factors_done)
    load(2).start()
    factors_copy.start()
    load(0).start()
    load(1).start()
    acts_copy.start()
    greet(at, at // 2, rows, mate)

    def ready():
        load(2).wait()
        factors_copy.wait()

    def expand(source):
        columns = pair_rows(source)
        grad_hidden = contract_last(w[2], grads[columns, :])
        for which in range(2):
            lefts[which, :, columns] = (
                lefts[which, :, columns].astype(jnp.float32) * grad_hidden
            ).astype(jnp.bfloat16)

    def reduce(target):
        columns = pair_rows(target)
        dims = (((0,), (0,)), ((), ()))
        total = lax.dot_general(
            lefts[0, :, columns], w[0], dims, preferred_element_type=jnp.float32
        ) + lax.dot_general(lefts[1, :, columns], w[1], dims, preferred_element_type=jnp.float32)
        part[pair_rows(target), :] = total.astype(jnp.bfloat16)

    pieces = width // FILL_COLUMNS
    total_pieces = 3 * pieces

    def piece_columns(item):
        return pl.ds(pl.multiple_of((item % pieces) * FILL_COLUMNS, FILL_COLUMNS), FILL_COLUMNS)

    def mate_copy(item):
        return push_sp(
            stage.at[item % 2, :, 1 - core],
            mate_part.at[item],
            mate_sent.at[item % 2],
            mate_landed.at[item],
            mate,
        )

    def put(item, side_chip, target):
        return pltpu.make_async_copy(
            mate_part.at[item, side_chip],
            target.at[item // pieces, :, piece_columns(item)],
            summed_done.at[item, side_chip],
        )

    def put_wait(item):
        put(item, chip, keep_ref).wait()
        put(item, 1 - chip, cross_ref).wait()

    def sum_one(item):
        mate_copy(item).wait_recv()
        mate_part[item] = (
            stage[item % 2, :, core].astype(jnp.float32) + mate_part[item].astype(jnp.float32)
        ).astype(jnp.bfloat16)
        put(item, chip, keep_ref).start()
        put(item, 1 - chip, cross_ref).start()

    def fill_one(item):
        which = item // pieces
        total = jnp.dot(
            lefts[which],
            rights[which // 2, :, piece_columns(item)],
            preferred_element_type=jnp.float32,
        )
        pl.when(item > 1)(lambda: mate_copy(item - 2).wait_send())
        stage[item % 2] = total.astype(jnp.bfloat16).reshape(
            2, 2, units // owners, FILL_COLUMNS
        )
        mate_copy(item).start()
        pl.when(item > 0)(lambda: sum_one(item - 1))

    each = pl.cdiv(total_pieces - FILL_FIRST, rows - 1)

    def fill(step):
        first = jnp.maximum(FILL_FIRST + (step - 1) * each, 0)
        last = jnp.minimum(FILL_FIRST + step * each, total_pieces)

        @pl.loop(0, each)
        def _(item):
            pl.when(first + item < last)(lambda: fill_one(first + item))

    line_gather(grad_ref, grads, *sems[:8], ready, expand)
    load(0).wait()
    load(1).wait()
    acts_copy.wait()
    line_scatter(part, side, lane, tail, out_ref, *sems[8:], reduce, fill)
    sum_one(total_pieces - 1)
    pl.loop(0, total_pieces)(put_wait)
    for item in range(total_pieces - 2, total_pieces):
        mate_copy(item).wait_send()


def ffn_back(grad_ffn, kept, w_parts, owners):
    size, width = grad_ffn.shape
    units = w_parts.shape[1]
    blocks = lax.axis_size("blk")
    rows = blocks // 2
    tokens = blocks * size
    items = 3 * width // FILL_COLUMNS
    whole = pl.BlockSpec(memory_space=pltpu.VMEM)
    far = pl.BlockSpec(memory_space=pl.ANY)
    return pl.pallas_call(
        functools.partial(ffn_back_kernel, owners),
        out_shape=(
            jax.ShapeDtypeStruct((size, width), jnp.float32),
            jax.ShapeDtypeStruct((3, units // owners, width), jnp.bfloat16),
            jax.ShapeDtypeStruct((3, units // owners, width), jnp.bfloat16),
        ),
        in_specs=[whole, far, far, far],
        out_specs=(whole, far, far),
        scratch_shapes=[
            pltpu.VMEM(w_parts.shape, jnp.bfloat16),
            pltpu.VMEM((2, tokens, width), jnp.bfloat16),
            pltpu.VMEM((3, units, tokens), jnp.bfloat16),
            *lane_buffers(rows, size, width),
            pltpu.VMEM((2, 2, 2, units // owners, FILL_COLUMNS), jnp.bfloat16),
            pltpu.VMEM((items, 2, units // owners, FILL_COLUMNS), jnp.bfloat16),
            pltpu.SemaphoreType.DMA((3,)),
            pltpu.SemaphoreType.DMA,
            pltpu.SemaphoreType.DMA,
            pltpu.SemaphoreType.DMA((2,)),
            pltpu.SemaphoreType.DMA((items,)),
            pltpu.SemaphoreType.DMA((items, 2)),
            *line_sems(rows),
            *lane_sems(rows),
        ],
        compiler_params=pltpu.CompilerParams(
            collective_id=3, has_side_effects=True, vmem_limit_bytes=VMEM_BYTES
        ),
        cost_estimate=cost_of(115),
        name="ffn_back",
    )(grad_ffn, *kept, w_parts)


def ffn_hidden(acts, w_parts):
    gate = contract_last(acts, w_parts[0])
    up = contract_last(acts, w_parts[1])
    return (gate, up, (gelu_value(gate) * up).astype(jnp.bfloat16))


def scatter_tokens(partial):
    return lax.psum_scatter(
        partial.astype(jnp.bfloat16), "blk", scatter_dimension=0, tiled=True
    ).astype(jnp.float32)


def ffn_forward_wide(act_ffn, w_parts, middle, cotangent, gains):
    acts = lax.all_gather(act_ffn, "blk", axis=0, tiled=True)
    hidden = ffn_hidden(acts, w_parts)[2]
    partial = jnp.dot(hidden, w_parts[2], preferred_element_type=jnp.float32)
    normed, inverse = norm_parts(scatter_tokens(partial))
    result = (middle + normed * gains[3]).astype(jnp.bfloat16)
    grad_v, gain_row = norm_back(cotangent.astype(jnp.float32), normed, inverse, gains[3])
    return (result, grad_v.astype(jnp.bfloat16), gain_row[None], acts)


def ffn_back_wide(grad_ffn, kept, w_parts, owners):
    (acts,) = kept
    grads = lax.all_gather(grad_ffn, "blk", axis=0, tiled=True)
    gate, up, hidden = ffn_hidden(acts, w_parts)
    grad_hidden = contract_last(grads, w_parts[2])
    grad_gate = (grad_hidden * up * gelu_slope(gate)).astype(jnp.bfloat16)
    grad_up = (grad_hidden * gelu_value(gate)).astype(jnp.bfloat16)
    partial = jnp.dot(grad_gate, w_parts[0], preferred_element_type=jnp.float32) + jnp.dot(
        grad_up, w_parts[1], preferred_element_type=jnp.float32
    )
    sums = jnp.stack(
        [
            jnp.einsum("tf,td->fd", left, right, preferred_element_type=jnp.float32)
            for left, right in ((grad_gate, acts), (grad_up, acts), (hidden, grads))
        ]
    ).astype(jnp.bfloat16)
    units = w_parts.shape[1]
    owned = sums.reshape(3, owners, units // owners, sums.shape[2])
    mine = lax.psum_scatter(
        jnp.transpose(owned, (1, 0, 2, 3)), "sp", scatter_dimension=0, tiled=True
    )
    return (scatter_tokens(partial), mine[0], None)


def cost_of(microseconds):
    return pl.CostEstimate(
        flops=int(microseconds * 1e9), bytes_accessed=int(microseconds * 3e6), transcendentals=0
    )


def push_sp(source, target, sent, landed, peer):
    return pltpu.make_async_remote_copy(
        src_ref=source,
        dst_ref=target,
        send_sem=sent,
        recv_sem=landed,
        device_id={"sp": peer},
        device_id_type=pl.DeviceIdType.MESH,
    )


def greet_sp(me, groups):
    barrier = pltpu.get_barrier_semaphore()
    for step in range(1, groups):
        pl.semaphore_signal(
            barrier,
            inc=1,
            device_id={"sp": (me + step) % groups},
            device_id_type=pl.DeviceIdType.MESH,
        )
    pl.semaphore_wait(barrier, groups - 1)


def gather_rows(x, w_ref, full_ref, w, w_done, own_done, sent, landed, prepare, project):
    me = lax.axis_index("sp")
    size = x.shape[0]
    units = w.shape[0]
    mate = me + 1 - 2 * (me % 2)
    across = (me + 2) % 4

    def spot(member):
        return full_ref.at[pl.ds(pl.multiple_of(member * size, size), size), :]

    load = pltpu.make_async_copy(
        w_ref.at[pl.ds(pl.multiple_of(me * units, units), units), :], w, w_done
    )
    load.start()
    prepare()
    greet_sp(me, 4)
    over = push_sp(x, spot(me), sent.at[0], landed.at[0], across)
    over.start()
    beside = push_sp(x, spot(me), sent.at[1], landed.at[1], mate)
    beside.start()
    keep = pltpu.make_async_copy(x, spot(me), own_done)
    keep.start()
    keep.wait()
    load.wait()

    def project_chip(chip):
        rows = pl.ds(pl.multiple_of(chip * 2 * size, 2 * size), 2 * size)
        project(rows, contract_last(full_ref[rows, :], w[...]).astype(jnp.bfloat16))

    beside.wait_recv()
    project_chip(me // 2)
    over.wait_recv()
    onward = push_sp(spot(across), spot(across), sent.at[2], landed.at[2], mate)
    onward.start()
    onward.wait_recv()
    project_chip(across // 2)
    over.wait_send()
    beside.wait_send()
    onward.wait_send()


def project_in_kernel(tokens_ref, gains_ref, w_ref, full_ref, out_ref, x, *scratch):
    def prepare():
        normed = norm_parts(tokens_ref[...].astype(jnp.float32))[0]
        x[...] = (normed * gains_ref[0:1, :]).astype(jnp.bfloat16)

    def project(rows, value):
        out_ref[rows, :] = value

    gather_rows(x, w_ref, full_ref, *scratch, prepare, project)


def gather_scratch(size, width, units):
    dma = pltpu.SemaphoreType.DMA
    return [
        pltpu.VMEM((size, width), jnp.bfloat16),
        pltpu.VMEM((units, width), jnp.bfloat16),
        dma,
        dma,
        dma((3,)),
        dma((3,)),
    ]


def project_in(tokens, gains, weights):
    size, width = tokens.shape
    units = weights.shape[0] // 4
    whole = pl.BlockSpec(memory_space=pltpu.VMEM)
    return pl.pallas_call(
        project_in_kernel,
        out_shape=(
            jax.ShapeDtypeStruct((4 * size, width), jnp.bfloat16),
            jax.ShapeDtypeStruct((4 * size, units), jnp.bfloat16),
        ),
        in_specs=[whole, whole, pl.BlockSpec(memory_space=pl.ANY)],
        out_specs=(whole, whole),
        scratch_shapes=gather_scratch(size, width, units),
        compiler_params=pltpu.CompilerParams(
            collective_id=4, has_side_effects=True, vmem_limit_bytes=VMEM_BYTES
        ),
        cost_estimate=cost_of(18),
        name="project_in",
    )(tokens, gains, weights)


def project_back_kernel(
    grad_ref,
    middle_ref,
    attn_ref,
    cotangent_ref,
    gains_ref,
    attended_ref,
    by_row_ref,
    totals_ref,
    w_ref,
    full_ref,
    scaled_ref,
    delta_ref,
    grad_middle_ref,
    rows_ref,
    x,
    *scratch,
):
    def prepare():
        grad_v, row_two = norm_back(
            grad_ref[...], *norm_parts(middle_ref[...]), gains_ref[2:3, :]
        )
        grad_middle = cotangent_ref[...].astype(jnp.float32) + grad_v
        grad_middle_ref[...] = grad_middle
        grad_v, row_one = norm_back(grad_middle, *norm_parts(attn_ref[...]), gains_ref[1:2, :])
        x[...] = grad_v.astype(jnp.bfloat16)
        rows_ref[...] = jnp.zeros_like(rows_ref)
        rows_ref[1:2, :] = row_one[None, :]
        rows_ref[2:3, :] = row_two[None, :]

    def project(rows, value):
        for head in range(value.shape[1] // HEAD):
            columns = slice(head * HEAD, (head + 1) * HEAD)
            grad = value[:, columns].astype(jnp.float32)
            scaled_ref[rows, columns] = (grad / by_row_ref[head, rows, :1]).astype(jnp.bfloat16)
            product = grad * attended_ref[rows, columns]
            delta_ref[head, :, rows] = (
                jnp.sum(product.T, axis=0, keepdims=True) / totals_ref[head, :, rows]
            )

    gather_rows(x, w_ref, full_ref, *scratch, prepare, project)


def project_back(
    grad_act, middle, attn, cotangent, gains, attended, by_row, totals, weights
):
    size, width = attn.shape
    units = weights.shape[0] // 4
    whole = pl.BlockSpec(memory_space=pltpu.VMEM)
    return pl.pallas_call(
        project_back_kernel,
        out_shape=(
            jax.ShapeDtypeStruct((4 * size, width), jnp.bfloat16),
            jax.ShapeDtypeStruct((4 * size, units), jnp.bfloat16),
            jax.ShapeDtypeStruct(totals.shape, jnp.float32),
            jax.ShapeDtypeStruct((size, width), jnp.float32),
            jax.ShapeDtypeStruct((8, width), jnp.float32),
        ),
        in_specs=[whole] * 8 + [pl.BlockSpec(memory_space=pl.ANY)],
        out_specs=(whole,) * 5,
        scratch_shapes=gather_scratch(size, width, units),
        compiler_params=pltpu.CompilerParams(
            collective_id=6, has_side_effects=True, vmem_limit_bytes=VMEM_BYTES
        ),
        cost_estimate=cost_of(20),
        name="project_back",
    )(grad_act, middle, attn, cotangent, gains, attended, by_row, totals, weights)


def exchange_norm_kernel(x_ref, w_ref, tokens_ref, gains_ref, out_ref, middle_ref, act_ref, *scratch):
    exchange_project_kernel(x_ref, w_ref, out_ref, *scratch)
    normed = norm_parts(out_ref[...])[0]
    middle = tokens_ref[...].astype(jnp.float32) + normed * gains_ref[1:2, :]
    middle_ref[...] = middle
    act_ref[...] = (norm_parts(middle)[0] * gains_ref[2:3, :]).astype(jnp.bfloat16)


def exchange_project_kernel(x_ref, w_ref, out_ref, w, got, w_done, own_done, sent, landed):
    me = lax.axis_index("sp")
    size = out_ref.shape[0]
    units = x_ref.shape[1]

    def rows_of(member):
        return x_ref.at[pl.ds(pl.multiple_of(member * size, size), size), :]

    def load(member):
        rows = pl.ds(pl.multiple_of(member * units, units), units)
        return pltpu.make_async_copy(w_ref.at[rows, :], w.at[rows, :], w_done.at[member])

    def send(step):
        peer = (me + step) % 4
        return push_sp(rows_of(peer), got.at[4 - step], sent.at[step], landed.at[4 - step], peer)

    greet_sp(me, 4)
    for step in (2, 1, 3):
        send(step).start()
    keep = pltpu.make_async_copy(rows_of(me), got.at[0], own_done)
    keep.start()
    for step in range(4):
        load((me + step) % 4).start()
    keep.wait()
    for step in (0, 1, 3, 2):
        member = (me + step) % 4
        load(member).wait()
        if step > 0:
            send(4 - step).wait_recv()
        rows = pl.ds(pl.multiple_of(member * units, units), units)
        term = jnp.dot(got[step], w[rows, :], preferred_element_type=jnp.float32)
        if step == 0:
            out_ref[...] = term
        else:
            out_ref[...] += term
    for step in (1, 2, 3):
        send(step).wait_send()


def exchange_project(columns, weights, identity, norm_inputs=()):
    size = columns.shape[0] // 4
    whole = pl.BlockSpec(memory_space=pltpu.VMEM)
    total = jax.ShapeDtypeStruct((size, weights.shape[1]), jnp.float32)
    low = jax.ShapeDtypeStruct(total.shape, jnp.bfloat16)
    shapes = [total, total, low] if norm_inputs else [total]
    return pl.pallas_call(
        exchange_norm_kernel if norm_inputs else exchange_project_kernel,
        out_shape=shapes,
        in_specs=[whole, pl.BlockSpec(memory_space=pl.ANY)] + [whole] * len(norm_inputs),
        out_specs=[whole] * len(shapes),
        scratch_shapes=[
            pltpu.VMEM(weights.shape, jnp.bfloat16),
            pltpu.VMEM((4, size, columns.shape[1]), jnp.bfloat16),
            pltpu.SemaphoreType.DMA((4,)),
            pltpu.SemaphoreType.DMA,
            pltpu.SemaphoreType.DMA((4,)),
            pltpu.SemaphoreType.DMA((4,)),
        ],
        compiler_params=pltpu.CompilerParams(
            collective_id=identity, has_side_effects=True, vmem_limit_bytes=VMEM_BYTES
        ),
        cost_estimate=cost_of(16),
        name="exchange_project",
    )(columns, weights, *norm_inputs)


def finish_kernel(
    cols_ref,
    act_ref,
    att_ref,
    grad_ref,
    w_ref,
    tokens_ref,
    middle_ref,
    gains_in_ref,
    rows_ref,
    row_three_ref,
    cross_ref,
    qkv_ref,
    out_ref,
    tokens_grad_ref,
    gains_ref,
    far_ref,
    w,
    got,
    grad_in,
    total,
    part,
    side,
    lane,
    tail,
    mine,
    from_sp,
    from_side,
    from_line,
    w_done,
    own_done,
    swap_sent,
    swap_landed,
    sp_sent,
    sp_landed,
    gain_side,
    line_sent,
    line_landed,
    cross_sent,
    cross_landed,
    *sems,
):
    at = lax.axis_index("blk")
    me = lax.axis_index("sp")
    rows = lax.axis_size("blk") // 2
    line, column = at // 2, at % 2
    partner = at + 1 - 2 * column
    block = total.shape[0]
    size = tokens_ref.shape[0]
    units = cols_ref.shape[1]
    extra = block - size

    barrier = pltpu.get_barrier_semaphore()
    for step in range(1, 4):
        pl.semaphore_signal(
            barrier, inc=1, device_id={"sp": (me + step) % 4}, device_id_type=pl.DeviceIdType.MESH
        )

    def line_peer(step):
        return 2 * ((line + step) % rows) + column

    for peer in [partner] + [line_peer(step) for step in range(1, rows)]:
        pl.semaphore_signal(
            barrier, inc=1, device_id={"blk": peer}, device_id_type=pl.DeviceIdType.MESH
        )

    def load(member):
        span = pl.ds(pl.multiple_of(member * units, units), units)
        return pltpu.make_async_copy(w_ref.at[span, :], w.at[span, :], w_done.at[member])

    def rows_of(member):
        return cols_ref.at[pl.ds(pl.multiple_of(member * size, size), size), :]

    def swap(step):
        peer = (me + step) % 4
        return push_sp(
            rows_of(peer), got.at[4 - step], swap_sent.at[step], swap_landed.at[4 - step], peer
        )

    for step in range(4):
        load((me + step) % 4).start()
    keep = pltpu.make_async_copy(rows_of(me), got.at[0], own_done)
    keep.start()
    pl.semaphore_wait(barrier, 3 + rows)
    for step in (2, 1, 3):
        swap(step).start()
    over = carry(
        cross_ref, far_ref, far_ref.shape[1], cross_sent, cross_landed, (me + 2) % 4
    )
    over.start()
    keep.wait()

    def sp_gains(step):
        return push_sp(
            mine, from_sp.at[4 - step], sp_sent.at[step], sp_landed.at[4 - step], (me + step) % 4
        )

    def side_gains():
        return push(from_sp.at[0], from_side, gain_side.at[0], gain_side.at[1], partner)

    def line_gains(step):
        return push(
            from_line.at[0],
            from_line.at[rows - step],
            line_sent.at[step],
            line_landed.at[rows - step],
            line_peer(step),
        )

    def reduce(target):
        dims = (((0,), (0,)), ((), ()))
        wide_columns = pl.ds(pl.multiple_of(target * 2 * size, 2 * size), 2 * size)
        term = lax.dot_general(
            cols_ref[:, wide_columns], act_ref[...], dims, preferred_element_type=jnp.float32
        ).astype(jnp.bfloat16)
        columns = pl.ds(pl.multiple_of(target * 2 * extra, 2 * extra), 2 * extra)
        more = lax.dot_general(
            att_ref[:, columns], grad_ref[...], dims, preferred_element_type=jnp.float32
        ).astype(jnp.bfloat16)
        for half in range(2):
            start = pl.multiple_of((2 * target + half) * block, block)
            part[pl.ds(start, size), :] = term[half * size : (half + 1) * size]
            start = pl.multiple_of((2 * target + half) * block + size, extra)
            part[pl.ds(start, extra), :] = more[half * extra : (half + 1) * extra]

    def inputs_back():
        for step in (0, 1, 3, 2):
            member = (me + step) % 4
            load(member).wait()
            if step > 0:
                swap(4 - step).wait_recv()
            span = pl.ds(pl.multiple_of(member * units, units), units)
            term = jnp.dot(got[step], w[span, :], preferred_element_type=jnp.float32)
            if step == 0:
                grad_in[...] = term
            else:
                grad_in[...] += term
        normed, inverse = norm_parts(tokens_ref[...].astype(jnp.float32))
        grad_v, gain_row = norm_back(grad_in[...], normed, inverse, gains_in_ref[0:1, :])
        tokens_grad_ref[...] = (middle_ref[...] + grad_v).astype(jnp.bfloat16)
        mine[...] = rows_ref[...]
        mine[0:1, :] = gain_row[None, :]
        mine[3:4, :] = row_three_ref[...]
        for step in range(1, 4):
            sp_gains(step).start()

    def fill(step):
        pl.when(step == 2)(inputs_back)

        @pl.when(step == 3)
        def _():
            gains = mine[...]
            for other in range(1, 4):
                sp_gains(4 - other).wait_recv()
                gains = gains + from_sp[other]
            from_sp[0] = gains
            side_gains().start()

        @pl.when(step == 3)
        def _():
            side_gains().wait_recv()
            from_line[0] = from_sp[0] + from_side[...]
            for other in range(1, rows):
                line_gains(other).start()

    line_scatter(part, side, lane, tail, total, *sems, reduce, fill)
    qkv_ref[...] = total[:size]
    out_ref[...] = total[size:]
    gains = from_line[0]
    for other in range(1, rows):
        line_gains(rows - other).wait_recv()
        gains = gains + from_line[other]
    gains_ref[...] = gains
    for step in (1, 2, 3):
        swap(step).wait_send()
        sp_gains(step).wait_send()
    over.wait()
    side_gains().wait_send()
    for step in range(1, rows):
        line_gains(step).wait_send()


def finish(
    cols, act_block, attended, grad_block, w_qkv, tokens, grad_middle, gains, rows, row_three, cross
):
    blocks = lax.axis_size("blk")
    lines = blocks // 2
    size, width = tokens.shape
    block = (cols.shape[1] + attended.shape[1]) // blocks
    whole = pl.BlockSpec(memory_space=pltpu.VMEM)
    any_space = pl.BlockSpec(memory_space=pl.ANY)
    dma = pltpu.SemaphoreType.DMA
    small = rows.shape
    return pl.pallas_call(
        finish_kernel,
        out_shape=(
            jax.ShapeDtypeStruct((cols.shape[1] // blocks, width), jnp.float32),
            jax.ShapeDtypeStruct((attended.shape[1] // blocks, width), jnp.float32),
            jax.ShapeDtypeStruct((size, width), jnp.bfloat16),
            jax.ShapeDtypeStruct(small, jnp.float32),
            half_of(cross),
        ),
        in_specs=[whole] * 4 + [any_space] + [whole] * 5 + [any_space],
        out_specs=(whole, whole, whole, whole, any_space),
        scratch_shapes=[
            pltpu.VMEM(w_qkv.shape, jnp.bfloat16),
            pltpu.VMEM((4, size, cols.shape[1]), jnp.bfloat16),
            pltpu.VMEM((size, width), jnp.float32),
            pltpu.VMEM((block, width), jnp.float32),
            *lane_buffers(lines, block, width),
            pltpu.VMEM(small, jnp.float32),
            pltpu.VMEM((4, *small), jnp.float32),
            pltpu.VMEM(small, jnp.float32),
            pltpu.VMEM((lines, *small), jnp.float32),
            dma((4,)),
            dma,
            dma((4,)),
            dma((4,)),
            dma((4,)),
            dma((4,)),
            dma((2,)),
            dma((lines,)),
            dma((lines,)),
            dma,
            dma,
            *lane_sems(lines),
        ],
        compiler_params=pltpu.CompilerParams(
            collective_id=8, has_side_effects=True, vmem_limit_bytes=VMEM_BYTES
        ),
        cost_estimate=cost_of(85),
        name="finish",
    )(
        cols,
        act_block,
        attended,
        grad_block,
        w_qkv,
        tokens,
        grad_middle,
        gains,
        rows,
        row_three,
        cross,
    )


def weight_sums_wide(left, right):
    term = jnp.einsum("tc,td->cd", left, right, preferred_element_type=jnp.float32)
    return scatter_tokens(term)


def finish_wide(
    cols, act_block, attended, grad_block, w_qkv, tokens, grad_middle, gains, rows, row_three, cross
):
    (grad_act_in,) = exchange_project(cols, w_qkv, 7)
    normed, inverse = norm_parts(tokens.astype(jnp.float32))
    grad_v, gain_row = norm_back(grad_act_in, normed, inverse, gains[0])
    gains_all = lax.psum(
        jnp.concatenate([gain_row[None], rows[1:3], row_three, rows[4:]]), ("blk", "sp")
    )
    return (
        weight_sums_wide(cols, act_block),
        weight_sums_wide(attended, grad_block),
        (grad_middle + grad_v).astype(jnp.bfloat16),
        gains_all,
        None,
    )


def body(tokens, w_qkv, w_out, gains, w_ffn, cotangent):
    groups = lax.axis_size("sp")
    wide = lax.axis_size("blk") > 8
    act_block, projected = project_in(tokens, gains, w_qkv)
    attended_low, attended, totals, by_row, kv_all = attend(projected, HEADS // groups)
    attn, middle, act_ffn = exchange_project(attended_low, w_out, 5, (tokens, gains))
    w_parts = jnp.transpose(w_ffn, (1, 0, 2))
    result, grad_ffn, row_three, *kept = (ffn_forward_wide if wide else ffn_forward)(
        act_ffn, w_parts, middle, cotangent, gains
    )
    grad_act_ffn, ffn_part, cross = (ffn_back_wide if wide else ffn_back)(
        grad_ffn, kept, w_parts, groups
    )
    grad_block, scaled, delta, grad_middle, rows = project_back(
        grad_act_ffn, middle, attn, cotangent, gains, attended, by_row, totals, w_out
    )
    grad_cols, *far_first = attend_back(projected, scaled, delta, kv_all, cross)
    qkv_grad, out_grad, tokens_grad, gains_all, far_last = (finish_wide if wide else finish)(
        grad_cols,
        act_block,
        attended_low,
        grad_block,
        w_qkv,
        tokens,
        grad_middle,
        gains,
        rows,
        row_three,
        cross,
    )
    ffn_sum = ffn_part.astype(jnp.float32)
    if not wide:
        ffn_sum = ffn_sum + jnp.concatenate([*far_first, far_last], axis=1).astype(jnp.float32)
    ffn_grad = jnp.transpose(ffn_sum, (1, 0, 2))
    share = gains_all.shape[1] // (groups * lax.axis_size("blk"))
    place = lax.axis_index("sp") * lax.axis_size("blk") + lax.axis_index("blk")
    gains_grad = lax.dynamic_slice_in_dim(gains_all[:4], place * share, share, 1)
    return (result, tokens_grad, qkv_grad, out_grad, gains_grad, ffn_grad)


def solution(mesh):
    return jax.shard_map(
        body,
        mesh=mesh,
        in_specs=(
            P(("blk", "sp"), None),
            P(),
            P(),
            P(),
            P("blk", None, None),
            P(("blk", "sp"), None),
        ),
        out_specs=(
            P(("blk", "sp"), None),
            P(("blk", "sp"), None),
            P(("sp", "blk"), None),
            P(("sp", "blk"), None),
            P(None, ("sp", "blk")),
            P(("blk", "sp"), None, None),
        ),
        check_vma=False,
    )
```

```python
import functools

import jax
import jax.numpy as jnp
from jax import lax
from jax.experimental import pallas as pl
from jax.experimental.pallas import tpu as pltpu
from jax.sharding import PartitionSpec as P

HEADS = 8
KV_HEADS = 4
HEAD = 256


VMEM_BYTES = 62 * 1024 * 1024
PIECES = 2
NORM_EPSILON = 1e-06
CAP_VALUE = 50.0
GELU_SCALE = 0.7978845608028654
GELU_CUBIC = 0.044715


def norm_parts(values):
    inverse = lax.rsqrt(jnp.mean(values * values, axis=-1, keepdims=True) + NORM_EPSILON)
    return (values * inverse, inverse)


def norm_back(grad_y, normed, inverse, gain):
    grad_n = grad_y * gain
    grad_v = inverse * (grad_n - normed * jnp.mean(grad_n * normed, axis=-1, keepdims=True))
    return (grad_v, jnp.sum(grad_y * normed, axis=0))


def gelu_value(values):
    return (
        0.5
        * values
        * (1.0 + jnp.tanh(GELU_SCALE * (values + GELU_CUBIC * values * values * values)))
    )


def gelu_slope(values):
    bent = jnp.tanh(GELU_SCALE * (values + GELU_CUBIC * values * values * values))
    return 0.5 * (1.0 + bent) + 0.5 * values * (1.0 - bent * bent) * GELU_SCALE * (
        1.0 + 3.0 * GELU_CUBIC * values * values
    )


def contract_last(left, right):
    return lax.dot_general(
        left, right, (((1,), (1,)), ((), ())), preferred_element_type=jnp.float32
    )


def push(source, target, sent, landed, block):
    return pltpu.make_async_remote_copy(
        src_ref=source,
        dst_ref=target,
        send_sem=sent,
        recv_sem=landed,
        device_id={"blk": block},
        device_id_type=pl.DeviceIdType.MESH,
    )


def greet(at, line, rows, sp_peer=None):
    barrier = pltpu.get_barrier_semaphore()
    others = 1
    if sp_peer is not None:
        others = 2
        pl.semaphore_signal(
            barrier, inc=1, device_id={"sp": sp_peer}, device_id_type=pl.DeviceIdType.MESH
        )

    def tell(block):
        pl.semaphore_signal(
            barrier, inc=1, device_id={"blk": block}, device_id_type=pl.DeviceIdType.MESH
        )

    tell(at + 1 - 2 * (at % 2))
    pl.when(line > 0)(lambda: tell(at - 2))
    pl.when(line < rows - 1)(lambda: tell(at + 2))
    pl.semaphore_wait(barrier, others + jnp.minimum(line, 1) + jnp.minimum(rows - 1 - line, 1))


def both(*terms):
    result = terms[0]
    for term in terms[1:]:
        result = jnp.logical_and(result, term)
    return result


def attend_kernel(
    heads,
    x_ref,
    low_ref,
    att_ref,
    tot_ref,
    by_row_ref,
    kv_ref,
    kv,
    acc,
    part,
    up_sent,
    up_landed,
    side_sent,
    side_landed,
    extra_sent,
    extra_landed,
    own_done,
    save_done,
):
    at = lax.axis_index("blk")
    blocks = lax.axis_size("blk")
    rows = blocks // 2
    line, column = at // 2, at % 2
    partner = at + 1 - 2 * column
    size = x_ref.shape[0]
    first = heads * HEAD
    own = x_ref.at[:, pl.ds(first, 2 * HEAD)]
    greet(at, line, rows)

    def halves(act):
        pl.loop(0, PIECES)(act)

    def span(piece):
        count = size // PIECES
        return pl.ds(pl.multiple_of(piece * count, count), count)

    def source_of(index, piece, is_own):
        if is_own:
            return x_ref.at[span(piece), pl.ds(first, 2 * HEAD)]
        return kv.at[index, span(piece)]

    def up_copy(index, piece, is_own=False):
        return push(
            source_of(index, piece, is_own),
            kv.at[index, span(piece)],
            up_sent.at[index // 2, piece],
            up_landed.at[index // 2, piece],
            at + 2,
        )

    def side_copy(index, piece, is_own=False):
        return push(
            source_of(index, piece, is_own),
            kv.at[index, span(piece)],
            side_sent.at[index // 2, piece],
            side_landed.at[index // 2, piece],
            partner,
        )

    def extra_copy():
        rows_now = kv.at[0, span(PIECES - 1)]
        return push(rows_now, rows_now, extra_sent.at[0], extra_landed.at[0], at + 2)

    def crossing(index):
        return jnp.where(both(index == 0, at > 0), PIECES - 1, PIECES)

    def save(index):
        return pltpu.make_async_copy(kv.at[index], kv_ref.at[index], save_done.at[index])

    @pl.loop(0, PIECES)
    def _(piece):
        pl.when(line < rows - 1)(lambda: up_copy(at, piece, True).start())
        pl.when(column == 0)(lambda: side_copy(at, PIECES - 1 - piece, True).start())

    keep = pltpu.make_async_copy(own, kv.at[at], own_done)
    keep.start()
    acc[...] = jnp.zeros_like(acc)
    part[...] = jnp.zeros_like(part)
    keep.wait()

    @pl.when(at == 1)
    def _():
        side_copy(0, PIECES - 1).wait_recv()
        extra_copy().start()

    ahead = lax.broadcasted_iota(jnp.int32, (size, size), 1) - lax.broadcasted_iota(
        jnp.int32, (size, size), 0
    )

    def compute(index):
        save(index).start()
        span = (at - index) * size
        for head in range(heads):
            raw = lax.dot_general(
                x_ref[:, head * HEAD : (head + 1) * HEAD],
                kv[index, :, :HEAD],
                (((1,), (1,)), ((), ())),
                preferred_element_type=jnp.float32,
            )
            weights = jnp.exp(CAP_VALUE * jnp.tanh(raw * (HEAD ** (-0.5) / CAP_VALUE)))
            weights = jnp.where(ahead <= span, weights, 0.0)
            total = weights[:, :128]
            for piece in range(1, size // 128):
                total = total + weights[:, piece * 128 : (piece + 1) * 128]
            part[head] += total
            acc[:, head * HEAD : (head + 1) * HEAD] += jnp.dot(
                weights.astype(jnp.bfloat16),
                kv[index, :, HEAD:],
                preferred_element_type=jnp.float32,
            )

    @pl.loop(0, rows + 1)
    def _(step):
        source = line - step
        index = 2 * source + column

        @pl.when(both(step > 0, source >= 0))
        def _():
            @pl.loop(0, PIECES)
            def _(piece):
                up_copy(index, piece).wait_recv()
                pl.when(line < rows - 1)(lambda: up_copy(index, piece).start())
                pl.when(piece < crossing(index))(lambda: side_copy(index, piece).start())

        @pl.when(both(step > 0, source == 0, column == 1))
        def _():
            extra_copy().wait_recv()
            pl.when(line < rows - 1)(lambda: extra_copy().start())

        @pl.loop(0, 2)
        def _(way):
            found = source + way
            here = 2 * found + jnp.where(way == 0, column, 1 - column)
            due = jnp.logical_or(way == 0, both(step > 0, jnp.logical_or(step > 1, column == 1)))

            @pl.when(both(found >= 0, due))
            def _():
                pl.when(way == 1)(
                    lambda: pl.loop(0, crossing(here))(
                        lambda piece: side_copy(here, piece).wait_recv()
                    )
                )
                compute(here)

    for head in range(heads):
        columns = slice(head * HEAD, (head + 1) * HEAD)
        total = jnp.sum(part[head], axis=1, keepdims=True)
        by_row_ref[head] = jnp.broadcast_to(total, by_row_ref.shape[1:])
        value = acc[:, columns] / total
        att_ref[:, columns] = value
        low_ref[:, columns] = value.astype(jnp.bfloat16)
        tot_ref[head] = jnp.sum(part[head].T, axis=0, keepdims=True)

    @pl.loop(0, rows)
    def _(source):
        index = 2 * source + column

        @pl.when(source <= line)
        def _():
            pl.when(line < rows - 1)(
                lambda: halves(lambda piece: up_copy(index, piece).wait_send())
            )
            pl.when(jnp.logical_or(source < line, column == 0))(
                lambda: pl.loop(0, crossing(index))(
                    lambda piece: side_copy(index, piece).wait_send()
                )
            )

    pl.when(both(column == 1, line < rows - 1))(lambda: extra_copy().wait_send())

    @pl.loop(0, blocks)
    def _(index):
        pl.when(index <= at)(lambda: save(index).wait())


def attend(projected, heads):
    size = projected.shape[0]
    blocks = lax.axis_size("blk")
    whole = pl.BlockSpec(memory_space=pltpu.VMEM)
    return pl.pallas_call(
        functools.partial(attend_kernel, heads),
        out_shape=(
            jax.ShapeDtypeStruct((size, heads * HEAD), jnp.bfloat16),
            jax.ShapeDtypeStruct((size, heads * HEAD), jnp.float32),
            jax.ShapeDtypeStruct((heads, 1, size), jnp.float32),
            jax.ShapeDtypeStruct((heads, size, 128), jnp.float32),
            jax.ShapeDtypeStruct((blocks, size, 2 * HEAD), jnp.bfloat16),
        ),
        in_specs=[whole],
        out_specs=(whole, whole, whole, whole, pl.BlockSpec(memory_space=pl.ANY)),
        scratch_shapes=[
            pltpu.VMEM((blocks, size, 2 * HEAD), jnp.bfloat16),
            pltpu.VMEM((size, heads * HEAD), jnp.float32),
            pltpu.VMEM((heads, size, 128), jnp.float32),
            pltpu.SemaphoreType.DMA((blocks // 2, PIECES)),
            pltpu.SemaphoreType.DMA((blocks // 2, PIECES)),
            pltpu.SemaphoreType.DMA((blocks // 2, PIECES)),
            pltpu.SemaphoreType.DMA((blocks // 2, PIECES)),
            pltpu.SemaphoreType.DMA((1,)),
            pltpu.SemaphoreType.DMA((1,)),
            pltpu.SemaphoreType.DMA,
            pltpu.SemaphoreType.DMA((blocks,)),
        ],
        compiler_params=pltpu.CompilerParams(
            collective_id=0, has_side_effects=True, vmem_limit_bytes=VMEM_BYTES
        ),
        cost_estimate=cost_of(50),
        name="attend",
    )(projected)


def carry(cross_ref, far_ref, first, sent, landed, across):
    return push_sp(
        cross_ref.at[:, pl.ds(first, far_ref.shape[1]), :], far_ref, sent, landed, across
    )


def attend_back_kernel(heads, carried, *refs):
    if carried:
        x_ref, scaled_ref, delta_ref, kv_ref, cross_ref, out_ref, far_ref, *scratch = refs
        *scratch, cross_sent, cross_landed = scratch
        across = (lax.axis_index("sp") + 2) % 4
        over = carry(cross_ref, far_ref, 0, cross_sent, cross_landed, across)
        after = over.start
    else:
        x_ref, scaled_ref, delta_ref, kv_ref, out_ref, *scratch = refs
        across, after = None, lambda: None
    attend_back_steps(
        heads, across, after, x_ref, scaled_ref, delta_ref, kv_ref, out_ref, *scratch
    )
    if carried:
        over.wait()


def attend_back_steps(
    heads,
    across,
    after_greeting,
    x_ref,
    scaled_ref,
    delta_ref,
    kv_ref,
    out_ref,
    kv,
    part,
    side,
    down,
    dq,
    dk,
    dv,
    load_done,
    side_sent,
    side_landed,
    down_sent,
    down_landed,
    extra,
    extra_done,
):
    at = lax.axis_index("blk")
    blocks = lax.axis_size("blk")
    rows = blocks // 2
    line, column = at // 2, at % 2
    partner = at + 1 - 2 * column
    size = x_ref.shape[0]

    def load(index):
        return pltpu.make_async_copy(kv_ref.at[index], kv.at[index], load_done.at[index])

    @pl.loop(0, blocks)
    def _(index):
        pl.when(index <= at)(lambda: load(index).start())

    greet(at, line, rows, across)
    after_greeting()

    def halves(act):
        pl.loop(0, PIECES)(act)

    def span(piece):
        count = size // PIECES
        return pl.ds(pl.multiple_of(piece * count, count), count)

    def side_copy(target, piece):
        return push(
            part.at[target, 1 - column, span(piece)],
            side.at[target, span(piece)],
            side_sent.at[target, piece],
            side_landed.at[target, piece],
            partner,
        )

    def down_copy(target, piece):
        return push(
            part.at[target, column, span(piece)],
            down.at[target, span(piece)],
            down_sent.at[target, piece],
            down_landed.at[target, piece],
            at - 2,
        )

    def extra_copy():
        return push(
            part.at[0, 0, span(PIECES - 1)], extra, extra_done.at[0], extra_done.at[1], at - 2
        )

    def crossing(target, receives):
        fewer = both(target == 0, line > 0, column == (0 if receives else 1))
        return jnp.where(fewer, PIECES - 1, PIECES)

    def extra_step():
        @pl.when(line < rows - 1)
        def _():
            extra_copy().wait_recv()
            part[0, 0, span(PIECES - 1)] = (
                part[0, 0, span(PIECES - 1)].astype(jnp.float32) + extra[...].astype(jnp.float32)
            ).astype(jnp.bfloat16)

        pl.when(line > 0)(lambda: extra_copy().start())
        pl.when(line == 0)(lambda: side_copy(0, PIECES - 1).start())

    dq[...] = jnp.zeros_like(dq)
    ahead = lax.broadcasted_iota(jnp.int32, (size, size), 0) - lax.broadcasted_iota(
        jnp.int32, (size, size), 1
    )

    def compute(target, half):
        index = 2 * target + half
        load(index).wait()
        span = (at - index) * size
        for head in range(heads):
            columns = slice(head * HEAD, (head + 1) * HEAD)
            query = x_ref[:, columns]
            scaled = scaled_ref[:, columns]
            key = kv[index, :, :HEAD]
            raw = lax.dot_general(
                key, query, (((1,), (1,)), ((), ())), preferred_element_type=jnp.float32
            )
            squashed = jnp.tanh(raw * (HEAD ** (-0.5) / CAP_VALUE))
            weights = jnp.exp(CAP_VALUE * squashed)
            weights = jnp.where(ahead <= span, weights, 0.0)
            inner = lax.dot_general(
                kv[index, :, HEAD:],
                scaled,
                (((1,), (1,)), ((), ())),
                preferred_element_type=jnp.float32,
            )
            grad_raw = (
                weights * (inner - delta_ref[head]) * (1.0 - squashed * squashed)
            ).astype(jnp.bfloat16)
            dv_now = jnp.dot(
                weights.astype(jnp.bfloat16), scaled, preferred_element_type=jnp.float32
            )
            dk_now = jnp.dot(grad_raw, query, preferred_element_type=jnp.float32)
            dq[:, columns] += lax.dot_general(
                grad_raw, key, (((0,), (0,)), ((), ())), preferred_element_type=jnp.float32
            )
            if head == 0:
                dv[...] = dv_now
                dk[...] = dk_now
            else:
                dv[...] += dv_now
                dk[...] += dk_now
        part[target, half, :, :HEAD] = (dk[...] * HEAD ** (-0.5)).astype(jnp.bfloat16)
        part[target, half, :, HEAD:] = dv[...].astype(jnp.bfloat16)

    def merge(target):
        def add(piece, more):
            part[target, column, span(piece)] = (
                part[target, column, span(piece)].astype(jnp.float32) + more.astype(jnp.float32)
            ).astype(jnp.bfloat16)

        def merge_piece(piece):
            meets = jnp.logical_or(target < line, column == 0)

            @pl.when(both(meets, piece < crossing(target, True)))
            def _():
                side_copy(target, piece).wait_recv()
                add(piece, side[target, span(piece)])

            @pl.when(line < rows - 1)
            def _():
                down_copy(target, piece).wait_recv()
                add(piece, down[target, span(piece)])

            pl.when(target < line)(lambda: down_copy(target, piece).start())

        pl.when(both(column == 1, target == 0, line == 0))(extra_step)
        halves(merge_piece)

        @pl.when(target == line)
        def _():
            out_ref[:, heads * HEAD :] = part[target, column]

    @pl.loop(0, rows)
    def _(target):
        away = jnp.logical_or(target < line, both(target == line, column == 1))

        @pl.loop(0, 2)
        def _(way):
            @pl.when(jnp.logical_or(both(way == 0, away), both(way == 1, target <= line)))
            def _():
                compute(target, jnp.where(way == 0, 1 - column, column))

                @pl.when(way == 0)
                def _():
                    now = jnp.where(at == 1, PIECES - 1, crossing(target, False))
                    pl.loop(0, now)(lambda piece: side_copy(target, piece).start())
                    due = jnp.where(line == rows - 1, target == 0, both(target == 1, line > 0))
                    pl.when(both(column == 1, due))(extra_step)

            pl.when(both(way == 0, line == rows - 1, target > 0))(lambda: merge(target - 1))


    out_ref[:, : heads * HEAD] = (dq[...] * HEAD ** (-0.5)).astype(jnp.bfloat16)

    @pl.loop(0, rows)
    def _(target):
        pl.when(both(target <= line, jnp.logical_or(line < rows - 1, target == rows - 1)))(
            lambda: merge(target)
        )

    @pl.loop(0, rows)
    def _(target):
        pl.when(jnp.logical_or(target < line, both(target == line, column == 1)))(
            lambda: pl.loop(0, crossing(target, False))(
                lambda piece: side_copy(target, piece).wait_send()
            )
        )
        pl.when(target < line)(lambda: halves(lambda piece: down_copy(target, piece).wait_send()))

    pl.when(both(column == 1, line > 0))(lambda: extra_copy().wait_send())


def half_of(cross):
    kinds, units, width = cross.shape
    return jax.ShapeDtypeStruct((kinds, units // 2, width), cross.dtype)


def attend_back(projected, scaled, delta, kv_all, cross=None):
    size = projected.shape[0]
    blocks = lax.axis_size("blk")
    rows = blocks // 2
    heads = scaled.shape[1] // HEAD
    whole = pl.BlockSpec(memory_space=pltpu.VMEM)
    far = pl.BlockSpec(memory_space=pl.ANY)
    carried = cross is not None
    far_shape, operands = [], [projected, scaled, delta, kv_all]
    if carried:
        far_shape = [half_of(cross)]
        operands.append(cross)
    return pl.pallas_call(
        functools.partial(attend_back_kernel, heads, carried),
        out_shape=[jax.ShapeDtypeStruct(projected.shape, jnp.bfloat16)] + far_shape,
        in_specs=[whole, whole, whole, far] + [far] * carried,
        out_specs=[whole] + [far] * carried,
        scratch_shapes=[
            pltpu.VMEM((blocks, size, 2 * HEAD), jnp.bfloat16),
            pltpu.VMEM((rows, 2, size, 2 * HEAD), jnp.bfloat16),
            pltpu.VMEM((rows, size, 2 * HEAD), jnp.bfloat16),
            pltpu.VMEM((rows, size, 2 * HEAD), jnp.bfloat16),
            pltpu.VMEM((size, heads * HEAD), jnp.float32),
            pltpu.VMEM((size, HEAD), jnp.float32),
            pltpu.VMEM((size, HEAD), jnp.float32),
            pltpu.SemaphoreType.DMA((blocks,)),
            pltpu.SemaphoreType.DMA((rows, PIECES)),
            pltpu.SemaphoreType.DMA((rows, PIECES)),
            pltpu.SemaphoreType.DMA((rows, PIECES)),
            pltpu.SemaphoreType.DMA((rows, PIECES)),
            pltpu.VMEM((size // PIECES, 2 * HEAD), jnp.bfloat16),
            pltpu.SemaphoreType.DMA((2,)),
        ]
        + [pltpu.SemaphoreType.DMA, pltpu.SemaphoreType.DMA] * carried,
        compiler_params=pltpu.CompilerParams(
            collective_id=1, has_side_effects=True, vmem_limit_bytes=VMEM_BYTES
        ),
        cost_estimate=cost_of(50),
        name="attend_back",
    )(*operands)


def line_gather(
    own_ref,
    full,
    line_sent,
    line_landed,
    extra_sent,
    extra_landed,
    side_sent,
    side_landed,
    first_done,
    own_done,
    ready,
    work,
):
    at = lax.axis_index("blk")
    rows = lax.axis_size("blk") // 2
    line, column = at // 2, at % 2
    partner = at + 1 - 2 * column
    size = own_ref.shape[0]
    half = size // 2

    def span(source, start, count):
        return full.at[pl.ds(pl.multiple_of(2 * source * size + start, half), count), :]

    def line_copy(source, sign, first=False):
        target = span(source, column * size, size)
        return push(
            own_ref if first else target,
            target,
            line_sent.at[(sign + 1) // 2, source],
            line_landed.at[source],
            at + 2 * sign,
        )

    def extra_copy(source, sign):
        target = span(source, (1 - column) * size + half, half)
        return push(
            target,
            target,
            extra_sent.at[(sign + 1) // 2, source],
            extra_landed.at[source],
            at + 2 * sign,
        )

    def side_copy(source, member, count, first=False):
        target = span(source, member * size, count)
        return push(
            own_ref.at[:count] if first else target,
            target,
            side_sent.at[source],
            side_landed.at[source],
            partner,
        )

    def first_copy(member):
        return push(
            own_ref.at[half:],
            span(line, member * size + half, half),
            first_done.at[0],
            first_done.at[1],
            partner,
        )

    def inside(row):
        return jnp.logical_and(row >= 0, row < rows)

    def end(row):
        return jnp.logical_or(row == 0, row == rows - 1)

    def by_end(source, act):
        pl.when(end(source))(lambda: act(half))
        pl.when(jnp.logical_not(end(source)))(lambda: act(size))

    pl.when(end(line))(lambda: first_copy(column).start())
    pl.when(line < rows - 1)(lambda: line_copy(line, 1, True).start())
    pl.when(line > 0)(lambda: line_copy(line, -1, True).start())
    by_end(line, lambda count: side_copy(line, column, count, True).start())
    keep = pltpu.make_async_copy(own_ref, span(line, column * size, size), own_done)
    keep.start()

    @pl.when(end(line))
    def _():
        first_copy(1 - column).wait_recv()
        pl.when(line < rows - 1)(lambda: extra_copy(line, 1).start())
        pl.when(line > 0)(lambda: extra_copy(line, -1).start())

    keep.wait()
    ready()

    @pl.loop(0, rows + 1)
    def _(step):
        @pl.loop(0, 2)
        def _(way):
            sign = 2 * way - 1
            source = line - sign * step

            @pl.when(both(step > 0, inside(source)))
            def _():
                line_copy(source, sign).wait_recv()
                pl.when(inside(line + sign))(lambda: line_copy(source, sign).start())
                by_end(source, lambda count: side_copy(source, column, count).start())

        @pl.loop(0, 2)
        def _(way):
            sign = 2 * way - 1
            source = line - sign * step

            @pl.when(both(step > 0, inside(source), end(source)))
            def _():
                extra_copy(source, sign).wait_recv()
                pl.when(inside(line + sign))(lambda: extra_copy(source, sign).start())

        @pl.loop(0, 2)
        def _(way):
            source = line - (2 * way - 1) * (step - 1)

            @pl.when(both(step > way, inside(source)))
            def _():
                by_end(source, lambda count: side_copy(source, 1 - column, count).wait_recv())
                work(source)

    @pl.loop(0, rows)
    def _(source):
        @pl.when(both(source <= line, line < rows - 1))
        def _():
            line_copy(source, 1).wait_send()
            pl.when(end(source))(lambda: extra_copy(source, 1).wait_send())

        @pl.when(both(source >= line, line > 0))
        def _():
            line_copy(source, -1).wait_send()
            pl.when(end(source))(lambda: extra_copy(source, -1).wait_send())

        by_end(source, lambda count: side_copy(source, column, count).wait_send())

    pl.when(end(line))(lambda: first_copy(column).wait_send())


def line_scatter(
    part,
    side,
    lane,
    tail,
    out_ref,
    side_sent,
    side_landed,
    lane_sent,
    lane_landed,
    tail_done,
    work,
    fill,
):
    at = lax.axis_index("blk")
    rows = lax.axis_size("blk") // 2
    line, column = at // 2, at % 2
    partner = at + 1 - 2 * column
    size = out_ref.shape[0]
    half = size // 2

    def span(target, start, count):
        return pl.ds(pl.multiple_of(2 * target * size + start, half), count)

    def piece(target, which):
        member = jnp.where(which == 2, 1 - column, column)
        return span(target, member * size + jnp.where(which == 0, 0, half), half)

    def side_copy(target, count):
        return push(
            part.at[span(target, (1 - column) * size, count), :],
            side.at[target, :count],
            side_sent.at[target],
            side_landed.at[target],
            partner,
        )

    def lane_copy(target, which, sign):
        slot = target if sign == 1 else jnp.where(target == line - 1, rows, target)
        return push(
            part.at[piece(target, which), :],
            lane.at[slot, which],
            lane_sent.at[target, which],
            lane_landed.at[slot, which],
            at + 2 * sign,
        )

    def lane_wait(slot, which):
        push(
            lane.at[slot, which],
            lane.at[slot, which],
            lane_sent.at[0, which],
            lane_landed.at[slot, which],
            partner,
        ).wait_recv()

    def tail_copy():
        return push(
            part.at[piece(line, 2), :], tail, tail_done.at[0], tail_done.at[1], partner
        )

    def inside(row):
        return jnp.logical_and(row >= 0, row < rows)

    def end(row):
        return jnp.logical_or(row == 0, row == rows - 1)

    def by_end(target, act):
        pl.when(end(target))(lambda: act(half))
        pl.when(jnp.logical_not(end(target)))(lambda: act(size))

    def add(where, more):
        part[where, :] = (
            part[where, :].astype(jnp.float32) + more.astype(jnp.float32)
        ).astype(jnp.bfloat16)

    def hop(target, which):
        sign = jnp.where(target > line, 1, -1)

        @pl.when(inside(line - sign))
        def _():
            lane_wait(target, which)
            add(piece(target, which), lane[target, which])

        pl.when(target > line)(lambda: lane_copy(target, which, 1).start())
        pl.when(target < line)(lambda: lane_copy(target, which, -1).start())

    def early(target):
        return both(end(target), end(line), target != line)

    @pl.loop(0, rows)
    def _(step):
        @pl.loop(0, 2)
        def _(way):
            target = line + (2 * way - 1) * (rows - 1 - step)

            @pl.when(both(step < rows - way, inside(target)))
            def _():
                work(target)
                by_end(target, lambda count: side_copy(target, count).start())

                pl.when(early(target))(lambda: pl.loop(1, 3)(lambda which: hop(target, which)))

    def gather_lanes(which):
        @pl.loop(0, 2)
        def _(above):
            slot = jnp.where(above == 0, line, rows)

            @pl.when(jnp.where(above == 0, line > 0, line < rows - 1))
            def _():
                lane_wait(slot, which)
                add(piece(line, which), lane[slot, which])

    def merge(target):
        @pl.when(both(end(target), target != line, jnp.logical_not(early(target))))
        def _():
            pl.loop(1, 3)(lambda which: hop(target, which))

        @pl.when(both(end(line), target == line))
        def _():
            gather_lanes(2)
            tail_copy().start()

        by_end(target, lambda count: side_copy(target, count).wait_recv())

        @pl.loop(0, 2)
        def _(which):
            @pl.when(jnp.logical_or(which == 0, jnp.logical_not(end(target))))
            def _():
                add(piece(target, which), side[target, pl.ds(which * half, half)])
                pl.when(target != line)(lambda: hop(target, which))

    @pl.loop(0, rows)
    def _(step):
        fill(step)

        @pl.loop(0, 2)
        def _(way):
            target = line + (2 * way - 1) * (rows - 1 - step)
            pl.when(both(step < rows - way, inside(target)))(lambda: merge(target))

    pl.loop(0, 2)(lambda which: gather_lanes(1 - which))
    out_ref[...] = part[span(line, column * size, size), :].astype(jnp.float32)

    @pl.when(end(line))
    def _():
        tail_copy().wait_recv()
        out_ref[half:, :] += tail[...].astype(jnp.float32)
        tail_copy().wait_send()

    @pl.loop(0, rows)
    def _(target):
        by_end(target, lambda count: side_copy(target, count).wait_send())

        def sent(sign):
            pl.loop(0, jnp.where(end(target), 3, 2))(
                lambda which: lane_copy(target, which, sign).wait_send()
            )

        pl.when(target > line)(lambda: sent(1))
        pl.when(target < line)(lambda: sent(-1))


def line_sems(rows):
    dma = pltpu.SemaphoreType.DMA
    ways, each = dma((2, rows)), dma((rows,))
    return [ways, each, ways, each, each, each, dma((2,)), dma]


def lane_sems(rows):
    dma = pltpu.SemaphoreType.DMA
    return [dma((rows,)), dma((rows,)), dma((rows, 3)), dma((rows + 1, 3)), dma((2,))]


def lane_buffers(rows, size, width):
    return [
        pltpu.VMEM((2 * rows * size, width), jnp.bfloat16),
        pltpu.VMEM((rows, size, width), jnp.bfloat16),
        pltpu.VMEM((rows + 1, 3, size // 2, width), jnp.bfloat16),
        pltpu.VMEM((size // 2, width), jnp.bfloat16),
    ]


def ffn_kernel(
    act_ref,
    w_ref,
    middle_ref,
    cotangent_ref,
    gains_ref,
    result_ref,
    grad_ref,
    row_ref,
    acts_ref,
    factors_ref,
    out_ref,
    w,
    acts,
    hidden,
    factors,
    part,
    side,
    lane,
    tail,
    w_done,
    save_done,
    factors_done,
    *sems,
):
    at = lax.axis_index("blk")
    rows = lax.axis_size("blk") // 2
    pair = 2 * act_ref.shape[0]

    def load(which):
        return pltpu.make_async_copy(w_ref.at[which], w.at[which], w_done.at[which])

    def pair_rows(source):
        return pl.ds(pl.multiple_of(source * pair, pair), pair)

    def save(source):
        return pltpu.make_async_copy(
            acts.at[pair_rows(source), :], acts_ref.at[pair_rows(source), :], save_done.at[source]
        )

    for which in range(3):
        load(which).start()
    greet(at, at // 2, rows)

    def ready():
        for which in range(3):
            load(which).wait()

    def expand(source):
        save(source).start()
        rows_now = acts[pair_rows(source), :]
        gate = contract_last(w[0], rows_now)
        up = contract_last(w[1], rows_now)
        hidden[source] = (gelu_value(gate) * up).astype(jnp.bfloat16)

    def reduce(target):
        part[pair_rows(target), :] = lax.dot_general(
            hidden[target], w[2], (((0,), (0,)), ((), ())), preferred_element_type=jnp.float32
        ).astype(jnp.bfloat16)

    line_gather(act_ref, acts, *sems[:8], ready, expand)
    def factors_copy(source):
        return pltpu.make_async_copy(
            factors.at[source % 2],
            factors_ref.at[:, :, pair_rows(source)],
            factors_done.at[source % 2],
        )

    def fill(source):
        rows_now = acts[pair_rows(source), :]
        gate = contract_last(w[0], rows_now)
        up = contract_last(w[1], rows_now)
        bent = jnp.tanh(GELU_SCALE * (gate + GELU_CUBIC * gate * gate * gate))
        slope = 0.5 * (1.0 + bent) + 0.5 * gate * (1.0 - bent * bent) * GELU_SCALE * (
            1.0 + 3.0 * GELU_CUBIC * gate * gate
        )
        pl.when(source > 1)(lambda: factors_copy(source - 2).wait())
        slot = source % 2
        factors[slot, 0] = (up * slope).astype(jnp.bfloat16)
        factors[slot, 1] = (0.5 * gate * (1.0 + bent)).astype(jnp.bfloat16)
        factors[slot, 2] = hidden[source]
        factors_copy(source).start()

    line_scatter(part, side, lane, tail, out_ref, *sems[8:], reduce, fill)
    normed, inverse = norm_parts(out_ref[...])
    result_ref[...] = (middle_ref[...] + normed * gains_ref[3:4, :]).astype(jnp.bfloat16)
    grad_v, gain_row = norm_back(
        cotangent_ref[...].astype(jnp.float32), normed, inverse, gains_ref[3:4, :]
    )
    grad_ref[...] = grad_v.astype(jnp.bfloat16)
    row_ref[...] = gain_row[None, :]
    factors_copy(rows - 2).wait()
    factors_copy(rows - 1).wait()
    pl.loop(0, rows)(lambda source: save(source).wait())


def ffn_forward(act_ffn, w_parts, middle, cotangent, gains):
    size, width = act_ffn.shape
    units = w_parts.shape[1]
    blocks = lax.axis_size("blk")
    rows = blocks // 2
    whole = pl.BlockSpec(memory_space=pltpu.VMEM)
    far = pl.BlockSpec(memory_space=pl.ANY)
    return pl.pallas_call(
        ffn_kernel,
        out_shape=(
            jax.ShapeDtypeStruct((size, width), jnp.bfloat16),
            jax.ShapeDtypeStruct((size, width), jnp.bfloat16),
            jax.ShapeDtypeStruct((1, width), jnp.float32),
            jax.ShapeDtypeStruct((blocks * size, width), jnp.bfloat16),
            jax.ShapeDtypeStruct((3, units, blocks * size), jnp.bfloat16),
        ),
        in_specs=[whole, far, whole, whole, whole],
        out_specs=(whole, whole, whole, far, far),
        scratch_shapes=[
            pltpu.VMEM((size, width), jnp.float32),
            pltpu.VMEM(w_parts.shape, jnp.bfloat16),
            pltpu.VMEM((blocks * size, width), jnp.bfloat16),
            pltpu.VMEM((rows, units, 2 * size), jnp.bfloat16),
            pltpu.VMEM((2, 3, units, 2 * size), jnp.bfloat16),
            *lane_buffers(rows, size, width),
            pltpu.SemaphoreType.DMA((3,)),
            pltpu.SemaphoreType.DMA((rows,)),
            pltpu.SemaphoreType.DMA((2,)),
            *line_sems(rows),
            *lane_sems(rows),
        ],
        compiler_params=pltpu.CompilerParams(
            collective_id=2, has_side_effects=True, vmem_limit_bytes=VMEM_BYTES
        ),
        cost_estimate=cost_of(115),
        name="ffn_forward",
    )(act_ffn, w_parts, middle, cotangent, gains)


FILL_COLUMNS = 768
FILL_FIRST = 0


def ffn_back_kernel(
    owners,
    grad_ref,
    acts_ref,
    factors_ref,
    w_ref,
    out_ref,
    keep_ref,
    cross_ref,
    w,
    rights,
    lefts,
    part,
    side,
    lane,
    tail,
    stage,
    mate_part,
    w_done,
    acts_done,
    factors_done,
    mate_sent,
    mate_landed,
    summed_done,
    *sems,
):
    at = lax.axis_index("blk")
    me = lax.axis_index("sp")
    chip, core = me // 2, me % 2
    mate = me + 1 - 2 * core
    rows = lax.axis_size("blk") // 2
    size, width = grad_ref.shape
    pair = 2 * size
    units = w.shape[1]
    acts, grads = rights.at[0], rights.at[1]

    def load(which):
        return pltpu.make_async_copy(w_ref.at[which], w.at[which], w_done.at[which])

    def pair_rows(source):
        return pl.ds(pl.multiple_of(source * pair, pair), pair)

    acts_copy = pltpu.make_async_copy(acts_ref, acts, acts_done)
    factors_copy = pltpu.make_async_copy(factors_ref, lefts, factors_done)
    load(2).start()
    factors_copy.start()
    load(0).start()
    load(1).start()
    acts_copy.start()
    greet(at, at // 2, rows, mate)

    def ready():
        load(2).wait()
        factors_copy.wait()

    def expand(source):
        columns = pair_rows(source)
        grad_hidden = contract_last(w[2], grads[columns, :])
        for which in range(2):
            lefts[which, :, columns] = (
                lefts[which, :, columns].astype(jnp.float32) * grad_hidden
            ).astype(jnp.bfloat16)

    def reduce(target):
        columns = pair_rows(target)
        dims = (((0,), (0,)), ((), ()))
        total = lax.dot_general(
            lefts[0, :, columns], w[0], dims, preferred_element_type=jnp.float32
        ) + lax.dot_general(lefts[1, :, columns], w[1], dims, preferred_element_type=jnp.float32)
        part[pair_rows(target), :] = total.astype(jnp.bfloat16)

    pieces = width // FILL_COLUMNS
    total_pieces = 3 * pieces

    def piece_columns(item):
        return pl.ds(pl.multiple_of((item % pieces) * FILL_COLUMNS, FILL_COLUMNS), FILL_COLUMNS)

    def mate_copy(item):
        return push_sp(
            stage.at[item % 2, :, 1 - core],
            mate_part.at[item],
            mate_sent.at[item % 2],
            mate_landed.at[item],
            mate,
        )

    def put(item, side_chip, target):
        return pltpu.make_async_copy(
            mate_part.at[item, side_chip],
            target.at[item // pieces, :, piece_columns(item)],
            summed_done.at[item, side_chip],
        )

    def put_wait(item):
        put(item, chip, keep_ref).wait()
        put(item, 1 - chip, cross_ref).wait()

    def sum_one(item):
        mate_copy(item).wait_recv()
        mate_part[item] = (
            stage[item % 2, :, core].astype(jnp.float32) + mate_part[item].astype(jnp.float32)
        ).astype(jnp.bfloat16)
        put(item, chip, keep_ref).start()
        put(item, 1 - chip, cross_ref).start()

    def fill_one(item):
        which = item // pieces
        total = jnp.dot(
            lefts[which],
            rights[which // 2, :, piece_columns(item)],
            preferred_element_type=jnp.float32,
        )
        pl.when(item > 1)(lambda: mate_copy(item - 2).wait_send())
        stage[item % 2] = total.astype(jnp.bfloat16).reshape(
            2, 2, units // owners, FILL_COLUMNS
        )
        mate_copy(item).start()
        pl.when(item > 0)(lambda: sum_one(item - 1))

    each = pl.cdiv(total_pieces - FILL_FIRST, rows - 1)

    def fill(step):
        first = jnp.maximum(FILL_FIRST + (step - 1) * each, 0)
        last = jnp.minimum(FILL_FIRST + step * each, total_pieces)

        @pl.loop(0, each)
        def _(item):
            pl.when(first + item < last)(lambda: fill_one(first + item))

    line_gather(grad_ref, grads, *sems[:8], ready, expand)
    load(0).wait()
    load(1).wait()
    acts_copy.wait()
    line_scatter(part, side, lane, tail, out_ref, *sems[8:], reduce, fill)
    sum_one(total_pieces - 1)
    pl.loop(0, total_pieces)(put_wait)
    for item in range(total_pieces - 2, total_pieces):
        mate_copy(item).wait_send()


def ffn_back(grad_ffn, kept, w_parts, owners):
    size, width = grad_ffn.shape
    units = w_parts.shape[1]
    blocks = lax.axis_size("blk")
    rows = blocks // 2
    tokens = blocks * size
    items = 3 * width // FILL_COLUMNS
    whole = pl.BlockSpec(memory_space=pltpu.VMEM)
    far = pl.BlockSpec(memory_space=pl.ANY)
    return pl.pallas_call(
        functools.partial(ffn_back_kernel, owners),
        out_shape=(
            jax.ShapeDtypeStruct((size, width), jnp.float32),
            jax.ShapeDtypeStruct((3, units // owners, width), jnp.bfloat16),
            jax.ShapeDtypeStruct((3, units // owners, width), jnp.bfloat16),
        ),
        in_specs=[whole, far, far, far],
        out_specs=(whole, far, far),
        scratch_shapes=[
            pltpu.VMEM(w_parts.shape, jnp.bfloat16),
            pltpu.VMEM((2, tokens, width), jnp.bfloat16),
            pltpu.VMEM((3, units, tokens), jnp.bfloat16),
            *lane_buffers(rows, size, width),
            pltpu.VMEM((2, 2, 2, units // owners, FILL_COLUMNS), jnp.bfloat16),
            pltpu.VMEM((items, 2, units // owners, FILL_COLUMNS), jnp.bfloat16),
            pltpu.SemaphoreType.DMA((3,)),
            pltpu.SemaphoreType.DMA,
            pltpu.SemaphoreType.DMA,
            pltpu.SemaphoreType.DMA((2,)),
            pltpu.SemaphoreType.DMA((items,)),
            pltpu.SemaphoreType.DMA((items, 2)),
            *line_sems(rows),
            *lane_sems(rows),
        ],
        compiler_params=pltpu.CompilerParams(
            collective_id=3, has_side_effects=True, vmem_limit_bytes=VMEM_BYTES
        ),
        cost_estimate=cost_of(115),
        name="ffn_back",
    )(grad_ffn, *kept, w_parts)


def ffn_hidden(acts, w_parts):
    gate = contract_last(acts, w_parts[0])
    up = contract_last(acts, w_parts[1])
    return (gate, up, (gelu_value(gate) * up).astype(jnp.bfloat16))


def scatter_tokens(partial):
    return lax.psum_scatter(
        partial.astype(jnp.bfloat16), "blk", scatter_dimension=0, tiled=True
    ).astype(jnp.float32)


def ffn_forward_wide(act_ffn, w_parts, middle, cotangent, gains):
    acts = lax.all_gather(act_ffn, "blk", axis=0, tiled=True)
    hidden = ffn_hidden(acts, w_parts)[2]
    partial = jnp.dot(hidden, w_parts[2], preferred_element_type=jnp.float32)
    normed, inverse = norm_parts(scatter_tokens(partial))
    result = (middle + normed * gains[3]).astype(jnp.bfloat16)
    grad_v, gain_row = norm_back(cotangent.astype(jnp.float32), normed, inverse, gains[3])
    return (result, grad_v.astype(jnp.bfloat16), gain_row[None], acts)


def ffn_back_wide(grad_ffn, kept, w_parts, owners):
    (acts,) = kept
    grads = lax.all_gather(grad_ffn, "blk", axis=0, tiled=True)
    gate, up, hidden = ffn_hidden(acts, w_parts)
    grad_hidden = contract_last(grads, w_parts[2])
    grad_gate = (grad_hidden * up * gelu_slope(gate)).astype(jnp.bfloat16)
    grad_up = (grad_hidden * gelu_value(gate)).astype(jnp.bfloat16)
    partial = jnp.dot(grad_gate, w_parts[0], preferred_element_type=jnp.float32) + jnp.dot(
        grad_up, w_parts[1], preferred_element_type=jnp.float32
    )
    sums = jnp.stack(
        [
            jnp.einsum("tf,td->fd", left, right, preferred_element_type=jnp.float32)
            for left, right in ((grad_gate, acts), (grad_up, acts), (hidden, grads))
        ]
    ).astype(jnp.bfloat16)
    units = w_parts.shape[1]
    owned = sums.reshape(3, owners, units // owners, sums.shape[2])
    mine = lax.psum_scatter(
        jnp.transpose(owned, (1, 0, 2, 3)), "sp", scatter_dimension=0, tiled=True
    )
    return (scatter_tokens(partial), mine[0], None)


def cost_of(microseconds):
    return pl.CostEstimate(
        flops=int(microseconds * 1e9), bytes_accessed=int(microseconds * 3e6), transcendentals=0
    )


def push_sp(source, target, sent, landed, peer):
    return pltpu.make_async_remote_copy(
        src_ref=source,
        dst_ref=target,
        send_sem=sent,
        recv_sem=landed,
        device_id={"sp": peer},
        device_id_type=pl.DeviceIdType.MESH,
    )


def greet_sp(me, groups):
    barrier = pltpu.get_barrier_semaphore()
    for step in range(1, groups):
        pl.semaphore_signal(
            barrier,
            inc=1,
            device_id={"sp": (me + step) % groups},
            device_id_type=pl.DeviceIdType.MESH,
        )
    pl.semaphore_wait(barrier, groups - 1)


def gather_rows(x, w_ref, full_ref, w, w_done, own_done, sent, landed, prepare, project):
    me = lax.axis_index("sp")
    size = x.shape[0]
    units = w.shape[0]
    mate = me + 1 - 2 * (me % 2)
    across = (me + 2) % 4

    def spot(member):
        return full_ref.at[pl.ds(pl.multiple_of(member * size, size), size), :]

    load = pltpu.make_async_copy(
        w_ref.at[pl.ds(pl.multiple_of(me * units, units), units), :], w, w_done
    )
    load.start()
    prepare()
    greet_sp(me, 4)
    half = size // 2

    def half_spot(member, piece):
        start = pl.multiple_of(member * size + piece * half, half)
        return full_ref.at[pl.ds(start, half), :]

    def over(piece):
        return push_sp(
            x.at[pl.ds(piece * half, half)],
            half_spot(me, piece),
            sent.at[piece],
            landed.at[piece],
            across,
        )

    def onward(piece):
        rows_now = half_spot(across, piece)
        return push_sp(rows_now, rows_now, sent.at[3 + piece], landed.at[3 + piece], mate)

    over(0).start()
    over(1).start()
    beside = push_sp(x, spot(me), sent.at[2], landed.at[2], mate)
    beside.start()
    keep = pltpu.make_async_copy(x, spot(me), own_done)
    keep.start()
    keep.wait()
    load.wait()

    def project_chip(chip):
        rows = pl.ds(pl.multiple_of(chip * 2 * size, 2 * size), 2 * size)
        project(rows, contract_last(full_ref[rows, :], w[...]).astype(jnp.bfloat16))

    beside.wait_recv()
    project_chip(me // 2)
    for piece in range(2):
        over(piece).wait_recv()
        onward(piece).start()
    for piece in range(2):
        onward(piece).wait_recv()
    project_chip(across // 2)
    beside.wait_send()
    for piece in range(2):
        over(piece).wait_send()
        onward(piece).wait_send()


def project_in_kernel(tokens_ref, gains_ref, w_ref, full_ref, out_ref, x, *scratch):
    def prepare():
        normed = norm_parts(tokens_ref[...].astype(jnp.float32))[0]
        x[...] = (normed * gains_ref[0:1, :]).astype(jnp.bfloat16)

    def project(rows, value):
        out_ref[rows, :] = value

    gather_rows(x, w_ref, full_ref, *scratch, prepare, project)


def gather_scratch(size, width, units):
    dma = pltpu.SemaphoreType.DMA
    return [
        pltpu.VMEM((size, width), jnp.bfloat16),
        pltpu.VMEM((units, width), jnp.bfloat16),
        dma,
        dma,
        dma((5,)),
        dma((5,)),
    ]


def project_in(tokens, gains, weights):
    size, width = tokens.shape
    units = weights.shape[0] // 4
    whole = pl.BlockSpec(memory_space=pltpu.VMEM)
    return pl.pallas_call(
        project_in_kernel,
        out_shape=(
            jax.ShapeDtypeStruct((4 * size, width), jnp.bfloat16),
            jax.ShapeDtypeStruct((4 * size, units), jnp.bfloat16),
        ),
        in_specs=[whole, whole, pl.BlockSpec(memory_space=pl.ANY)],
        out_specs=(whole, whole),
        scratch_shapes=gather_scratch(size, width, units),
        compiler_params=pltpu.CompilerParams(
            collective_id=4, has_side_effects=True, vmem_limit_bytes=VMEM_BYTES
        ),
        cost_estimate=cost_of(18),
        name="project_in",
    )(tokens, gains, weights)


def project_back_kernel(
    grad_ref,
    middle_ref,
    attn_ref,
    cotangent_ref,
    gains_ref,
    attended_ref,
    by_row_ref,
    totals_ref,
    w_ref,
    full_ref,
    scaled_ref,
    delta_ref,
    grad_middle_ref,
    rows_ref,
    x,
    *scratch,
):
    def prepare():
        grad_v, row_two = norm_back(
            grad_ref[...], *norm_parts(middle_ref[...]), gains_ref[2:3, :]
        )
        grad_middle = cotangent_ref[...].astype(jnp.float32) + grad_v
        grad_middle_ref[...] = grad_middle
        grad_v, row_one = norm_back(grad_middle, *norm_parts(attn_ref[...]), gains_ref[1:2, :])
        x[...] = grad_v.astype(jnp.bfloat16)
        rows_ref[...] = jnp.zeros_like(rows_ref)
        rows_ref[1:2, :] = row_one[None, :]
        rows_ref[2:3, :] = row_two[None, :]

    def project(rows, value):
        for head in range(value.shape[1] // HEAD):
            columns = slice(head * HEAD, (head + 1) * HEAD)
            grad = value[:, columns].astype(jnp.float32)
            scaled_ref[rows, columns] = (grad / by_row_ref[head, rows, :1]).astype(jnp.bfloat16)
            product = grad * attended_ref[rows, columns]
            delta_ref[head, :, rows] = (
                jnp.sum(product.T, axis=0, keepdims=True) / totals_ref[head, :, rows]
            )

    gather_rows(x, w_ref, full_ref, *scratch, prepare, project)


def project_back(
    grad_act, middle, attn, cotangent, gains, attended, by_row, totals, weights
):
    size, width = attn.shape
    units = weights.shape[0] // 4
    whole = pl.BlockSpec(memory_space=pltpu.VMEM)
    return pl.pallas_call(
        project_back_kernel,
        out_shape=(
            jax.ShapeDtypeStruct((4 * size, width), jnp.bfloat16),
            jax.ShapeDtypeStruct((4 * size, units), jnp.bfloat16),
            jax.ShapeDtypeStruct(totals.shape, jnp.float32),
            jax.ShapeDtypeStruct((size, width), jnp.float32),
            jax.ShapeDtypeStruct((8, width), jnp.float32),
        ),
        in_specs=[whole] * 8 + [pl.BlockSpec(memory_space=pl.ANY)],
        out_specs=(whole,) * 5,
        scratch_shapes=gather_scratch(size, width, units),
        compiler_params=pltpu.CompilerParams(
            collective_id=6, has_side_effects=True, vmem_limit_bytes=VMEM_BYTES
        ),
        cost_estimate=cost_of(20),
        name="project_back",
    )(grad_act, middle, attn, cotangent, gains, attended, by_row, totals, weights)


def exchange_norm_kernel(x_ref, w_ref, tokens_ref, gains_ref, out_ref, middle_ref, act_ref, *scratch):
    exchange_project_kernel(x_ref, w_ref, out_ref, *scratch)
    normed = norm_parts(out_ref[...])[0]
    middle = tokens_ref[...].astype(jnp.float32) + normed * gains_ref[1:2, :]
    middle_ref[...] = middle
    act_ref[...] = (norm_parts(middle)[0] * gains_ref[2:3, :]).astype(jnp.bfloat16)


def exchange_project_kernel(x_ref, w_ref, out_ref, w, got, w_done, own_done, sent, landed):
    me = lax.axis_index("sp")
    size = out_ref.shape[0]
    units = x_ref.shape[1]

    def rows_of(member):
        return x_ref.at[pl.ds(pl.multiple_of(member * size, size), size), :]

    def load(member):
        rows = pl.ds(pl.multiple_of(member * units, units), units)
        return pltpu.make_async_copy(w_ref.at[rows, :], w.at[rows, :], w_done.at[member])

    def send(step):
        peer = (me + step) % 4
        return push_sp(rows_of(peer), got.at[4 - step], sent.at[step], landed.at[4 - step], peer)

    greet_sp(me, 4)
    for step in (2, 1, 3):
        send(step).start()
    keep = pltpu.make_async_copy(rows_of(me), got.at[0], own_done)
    keep.start()
    for step in range(4):
        load((me + step) % 4).start()
    keep.wait()
    for step in (0, 1, 3, 2):
        member = (me + step) % 4
        load(member).wait()
        if step > 0:
            send(4 - step).wait_recv()
        rows = pl.ds(pl.multiple_of(member * units, units), units)
        term = jnp.dot(got[step], w[rows, :], preferred_element_type=jnp.float32)
        if step == 0:
            out_ref[...] = term
        else:
            out_ref[...] += term
    for step in (1, 2, 3):
        send(step).wait_send()


def exchange_project(columns, weights, identity, norm_inputs=()):
    size = columns.shape[0] // 4
    whole = pl.BlockSpec(memory_space=pltpu.VMEM)
    total = jax.ShapeDtypeStruct((size, weights.shape[1]), jnp.float32)
    low = jax.ShapeDtypeStruct(total.shape, jnp.bfloat16)
    shapes = [total, total, low] if norm_inputs else [total]
    return pl.pallas_call(
        exchange_norm_kernel if norm_inputs else exchange_project_kernel,
        out_shape=shapes,
        in_specs=[whole, pl.BlockSpec(memory_space=pl.ANY)] + [whole] * len(norm_inputs),
        out_specs=[whole] * len(shapes),
        scratch_shapes=[
            pltpu.VMEM(weights.shape, jnp.bfloat16),
            pltpu.VMEM((4, size, columns.shape[1]), jnp.bfloat16),
            pltpu.SemaphoreType.DMA((4,)),
            pltpu.SemaphoreType.DMA,
            pltpu.SemaphoreType.DMA((4,)),
            pltpu.SemaphoreType.DMA((4,)),
        ],
        compiler_params=pltpu.CompilerParams(
            collective_id=identity, has_side_effects=True, vmem_limit_bytes=VMEM_BYTES
        ),
        cost_estimate=cost_of(16),
        name="exchange_project",
    )(columns, weights, *norm_inputs)


def finish_kernel(
    cols_ref,
    act_ref,
    att_ref,
    grad_ref,
    w_ref,
    tokens_ref,
    middle_ref,
    gains_in_ref,
    rows_ref,
    row_three_ref,
    cross_ref,
    qkv_ref,
    out_ref,
    tokens_grad_ref,
    gains_ref,
    far_ref,
    w,
    got,
    grad_in,
    total,
    part,
    side,
    lane,
    tail,
    mine,
    from_sp,
    from_side,
    from_line,
    w_done,
    own_done,
    swap_sent,
    swap_landed,
    sp_sent,
    sp_landed,
    gain_side,
    line_sent,
    line_landed,
    cross_sent,
    cross_landed,
    *sems,
):
    at = lax.axis_index("blk")
    me = lax.axis_index("sp")
    rows = lax.axis_size("blk") // 2
    line, column = at // 2, at % 2
    partner = at + 1 - 2 * column
    block = total.shape[0]
    size = tokens_ref.shape[0]
    units = cols_ref.shape[1]
    extra = block - size

    barrier = pltpu.get_barrier_semaphore()
    for step in range(1, 4):
        pl.semaphore_signal(
            barrier, inc=1, device_id={"sp": (me + step) % 4}, device_id_type=pl.DeviceIdType.MESH
        )

    def line_peer(step):
        return 2 * ((line + step) % rows) + column

    for peer in [partner] + [line_peer(step) for step in range(1, rows)]:
        pl.semaphore_signal(
            barrier, inc=1, device_id={"blk": peer}, device_id_type=pl.DeviceIdType.MESH
        )

    def load(member):
        span = pl.ds(pl.multiple_of(member * units, units), units)
        return pltpu.make_async_copy(w_ref.at[span, :], w.at[span, :], w_done.at[member])

    def rows_of(member):
        return cols_ref.at[pl.ds(pl.multiple_of(member * size, size), size), :]

    def swap(step):
        peer = (me + step) % 4
        return push_sp(
            rows_of(peer), got.at[4 - step], swap_sent.at[step], swap_landed.at[4 - step], peer
        )

    for step in range(4):
        load((me + step) % 4).start()
    keep = pltpu.make_async_copy(rows_of(me), got.at[0], own_done)
    keep.start()
    pl.semaphore_wait(barrier, 3 + rows)
    for step in (2, 1, 3):
        swap(step).start()
    over = carry(
        cross_ref, far_ref, far_ref.shape[1], cross_sent, cross_landed, (me + 2) % 4
    )
    over.start()
    keep.wait()

    def sp_gains(step):
        return push_sp(
            mine, from_sp.at[4 - step], sp_sent.at[step], sp_landed.at[4 - step], (me + step) % 4
        )

    def side_gains():
        return push(from_sp.at[0], from_side, gain_side.at[0], gain_side.at[1], partner)

    def line_gains(step):
        return push(
            from_line.at[0],
            from_line.at[rows - step],
            line_sent.at[step],
            line_landed.at[rows - step],
            line_peer(step),
        )

    def reduce(target):
        dims = (((0,), (0,)), ((), ()))
        wide_columns = pl.ds(pl.multiple_of(target * 2 * size, 2 * size), 2 * size)
        term = lax.dot_general(
            cols_ref[:, wide_columns], act_ref[...], dims, preferred_element_type=jnp.float32
        ).astype(jnp.bfloat16)
        columns = pl.ds(pl.multiple_of(target * 2 * extra, 2 * extra), 2 * extra)
        more = lax.dot_general(
            att_ref[:, columns], grad_ref[...], dims, preferred_element_type=jnp.float32
        ).astype(jnp.bfloat16)
        for half in range(2):
            start = pl.multiple_of((2 * target + half) * block, block)
            part[pl.ds(start, size), :] = term[half * size : (half + 1) * size]
            start = pl.multiple_of((2 * target + half) * block + size, extra)
            part[pl.ds(start, extra), :] = more[half * extra : (half + 1) * extra]

    def inputs_back():
        for step in (0, 1, 3, 2):
            member = (me + step) % 4
            load(member).wait()
            if step > 0:
                swap(4 - step).wait_recv()
            span = pl.ds(pl.multiple_of(member * units, units), units)
            term = jnp.dot(got[step], w[span, :], preferred_element_type=jnp.float32)
            if step == 0:
                grad_in[...] = term
            else:
                grad_in[...] += term
        normed, inverse = norm_parts(tokens_ref[...].astype(jnp.float32))
        grad_v, gain_row = norm_back(grad_in[...], normed, inverse, gains_in_ref[0:1, :])
        tokens_grad_ref[...] = (middle_ref[...] + grad_v).astype(jnp.bfloat16)
        mine[...] = rows_ref[...]
        mine[0:1, :] = gain_row[None, :]
        mine[3:4, :] = row_three_ref[...]
        for step in range(1, 4):
            sp_gains(step).start()

    def fill(step):
        pl.when(step == 2)(inputs_back)

        @pl.when(step == 3)
        def _():
            gains = mine[...]
            for other in range(1, 4):
                sp_gains(4 - other).wait_recv()
                gains = gains + from_sp[other]
            from_sp[0] = gains
            side_gains().start()

        @pl.when(step == 3)
        def _():
            side_gains().wait_recv()
            from_line[0] = from_sp[0] + from_side[...]
            for other in range(1, rows):
                line_gains(other).start()

    line_scatter(part, side, lane, tail, total, *sems, reduce, fill)
    qkv_ref[...] = total[:size]
    out_ref[...] = total[size:]
    gains = from_line[0]
    for other in range(1, rows):
        line_gains(rows - other).wait_recv()
        gains = gains + from_line[other]
    gains_ref[...] = gains
    for step in (1, 2, 3):
        swap(step).wait_send()
        sp_gains(step).wait_send()
    over.wait()
    side_gains().wait_send()
    for step in range(1, rows):
        line_gains(step).wait_send()


def finish(
    cols, act_block, attended, grad_block, w_qkv, tokens, grad_middle, gains, rows, row_three, cross
):
    blocks = lax.axis_size("blk")
    lines = blocks // 2
    size, width = tokens.shape
    block = (cols.shape[1] + attended.shape[1]) // blocks
    whole = pl.BlockSpec(memory_space=pltpu.VMEM)
    any_space = pl.BlockSpec(memory_space=pl.ANY)
    dma = pltpu.SemaphoreType.DMA
    small = rows.shape
    return pl.pallas_call(
        finish_kernel,
        out_shape=(
            jax.ShapeDtypeStruct((cols.shape[1] // blocks, width), jnp.float32),
            jax.ShapeDtypeStruct((attended.shape[1] // blocks, width), jnp.float32),
            jax.ShapeDtypeStruct((size, width), jnp.bfloat16),
            jax.ShapeDtypeStruct(small, jnp.float32),
            half_of(cross),
        ),
        in_specs=[whole] * 4 + [any_space] + [whole] * 5 + [any_space],
        out_specs=(whole, whole, whole, whole, any_space),
        scratch_shapes=[
            pltpu.VMEM(w_qkv.shape, jnp.bfloat16),
            pltpu.VMEM((4, size, cols.shape[1]), jnp.bfloat16),
            pltpu.VMEM((size, width), jnp.float32),
            pltpu.VMEM((block, width), jnp.float32),
            *lane_buffers(lines, block, width),
            pltpu.VMEM(small, jnp.float32),
            pltpu.VMEM((4, *small), jnp.float32),
            pltpu.VMEM(small, jnp.float32),
            pltpu.VMEM((lines, *small), jnp.float32),
            dma((4,)),
            dma,
            dma((4,)),
            dma((4,)),
            dma((4,)),
            dma((4,)),
            dma((2,)),
            dma((lines,)),
            dma((lines,)),
            dma,
            dma,
            *lane_sems(lines),
        ],
        compiler_params=pltpu.CompilerParams(
            collective_id=8, has_side_effects=True, vmem_limit_bytes=VMEM_BYTES
        ),
        cost_estimate=cost_of(85),
        name="finish",
    )(
        cols,
        act_block,
        attended,
        grad_block,
        w_qkv,
        tokens,
        grad_middle,
        gains,
        rows,
        row_three,
        cross,
    )


def weight_sums_wide(left, right):
    term = jnp.einsum("tc,td->cd", left, right, preferred_element_type=jnp.float32)
    return scatter_tokens(term)


def finish_wide(
    cols, act_block, attended, grad_block, w_qkv, tokens, grad_middle, gains, rows, row_three, cross
):
    (grad_act_in,) = exchange_project(cols, w_qkv, 7)
    normed, inverse = norm_parts(tokens.astype(jnp.float32))
    grad_v, gain_row = norm_back(grad_act_in, normed, inverse, gains[0])
    gains_all = lax.psum(
        jnp.concatenate([gain_row[None], rows[1:3], row_three, rows[4:]]), ("blk", "sp")
    )
    return (
        weight_sums_wide(cols, act_block),
        weight_sums_wide(attended, grad_block),
        (grad_middle + grad_v).astype(jnp.bfloat16),
        gains_all,
        None,
    )


def deliver_kernel(*refs):
    keep_ref, first_ref, last_ref, *others = refs
    ins, sum_ref, outs = others[:4], others[4], others[5:]
    half = first_ref.shape[1]
    for start, far_ref in ((0, first_ref), (half, last_ref)):
        rows = slice(start, start + half)
        sum_ref[:, rows] = keep_ref[:, rows].astype(jnp.float32) + far_ref[...].astype(
            jnp.float32
        )
    for source, target in zip(ins, outs):
        target[...] = source[...]


def deliver(keep, first, last, *results):
    kinds, units, width = keep.shape
    copies = [
        pl.BlockSpec((result.shape[0] // 2, width), lambda i: (jnp.minimum(i, 1), 0))
        for result in results
    ]
    sums = pl.BlockSpec((1, units, width), lambda i: (i, 0, 0))
    halves = pl.BlockSpec((1, units // 2, width), lambda i: (i, 0, 0))
    return pl.pallas_call(
        deliver_kernel,
        grid=(kinds,),
        out_shape=[jax.ShapeDtypeStruct(keep.shape, jnp.float32)]
        + [jax.ShapeDtypeStruct(result.shape, result.dtype) for result in results],
        in_specs=[sums, halves, halves] + copies,
        out_specs=[sums] + copies,
        compiler_params=pltpu.CompilerParams(vmem_limit_bytes=VMEM_BYTES),
        cost_estimate=cost_of(8),
        name="deliver",
    )(keep, first, last, *results)


def body(tokens, w_qkv, w_out, gains, w_ffn, cotangent):
    groups = lax.axis_size("sp")
    wide = lax.axis_size("blk") > 8
    act_block, projected = project_in(tokens, gains, w_qkv)
    attended_low, attended, totals, by_row, kv_all = attend(projected, HEADS // groups)
    attn, middle, act_ffn = exchange_project(attended_low, w_out, 5, (tokens, gains))
    w_parts = jnp.transpose(w_ffn, (1, 0, 2))
    result, grad_ffn, row_three, *kept = (ffn_forward_wide if wide else ffn_forward)(
        act_ffn, w_parts, middle, cotangent, gains
    )
    grad_act_ffn, ffn_part, cross = (ffn_back_wide if wide else ffn_back)(
        grad_ffn, kept, w_parts, groups
    )
    grad_block, scaled, delta, grad_middle, rows = project_back(
        grad_act_ffn, middle, attn, cotangent, gains, attended, by_row, totals, w_out
    )
    grad_cols, *far_first = attend_back(projected, scaled, delta, kv_all, cross)
    qkv_grad, out_grad, tokens_grad, gains_all, far_last = (finish_wide if wide else finish)(
        grad_cols,
        act_block,
        attended_low,
        grad_block,
        w_qkv,
        tokens,
        grad_middle,
        gains,
        rows,
        row_three,
        cross,
    )
    if wide:
        ffn_sum = ffn_part.astype(jnp.float32)
    else:
        ffn_sum, result, tokens_grad, qkv_grad, out_grad = deliver(
            ffn_part, *far_first, far_last, result, tokens_grad, qkv_grad, out_grad
        )
    ffn_grad = jnp.transpose(ffn_sum, (1, 0, 2))
    share = gains_all.shape[1] // (groups * lax.axis_size("blk"))
    place = lax.axis_index("sp") * lax.axis_size("blk") + lax.axis_index("blk")
    gains_grad = lax.dynamic_slice_in_dim(gains_all[:4], place * share, share, 1)
    return (result, tokens_grad, qkv_grad, out_grad, gains_grad, ffn_grad)


def solution(mesh):
    return jax.shard_map(
        body,
        mesh=mesh,
        in_specs=(
            P(("blk", "sp"), None),
            P(),
            P(),
            P(),
            P("blk", None, None),
            P(("blk", "sp"), None),
        ),
        out_specs=(
            P(("blk", "sp"), None),
            P(("blk", "sp"), None),
            P(("sp", "blk"), None),
            P(("sp", "blk"), None),
            P(None, ("sp", "blk")),
            P(("blk", "sp"), None, None),
        ),
        check_vma=False,
    )
```

```python
import functools

import jax
import jax.numpy as jnp
from jax import lax
from jax.experimental import pallas as pl
from jax.experimental.pallas import tpu as pltpu
from jax.sharding import PartitionSpec as P

HEADS = 8
KV_HEADS = 4
HEAD = 256


VMEM_BYTES = 62 * 1024 * 1024
PIECES = 2
NORM_EPSILON = 1e-06
CAP_VALUE = 50.0
GELU_SCALE = 0.7978845608028654
GELU_CUBIC = 0.044715


def norm_parts(values):
    inverse = lax.rsqrt(jnp.mean(values * values, axis=-1, keepdims=True) + NORM_EPSILON)
    return (values * inverse, inverse)


def norm_back(grad_y, normed, inverse, gain):
    grad_n = grad_y * gain
    grad_v = inverse * (grad_n - normed * jnp.mean(grad_n * normed, axis=-1, keepdims=True))
    return (grad_v, jnp.sum(grad_y * normed, axis=0))


def gelu_value(values):
    return (
        0.5
        * values
        * (1.0 + jnp.tanh(GELU_SCALE * (values + GELU_CUBIC * values * values * values)))
    )


def gelu_slope(values):
    bent = jnp.tanh(GELU_SCALE * (values + GELU_CUBIC * values * values * values))
    return 0.5 * (1.0 + bent) + 0.5 * values * (1.0 - bent * bent) * GELU_SCALE * (
        1.0 + 3.0 * GELU_CUBIC * values * values
    )


def contract_last(left, right):
    return lax.dot_general(
        left, right, (((1,), (1,)), ((), ())), preferred_element_type=jnp.float32
    )


def push(source, target, sent, landed, block):
    return pltpu.make_async_remote_copy(
        src_ref=source,
        dst_ref=target,
        send_sem=sent,
        recv_sem=landed,
        device_id={"blk": block},
        device_id_type=pl.DeviceIdType.MESH,
    )


def greet(at, line, rows, sp_peer=None):
    barrier = pltpu.get_barrier_semaphore()
    others = 1
    if sp_peer is not None:
        others = 2
        pl.semaphore_signal(
            barrier, inc=1, device_id={"sp": sp_peer}, device_id_type=pl.DeviceIdType.MESH
        )

    def tell(block):
        pl.semaphore_signal(
            barrier, inc=1, device_id={"blk": block}, device_id_type=pl.DeviceIdType.MESH
        )

    tell(at + 1 - 2 * (at % 2))
    pl.when(line > 0)(lambda: tell(at - 2))
    pl.when(line < rows - 1)(lambda: tell(at + 2))
    pl.semaphore_wait(barrier, others + jnp.minimum(line, 1) + jnp.minimum(rows - 1 - line, 1))


def both(*terms):
    result = terms[0]
    for term in terms[1:]:
        result = jnp.logical_and(result, term)
    return result


def attend_kernel(
    heads,
    x_ref,
    low_ref,
    att_ref,
    tot_ref,
    by_row_ref,
    kv_ref,
    kv,
    acc,
    part,
    up_sent,
    up_landed,
    side_sent,
    side_landed,
    extra_sent,
    extra_landed,
    own_done,
    save_done,
):
    at = lax.axis_index("blk")
    blocks = lax.axis_size("blk")
    rows = blocks // 2
    line, column = at // 2, at % 2
    partner = at + 1 - 2 * column
    size = x_ref.shape[0]
    first = heads * HEAD
    own = x_ref.at[:, pl.ds(first, 2 * HEAD)]
    greet(at, line, rows)

    def halves(act):
        pl.loop(0, PIECES)(act)

    def span(piece):
        count = size // PIECES
        return pl.ds(pl.multiple_of(piece * count, count), count)

    def source_of(index, piece, is_own):
        if is_own:
            return x_ref.at[span(piece), pl.ds(first, 2 * HEAD)]
        return kv.at[index, span(piece)]

    def up_copy(index, piece, is_own=False):
        return push(
            source_of(index, piece, is_own),
            kv.at[index, span(piece)],
            up_sent.at[index // 2, piece],
            up_landed.at[index // 2, piece],
            at + 2,
        )

    def side_copy(index, piece, is_own=False):
        return push(
            source_of(index, piece, is_own),
            kv.at[index, span(piece)],
            side_sent.at[index // 2, piece],
            side_landed.at[index // 2, piece],
            partner,
        )

    def extra_copy():
        rows_now = kv.at[0, span(PIECES - 1)]
        return push(rows_now, rows_now, extra_sent.at[0], extra_landed.at[0], at + 2)

    def crossing(index):
        return jnp.where(both(index == 0, at > 0), PIECES - 1, PIECES)

    def save(index):
        return pltpu.make_async_copy(kv.at[index], kv_ref.at[index], save_done.at[index])

    @pl.loop(0, PIECES)
    def _(piece):
        pl.when(line < rows - 1)(lambda: up_copy(at, piece, True).start())
        pl.when(column == 0)(lambda: side_copy(at, PIECES - 1 - piece, True).start())

    keep = pltpu.make_async_copy(own, kv.at[at], own_done)
    keep.start()
    acc[...] = jnp.zeros_like(acc)
    part[...] = jnp.zeros_like(part)
    keep.wait()

    @pl.when(at == 1)
    def _():
        side_copy(0, PIECES - 1).wait_recv()
        extra_copy().start()

    ahead = lax.broadcasted_iota(jnp.int32, (size, size), 1) - lax.broadcasted_iota(
        jnp.int32, (size, size), 0
    )

    def compute(index):
        save(index).start()
        span = (at - index) * size
        for head in range(heads):
            raw = lax.dot_general(
                x_ref[:, head * HEAD : (head + 1) * HEAD],
                kv[index, :, :HEAD],
                (((1,), (1,)), ((), ())),
                preferred_element_type=jnp.float32,
            )
            weights = jnp.exp(CAP_VALUE * jnp.tanh(raw * (HEAD ** (-0.5) / CAP_VALUE)))
            weights = jnp.where(ahead <= span, weights, 0.0)
            total = weights[:, :128]
            for piece in range(1, size // 128):
                total = total + weights[:, piece * 128 : (piece + 1) * 128]
            part[head] += total
            acc[:, head * HEAD : (head + 1) * HEAD] += jnp.dot(
                weights.astype(jnp.bfloat16),
                kv[index, :, HEAD:],
                preferred_element_type=jnp.float32,
            )

    @pl.loop(0, rows + 1)
    def _(step):
        source = line - step
        index = 2 * source + column

        @pl.when(both(step > 0, source >= 0))
        def _():
            @pl.loop(0, PIECES)
            def _(piece):
                up_copy(index, piece).wait_recv()
                pl.when(line < rows - 1)(lambda: up_copy(index, piece).start())
                pl.when(piece < crossing(index))(lambda: side_copy(index, piece).start())

        @pl.when(both(step > 0, source == 0, column == 1))
        def _():
            extra_copy().wait_recv()
            pl.when(line < rows - 1)(lambda: extra_copy().start())

        @pl.loop(0, 2)
        def _(way):
            found = source + way
            here = 2 * found + jnp.where(way == 0, column, 1 - column)
            due = jnp.logical_or(way == 0, both(step > 0, jnp.logical_or(step > 1, column == 1)))

            @pl.when(both(found >= 0, due))
            def _():
                pl.when(way == 1)(
                    lambda: pl.loop(0, crossing(here))(
                        lambda piece: side_copy(here, piece).wait_recv()
                    )
                )
                compute(here)

    for head in range(heads):
        columns = slice(head * HEAD, (head + 1) * HEAD)
        total = jnp.sum(part[head], axis=1, keepdims=True)
        by_row_ref[head] = jnp.broadcast_to(total, by_row_ref.shape[1:])
        value = acc[:, columns] / total
        att_ref[:, columns] = value
        low_ref[:, columns] = value.astype(jnp.bfloat16)
        tot_ref[head] = jnp.sum(part[head].T, axis=0, keepdims=True)

    @pl.loop(0, rows)
    def _(source):
        index = 2 * source + column

        @pl.when(source <= line)
        def _():
            pl.when(line < rows - 1)(
                lambda: halves(lambda piece: up_copy(index, piece).wait_send())
            )
            pl.when(jnp.logical_or(source < line, column == 0))(
                lambda: pl.loop(0, crossing(index))(
                    lambda piece: side_copy(index, piece).wait_send()
                )
            )

    pl.when(both(column == 1, line < rows - 1))(lambda: extra_copy().wait_send())

    @pl.loop(0, blocks)
    def _(index):
        pl.when(index <= at)(lambda: save(index).wait())


def attend(projected, heads):
    size = projected.shape[0]
    blocks = lax.axis_size("blk")
    whole = pl.BlockSpec(memory_space=pltpu.VMEM)
    return pl.pallas_call(
        functools.partial(attend_kernel, heads),
        out_shape=(
            jax.ShapeDtypeStruct((size, heads * HEAD), jnp.bfloat16),
            jax.ShapeDtypeStruct((size, heads * HEAD), jnp.float32),
            jax.ShapeDtypeStruct((heads, 1, size), jnp.float32),
            jax.ShapeDtypeStruct((heads, size, 128), jnp.float32),
            jax.ShapeDtypeStruct((blocks, size, 2 * HEAD), jnp.bfloat16),
        ),
        in_specs=[whole],
        out_specs=(whole, whole, whole, whole, pl.BlockSpec(memory_space=pl.ANY)),
        scratch_shapes=[
            pltpu.VMEM((blocks, size, 2 * HEAD), jnp.bfloat16),
            pltpu.VMEM((size, heads * HEAD), jnp.float32),
            pltpu.VMEM((heads, size, 128), jnp.float32),
            pltpu.SemaphoreType.DMA((blocks // 2, PIECES)),
            pltpu.SemaphoreType.DMA((blocks // 2, PIECES)),
            pltpu.SemaphoreType.DMA((blocks // 2, PIECES)),
            pltpu.SemaphoreType.DMA((blocks // 2, PIECES)),
            pltpu.SemaphoreType.DMA((1,)),
            pltpu.SemaphoreType.DMA((1,)),
            pltpu.SemaphoreType.DMA,
            pltpu.SemaphoreType.DMA((blocks,)),
        ],
        compiler_params=pltpu.CompilerParams(
            collective_id=0, has_side_effects=True, vmem_limit_bytes=VMEM_BYTES
        ),
        cost_estimate=cost_of(50),
        name="attend",
    )(projected)


def carry(cross_ref, far_ref, first, sent, landed, across):
    return push_sp(
        cross_ref.at[:, pl.ds(first, far_ref.shape[1]), :], far_ref, sent, landed, across
    )


def attend_back_kernel(heads, carried, *refs):
    if carried:
        x_ref, scaled_ref, delta_ref, kv_ref, cross_ref, out_ref, far_ref, *scratch = refs
        *scratch, cross_sent, cross_landed = scratch
        across = (lax.axis_index("sp") + 2) % 4
        over = carry(cross_ref, far_ref, 0, cross_sent, cross_landed, across)
        after = over.start
    else:
        x_ref, scaled_ref, delta_ref, kv_ref, out_ref, *scratch = refs
        across, after = None, lambda: None
    attend_back_steps(
        heads, across, after, x_ref, scaled_ref, delta_ref, kv_ref, out_ref, *scratch
    )
    if carried:
        over.wait()


def attend_back_steps(
    heads,
    across,
    after_greeting,
    x_ref,
    scaled_ref,
    delta_ref,
    kv_ref,
    out_ref,
    kv,
    part,
    side,
    down,
    dq,
    dk,
    dv,
    load_done,
    side_sent,
    side_landed,
    down_sent,
    down_landed,
    extra,
    extra_done,
):
    at = lax.axis_index("blk")
    blocks = lax.axis_size("blk")
    rows = blocks // 2
    line, column = at // 2, at % 2
    partner = at + 1 - 2 * column
    size = x_ref.shape[0]

    def load(index):
        return pltpu.make_async_copy(kv_ref.at[index], kv.at[index], load_done.at[index])

    @pl.loop(0, blocks)
    def _(index):
        pl.when(index <= at)(lambda: load(index).start())

    greet(at, line, rows, across)
    after_greeting()

    def halves(act):
        pl.loop(0, PIECES)(act)

    def span(piece):
        count = size // PIECES
        return pl.ds(pl.multiple_of(piece * count, count), count)

    def side_copy(target, piece):
        return push(
            part.at[target, 1 - column, span(piece)],
            side.at[target, span(piece)],
            side_sent.at[target, piece],
            side_landed.at[target, piece],
            partner,
        )

    def down_copy(target, piece):
        return push(
            part.at[target, column, span(piece)],
            down.at[target, span(piece)],
            down_sent.at[target, piece],
            down_landed.at[target, piece],
            at - 2,
        )

    def extra_copy():
        return push(
            part.at[0, 0, span(PIECES - 1)], extra, extra_done.at[0], extra_done.at[1], at - 2
        )

    def crossing(target, receives):
        fewer = both(target == 0, line > 0, column == (0 if receives else 1))
        return jnp.where(fewer, PIECES - 1, PIECES)

    def extra_step():
        @pl.when(line < rows - 1)
        def _():
            extra_copy().wait_recv()
            part[0, 0, span(PIECES - 1)] = (
                part[0, 0, span(PIECES - 1)].astype(jnp.float32) + extra[...].astype(jnp.float32)
            ).astype(jnp.bfloat16)

        pl.when(line > 0)(lambda: extra_copy().start())
        pl.when(line == 0)(lambda: side_copy(0, PIECES - 1).start())

    dq[...] = jnp.zeros_like(dq)
    ahead = lax.broadcasted_iota(jnp.int32, (size, size), 0) - lax.broadcasted_iota(
        jnp.int32, (size, size), 1
    )

    def compute(target, half):
        index = 2 * target + half
        load(index).wait()
        span = (at - index) * size
        for head in range(heads):
            columns = slice(head * HEAD, (head + 1) * HEAD)
            query = x_ref[:, columns]
            scaled = scaled_ref[:, columns]
            key = kv[index, :, :HEAD]
            raw = lax.dot_general(
                key, query, (((1,), (1,)), ((), ())), preferred_element_type=jnp.float32
            )
            squashed = jnp.tanh(raw * (HEAD ** (-0.5) / CAP_VALUE))
            weights = jnp.exp(CAP_VALUE * squashed)
            weights = jnp.where(ahead <= span, weights, 0.0)
            inner = lax.dot_general(
                kv[index, :, HEAD:],
                scaled,
                (((1,), (1,)), ((), ())),
                preferred_element_type=jnp.float32,
            )
            grad_raw = (
                weights * (inner - delta_ref[head]) * (1.0 - squashed * squashed)
            ).astype(jnp.bfloat16)
            dv_now = jnp.dot(
                weights.astype(jnp.bfloat16), scaled, preferred_element_type=jnp.float32
            )
            dk_now = jnp.dot(grad_raw, query, preferred_element_type=jnp.float32)
            dq[:, columns] += lax.dot_general(
                grad_raw, key, (((0,), (0,)), ((), ())), preferred_element_type=jnp.float32
            )
            if head == 0:
                dv[...] = dv_now
                dk[...] = dk_now
            else:
                dv[...] += dv_now
                dk[...] += dk_now
        part[target, half, :, :HEAD] = (dk[...] * HEAD ** (-0.5)).astype(jnp.bfloat16)
        part[target, half, :, HEAD:] = dv[...].astype(jnp.bfloat16)

    def merge(target):
        def add(piece, more):
            part[target, column, span(piece)] = (
                part[target, column, span(piece)].astype(jnp.float32) + more.astype(jnp.float32)
            ).astype(jnp.bfloat16)

        def merge_piece(piece):
            meets = jnp.logical_or(target < line, column == 0)

            @pl.when(both(meets, piece < crossing(target, True)))
            def _():
                side_copy(target, piece).wait_recv()
                add(piece, side[target, span(piece)])

            @pl.when(line < rows - 1)
            def _():
                down_copy(target, piece).wait_recv()
                add(piece, down[target, span(piece)])

            pl.when(target < line)(lambda: down_copy(target, piece).start())

        pl.when(both(column == 1, target == 0, line == 0))(extra_step)
        halves(merge_piece)

        @pl.when(target == line)
        def _():
            out_ref[:, heads * HEAD :] = part[target, column]

    @pl.loop(0, rows)
    def _(target):
        away = jnp.logical_or(target < line, both(target == line, column == 1))

        @pl.loop(0, 2)
        def _(way):
            @pl.when(jnp.logical_or(both(way == 0, away), both(way == 1, target <= line)))
            def _():
                compute(target, jnp.where(way == 0, 1 - column, column))

                @pl.when(way == 0)
                def _():
                    now = jnp.where(at == 1, PIECES - 1, crossing(target, False))
                    pl.loop(0, now)(lambda piece: side_copy(target, piece).start())
                    due = jnp.where(line == rows - 1, target == 0, both(target == 1, line > 0))
                    pl.when(both(column == 1, due))(extra_step)

            pl.when(both(way == 0, line == rows - 1, target > 0))(lambda: merge(target - 1))


    out_ref[:, : heads * HEAD] = (dq[...] * HEAD ** (-0.5)).astype(jnp.bfloat16)

    @pl.loop(0, rows)
    def _(target):
        pl.when(both(target <= line, jnp.logical_or(line < rows - 1, target == rows - 1)))(
            lambda: merge(target)
        )

    @pl.loop(0, rows)
    def _(target):
        pl.when(jnp.logical_or(target < line, both(target == line, column == 1)))(
            lambda: pl.loop(0, crossing(target, False))(
                lambda piece: side_copy(target, piece).wait_send()
            )
        )
        pl.when(target < line)(lambda: halves(lambda piece: down_copy(target, piece).wait_send()))

    pl.when(both(column == 1, line > 0))(lambda: extra_copy().wait_send())


def half_of(cross):
    kinds, units, width = cross.shape
    return jax.ShapeDtypeStruct((kinds, units // 2, width), cross.dtype)


def attend_back(projected, scaled, delta, kv_all, cross=None):
    size = projected.shape[0]
    blocks = lax.axis_size("blk")
    rows = blocks // 2
    heads = scaled.shape[1] // HEAD
    whole = pl.BlockSpec(memory_space=pltpu.VMEM)
    far = pl.BlockSpec(memory_space=pl.ANY)
    carried = cross is not None
    far_shape, operands = [], [projected, scaled, delta, kv_all]
    if carried:
        far_shape = [half_of(cross)]
        operands.append(cross)
    return pl.pallas_call(
        functools.partial(attend_back_kernel, heads, carried),
        out_shape=[jax.ShapeDtypeStruct(projected.shape, jnp.bfloat16)] + far_shape,
        in_specs=[whole, whole, whole, far] + [far] * carried,
        out_specs=[whole] + [far] * carried,
        scratch_shapes=[
            pltpu.VMEM((blocks, size, 2 * HEAD), jnp.bfloat16),
            pltpu.VMEM((rows, 2, size, 2 * HEAD), jnp.bfloat16),
            pltpu.VMEM((rows, size, 2 * HEAD), jnp.bfloat16),
            pltpu.VMEM((rows, size, 2 * HEAD), jnp.bfloat16),
            pltpu.VMEM((size, heads * HEAD), jnp.float32),
            pltpu.VMEM((size, HEAD), jnp.float32),
            pltpu.VMEM((size, HEAD), jnp.float32),
            pltpu.SemaphoreType.DMA((blocks,)),
            pltpu.SemaphoreType.DMA((rows, PIECES)),
            pltpu.SemaphoreType.DMA((rows, PIECES)),
            pltpu.SemaphoreType.DMA((rows, PIECES)),
            pltpu.SemaphoreType.DMA((rows, PIECES)),
            pltpu.VMEM((size // PIECES, 2 * HEAD), jnp.bfloat16),
            pltpu.SemaphoreType.DMA((2,)),
        ]
        + [pltpu.SemaphoreType.DMA, pltpu.SemaphoreType.DMA] * carried,
        compiler_params=pltpu.CompilerParams(
            collective_id=1, has_side_effects=True, vmem_limit_bytes=VMEM_BYTES
        ),
        cost_estimate=cost_of(50),
        name="attend_back",
    )(*operands)


def line_gather(
    own_ref,
    full,
    line_sent,
    line_landed,
    extra_sent,
    extra_landed,
    side_sent,
    side_landed,
    first_done,
    own_done,
    ready,
    work,
):
    at = lax.axis_index("blk")
    rows = lax.axis_size("blk") // 2
    line, column = at // 2, at % 2
    partner = at + 1 - 2 * column
    size = own_ref.shape[0]
    half = size // 2

    def span(source, start, count):
        return full.at[pl.ds(pl.multiple_of(2 * source * size + start, half), count), :]

    def line_copy(source, sign, first=False):
        target = span(source, column * size, size)
        return push(
            own_ref if first else target,
            target,
            line_sent.at[(sign + 1) // 2, source],
            line_landed.at[source],
            at + 2 * sign,
        )

    def extra_copy(source, sign):
        target = span(source, (1 - column) * size + half, half)
        return push(
            target,
            target,
            extra_sent.at[(sign + 1) // 2, source],
            extra_landed.at[source],
            at + 2 * sign,
        )

    def side_copy(source, member, count, first=False):
        target = span(source, member * size, count)
        return push(
            own_ref.at[:count] if first else target,
            target,
            side_sent.at[source],
            side_landed.at[source],
            partner,
        )

    def first_copy(member):
        return push(
            own_ref.at[half:],
            span(line, member * size + half, half),
            first_done.at[0],
            first_done.at[1],
            partner,
        )

    def inside(row):
        return jnp.logical_and(row >= 0, row < rows)

    def end(row):
        return jnp.logical_or(row == 0, row == rows - 1)

    def by_end(source, act):
        pl.when(end(source))(lambda: act(half))
        pl.when(jnp.logical_not(end(source)))(lambda: act(size))

    pl.when(end(line))(lambda: first_copy(column).start())
    pl.when(line < rows - 1)(lambda: line_copy(line, 1, True).start())
    pl.when(line > 0)(lambda: line_copy(line, -1, True).start())
    by_end(line, lambda count: side_copy(line, column, count, True).start())
    keep = pltpu.make_async_copy(own_ref, span(line, column * size, size), own_done)
    keep.start()

    @pl.when(end(line))
    def _():
        first_copy(1 - column).wait_recv()
        pl.when(line < rows - 1)(lambda: extra_copy(line, 1).start())
        pl.when(line > 0)(lambda: extra_copy(line, -1).start())

    keep.wait()
    ready()

    @pl.loop(0, rows + 1)
    def _(step):
        @pl.loop(0, 2)
        def _(way):
            sign = 2 * way - 1
            source = line - sign * step

            @pl.when(both(step > 0, inside(source)))
            def _():
                line_copy(source, sign).wait_recv()
                pl.when(inside(line + sign))(lambda: line_copy(source, sign).start())
                by_end(source, lambda count: side_copy(source, column, count).start())

        @pl.loop(0, 2)
        def _(way):
            sign = 2 * way - 1
            source = line - sign * step

            @pl.when(both(step > 0, inside(source), end(source)))
            def _():
                extra_copy(source, sign).wait_recv()
                pl.when(inside(line + sign))(lambda: extra_copy(source, sign).start())

        @pl.loop(0, 2)
        def _(way):
            source = line - (2 * way - 1) * (step - 1)

            @pl.when(both(step > way, inside(source)))
            def _():
                by_end(source, lambda count: side_copy(source, 1 - column, count).wait_recv())
                work(source)

    @pl.loop(0, rows)
    def _(source):
        @pl.when(both(source <= line, line < rows - 1))
        def _():
            line_copy(source, 1).wait_send()
            pl.when(end(source))(lambda: extra_copy(source, 1).wait_send())

        @pl.when(both(source >= line, line > 0))
        def _():
            line_copy(source, -1).wait_send()
            pl.when(end(source))(lambda: extra_copy(source, -1).wait_send())

        by_end(source, lambda count: side_copy(source, column, count).wait_send())

    pl.when(end(line))(lambda: first_copy(column).wait_send())


def line_scatter(
    part,
    side,
    lane,
    tail,
    out_ref,
    side_sent,
    side_landed,
    lane_sent,
    lane_landed,
    tail_done,
    work,
    fill,
    split=False,
):
    at = lax.axis_index("blk")
    rows = lax.axis_size("blk") // 2
    line, column = at // 2, at % 2
    partner = at + 1 - 2 * column
    size = out_ref.shape[0]
    half = size // 2

    def span(target, start, count):
        return pl.ds(pl.multiple_of(2 * target * size + start, half), count)

    def piece(target, which):
        member = jnp.where(which == 2, 1 - column, column)
        return span(target, member * size + jnp.where(which == 0, 0, half), half)

    def side_copy(target, which, count):
        start = which * half
        return push(
            part.at[span(target, (1 - column) * size + start, count), :],
            side.at[target, pl.ds(start, count)],
            side_sent.at[target, which],
            side_landed.at[target, which],
            partner,
        )

    def lane_copy(target, which, sign):
        slot = target if sign == 1 else jnp.where(target == line - 1, rows, target)
        return push(
            part.at[piece(target, which), :],
            lane.at[slot, which],
            lane_sent.at[target, which],
            lane_landed.at[slot, which],
            at + 2 * sign,
        )

    def lane_wait(slot, which):
        push(
            lane.at[slot, which],
            lane.at[slot, which],
            lane_sent.at[0, which],
            lane_landed.at[slot, which],
            partner,
        ).wait_recv()

    def tail_copy():
        return push(
            part.at[piece(line, 2), :], tail, tail_done.at[0], tail_done.at[1], partner
        )

    def inside(row):
        return jnp.logical_and(row >= 0, row < rows)

    def end(row):
        return jnp.logical_or(row == 0, row == rows - 1)

    def sides(target, act):
        pl.when(end(target))(lambda: act(side_copy(target, 0, half)))

        @pl.when(jnp.logical_not(end(target)))
        def _():
            if split:
                pl.loop(0, 2)(lambda which: act(side_copy(target, which, half)))
            else:
                act(side_copy(target, 0, size))

    def add(where, more):
        part[where, :] = (
            part[where, :].astype(jnp.float32) + more.astype(jnp.float32)
        ).astype(jnp.bfloat16)

    def hop(target, which):
        sign = jnp.where(target > line, 1, -1)

        @pl.when(inside(line - sign))
        def _():
            lane_wait(target, which)
            add(piece(target, which), lane[target, which])

        pl.when(target > line)(lambda: lane_copy(target, which, 1).start())
        pl.when(target < line)(lambda: lane_copy(target, which, -1).start())

    def early(target):
        return both(end(target), end(line), target != line)

    @pl.loop(0, rows)
    def _(step):
        @pl.loop(0, 2)
        def _(way):
            target = line + (2 * way - 1) * (rows - 1 - step)

            @pl.when(both(step < rows - way, inside(target)))
            def _():
                work(target)
                sides(target, lambda copy: copy.start())

                pl.when(early(target))(lambda: pl.loop(1, 3)(lambda which: hop(target, which)))

    def gather_lanes(which):
        @pl.loop(0, 2)
        def _(above):
            slot = jnp.where(above == 0, line, rows)

            @pl.when(jnp.where(above == 0, line > 0, line < rows - 1))
            def _():
                lane_wait(slot, which)
                add(piece(line, which), lane[slot, which])

    def merge(target):
        @pl.when(both(end(target), target != line, jnp.logical_not(early(target))))
        def _():
            pl.loop(1, 3)(lambda which: hop(target, which))

        @pl.when(both(end(line), target == line))
        def _():
            gather_lanes(2)
            tail_copy().start()

        if not split:
            sides(target, lambda copy: copy.wait_recv())

        @pl.loop(0, 2)
        def _(which):
            @pl.when(jnp.logical_or(which == 0, jnp.logical_not(end(target))))
            def _():
                if split:
                    side_copy(target, which, half).wait_recv()
                add(piece(target, which), side[target, pl.ds(which * half, half)])
                pl.when(target != line)(lambda: hop(target, which))

    @pl.loop(0, rows)
    def _(step):
        fill(step)

        @pl.loop(0, 2)
        def _(way):
            target = line + (2 * way - 1) * (rows - 1 - step)
            pl.when(both(step < rows - way, inside(target)))(lambda: merge(target))

    pl.loop(0, 2)(lambda which: gather_lanes(1 - which))
    out_ref[...] = part[span(line, column * size, size), :].astype(jnp.float32)

    @pl.when(end(line))
    def _():
        tail_copy().wait_recv()
        out_ref[half:, :] += tail[...].astype(jnp.float32)
        tail_copy().wait_send()

    @pl.loop(0, rows)
    def _(target):
        sides(target, lambda copy: copy.wait_send())

        def sent(sign):
            pl.loop(0, jnp.where(end(target), 3, 2))(
                lambda which: lane_copy(target, which, sign).wait_send()
            )

        pl.when(target > line)(lambda: sent(1))
        pl.when(target < line)(lambda: sent(-1))


def line_sems(rows):
    dma = pltpu.SemaphoreType.DMA
    ways, each = dma((2, rows)), dma((rows,))
    return [ways, each, ways, each, each, each, dma((2,)), dma]


def lane_sems(rows):
    dma = pltpu.SemaphoreType.DMA
    return [dma((rows, 2)), dma((rows, 2)), dma((rows, 3)), dma((rows + 1, 3)), dma((2,))]


def lane_buffers(rows, size, width):
    return [
        pltpu.VMEM((2 * rows * size, width), jnp.bfloat16),
        pltpu.VMEM((rows, size, width), jnp.bfloat16),
        pltpu.VMEM((rows + 1, 3, size // 2, width), jnp.bfloat16),
        pltpu.VMEM((size // 2, width), jnp.bfloat16),
    ]


def ffn_kernel(
    act_ref,
    w_ref,
    middle_ref,
    cotangent_ref,
    gains_ref,
    result_ref,
    grad_ref,
    row_ref,
    acts_ref,
    factors_ref,
    out_ref,
    w,
    acts,
    hidden,
    factors,
    part,
    side,
    lane,
    tail,
    w_done,
    save_done,
    factors_done,
    *sems,
):
    at = lax.axis_index("blk")
    rows = lax.axis_size("blk") // 2
    pair = 2 * act_ref.shape[0]

    def load(which):
        return pltpu.make_async_copy(w_ref.at[which], w.at[which], w_done.at[which])

    def pair_rows(source):
        return pl.ds(pl.multiple_of(source * pair, pair), pair)

    def save(source):
        return pltpu.make_async_copy(
            acts.at[pair_rows(source), :], acts_ref.at[pair_rows(source), :], save_done.at[source]
        )

    for which in range(3):
        load(which).start()
    greet(at, at // 2, rows)

    def ready():
        for which in range(3):
            load(which).wait()

    def expand(source):
        save(source).start()
        rows_now = acts[pair_rows(source), :]
        gate = contract_last(w[0], rows_now)
        up = contract_last(w[1], rows_now)
        hidden[source] = (gelu_value(gate) * up).astype(jnp.bfloat16)

    def reduce(target):
        part[pair_rows(target), :] = lax.dot_general(
            hidden[target], w[2], (((0,), (0,)), ((), ())), preferred_element_type=jnp.float32
        ).astype(jnp.bfloat16)

    line_gather(act_ref, acts, *sems[:8], ready, expand)
    def factors_copy(source):
        return pltpu.make_async_copy(
            factors.at[source % 2],
            factors_ref.at[:, :, pair_rows(source)],
            factors_done.at[source % 2],
        )

    def fill(source):
        rows_now = acts[pair_rows(source), :]
        gate = contract_last(w[0], rows_now)
        up = contract_last(w[1], rows_now)
        bent = jnp.tanh(GELU_SCALE * (gate + GELU_CUBIC * gate * gate * gate))
        slope = 0.5 * (1.0 + bent) + 0.5 * gate * (1.0 - bent * bent) * GELU_SCALE * (
            1.0 + 3.0 * GELU_CUBIC * gate * gate
        )
        pl.when(source > 1)(lambda: factors_copy(source - 2).wait())
        slot = source % 2
        factors[slot, 0] = (up * slope).astype(jnp.bfloat16)
        factors[slot, 1] = (0.5 * gate * (1.0 + bent)).astype(jnp.bfloat16)
        factors[slot, 2] = hidden[source]
        factors_copy(source).start()

    line_scatter(part, side, lane, tail, out_ref, *sems[8:], reduce, fill)
    normed, inverse = norm_parts(out_ref[...])
    result_ref[...] = (middle_ref[...] + normed * gains_ref[3:4, :]).astype(jnp.bfloat16)
    grad_v, gain_row = norm_back(
        cotangent_ref[...].astype(jnp.float32), normed, inverse, gains_ref[3:4, :]
    )
    grad_ref[...] = grad_v.astype(jnp.bfloat16)
    row_ref[...] = gain_row[None, :]
    factors_copy(rows - 2).wait()
    factors_copy(rows - 1).wait()
    pl.loop(0, rows)(lambda source: save(source).wait())


def ffn_forward(act_ffn, w_parts, middle, cotangent, gains):
    size, width = act_ffn.shape
    units = w_parts.shape[1]
    blocks = lax.axis_size("blk")
    rows = blocks // 2
    whole = pl.BlockSpec(memory_space=pltpu.VMEM)
    far = pl.BlockSpec(memory_space=pl.ANY)
    return pl.pallas_call(
        ffn_kernel,
        out_shape=(
            jax.ShapeDtypeStruct((size, width), jnp.bfloat16),
            jax.ShapeDtypeStruct((size, width), jnp.bfloat16),
            jax.ShapeDtypeStruct((1, width), jnp.float32),
            jax.ShapeDtypeStruct((blocks * size, width), jnp.bfloat16),
            jax.ShapeDtypeStruct((3, units, blocks * size), jnp.bfloat16),
        ),
        in_specs=[whole, far, whole, whole, whole],
        out_specs=(whole, whole, whole, far, far),
        scratch_shapes=[
            pltpu.VMEM((size, width), jnp.float32),
            pltpu.VMEM(w_parts.shape, jnp.bfloat16),
            pltpu.VMEM((blocks * size, width), jnp.bfloat16),
            pltpu.VMEM((rows, units, 2 * size), jnp.bfloat16),
            pltpu.VMEM((2, 3, units, 2 * size), jnp.bfloat16),
            *lane_buffers(rows, size, width),
            pltpu.SemaphoreType.DMA((3,)),
            pltpu.SemaphoreType.DMA((rows,)),
            pltpu.SemaphoreType.DMA((2,)),
            *line_sems(rows),
            *lane_sems(rows),
        ],
        compiler_params=pltpu.CompilerParams(
            collective_id=2, has_side_effects=True, vmem_limit_bytes=VMEM_BYTES
        ),
        cost_estimate=cost_of(115),
        name="ffn_forward",
    )(act_ffn, w_parts, middle, cotangent, gains)


FILL_COLUMNS = 768
FILL_FIRST = 0


def ffn_back_kernel(
    owners,
    grad_ref,
    acts_ref,
    factors_ref,
    w_ref,
    out_ref,
    keep_ref,
    cross_ref,
    w,
    rights,
    lefts,
    part,
    side,
    lane,
    tail,
    stage,
    mate_part,
    w_done,
    acts_done,
    factors_done,
    mate_sent,
    mate_landed,
    summed_done,
    *sems,
):
    at = lax.axis_index("blk")
    me = lax.axis_index("sp")
    chip, core = me // 2, me % 2
    mate = me + 1 - 2 * core
    rows = lax.axis_size("blk") // 2
    size, width = grad_ref.shape
    pair = 2 * size
    units = w.shape[1]
    acts, grads = rights.at[0], rights.at[1]

    def load(which):
        return pltpu.make_async_copy(w_ref.at[which], w.at[which], w_done.at[which])

    def pair_rows(source):
        return pl.ds(pl.multiple_of(source * pair, pair), pair)

    acts_copy = pltpu.make_async_copy(acts_ref, acts, acts_done)
    factors_copy = pltpu.make_async_copy(factors_ref, lefts, factors_done)
    load(2).start()
    factors_copy.start()
    load(0).start()
    load(1).start()
    acts_copy.start()
    greet(at, at // 2, rows, mate)

    def ready():
        load(2).wait()
        factors_copy.wait()

    def expand(source):
        columns = pair_rows(source)
        grad_hidden = contract_last(w[2], grads[columns, :])
        for which in range(2):
            lefts[which, :, columns] = (
                lefts[which, :, columns].astype(jnp.float32) * grad_hidden
            ).astype(jnp.bfloat16)

    def reduce(target):
        columns = pair_rows(target)
        dims = (((0,), (0,)), ((), ()))
        total = lax.dot_general(
            lefts[0, :, columns], w[0], dims, preferred_element_type=jnp.float32
        ) + lax.dot_general(lefts[1, :, columns], w[1], dims, preferred_element_type=jnp.float32)
        part[pair_rows(target), :] = total.astype(jnp.bfloat16)

    pieces = width // FILL_COLUMNS
    total_pieces = 3 * pieces

    def piece_columns(item):
        return pl.ds(pl.multiple_of((item % pieces) * FILL_COLUMNS, FILL_COLUMNS), FILL_COLUMNS)

    def mate_copy(item):
        return push_sp(
            stage.at[item % 2, :, 1 - core],
            mate_part.at[item],
            mate_sent.at[item % 2],
            mate_landed.at[item],
            mate,
        )

    def put(item, side_chip, target):
        return pltpu.make_async_copy(
            mate_part.at[item, side_chip],
            target.at[item // pieces, :, piece_columns(item)],
            summed_done.at[item, side_chip],
        )

    def put_wait(item):
        put(item, chip, keep_ref).wait()
        put(item, 1 - chip, cross_ref).wait()

    def sum_one(item):
        mate_copy(item).wait_recv()
        mate_part[item] = (
            stage[item % 2, :, core].astype(jnp.float32) + mate_part[item].astype(jnp.float32)
        ).astype(jnp.bfloat16)
        put(item, chip, keep_ref).start()
        put(item, 1 - chip, cross_ref).start()

    def fill_one(item):
        which = item // pieces
        total = jnp.dot(
            lefts[which],
            rights[which // 2, :, piece_columns(item)],
            preferred_element_type=jnp.float32,
        )
        pl.when(item > 1)(lambda: mate_copy(item - 2).wait_send())
        stage[item % 2] = total.astype(jnp.bfloat16).reshape(
            2, 2, units // owners, FILL_COLUMNS
        )
        mate_copy(item).start()
        pl.when(item > 0)(lambda: sum_one(item - 1))

    each = pl.cdiv(total_pieces - FILL_FIRST, rows - 1)

    def fill(step):
        first = jnp.maximum(FILL_FIRST + (step - 1) * each, 0)
        last = jnp.minimum(FILL_FIRST + step * each, total_pieces)

        @pl.loop(0, each)
        def _(item):
            pl.when(first + item < last)(lambda: fill_one(first + item))

    line_gather(grad_ref, grads, *sems[:8], ready, expand)
    load(0).wait()
    load(1).wait()
    acts_copy.wait()
    line_scatter(part, side, lane, tail, out_ref, *sems[8:], reduce, fill)
    sum_one(total_pieces - 1)
    pl.loop(0, total_pieces)(put_wait)
    for item in range(total_pieces - 2, total_pieces):
        mate_copy(item).wait_send()


def ffn_back(grad_ffn, kept, w_parts, owners):
    size, width = grad_ffn.shape
    units = w_parts.shape[1]
    blocks = lax.axis_size("blk")
    rows = blocks // 2
    tokens = blocks * size
    items = 3 * width // FILL_COLUMNS
    whole = pl.BlockSpec(memory_space=pltpu.VMEM)
    far = pl.BlockSpec(memory_space=pl.ANY)
    return pl.pallas_call(
        functools.partial(ffn_back_kernel, owners),
        out_shape=(
            jax.ShapeDtypeStruct((size, width), jnp.float32),
            jax.ShapeDtypeStruct((3, units // owners, width), jnp.bfloat16),
            jax.ShapeDtypeStruct((3, units // owners, width), jnp.bfloat16),
        ),
        in_specs=[whole, far, far, far],
        out_specs=(whole, far, far),
        scratch_shapes=[
            pltpu.VMEM(w_parts.shape, jnp.bfloat16),
            pltpu.VMEM((2, tokens, width), jnp.bfloat16),
            pltpu.VMEM((3, units, tokens), jnp.bfloat16),
            *lane_buffers(rows, size, width),
            pltpu.VMEM((2, 2, 2, units // owners, FILL_COLUMNS), jnp.bfloat16),
            pltpu.VMEM((items, 2, units // owners, FILL_COLUMNS), jnp.bfloat16),
            pltpu.SemaphoreType.DMA((3,)),
            pltpu.SemaphoreType.DMA,
            pltpu.SemaphoreType.DMA,
            pltpu.SemaphoreType.DMA((2,)),
            pltpu.SemaphoreType.DMA((items,)),
            pltpu.SemaphoreType.DMA((items, 2)),
            *line_sems(rows),
            *lane_sems(rows),
        ],
        compiler_params=pltpu.CompilerParams(
            collective_id=3, has_side_effects=True, vmem_limit_bytes=VMEM_BYTES
        ),
        cost_estimate=cost_of(115),
        name="ffn_back",
    )(grad_ffn, *kept, w_parts)


def ffn_hidden(acts, w_parts):
    gate = contract_last(acts, w_parts[0])
    up = contract_last(acts, w_parts[1])
    return (gate, up, (gelu_value(gate) * up).astype(jnp.bfloat16))


def scatter_tokens(partial):
    return lax.psum_scatter(
        partial.astype(jnp.bfloat16), "blk", scatter_dimension=0, tiled=True
    ).astype(jnp.float32)


def ffn_forward_wide(act_ffn, w_parts, middle, cotangent, gains):
    acts = lax.all_gather(act_ffn, "blk", axis=0, tiled=True)
    hidden = ffn_hidden(acts, w_parts)[2]
    partial = jnp.dot(hidden, w_parts[2], preferred_element_type=jnp.float32)
    normed, inverse = norm_parts(scatter_tokens(partial))
    result = (middle + normed * gains[3]).astype(jnp.bfloat16)
    grad_v, gain_row = norm_back(cotangent.astype(jnp.float32), normed, inverse, gains[3])
    return (result, grad_v.astype(jnp.bfloat16), gain_row[None], acts)


def ffn_back_wide(grad_ffn, kept, w_parts, owners):
    (acts,) = kept
    grads = lax.all_gather(grad_ffn, "blk", axis=0, tiled=True)
    gate, up, hidden = ffn_hidden(acts, w_parts)
    grad_hidden = contract_last(grads, w_parts[2])
    grad_gate = (grad_hidden * up * gelu_slope(gate)).astype(jnp.bfloat16)
    grad_up = (grad_hidden * gelu_value(gate)).astype(jnp.bfloat16)
    partial = jnp.dot(grad_gate, w_parts[0], preferred_element_type=jnp.float32) + jnp.dot(
        grad_up, w_parts[1], preferred_element_type=jnp.float32
    )
    sums = jnp.stack(
        [
            jnp.einsum("tf,td->fd", left, right, preferred_element_type=jnp.float32)
            for left, right in ((grad_gate, acts), (grad_up, acts), (hidden, grads))
        ]
    ).astype(jnp.bfloat16)
    units = w_parts.shape[1]
    owned = sums.reshape(3, owners, units // owners, sums.shape[2])
    mine = lax.psum_scatter(
        jnp.transpose(owned, (1, 0, 2, 3)), "sp", scatter_dimension=0, tiled=True
    )
    return (scatter_tokens(partial), mine[0], None)


def cost_of(microseconds):
    return pl.CostEstimate(
        flops=int(microseconds * 1e9), bytes_accessed=int(microseconds * 3e6), transcendentals=0
    )


def push_sp(source, target, sent, landed, peer):
    return pltpu.make_async_remote_copy(
        src_ref=source,
        dst_ref=target,
        send_sem=sent,
        recv_sem=landed,
        device_id={"sp": peer},
        device_id_type=pl.DeviceIdType.MESH,
    )


def greet_sp(me, groups, before_wait=lambda: None):
    barrier = pltpu.get_barrier_semaphore()
    for step in range(1, groups):
        pl.semaphore_signal(
            barrier,
            inc=1,
            device_id={"sp": (me + step) % groups},
            device_id_type=pl.DeviceIdType.MESH,
        )
    before_wait()
    pl.semaphore_wait(barrier, groups - 1)


def gather_rows(x, w_ref, full_ref, w, w_done, own_done, sent, landed, prepare, project):
    me = lax.axis_index("sp")
    size = x.shape[0]
    units = w.shape[0]
    mate = me + 1 - 2 * (me % 2)
    across = (me + 2) % 4

    def spot(member):
        return full_ref.at[pl.ds(pl.multiple_of(member * size, size), size), :]

    load = pltpu.make_async_copy(
        w_ref.at[pl.ds(pl.multiple_of(me * units, units), units), :], w, w_done
    )
    load.start()
    greet_sp(me, 4, prepare)
    half = size // 2

    def half_spot(member, piece):
        start = pl.multiple_of(member * size + piece * half, half)
        return full_ref.at[pl.ds(start, half), :]

    def over(piece):
        return push_sp(
            x.at[pl.ds(piece * half, half)],
            half_spot(me, piece),
            sent.at[piece],
            landed.at[piece],
            across,
        )

    def onward(piece):
        rows_now = half_spot(across, piece)
        return push_sp(rows_now, rows_now, sent.at[3 + piece], landed.at[3 + piece], mate)

    over(0).start()
    over(1).start()
    beside = push_sp(x, spot(me), sent.at[2], landed.at[2], mate)
    beside.start()
    keep = pltpu.make_async_copy(x, spot(me), own_done)
    keep.start()
    keep.wait()
    load.wait()

    def project_chip(chip):
        rows = pl.ds(pl.multiple_of(chip * 2 * size, 2 * size), 2 * size)
        project(rows, contract_last(full_ref[rows, :], w[...]).astype(jnp.bfloat16))

    beside.wait_recv()
    project_chip(me // 2)
    for piece in range(2):
        over(piece).wait_recv()
        onward(piece).start()
    for piece in range(2):
        onward(piece).wait_recv()
    project_chip(across // 2)
    beside.wait_send()
    for piece in range(2):
        over(piece).wait_send()
        onward(piece).wait_send()


def project_in_kernel(tokens_ref, gains_ref, w_ref, full_ref, out_ref, x, *scratch):
    def prepare():
        normed = norm_parts(tokens_ref[...].astype(jnp.float32))[0]
        x[...] = (normed * gains_ref[0:1, :]).astype(jnp.bfloat16)

    def project(rows, value):
        out_ref[rows, :] = value

    gather_rows(x, w_ref, full_ref, *scratch, prepare, project)


def gather_scratch(size, width, units):
    dma = pltpu.SemaphoreType.DMA
    return [
        pltpu.VMEM((size, width), jnp.bfloat16),
        pltpu.VMEM((units, width), jnp.bfloat16),
        dma,
        dma,
        dma((5,)),
        dma((5,)),
    ]


def project_in(tokens, gains, weights):
    size, width = tokens.shape
    units = weights.shape[0] // 4
    whole = pl.BlockSpec(memory_space=pltpu.VMEM)
    return pl.pallas_call(
        project_in_kernel,
        out_shape=(
            jax.ShapeDtypeStruct((4 * size, width), jnp.bfloat16),
            jax.ShapeDtypeStruct((4 * size, units), jnp.bfloat16),
        ),
        in_specs=[whole, whole, pl.BlockSpec(memory_space=pl.ANY)],
        out_specs=(whole, whole),
        scratch_shapes=gather_scratch(size, width, units),
        compiler_params=pltpu.CompilerParams(
            collective_id=4, has_side_effects=True, vmem_limit_bytes=VMEM_BYTES
        ),
        cost_estimate=cost_of(18),
        name="project_in",
    )(tokens, gains, weights)


def project_back_kernel(
    grad_ref,
    middle_ref,
    attn_ref,
    cotangent_ref,
    gains_ref,
    attended_ref,
    by_row_ref,
    totals_ref,
    w_ref,
    full_ref,
    scaled_ref,
    delta_ref,
    grad_middle_ref,
    rows_ref,
    x,
    *scratch,
):
    def prepare():
        grad_v, row_two = norm_back(
            grad_ref[...], *norm_parts(middle_ref[...]), gains_ref[2:3, :]
        )
        grad_middle = cotangent_ref[...].astype(jnp.float32) + grad_v
        grad_middle_ref[...] = grad_middle
        grad_v, row_one = norm_back(grad_middle, *norm_parts(attn_ref[...]), gains_ref[1:2, :])
        x[...] = grad_v.astype(jnp.bfloat16)
        rows_ref[...] = jnp.zeros_like(rows_ref)
        rows_ref[1:2, :] = row_one[None, :]
        rows_ref[2:3, :] = row_two[None, :]

    def project(rows, value):
        for head in range(value.shape[1] // HEAD):
            columns = slice(head * HEAD, (head + 1) * HEAD)
            grad = value[:, columns].astype(jnp.float32)
            scaled_ref[rows, columns] = (grad / by_row_ref[head, rows, :1]).astype(jnp.bfloat16)
            product = grad * attended_ref[rows, columns]
            delta_ref[head, :, rows] = (
                jnp.sum(product.T, axis=0, keepdims=True) / totals_ref[head, :, rows]
            )

    gather_rows(x, w_ref, full_ref, *scratch, prepare, project)


def project_back(
    grad_act, middle, attn, cotangent, gains, attended, by_row, totals, weights
):
    size, width = attn.shape
    units = weights.shape[0] // 4
    whole = pl.BlockSpec(memory_space=pltpu.VMEM)
    return pl.pallas_call(
        project_back_kernel,
        out_shape=(
            jax.ShapeDtypeStruct((4 * size, width), jnp.bfloat16),
            jax.ShapeDtypeStruct((4 * size, units), jnp.bfloat16),
            jax.ShapeDtypeStruct(totals.shape, jnp.float32),
            jax.ShapeDtypeStruct((size, width), jnp.float32),
            jax.ShapeDtypeStruct((8, width), jnp.float32),
        ),
        in_specs=[whole] * 8 + [pl.BlockSpec(memory_space=pl.ANY)],
        out_specs=(whole,) * 5,
        scratch_shapes=gather_scratch(size, width, units),
        compiler_params=pltpu.CompilerParams(
            collective_id=6, has_side_effects=True, vmem_limit_bytes=VMEM_BYTES
        ),
        cost_estimate=cost_of(20),
        name="project_back",
    )(grad_act, middle, attn, cotangent, gains, attended, by_row, totals, weights)


def exchange_norm_kernel(x_ref, w_ref, tokens_ref, gains_ref, out_ref, middle_ref, act_ref, *scratch):
    exchange_project_kernel(x_ref, w_ref, out_ref, *scratch)
    normed = norm_parts(out_ref[...])[0]
    middle = tokens_ref[...].astype(jnp.float32) + normed * gains_ref[1:2, :]
    middle_ref[...] = middle
    act_ref[...] = (norm_parts(middle)[0] * gains_ref[2:3, :]).astype(jnp.bfloat16)


def exchange_project_kernel(x_ref, w_ref, out_ref, w, got, w_done, own_done, sent, landed):
    me = lax.axis_index("sp")
    size = out_ref.shape[0]
    units = x_ref.shape[1]

    def rows_of(member):
        return x_ref.at[pl.ds(pl.multiple_of(member * size, size), size), :]

    def load(member):
        rows = pl.ds(pl.multiple_of(member * units, units), units)
        return pltpu.make_async_copy(w_ref.at[rows, :], w.at[rows, :], w_done.at[member])

    def send(step):
        peer = (me + step) % 4
        return push_sp(rows_of(peer), got.at[4 - step], sent.at[step], landed.at[4 - step], peer)

    greet_sp(me, 4)
    for step in (2, 1, 3):
        send(step).start()
    keep = pltpu.make_async_copy(rows_of(me), got.at[0], own_done)
    keep.start()
    for step in range(4):
        load((me + step) % 4).start()
    keep.wait()
    for step in (0, 1, 3, 2):
        member = (me + step) % 4
        load(member).wait()
        if step > 0:
            send(4 - step).wait_recv()
        rows = pl.ds(pl.multiple_of(member * units, units), units)
        term = jnp.dot(got[step], w[rows, :], preferred_element_type=jnp.float32)
        if step == 0:
            out_ref[...] = term
        else:
            out_ref[...] += term
    for step in (1, 2, 3):
        send(step).wait_send()


def exchange_project(columns, weights, identity, norm_inputs=()):
    size = columns.shape[0] // 4
    whole = pl.BlockSpec(memory_space=pltpu.VMEM)
    total = jax.ShapeDtypeStruct((size, weights.shape[1]), jnp.float32)
    low = jax.ShapeDtypeStruct(total.shape, jnp.bfloat16)
    shapes = [total, total, low] if norm_inputs else [total]
    return pl.pallas_call(
        exchange_norm_kernel if norm_inputs else exchange_project_kernel,
        out_shape=shapes,
        in_specs=[whole, pl.BlockSpec(memory_space=pl.ANY)] + [whole] * len(norm_inputs),
        out_specs=[whole] * len(shapes),
        scratch_shapes=[
            pltpu.VMEM(weights.shape, jnp.bfloat16),
            pltpu.VMEM((4, size, columns.shape[1]), jnp.bfloat16),
            pltpu.SemaphoreType.DMA((4,)),
            pltpu.SemaphoreType.DMA,
            pltpu.SemaphoreType.DMA((4,)),
            pltpu.SemaphoreType.DMA((4,)),
        ],
        compiler_params=pltpu.CompilerParams(
            collective_id=identity, has_side_effects=True, vmem_limit_bytes=VMEM_BYTES
        ),
        cost_estimate=cost_of(16),
        name="exchange_project",
    )(columns, weights, *norm_inputs)


def finish_kernel(
    cols_ref,
    act_ref,
    att_ref,
    grad_ref,
    w_ref,
    tokens_ref,
    middle_ref,
    gains_in_ref,
    rows_ref,
    row_three_ref,
    cross_ref,
    qkv_ref,
    out_ref,
    tokens_grad_ref,
    gains_ref,
    far_ref,
    w,
    got,
    grad_in,
    total,
    part,
    side,
    lane,
    tail,
    mine,
    from_sp,
    from_side,
    from_line,
    w_done,
    own_done,
    swap_sent,
    swap_landed,
    sp_sent,
    sp_landed,
    gain_side,
    line_sent,
    line_landed,
    cross_sent,
    cross_landed,
    *sems,
):
    at = lax.axis_index("blk")
    me = lax.axis_index("sp")
    rows = lax.axis_size("blk") // 2
    line, column = at // 2, at % 2
    partner = at + 1 - 2 * column
    block = total.shape[0]
    size = tokens_ref.shape[0]
    units = cols_ref.shape[1]
    extra = block - size

    barrier = pltpu.get_barrier_semaphore()
    for step in range(1, 4):
        pl.semaphore_signal(
            barrier, inc=1, device_id={"sp": (me + step) % 4}, device_id_type=pl.DeviceIdType.MESH
        )

    def line_peer(step):
        return 2 * ((line + step) % rows) + column

    for peer in [partner] + [line_peer(step) for step in range(1, rows)]:
        pl.semaphore_signal(
            barrier, inc=1, device_id={"blk": peer}, device_id_type=pl.DeviceIdType.MESH
        )

    def load(member):
        span = pl.ds(pl.multiple_of(member * units, units), units)
        return pltpu.make_async_copy(w_ref.at[span, :], w.at[span, :], w_done.at[member])

    def rows_of(member):
        return cols_ref.at[pl.ds(pl.multiple_of(member * size, size), size), :]

    def swap(step):
        peer = (me + step) % 4
        return push_sp(
            rows_of(peer), got.at[4 - step], swap_sent.at[step], swap_landed.at[4 - step], peer
        )

    for step in range(4):
        load((me + step) % 4).start()
    keep = pltpu.make_async_copy(rows_of(me), got.at[0], own_done)
    keep.start()
    pl.semaphore_wait(barrier, 3 + rows)
    for step in (2, 1, 3):
        swap(step).start()
    over = carry(
        cross_ref, far_ref, far_ref.shape[1], cross_sent, cross_landed, (me + 2) % 4
    )
    over.start()
    keep.wait()

    def sp_gains(step):
        return push_sp(
            mine, from_sp.at[4 - step], sp_sent.at[step], sp_landed.at[4 - step], (me + step) % 4
        )

    def side_gains():
        return push(from_sp.at[0], from_side, gain_side.at[0], gain_side.at[1], partner)

    def line_gains(step):
        return push(
            from_line.at[0],
            from_line.at[rows - step],
            line_sent.at[step],
            line_landed.at[rows - step],
            line_peer(step),
        )

    def reduce(target):
        dims = (((0,), (0,)), ((), ()))
        wide_columns = pl.ds(pl.multiple_of(target * 2 * size, 2 * size), 2 * size)
        term = lax.dot_general(
            cols_ref[:, wide_columns], act_ref[...], dims, preferred_element_type=jnp.float32
        ).astype(jnp.bfloat16)
        columns = pl.ds(pl.multiple_of(target * 2 * extra, 2 * extra), 2 * extra)
        more = lax.dot_general(
            att_ref[:, columns], grad_ref[...], dims, preferred_element_type=jnp.float32
        ).astype(jnp.bfloat16)
        for half in range(2):
            start = pl.multiple_of((2 * target + half) * block, block)
            part[pl.ds(start, size), :] = term[half * size : (half + 1) * size]
            start = pl.multiple_of((2 * target + half) * block + size, extra)
            part[pl.ds(start, extra), :] = more[half * extra : (half + 1) * extra]

    def inputs_back():
        for step in (0, 1, 3, 2):
            member = (me + step) % 4
            load(member).wait()
            if step > 0:
                swap(4 - step).wait_recv()
            span = pl.ds(pl.multiple_of(member * units, units), units)
            term = jnp.dot(got[step], w[span, :], preferred_element_type=jnp.float32)
            if step == 0:
                grad_in[...] = term
            else:
                grad_in[...] += term
        normed, inverse = norm_parts(tokens_ref[...].astype(jnp.float32))
        grad_v, gain_row = norm_back(grad_in[...], normed, inverse, gains_in_ref[0:1, :])
        tokens_grad_ref[...] = (middle_ref[...] + grad_v).astype(jnp.bfloat16)
        mine[...] = rows_ref[...]
        mine[0:1, :] = gain_row[None, :]
        mine[3:4, :] = row_three_ref[...]
        for step in range(1, 4):
            sp_gains(step).start()

    def fill(step):
        pl.when(step == 2)(inputs_back)

        @pl.when(step == 3)
        def _():
            gains = mine[...]
            for other in range(1, 4):
                sp_gains(4 - other).wait_recv()
                gains = gains + from_sp[other]
            from_sp[0] = gains
            side_gains().start()

        @pl.when(step == 3)
        def _():
            side_gains().wait_recv()
            from_line[0] = from_sp[0] + from_side[...]
            for other in range(1, rows):
                line_gains(other).start()

    line_scatter(part, side, lane, tail, total, *sems, reduce, fill, split=True)
    qkv_ref[...] = total[:size]
    out_ref[...] = total[size:]
    gains = from_line[0]
    for other in range(1, rows):
        line_gains(rows - other).wait_recv()
        gains = gains + from_line[other]
    gains_ref[...] = gains
    for step in (1, 2, 3):
        swap(step).wait_send()
        sp_gains(step).wait_send()
    over.wait()
    side_gains().wait_send()
    for step in range(1, rows):
        line_gains(step).wait_send()


def finish(
    cols, act_block, attended, grad_block, w_qkv, tokens, grad_middle, gains, rows, row_three, cross
):
    blocks = lax.axis_size("blk")
    lines = blocks // 2
    size, width = tokens.shape
    block = (cols.shape[1] + attended.shape[1]) // blocks
    whole = pl.BlockSpec(memory_space=pltpu.VMEM)
    any_space = pl.BlockSpec(memory_space=pl.ANY)
    dma = pltpu.SemaphoreType.DMA
    small = rows.shape
    return pl.pallas_call(
        finish_kernel,
        out_shape=(
            jax.ShapeDtypeStruct((cols.shape[1] // blocks, width), jnp.float32),
            jax.ShapeDtypeStruct((attended.shape[1] // blocks, width), jnp.float32),
            jax.ShapeDtypeStruct((size, width), jnp.bfloat16),
            jax.ShapeDtypeStruct(small, jnp.float32),
            half_of(cross),
        ),
        in_specs=[whole] * 4 + [any_space] + [whole] * 5 + [any_space],
        out_specs=(whole, whole, whole, whole, any_space),
        scratch_shapes=[
            pltpu.VMEM(w_qkv.shape, jnp.bfloat16),
            pltpu.VMEM((4, size, cols.shape[1]), jnp.bfloat16),
            pltpu.VMEM((size, width), jnp.float32),
            pltpu.VMEM((block, width), jnp.float32),
            *lane_buffers(lines, block, width),
            pltpu.VMEM(small, jnp.float32),
            pltpu.VMEM((4, *small), jnp.float32),
            pltpu.VMEM(small, jnp.float32),
            pltpu.VMEM((lines, *small), jnp.float32),
            dma((4,)),
            dma,
            dma((4,)),
            dma((4,)),
            dma((4,)),
            dma((4,)),
            dma((2,)),
            dma((lines,)),
            dma((lines,)),
            dma,
            dma,
            *lane_sems(lines),
        ],
        compiler_params=pltpu.CompilerParams(
            collective_id=8, has_side_effects=True, vmem_limit_bytes=VMEM_BYTES
        ),
        cost_estimate=cost_of(85),
        name="finish",
    )(
        cols,
        act_block,
        attended,
        grad_block,
        w_qkv,
        tokens,
        grad_middle,
        gains,
        rows,
        row_three,
        cross,
    )


def weight_sums_wide(left, right):
    term = jnp.einsum("tc,td->cd", left, right, preferred_element_type=jnp.float32)
    return scatter_tokens(term)


def finish_wide(
    cols, act_block, attended, grad_block, w_qkv, tokens, grad_middle, gains, rows, row_three, cross
):
    (grad_act_in,) = exchange_project(cols, w_qkv, 7)
    normed, inverse = norm_parts(tokens.astype(jnp.float32))
    grad_v, gain_row = norm_back(grad_act_in, normed, inverse, gains[0])
    gains_all = lax.psum(
        jnp.concatenate([gain_row[None], rows[1:3], row_three, rows[4:]]), ("blk", "sp")
    )
    return (
        weight_sums_wide(cols, act_block),
        weight_sums_wide(attended, grad_block),
        (grad_middle + grad_v).astype(jnp.bfloat16),
        gains_all,
        None,
    )


def deliver_kernel(*refs):
    keep_ref, first_ref, last_ref, *others = refs
    ins, sum_ref, outs = others[:4], others[4], others[5:]
    half = first_ref.shape[1]
    for start, far_ref in ((0, first_ref), (half, last_ref)):
        rows = slice(start, start + half)
        sum_ref[:, rows] = keep_ref[:, rows].astype(jnp.float32) + far_ref[...].astype(
            jnp.float32
        )
    for source, target in zip(ins, outs):
        target[...] = source[...]


def deliver(keep, first, last, *results):
    kinds, units, width = keep.shape
    copies = [
        pl.BlockSpec((result.shape[0] // 2, width), lambda i: (jnp.minimum(i, 1), 0))
        for result in results
    ]
    sums = pl.BlockSpec((1, units, width), lambda i: (i, 0, 0))
    halves = pl.BlockSpec((1, units // 2, width), lambda i: (i, 0, 0))
    return pl.pallas_call(
        deliver_kernel,
        grid=(kinds,),
        out_shape=[jax.ShapeDtypeStruct(keep.shape, jnp.float32)]
        + [jax.ShapeDtypeStruct(result.shape, result.dtype) for result in results],
        in_specs=[sums, halves, halves] + copies,
        out_specs=[sums] + copies,
        compiler_params=pltpu.CompilerParams(vmem_limit_bytes=VMEM_BYTES),
        cost_estimate=cost_of(8),
        name="deliver",
    )(keep, first, last, *results)


def body(tokens, w_qkv, w_out, gains, w_ffn, cotangent):
    groups = lax.axis_size("sp")
    wide = lax.axis_size("blk") > 8
    act_block, projected = project_in(tokens, gains, w_qkv)
    attended_low, attended, totals, by_row, kv_all = attend(projected, HEADS // groups)
    attn, middle, act_ffn = exchange_project(attended_low, w_out, 5, (tokens, gains))
    w_parts = jnp.transpose(w_ffn, (1, 0, 2))
    result, grad_ffn, row_three, *kept = (ffn_forward_wide if wide else ffn_forward)(
        act_ffn, w_parts, middle, cotangent, gains
    )
    grad_act_ffn, ffn_part, cross = (ffn_back_wide if wide else ffn_back)(
        grad_ffn, kept, w_parts, groups
    )
    grad_block, scaled, delta, grad_middle, rows = project_back(
        grad_act_ffn, middle, attn, cotangent, gains, attended, by_row, totals, w_out
    )
    grad_cols, *far_first = attend_back(projected, scaled, delta, kv_all, cross)
    qkv_grad, out_grad, tokens_grad, gains_all, far_last = (finish_wide if wide else finish)(
        grad_cols,
        act_block,
        attended_low,
        grad_block,
        w_qkv,
        tokens,
        grad_middle,
        gains,
        rows,
        row_three,
        cross,
    )
    if wide:
        ffn_sum = ffn_part.astype(jnp.float32)
    else:
        ffn_sum, result, tokens_grad, qkv_grad, out_grad = deliver(
            ffn_part, *far_first, far_last, result, tokens_grad, qkv_grad, out_grad
        )
    ffn_grad = jnp.transpose(ffn_sum, (1, 0, 2))
    share = gains_all.shape[1] // (groups * lax.axis_size("blk"))
    place = lax.axis_index("sp") * lax.axis_size("blk") + lax.axis_index("blk")
    gains_grad = lax.dynamic_slice_in_dim(gains_all[:4], place * share, share, 1)
    return (result, tokens_grad, qkv_grad, out_grad, gains_grad, ffn_grad)


def solution(mesh):
    return jax.shard_map(
        body,
        mesh=mesh,
        in_specs=(
            P(("blk", "sp"), None),
            P(),
            P(),
            P(),
            P("blk", None, None),
            P(("blk", "sp"), None),
        ),
        out_specs=(
            P(("blk", "sp"), None),
            P(("blk", "sp"), None),
            P(("sp", "blk"), None),
            P(("sp", "blk"), None),
            P(None, ("sp", "blk")),
            P(("blk", "sp"), None, None),
        ),
        check_vma=False,
    )
```

```python
import functools

import jax
import jax.numpy as jnp
from jax import lax
from jax.experimental import pallas as pl
from jax.experimental.pallas import tpu as pltpu
from jax.sharding import PartitionSpec as P

HEADS = 8
KV_HEADS = 4
HEAD = 256


VMEM_BYTES = 62 * 1024 * 1024
PIECES = 2
NORM_EPSILON = 1e-06
CAP_VALUE = 50.0
GELU_SCALE = 0.7978845608028654
GELU_CUBIC = 0.044715


def norm_parts(values):
    inverse = lax.rsqrt(jnp.mean(values * values, axis=-1, keepdims=True) + NORM_EPSILON)
    return (values * inverse, inverse)


def norm_back(grad_y, normed, inverse, gain):
    grad_n = grad_y * gain
    grad_v = inverse * (grad_n - normed * jnp.mean(grad_n * normed, axis=-1, keepdims=True))
    return (grad_v, jnp.sum(grad_y * normed, axis=0))


def gelu_value(values):
    return (
        0.5
        * values
        * (1.0 + jnp.tanh(GELU_SCALE * (values + GELU_CUBIC * values * values * values)))
    )


def gelu_slope(values):
    bent = jnp.tanh(GELU_SCALE * (values + GELU_CUBIC * values * values * values))
    return 0.5 * (1.0 + bent) + 0.5 * values * (1.0 - bent * bent) * GELU_SCALE * (
        1.0 + 3.0 * GELU_CUBIC * values * values
    )


def contract_last(left, right):
    return lax.dot_general(
        left, right, (((1,), (1,)), ((), ())), preferred_element_type=jnp.float32
    )


def push(source, target, sent, landed, block):
    return pltpu.make_async_remote_copy(
        src_ref=source,
        dst_ref=target,
        send_sem=sent,
        recv_sem=landed,
        device_id={"blk": block},
        device_id_type=pl.DeviceIdType.MESH,
    )


def greet(at, line, rows, sp_peer=None):
    barrier = pltpu.get_barrier_semaphore()
    others = 1
    if sp_peer is not None:
        others = 2
        pl.semaphore_signal(
            barrier, inc=1, device_id={"sp": sp_peer}, device_id_type=pl.DeviceIdType.MESH
        )

    def tell(block):
        pl.semaphore_signal(
            barrier, inc=1, device_id={"blk": block}, device_id_type=pl.DeviceIdType.MESH
        )

    tell(at + 1 - 2 * (at % 2))
    pl.when(line > 0)(lambda: tell(at - 2))
    pl.when(line < rows - 1)(lambda: tell(at + 2))
    pl.semaphore_wait(barrier, others + jnp.minimum(line, 1) + jnp.minimum(rows - 1 - line, 1))


def both(*terms):
    result = terms[0]
    for term in terms[1:]:
        result = jnp.logical_and(result, term)
    return result


def attend_kernel(
    heads,
    x_ref,
    low_ref,
    att_ref,
    tot_ref,
    by_row_ref,
    kv_ref,
    kv,
    acc,
    part,
    up_sent,
    up_landed,
    side_sent,
    side_landed,
    extra_sent,
    extra_landed,
    own_done,
    save_done,
):
    at = lax.axis_index("blk")
    blocks = lax.axis_size("blk")
    rows = blocks // 2
    line, column = at // 2, at % 2
    partner = at + 1 - 2 * column
    size = x_ref.shape[0]
    first = heads * HEAD
    own = x_ref.at[:, pl.ds(first, 2 * HEAD)]
    greet(at, line, rows)

    def halves(act):
        pl.loop(0, PIECES)(act)

    def span(piece):
        count = size // PIECES
        return pl.ds(pl.multiple_of(piece * count, count), count)

    def source_of(index, piece, is_own):
        if is_own:
            return x_ref.at[span(piece), pl.ds(first, 2 * HEAD)]
        return kv.at[index, span(piece)]

    def up_copy(index, piece, is_own=False):
        return push(
            source_of(index, piece, is_own),
            kv.at[index, span(piece)],
            up_sent.at[index // 2, piece],
            up_landed.at[index // 2, piece],
            at + 2,
        )

    def side_copy(index, piece, is_own=False):
        return push(
            source_of(index, piece, is_own),
            kv.at[index, span(piece)],
            side_sent.at[index // 2, piece],
            side_landed.at[index // 2, piece],
            partner,
        )

    def extra_copy():
        rows_now = kv.at[0, span(PIECES - 1)]
        return push(rows_now, rows_now, extra_sent.at[0], extra_landed.at[0], at + 2)

    def crossing(index):
        return jnp.where(both(index == 0, at > 0), PIECES - 1, PIECES)

    def save(index):
        return pltpu.make_async_copy(kv.at[index], kv_ref.at[index], save_done.at[index])

    @pl.loop(0, PIECES)
    def _(piece):
        pl.when(line < rows - 1)(lambda: up_copy(at, piece, True).start())
        pl.when(column == 0)(lambda: side_copy(at, PIECES - 1 - piece, True).start())

    keep = pltpu.make_async_copy(own, kv.at[at], own_done)
    keep.start()
    acc[...] = jnp.zeros_like(acc)
    part[...] = jnp.zeros_like(part)
    keep.wait()

    @pl.when(at == 1)
    def _():
        side_copy(0, PIECES - 1).wait_recv()
        extra_copy().start()

    ahead = lax.broadcasted_iota(jnp.int32, (size, size), 1) - lax.broadcasted_iota(
        jnp.int32, (size, size), 0
    )

    def compute(index):
        save(index).start()
        span = (at - index) * size
        for head in range(heads):
            raw = lax.dot_general(
                x_ref[:, head * HEAD : (head + 1) * HEAD],
                kv[index, :, :HEAD],
                (((1,), (1,)), ((), ())),
                preferred_element_type=jnp.float32,
            )
            weights = jnp.exp(CAP_VALUE * jnp.tanh(raw * (HEAD ** (-0.5) / CAP_VALUE)))
            weights = jnp.where(ahead <= span, weights, 0.0)
            total = weights[:, :128]
            for piece in range(1, size // 128):
                total = total + weights[:, piece * 128 : (piece + 1) * 128]
            part[head] += total
            acc[:, head * HEAD : (head + 1) * HEAD] += jnp.dot(
                weights.astype(jnp.bfloat16),
                kv[index, :, HEAD:],
                preferred_element_type=jnp.float32,
            )

    @pl.loop(0, rows + 1)
    def _(step):
        source = line - step
        index = 2 * source + column

        @pl.when(both(step > 0, source >= 0))
        def _():
            @pl.loop(0, PIECES)
            def _(piece):
                up_copy(index, piece).wait_recv()
                pl.when(line < rows - 1)(lambda: up_copy(index, piece).start())
                pl.when(piece < crossing(index))(lambda: side_copy(index, piece).start())

        @pl.when(both(step > 0, source == 0, column == 1))
        def _():
            extra_copy().wait_recv()
            pl.when(line < rows - 1)(lambda: extra_copy().start())

        @pl.loop(0, 2)
        def _(way):
            found = source + way
            here = 2 * found + jnp.where(way == 0, column, 1 - column)
            due = jnp.logical_or(way == 0, both(step > 0, jnp.logical_or(step > 1, column == 1)))

            @pl.when(both(found >= 0, due))
            def _():
                pl.when(way == 1)(
                    lambda: pl.loop(0, crossing(here))(
                        lambda piece: side_copy(here, piece).wait_recv()
                    )
                )
                compute(here)

    for head in range(heads):
        columns = slice(head * HEAD, (head + 1) * HEAD)
        total = jnp.sum(part[head], axis=1, keepdims=True)
        by_row_ref[head] = jnp.broadcast_to(total, by_row_ref.shape[1:])
        value = acc[:, columns] / total
        att_ref[:, columns] = value
        low_ref[:, columns] = value.astype(jnp.bfloat16)
        tot_ref[head] = jnp.sum(part[head].T, axis=0, keepdims=True)

    @pl.loop(0, rows)
    def _(source):
        index = 2 * source + column

        @pl.when(source <= line)
        def _():
            pl.when(line < rows - 1)(
                lambda: halves(lambda piece: up_copy(index, piece).wait_send())
            )
            pl.when(jnp.logical_or(source < line, column == 0))(
                lambda: pl.loop(0, crossing(index))(
                    lambda piece: side_copy(index, piece).wait_send()
                )
            )

    pl.when(both(column == 1, line < rows - 1))(lambda: extra_copy().wait_send())

    @pl.loop(0, blocks)
    def _(index):
        pl.when(index <= at)(lambda: save(index).wait())


def attend(projected, heads):
    size = projected.shape[0]
    blocks = lax.axis_size("blk")
    whole = pl.BlockSpec(memory_space=pltpu.VMEM)
    return pl.pallas_call(
        functools.partial(attend_kernel, heads),
        out_shape=(
            jax.ShapeDtypeStruct((size, heads * HEAD), jnp.bfloat16),
            jax.ShapeDtypeStruct((size, heads * HEAD), jnp.float32),
            jax.ShapeDtypeStruct((heads, 1, size), jnp.float32),
            jax.ShapeDtypeStruct((heads, size, 128), jnp.float32),
            jax.ShapeDtypeStruct((blocks, size, 2 * HEAD), jnp.bfloat16),
        ),
        in_specs=[whole],
        out_specs=(whole, whole, whole, whole, pl.BlockSpec(memory_space=pl.ANY)),
        scratch_shapes=[
            pltpu.VMEM((blocks, size, 2 * HEAD), jnp.bfloat16),
            pltpu.VMEM((size, heads * HEAD), jnp.float32),
            pltpu.VMEM((heads, size, 128), jnp.float32),
            pltpu.SemaphoreType.DMA((blocks // 2, PIECES)),
            pltpu.SemaphoreType.DMA((blocks // 2, PIECES)),
            pltpu.SemaphoreType.DMA((blocks // 2, PIECES)),
            pltpu.SemaphoreType.DMA((blocks // 2, PIECES)),
            pltpu.SemaphoreType.DMA((1,)),
            pltpu.SemaphoreType.DMA((1,)),
            pltpu.SemaphoreType.DMA,
            pltpu.SemaphoreType.DMA((blocks,)),
        ],
        compiler_params=pltpu.CompilerParams(
            collective_id=0, has_side_effects=True, vmem_limit_bytes=VMEM_BYTES
        ),
        cost_estimate=cost_of(50),
        name="attend",
    )(projected)


def carry(cross_ref, far_ref, first, sent, landed, across):
    return push_sp(
        cross_ref.at[:, pl.ds(first, far_ref.shape[1]), :], far_ref, sent, landed, across
    )


def attend_back_kernel(heads, carried, *refs):
    if carried:
        x_ref, scaled_ref, delta_ref, kv_ref, cross_ref, out_ref, far_ref, *scratch = refs
        *scratch, cross_sent, cross_landed = scratch
        across = (lax.axis_index("sp") + 2) % 4
        over = carry(cross_ref, far_ref, 0, cross_sent, cross_landed, across)
        after = over.start
    else:
        x_ref, scaled_ref, delta_ref, kv_ref, out_ref, *scratch = refs
        across, after = None, lambda: None
    attend_back_steps(
        heads, across, after, x_ref, scaled_ref, delta_ref, kv_ref, out_ref, *scratch
    )
    if carried:
        over.wait()


def attend_back_steps(
    heads,
    across,
    after_greeting,
    x_ref,
    scaled_ref,
    delta_ref,
    kv_ref,
    out_ref,
    kv,
    part,
    side,
    down,
    dq,
    dk,
    dv,
    load_done,
    side_sent,
    side_landed,
    down_sent,
    down_landed,
    extra,
    extra_done,
):
    at = lax.axis_index("blk")
    blocks = lax.axis_size("blk")
    rows = blocks // 2
    line, column = at // 2, at % 2
    partner = at + 1 - 2 * column
    size = x_ref.shape[0]

    def load(index):
        return pltpu.make_async_copy(kv_ref.at[index], kv.at[index], load_done.at[index])

    @pl.loop(0, blocks)
    def _(index):
        pl.when(index <= at)(lambda: load(index).start())

    greet(at, line, rows, across)
    after_greeting()

    def halves(act):
        pl.loop(0, PIECES)(act)

    def span(piece):
        count = size // PIECES
        return pl.ds(pl.multiple_of(piece * count, count), count)

    def side_copy(target, piece):
        return push(
            part.at[target, 1 - column, span(piece)],
            side.at[target, span(piece)],
            side_sent.at[target, piece],
            side_landed.at[target, piece],
            partner,
        )

    def down_copy(target, piece):
        return push(
            part.at[target, column, span(piece)],
            down.at[target, span(piece)],
            down_sent.at[target, piece],
            down_landed.at[target, piece],
            at - 2,
        )

    def extra_copy():
        return push(
            part.at[0, 0, span(PIECES - 1)], extra, extra_done.at[0], extra_done.at[1], at - 2
        )

    def crossing(target, receives):
        fewer = both(target == 0, line > 0, column == (0 if receives else 1))
        return jnp.where(fewer, PIECES - 1, PIECES)

    def extra_step():
        @pl.when(line < rows - 1)
        def _():
            extra_copy().wait_recv()
            part[0, 0, span(PIECES - 1)] = (
                part[0, 0, span(PIECES - 1)].astype(jnp.float32) + extra[...].astype(jnp.float32)
            ).astype(jnp.bfloat16)

        pl.when(line > 0)(lambda: extra_copy().start())
        pl.when(line == 0)(lambda: side_copy(0, PIECES - 1).start())

    dq[...] = jnp.zeros_like(dq)
    ahead = lax.broadcasted_iota(jnp.int32, (size, size), 0) - lax.broadcasted_iota(
        jnp.int32, (size, size), 1
    )

    def compute(target, half):
        index = 2 * target + half
        load(index).wait()
        span = (at - index) * size
        for head in range(heads):
            columns = slice(head * HEAD, (head + 1) * HEAD)
            query = x_ref[:, columns]
            scaled = scaled_ref[:, columns]
            key = kv[index, :, :HEAD]
            raw = lax.dot_general(
                key, query, (((1,), (1,)), ((), ())), preferred_element_type=jnp.float32
            )
            squashed = jnp.tanh(raw * (HEAD ** (-0.5) / CAP_VALUE))
            weights = jnp.exp(CAP_VALUE * squashed)
            weights = jnp.where(ahead <= span, weights, 0.0)
            inner = lax.dot_general(
                kv[index, :, HEAD:],
                scaled,
                (((1,), (1,)), ((), ())),
                preferred_element_type=jnp.float32,
            )
            grad_raw = (
                weights * (inner - delta_ref[head]) * (1.0 - squashed * squashed)
            ).astype(jnp.bfloat16)
            dv_now = jnp.dot(
                weights.astype(jnp.bfloat16), scaled, preferred_element_type=jnp.float32
            )
            dk_now = jnp.dot(grad_raw, query, preferred_element_type=jnp.float32)
            dq[:, columns] += lax.dot_general(
                grad_raw, key, (((0,), (0,)), ((), ())), preferred_element_type=jnp.float32
            )
            if head == 0:
                dv[...] = dv_now
                dk[...] = dk_now
            else:
                dv[...] += dv_now
                dk[...] += dk_now
        part[target, half, :, :HEAD] = (dk[...] * HEAD ** (-0.5)).astype(jnp.bfloat16)
        part[target, half, :, HEAD:] = dv[...].astype(jnp.bfloat16)

    def merge(target):
        def add(piece, more):
            part[target, column, span(piece)] = (
                part[target, column, span(piece)].astype(jnp.float32) + more.astype(jnp.float32)
            ).astype(jnp.bfloat16)

        def merge_piece(piece):
            meets = jnp.logical_or(target < line, column == 0)

            @pl.when(both(meets, piece < crossing(target, True)))
            def _():
                side_copy(target, piece).wait_recv()
                add(piece, side[target, span(piece)])

            @pl.when(line < rows - 1)
            def _():
                down_copy(target, piece).wait_recv()
                add(piece, down[target, span(piece)])

            pl.when(target < line)(lambda: down_copy(target, piece).start())

        pl.when(both(column == 1, target == 0, line == 0))(extra_step)
        halves(merge_piece)

        @pl.when(target == line)
        def _():
            out_ref[:, heads * HEAD :] = part[target, column]

    @pl.loop(0, rows)
    def _(target):
        away = jnp.logical_or(target < line, both(target == line, column == 1))

        @pl.loop(0, 2)
        def _(way):
            @pl.when(jnp.logical_or(both(way == 0, away), both(way == 1, target <= line)))
            def _():
                compute(target, jnp.where(way == 0, 1 - column, column))

                @pl.when(way == 0)
                def _():
                    now = jnp.where(at == 1, PIECES - 1, crossing(target, False))
                    pl.loop(0, now)(lambda piece: side_copy(target, piece).start())
                    due = jnp.where(line == rows - 1, target == 0, both(target == 1, line > 0))
                    pl.when(both(column == 1, due))(extra_step)

            pl.when(both(way == 0, line == rows - 1, target > 0))(lambda: merge(target - 1))


    out_ref[:, : heads * HEAD] = (dq[...] * HEAD ** (-0.5)).astype(jnp.bfloat16)

    @pl.loop(0, rows)
    def _(target):
        pl.when(both(target <= line, jnp.logical_or(line < rows - 1, target == rows - 1)))(
            lambda: merge(target)
        )

    @pl.loop(0, rows)
    def _(target):
        pl.when(jnp.logical_or(target < line, both(target == line, column == 1)))(
            lambda: pl.loop(0, crossing(target, False))(
                lambda piece: side_copy(target, piece).wait_send()
            )
        )
        pl.when(target < line)(lambda: halves(lambda piece: down_copy(target, piece).wait_send()))

    pl.when(both(column == 1, line > 0))(lambda: extra_copy().wait_send())


def half_of(cross):
    kinds, units, width = cross.shape
    return jax.ShapeDtypeStruct((kinds, units // 2, width), cross.dtype)


def attend_back(projected, scaled, delta, kv_all, cross=None):
    size = projected.shape[0]
    blocks = lax.axis_size("blk")
    rows = blocks // 2
    heads = scaled.shape[1] // HEAD
    whole = pl.BlockSpec(memory_space=pltpu.VMEM)
    far = pl.BlockSpec(memory_space=pl.ANY)
    carried = cross is not None
    far_shape, operands = [], [projected, scaled, delta, kv_all]
    if carried:
        far_shape = [half_of(cross)]
        operands.append(cross)
    return pl.pallas_call(
        functools.partial(attend_back_kernel, heads, carried),
        out_shape=[jax.ShapeDtypeStruct(projected.shape, jnp.bfloat16)] + far_shape,
        in_specs=[whole, whole, whole, far] + [far] * carried,
        out_specs=[whole] + [far] * carried,
        scratch_shapes=[
            pltpu.VMEM((blocks, size, 2 * HEAD), jnp.bfloat16),
            pltpu.VMEM((rows, 2, size, 2 * HEAD), jnp.bfloat16),
            pltpu.VMEM((rows, size, 2 * HEAD), jnp.bfloat16),
            pltpu.VMEM((rows, size, 2 * HEAD), jnp.bfloat16),
            pltpu.VMEM((size, heads * HEAD), jnp.float32),
            pltpu.VMEM((size, HEAD), jnp.float32),
            pltpu.VMEM((size, HEAD), jnp.float32),
            pltpu.SemaphoreType.DMA((blocks,)),
            pltpu.SemaphoreType.DMA((rows, PIECES)),
            pltpu.SemaphoreType.DMA((rows, PIECES)),
            pltpu.SemaphoreType.DMA((rows, PIECES)),
            pltpu.SemaphoreType.DMA((rows, PIECES)),
            pltpu.VMEM((size // PIECES, 2 * HEAD), jnp.bfloat16),
            pltpu.SemaphoreType.DMA((2,)),
        ]
        + [pltpu.SemaphoreType.DMA, pltpu.SemaphoreType.DMA] * carried,
        compiler_params=pltpu.CompilerParams(
            collective_id=1, has_side_effects=True, vmem_limit_bytes=VMEM_BYTES
        ),
        cost_estimate=cost_of(50),
        name="attend_back",
    )(*operands)


def line_gather(
    own_ref,
    full,
    line_sent,
    line_landed,
    extra_sent,
    extra_landed,
    side_sent,
    side_landed,
    first_done,
    own_done,
    ready,
    work,
):
    at = lax.axis_index("blk")
    rows = lax.axis_size("blk") // 2
    line, column = at // 2, at % 2
    partner = at + 1 - 2 * column
    size = own_ref.shape[0]
    half = size // 2

    def span(source, start, count):
        return full.at[pl.ds(pl.multiple_of(2 * source * size + start, half), count), :]

    def line_copy(source, sign, first=False):
        target = span(source, column * size, size)
        return push(
            own_ref if first else target,
            target,
            line_sent.at[(sign + 1) // 2, source],
            line_landed.at[source],
            at + 2 * sign,
        )

    def extra_copy(source, sign):
        target = span(source, (1 - column) * size + half, half)
        return push(
            target,
            target,
            extra_sent.at[(sign + 1) // 2, source],
            extra_landed.at[source],
            at + 2 * sign,
        )

    def side_copy(source, member, count, first=False):
        target = span(source, member * size, count)
        return push(
            own_ref.at[:count] if first else target,
            target,
            side_sent.at[source],
            side_landed.at[source],
            partner,
        )

    def first_copy(member):
        return push(
            own_ref.at[half:],
            span(line, member * size + half, half),
            first_done.at[0],
            first_done.at[1],
            partner,
        )

    def inside(row):
        return jnp.logical_and(row >= 0, row < rows)

    def end(row):
        return jnp.logical_or(row == 0, row == rows - 1)

    def by_end(source, act):
        pl.when(end(source))(lambda: act(half))
        pl.when(jnp.logical_not(end(source)))(lambda: act(size))

    pl.when(end(line))(lambda: first_copy(column).start())
    pl.when(line < rows - 1)(lambda: line_copy(line, 1, True).start())
    pl.when(line > 0)(lambda: line_copy(line, -1, True).start())
    by_end(line, lambda count: side_copy(line, column, count, True).start())
    keep = pltpu.make_async_copy(own_ref, span(line, column * size, size), own_done)
    keep.start()

    @pl.when(end(line))
    def _():
        first_copy(1 - column).wait_recv()
        pl.when(line < rows - 1)(lambda: extra_copy(line, 1).start())
        pl.when(line > 0)(lambda: extra_copy(line, -1).start())

    keep.wait()
    ready()

    @pl.loop(0, rows + 1)
    def _(step):
        @pl.loop(0, 2)
        def _(way):
            sign = 2 * way - 1
            source = line - sign * step

            @pl.when(both(step > 0, inside(source)))
            def _():
                line_copy(source, sign).wait_recv()
                pl.when(inside(line + sign))(lambda: line_copy(source, sign).start())
                by_end(source, lambda count: side_copy(source, column, count).start())

        @pl.loop(0, 2)
        def _(way):
            sign = 2 * way - 1
            source = line - sign * step

            @pl.when(both(step > 0, inside(source), end(source)))
            def _():
                extra_copy(source, sign).wait_recv()
                pl.when(inside(line + sign))(lambda: extra_copy(source, sign).start())

        @pl.loop(0, 2)
        def _(way):
            source = line - (2 * way - 1) * (step - 1)

            @pl.when(both(step > way, inside(source)))
            def _():
                by_end(source, lambda count: side_copy(source, 1 - column, count).wait_recv())
                work(source)

    @pl.loop(0, rows)
    def _(source):
        @pl.when(both(source <= line, line < rows - 1))
        def _():
            line_copy(source, 1).wait_send()
            pl.when(end(source))(lambda: extra_copy(source, 1).wait_send())

        @pl.when(both(source >= line, line > 0))
        def _():
            line_copy(source, -1).wait_send()
            pl.when(end(source))(lambda: extra_copy(source, -1).wait_send())

        by_end(source, lambda count: side_copy(source, column, count).wait_send())

    pl.when(end(line))(lambda: first_copy(column).wait_send())


def line_scatter(
    part,
    side,
    lane,
    tail,
    out_ref,
    side_sent,
    side_landed,
    lane_sent,
    lane_landed,
    tail_done,
    work,
    fill,
    split=False,
):
    at = lax.axis_index("blk")
    rows = lax.axis_size("blk") // 2
    line, column = at // 2, at % 2
    partner = at + 1 - 2 * column
    size = out_ref.shape[0]
    half = size // 2

    def span(target, start, count):
        return pl.ds(pl.multiple_of(2 * target * size + start, half), count)

    def piece(target, which):
        member = jnp.where(which == 2, 1 - column, column)
        return span(target, member * size + jnp.where(which == 0, 0, half), half)

    def side_copy(target, which, count):
        start = which * half
        return push(
            part.at[span(target, (1 - column) * size + start, count), :],
            side.at[target, pl.ds(start, count)],
            side_sent.at[target, which],
            side_landed.at[target, which],
            partner,
        )

    def lane_copy(target, which, sign):
        slot = target if sign == 1 else jnp.where(target == line - 1, rows, target)
        return push(
            part.at[piece(target, which), :],
            lane.at[slot, which],
            lane_sent.at[target, which],
            lane_landed.at[slot, which],
            at + 2 * sign,
        )

    def lane_wait(slot, which):
        push(
            lane.at[slot, which],
            lane.at[slot, which],
            lane_sent.at[0, which],
            lane_landed.at[slot, which],
            partner,
        ).wait_recv()

    def tail_copy():
        return push(
            part.at[piece(line, 2), :], tail, tail_done.at[0], tail_done.at[1], partner
        )

    def inside(row):
        return jnp.logical_and(row >= 0, row < rows)

    def end(row):
        return jnp.logical_or(row == 0, row == rows - 1)

    def sides(target, act):
        pl.when(end(target))(lambda: act(side_copy(target, 0, half)))

        @pl.when(jnp.logical_not(end(target)))
        def _():
            if split:
                pl.loop(0, 2)(lambda which: act(side_copy(target, which, half)))
            else:
                act(side_copy(target, 0, size))

    def add(where, more):
        part[where, :] = (
            part[where, :].astype(jnp.float32) + more.astype(jnp.float32)
        ).astype(jnp.bfloat16)

    def hop(target, which):
        sign = jnp.where(target > line, 1, -1)

        @pl.when(inside(line - sign))
        def _():
            lane_wait(target, which)
            add(piece(target, which), lane[target, which])

        pl.when(target > line)(lambda: lane_copy(target, which, 1).start())
        pl.when(target < line)(lambda: lane_copy(target, which, -1).start())

    def early(target):
        return both(end(target), end(line), target != line)

    @pl.loop(0, rows)
    def _(step):
        @pl.loop(0, 2)
        def _(way):
            target = line + (2 * way - 1) * (rows - 1 - step)

            @pl.when(both(step < rows - way, inside(target)))
            def _():
                work(target)
                sides(target, lambda copy: copy.start())

                pl.when(early(target))(lambda: pl.loop(1, 3)(lambda which: hop(target, which)))

    def gather_lanes(which):
        @pl.loop(0, 2)
        def _(above):
            slot = jnp.where(above == 0, line, rows)

            @pl.when(jnp.where(above == 0, line > 0, line < rows - 1))
            def _():
                lane_wait(slot, which)
                add(piece(line, which), lane[slot, which])

    def merge(target):
        @pl.when(both(end(target), target != line, jnp.logical_not(early(target))))
        def _():
            pl.loop(1, 3)(lambda which: hop(target, which))

        @pl.when(both(end(line), target == line))
        def _():
            gather_lanes(2)
            tail_copy().start()

        if not split:
            sides(target, lambda copy: copy.wait_recv())

        @pl.loop(0, 2)
        def _(which):
            @pl.when(jnp.logical_or(which == 0, jnp.logical_not(end(target))))
            def _():
                if split:
                    side_copy(target, which, half).wait_recv()
                add(piece(target, which), side[target, pl.ds(which * half, half)])
                pl.when(target != line)(lambda: hop(target, which))

    @pl.loop(0, rows)
    def _(step):
        fill(step)

        @pl.loop(0, 2)
        def _(way):
            target = line + (2 * way - 1) * (rows - 1 - step)
            pl.when(both(step < rows - way, inside(target)))(lambda: merge(target))

    pl.loop(0, 2)(lambda which: gather_lanes(1 - which))
    out_ref[...] = part[span(line, column * size, size), :].astype(jnp.float32)

    @pl.when(end(line))
    def _():
        tail_copy().wait_recv()
        out_ref[half:, :] += tail[...].astype(jnp.float32)
        tail_copy().wait_send()

    @pl.loop(0, rows)
    def _(target):
        sides(target, lambda copy: copy.wait_send())

        def sent(sign):
            pl.loop(0, jnp.where(end(target), 3, 2))(
                lambda which: lane_copy(target, which, sign).wait_send()
            )

        pl.when(target > line)(lambda: sent(1))
        pl.when(target < line)(lambda: sent(-1))


def line_sems(rows):
    dma = pltpu.SemaphoreType.DMA
    ways, each = dma((2, rows)), dma((rows,))
    return [ways, each, ways, each, each, each, dma((2,)), dma]


def lane_sems(rows):
    dma = pltpu.SemaphoreType.DMA
    return [dma((rows, 2)), dma((rows, 2)), dma((rows, 3)), dma((rows + 1, 3)), dma((2,))]


def lane_buffers(rows, size, width):
    return [
        pltpu.VMEM((2 * rows * size, width), jnp.bfloat16),
        pltpu.VMEM((rows, size, width), jnp.bfloat16),
        pltpu.VMEM((rows + 1, 3, size // 2, width), jnp.bfloat16),
        pltpu.VMEM((size // 2, width), jnp.bfloat16),
    ]


def ffn_kernel(
    act_ref,
    w_ref,
    middle_ref,
    cotangent_ref,
    gains_ref,
    result_ref,
    grad_ref,
    row_ref,
    acts_ref,
    factors_ref,
    out_ref,
    w,
    acts,
    hidden,
    factors,
    part,
    side,
    lane,
    tail,
    w_done,
    save_done,
    factors_done,
    *sems,
):
    at = lax.axis_index("blk")
    rows = lax.axis_size("blk") // 2
    pair = 2 * act_ref.shape[0]

    def load(which):
        return pltpu.make_async_copy(w_ref.at[which], w.at[which], w_done.at[which])

    def pair_rows(source):
        return pl.ds(pl.multiple_of(source * pair, pair), pair)

    def save(source):
        return pltpu.make_async_copy(
            acts.at[pair_rows(source), :], acts_ref.at[pair_rows(source), :], save_done.at[source]
        )

    for which in range(3):
        load(which).start()
    greet(at, at // 2, rows)

    def ready():
        for which in range(3):
            load(which).wait()

    def expand(source):
        save(source).start()
        rows_now = acts[pair_rows(source), :]
        gate = contract_last(w[0], rows_now)
        up = contract_last(w[1], rows_now)
        hidden[source] = (gelu_value(gate) * up).astype(jnp.bfloat16)

    def reduce(target):
        part[pair_rows(target), :] = lax.dot_general(
            hidden[target], w[2], (((0,), (0,)), ((), ())), preferred_element_type=jnp.float32
        ).astype(jnp.bfloat16)

    line_gather(act_ref, acts, *sems[:8], ready, expand)
    def factors_copy(source):
        return pltpu.make_async_copy(
            factors.at[source % 2],
            factors_ref.at[:, :, pair_rows(source)],
            factors_done.at[source % 2],
        )

    def fill(source):
        rows_now = acts[pair_rows(source), :]
        gate = contract_last(w[0], rows_now)
        up = contract_last(w[1], rows_now)
        bent = jnp.tanh(GELU_SCALE * (gate + GELU_CUBIC * gate * gate * gate))
        slope = 0.5 * (1.0 + bent) + 0.5 * gate * (1.0 - bent * bent) * GELU_SCALE * (
            1.0 + 3.0 * GELU_CUBIC * gate * gate
        )
        pl.when(source > 1)(lambda: factors_copy(source - 2).wait())
        slot = source % 2
        factors[slot, 0] = (up * slope).astype(jnp.bfloat16)
        factors[slot, 1] = (0.5 * gate * (1.0 + bent)).astype(jnp.bfloat16)
        factors[slot, 2] = hidden[source]
        factors_copy(source).start()

    line_scatter(part, side, lane, tail, out_ref, *sems[8:], reduce, fill)
    normed, inverse = norm_parts(out_ref[...])
    result_ref[...] = (middle_ref[...] + normed * gains_ref[3:4, :]).astype(jnp.bfloat16)
    grad_v, gain_row = norm_back(
        cotangent_ref[...].astype(jnp.float32), normed, inverse, gains_ref[3:4, :]
    )
    grad_ref[...] = grad_v.astype(jnp.bfloat16)
    row_ref[...] = gain_row[None, :]
    factors_copy(rows - 2).wait()
    factors_copy(rows - 1).wait()
    pl.loop(0, rows)(lambda source: save(source).wait())


def ffn_forward(act_ffn, w_parts, middle, cotangent, gains):
    size, width = act_ffn.shape
    units = w_parts.shape[1]
    blocks = lax.axis_size("blk")
    rows = blocks // 2
    whole = pl.BlockSpec(memory_space=pltpu.VMEM)
    far = pl.BlockSpec(memory_space=pl.ANY)
    return pl.pallas_call(
        ffn_kernel,
        out_shape=(
            jax.ShapeDtypeStruct((size, width), jnp.bfloat16),
            jax.ShapeDtypeStruct((size, width), jnp.bfloat16),
            jax.ShapeDtypeStruct((1, width), jnp.float32),
            jax.ShapeDtypeStruct((blocks * size, width), jnp.bfloat16),
            jax.ShapeDtypeStruct((3, units, blocks * size), jnp.bfloat16),
        ),
        in_specs=[whole, far, whole, whole, whole],
        out_specs=(whole, whole, whole, far, far),
        scratch_shapes=[
            pltpu.VMEM((size, width), jnp.float32),
            pltpu.VMEM(w_parts.shape, jnp.bfloat16),
            pltpu.VMEM((blocks * size, width), jnp.bfloat16),
            pltpu.VMEM((rows, units, 2 * size), jnp.bfloat16),
            pltpu.VMEM((2, 3, units, 2 * size), jnp.bfloat16),
            *lane_buffers(rows, size, width),
            pltpu.SemaphoreType.DMA((3,)),
            pltpu.SemaphoreType.DMA((rows,)),
            pltpu.SemaphoreType.DMA((2,)),
            *line_sems(rows),
            *lane_sems(rows),
        ],
        compiler_params=pltpu.CompilerParams(
            collective_id=2, has_side_effects=True, vmem_limit_bytes=VMEM_BYTES
        ),
        cost_estimate=cost_of(115),
        name="ffn_forward",
    )(act_ffn, w_parts, middle, cotangent, gains)


FILL_COLUMNS = 768
FILL_FIRST = 0


def ffn_back_kernel(
    owners,
    grad_ref,
    acts_ref,
    factors_ref,
    w_ref,
    out_ref,
    keep_ref,
    cross_ref,
    w,
    rights,
    lefts,
    part,
    side,
    lane,
    tail,
    stage,
    mate_part,
    w_done,
    acts_done,
    factors_done,
    mate_sent,
    mate_landed,
    summed_done,
    *sems,
):
    at = lax.axis_index("blk")
    me = lax.axis_index("sp")
    chip, core = me // 2, me % 2
    mate = me + 1 - 2 * core
    rows = lax.axis_size("blk") // 2
    size, width = grad_ref.shape
    pair = 2 * size
    units = w.shape[1]
    acts, grads = rights.at[0], rights.at[1]

    def load(which):
        return pltpu.make_async_copy(w_ref.at[which], w.at[which], w_done.at[which])

    def pair_rows(source):
        return pl.ds(pl.multiple_of(source * pair, pair), pair)

    acts_copy = pltpu.make_async_copy(acts_ref, acts, acts_done)
    factors_copy = pltpu.make_async_copy(factors_ref, lefts, factors_done)
    load(2).start()
    factors_copy.start()
    load(0).start()
    load(1).start()
    acts_copy.start()
    greet(at, at // 2, rows, mate)

    def ready():
        load(2).wait()
        factors_copy.wait()

    def expand(source):
        columns = pair_rows(source)
        grad_hidden = contract_last(w[2], grads[columns, :])
        for which in range(2):
            lefts[which, :, columns] = (
                lefts[which, :, columns].astype(jnp.float32) * grad_hidden
            ).astype(jnp.bfloat16)

    def reduce(target):
        columns = pair_rows(target)
        dims = (((0,), (0,)), ((), ()))
        total = lax.dot_general(
            lefts[0, :, columns], w[0], dims, preferred_element_type=jnp.float32
        ) + lax.dot_general(lefts[1, :, columns], w[1], dims, preferred_element_type=jnp.float32)
        part[pair_rows(target), :] = total.astype(jnp.bfloat16)

    pieces = width // FILL_COLUMNS
    total_pieces = 3 * pieces

    def piece_columns(item):
        return pl.ds(pl.multiple_of((item % pieces) * FILL_COLUMNS, FILL_COLUMNS), FILL_COLUMNS)

    def mate_copy(item):
        return push_sp(
            stage.at[item % 2, :, 1 - core],
            mate_part.at[item],
            mate_sent.at[item % 2],
            mate_landed.at[item],
            mate,
        )

    def put(item, side_chip, target):
        return pltpu.make_async_copy(
            mate_part.at[item, side_chip],
            target.at[item // pieces, :, piece_columns(item)],
            summed_done.at[item, side_chip],
        )

    def put_wait(item):
        put(item, chip, keep_ref).wait()
        put(item, 1 - chip, cross_ref).wait()

    def sum_one(item):
        mate_copy(item).wait_recv()
        mate_part[item] = (
            stage[item % 2, :, core].astype(jnp.float32) + mate_part[item].astype(jnp.float32)
        ).astype(jnp.bfloat16)
        put(item, chip, keep_ref).start()
        put(item, 1 - chip, cross_ref).start()

    def fill_one(item):
        which = item // pieces
        total = jnp.dot(
            lefts[which],
            rights[which // 2, :, piece_columns(item)],
            preferred_element_type=jnp.float32,
        )
        pl.when(item > 1)(lambda: mate_copy(item - 2).wait_send())
        stage[item % 2] = total.astype(jnp.bfloat16).reshape(
            2, 2, units // owners, FILL_COLUMNS
        )
        mate_copy(item).start()
        pl.when(item > 0)(lambda: sum_one(item - 1))

    each = pl.cdiv(total_pieces - FILL_FIRST, rows - 1)

    def fill(step):
        first = jnp.maximum(FILL_FIRST + (step - 1) * each, 0)
        last = jnp.minimum(FILL_FIRST + step * each, total_pieces)

        @pl.loop(0, each)
        def _(item):
            pl.when(first + item < last)(lambda: fill_one(first + item))

    line_gather(grad_ref, grads, *sems[:8], ready, expand)
    load(0).wait()
    load(1).wait()
    acts_copy.wait()
    line_scatter(part, side, lane, tail, out_ref, *sems[8:], reduce, fill)
    sum_one(total_pieces - 1)
    pl.loop(0, total_pieces)(put_wait)
    for item in range(total_pieces - 2, total_pieces):
        mate_copy(item).wait_send()


def ffn_back(grad_ffn, kept, w_parts, owners):
    size, width = grad_ffn.shape
    units = w_parts.shape[1]
    blocks = lax.axis_size("blk")
    rows = blocks // 2
    tokens = blocks * size
    items = 3 * width // FILL_COLUMNS
    whole = pl.BlockSpec(memory_space=pltpu.VMEM)
    far = pl.BlockSpec(memory_space=pl.ANY)
    return pl.pallas_call(
        functools.partial(ffn_back_kernel, owners),
        out_shape=(
            jax.ShapeDtypeStruct((size, width), jnp.float32),
            jax.ShapeDtypeStruct((3, units // owners, width), jnp.bfloat16),
            jax.ShapeDtypeStruct((3, units // owners, width), jnp.bfloat16),
        ),
        in_specs=[whole, far, far, far],
        out_specs=(whole, far, far),
        scratch_shapes=[
            pltpu.VMEM(w_parts.shape, jnp.bfloat16),
            pltpu.VMEM((2, tokens, width), jnp.bfloat16),
            pltpu.VMEM((3, units, tokens), jnp.bfloat16),
            *lane_buffers(rows, size, width),
            pltpu.VMEM((2, 2, 2, units // owners, FILL_COLUMNS), jnp.bfloat16),
            pltpu.VMEM((items, 2, units // owners, FILL_COLUMNS), jnp.bfloat16),
            pltpu.SemaphoreType.DMA((3,)),
            pltpu.SemaphoreType.DMA,
            pltpu.SemaphoreType.DMA,
            pltpu.SemaphoreType.DMA((2,)),
            pltpu.SemaphoreType.DMA((items,)),
            pltpu.SemaphoreType.DMA((items, 2)),
            *line_sems(rows),
            *lane_sems(rows),
        ],
        compiler_params=pltpu.CompilerParams(
            collective_id=3, has_side_effects=True, vmem_limit_bytes=VMEM_BYTES
        ),
        cost_estimate=cost_of(115),
        name="ffn_back",
    )(grad_ffn, *kept, w_parts)


def ffn_hidden(acts, w_parts):
    gate = contract_last(acts, w_parts[0])
    up = contract_last(acts, w_parts[1])
    return (gate, up, (gelu_value(gate) * up).astype(jnp.bfloat16))


def scatter_tokens(partial):
    return lax.psum_scatter(
        partial.astype(jnp.bfloat16), "blk", scatter_dimension=0, tiled=True
    ).astype(jnp.float32)


def ffn_forward_wide(act_ffn, w_parts, middle, cotangent, gains):
    acts = lax.all_gather(act_ffn, "blk", axis=0, tiled=True)
    hidden = ffn_hidden(acts, w_parts)[2]
    partial = jnp.dot(hidden, w_parts[2], preferred_element_type=jnp.float32)
    normed, inverse = norm_parts(scatter_tokens(partial))
    result = (middle + normed * gains[3]).astype(jnp.bfloat16)
    grad_v, gain_row = norm_back(cotangent.astype(jnp.float32), normed, inverse, gains[3])
    return (result, grad_v.astype(jnp.bfloat16), gain_row[None], acts)


def ffn_back_wide(grad_ffn, kept, w_parts, owners):
    (acts,) = kept
    grads = lax.all_gather(grad_ffn, "blk", axis=0, tiled=True)
    gate, up, hidden = ffn_hidden(acts, w_parts)
    grad_hidden = contract_last(grads, w_parts[2])
    grad_gate = (grad_hidden * up * gelu_slope(gate)).astype(jnp.bfloat16)
    grad_up = (grad_hidden * gelu_value(gate)).astype(jnp.bfloat16)
    partial = jnp.dot(grad_gate, w_parts[0], preferred_element_type=jnp.float32) + jnp.dot(
        grad_up, w_parts[1], preferred_element_type=jnp.float32
    )
    sums = jnp.stack(
        [
            jnp.einsum("tf,td->fd", left, right, preferred_element_type=jnp.float32)
            for left, right in ((grad_gate, acts), (grad_up, acts), (hidden, grads))
        ]
    ).astype(jnp.bfloat16)
    units = w_parts.shape[1]
    owned = sums.reshape(3, owners, units // owners, sums.shape[2])
    mine = lax.psum_scatter(
        jnp.transpose(owned, (1, 0, 2, 3)), "sp", scatter_dimension=0, tiled=True
    )
    return (scatter_tokens(partial), mine[0], None)


def cost_of(microseconds):
    return pl.CostEstimate(
        flops=int(microseconds * 1e9), bytes_accessed=int(microseconds * 3e6), transcendentals=0
    )


def push_sp(source, target, sent, landed, peer):
    return pltpu.make_async_remote_copy(
        src_ref=source,
        dst_ref=target,
        send_sem=sent,
        recv_sem=landed,
        device_id={"sp": peer},
        device_id_type=pl.DeviceIdType.MESH,
    )


def greet_sp(me, groups, before_wait=lambda: None):
    barrier = pltpu.get_barrier_semaphore()
    for step in range(1, groups):
        pl.semaphore_signal(
            barrier,
            inc=1,
            device_id={"sp": (me + step) % groups},
            device_id_type=pl.DeviceIdType.MESH,
        )
    before_wait()
    pl.semaphore_wait(barrier, groups - 1)


def gather_rows(x, w_ref, full_ref, w, w_done, own_done, sent, landed, prepare, project):
    me = lax.axis_index("sp")
    size = x.shape[0]
    units = w.shape[0]
    mate = me + 1 - 2 * (me % 2)
    across = (me + 2) % 4

    def spot(member):
        return full_ref.at[pl.ds(pl.multiple_of(member * size, size), size), :]

    load = pltpu.make_async_copy(
        w_ref.at[pl.ds(pl.multiple_of(me * units, units), units), :], w, w_done
    )
    load.start()
    greet_sp(me, 4, prepare)
    half = size // 2

    def half_spot(member, piece):
        start = pl.multiple_of(member * size + piece * half, half)
        return full_ref.at[pl.ds(start, half), :]

    def over(piece):
        return push_sp(
            x.at[pl.ds(piece * half, half)],
            half_spot(me, piece),
            sent.at[piece],
            landed.at[piece],
            across,
        )

    def onward(piece):
        rows_now = half_spot(across, piece)
        return push_sp(rows_now, rows_now, sent.at[3 + piece], landed.at[3 + piece], mate)

    over(0).start()
    over(1).start()
    beside = push_sp(x, spot(me), sent.at[2], landed.at[2], mate)
    beside.start()
    keep = pltpu.make_async_copy(x, spot(me), own_done)
    keep.start()
    keep.wait()
    load.wait()

    def project_chip(chip):
        rows = pl.ds(pl.multiple_of(chip * 2 * size, 2 * size), 2 * size)
        project(rows, contract_last(full_ref[rows, :], w[...]).astype(jnp.bfloat16))

    beside.wait_recv()
    project_chip(me // 2)
    for piece in range(2):
        over(piece).wait_recv()
        onward(piece).start()
    for piece in range(2):
        onward(piece).wait_recv()
    project_chip(across // 2)
    beside.wait_send()
    for piece in range(2):
        over(piece).wait_send()
        onward(piece).wait_send()


def project_in_kernel(tokens_ref, gains_ref, w_ref, full_ref, out_ref, x, *scratch):
    def prepare():
        normed = norm_parts(tokens_ref[...].astype(jnp.float32))[0]
        x[...] = (normed * gains_ref[0:1, :]).astype(jnp.bfloat16)

    def project(rows, value):
        out_ref[rows, :] = value

    gather_rows(x, w_ref, full_ref, *scratch, prepare, project)


def gather_scratch(size, width, units):
    dma = pltpu.SemaphoreType.DMA
    return [
        pltpu.VMEM((size, width), jnp.bfloat16),
        pltpu.VMEM((units, width), jnp.bfloat16),
        dma,
        dma,
        dma((5,)),
        dma((5,)),
    ]


def project_in(tokens, gains, weights):
    size, width = tokens.shape
    units = weights.shape[0] // 4
    whole = pl.BlockSpec(memory_space=pltpu.VMEM)
    return pl.pallas_call(
        project_in_kernel,
        out_shape=(
            jax.ShapeDtypeStruct((4 * size, width), jnp.bfloat16),
            jax.ShapeDtypeStruct((4 * size, units), jnp.bfloat16),
        ),
        in_specs=[whole, whole, pl.BlockSpec(memory_space=pl.ANY)],
        out_specs=(whole, whole),
        scratch_shapes=gather_scratch(size, width, units),
        compiler_params=pltpu.CompilerParams(
            collective_id=4, has_side_effects=True, vmem_limit_bytes=VMEM_BYTES
        ),
        cost_estimate=cost_of(18),
        name="project_in",
    )(tokens, gains, weights)


def project_back_kernel(
    grad_ref,
    middle_ref,
    attn_ref,
    cotangent_ref,
    gains_ref,
    attended_ref,
    by_row_ref,
    totals_ref,
    w_ref,
    full_ref,
    scaled_ref,
    delta_ref,
    grad_middle_ref,
    rows_ref,
    x,
    *scratch,
):
    def prepare():
        grad_v, row_two = norm_back(
            grad_ref[...], *norm_parts(middle_ref[...]), gains_ref[2:3, :]
        )
        grad_middle = cotangent_ref[...].astype(jnp.float32) + grad_v
        grad_middle_ref[...] = grad_middle
        grad_v, row_one = norm_back(grad_middle, *norm_parts(attn_ref[...]), gains_ref[1:2, :])
        x[...] = grad_v.astype(jnp.bfloat16)
        rows_ref[...] = jnp.zeros_like(rows_ref)
        rows_ref[1:2, :] = row_one[None, :]
        rows_ref[2:3, :] = row_two[None, :]

    def project(rows, value):
        for head in range(value.shape[1] // HEAD):
            columns = slice(head * HEAD, (head + 1) * HEAD)
            grad = value[:, columns].astype(jnp.float32)
            scaled_ref[rows, columns] = (grad / by_row_ref[head, rows, :1]).astype(jnp.bfloat16)
            product = grad * attended_ref[rows, columns]
            delta_ref[head, :, rows] = (
                jnp.sum(product.T, axis=0, keepdims=True) / totals_ref[head, :, rows]
            )

    gather_rows(x, w_ref, full_ref, *scratch, prepare, project)


def project_back(
    grad_act, middle, attn, cotangent, gains, attended, by_row, totals, weights
):
    size, width = attn.shape
    units = weights.shape[0] // 4
    whole = pl.BlockSpec(memory_space=pltpu.VMEM)
    return pl.pallas_call(
        project_back_kernel,
        out_shape=(
            jax.ShapeDtypeStruct((4 * size, width), jnp.bfloat16),
            jax.ShapeDtypeStruct((4 * size, units), jnp.bfloat16),
            jax.ShapeDtypeStruct(totals.shape, jnp.float32),
            jax.ShapeDtypeStruct((size, width), jnp.float32),
            jax.ShapeDtypeStruct((8, width), jnp.float32),
        ),
        in_specs=[whole] * 8 + [pl.BlockSpec(memory_space=pl.ANY)],
        out_specs=(whole,) * 5,
        scratch_shapes=gather_scratch(size, width, units),
        compiler_params=pltpu.CompilerParams(
            collective_id=6, has_side_effects=True, vmem_limit_bytes=VMEM_BYTES
        ),
        cost_estimate=cost_of(20),
        name="project_back",
    )(grad_act, middle, attn, cotangent, gains, attended, by_row, totals, weights)


def exchange_norm_kernel(x_ref, w_ref, tokens_ref, gains_ref, out_ref, middle_ref, act_ref, *scratch):
    exchange_project_kernel(x_ref, w_ref, out_ref, *scratch)
    normed = norm_parts(out_ref[...])[0]
    middle = tokens_ref[...].astype(jnp.float32) + normed * gains_ref[1:2, :]
    middle_ref[...] = middle
    act_ref[...] = (norm_parts(middle)[0] * gains_ref[2:3, :]).astype(jnp.bfloat16)


def exchange_project_kernel(x_ref, w_ref, out_ref, w, got, w_done, own_done, sent, landed):
    me = lax.axis_index("sp")
    size = out_ref.shape[0]
    units = x_ref.shape[1]

    def rows_of(member):
        return x_ref.at[pl.ds(pl.multiple_of(member * size, size), size), :]

    def load(member):
        rows = pl.ds(pl.multiple_of(member * units, units), units)
        return pltpu.make_async_copy(w_ref.at[rows, :], w.at[rows, :], w_done.at[member])

    def send(step):
        peer = (me + step) % 4
        return push_sp(rows_of(peer), got.at[4 - step], sent.at[step], landed.at[4 - step], peer)

    greet_sp(me, 4)
    for step in (2, 1, 3):
        send(step).start()
    keep = pltpu.make_async_copy(rows_of(me), got.at[0], own_done)
    keep.start()
    for step in range(4):
        load((me + step) % 4).start()
    keep.wait()
    core = me % 2
    for place, step in enumerate((0, 1 + 2 * core, 2, 3 - 2 * core)):
        member = (me + step) % 4
        load(member).wait()
        if place > 0:
            send(4 - step).wait_recv()
        rows = pl.ds(pl.multiple_of(member * units, units), units)
        term = jnp.dot(got[step], w[rows, :], preferred_element_type=jnp.float32)
        if place == 0:
            out_ref[...] = term
        else:
            out_ref[...] += term
    for step in (1, 2, 3):
        send(step).wait_send()


def exchange_project(columns, weights, identity, norm_inputs=()):
    size = columns.shape[0] // 4
    whole = pl.BlockSpec(memory_space=pltpu.VMEM)
    total = jax.ShapeDtypeStruct((size, weights.shape[1]), jnp.float32)
    low = jax.ShapeDtypeStruct(total.shape, jnp.bfloat16)
    shapes = [total, total, low] if norm_inputs else [total]
    return pl.pallas_call(
        exchange_norm_kernel if norm_inputs else exchange_project_kernel,
        out_shape=shapes,
        in_specs=[whole, pl.BlockSpec(memory_space=pl.ANY)] + [whole] * len(norm_inputs),
        out_specs=[whole] * len(shapes),
        scratch_shapes=[
            pltpu.VMEM(weights.shape, jnp.bfloat16),
            pltpu.VMEM((4, size, columns.shape[1]), jnp.bfloat16),
            pltpu.SemaphoreType.DMA((4,)),
            pltpu.SemaphoreType.DMA,
            pltpu.SemaphoreType.DMA((4,)),
            pltpu.SemaphoreType.DMA((4,)),
        ],
        compiler_params=pltpu.CompilerParams(
            collective_id=identity, has_side_effects=True, vmem_limit_bytes=VMEM_BYTES
        ),
        cost_estimate=cost_of(16),
        name="exchange_project",
    )(columns, weights, *norm_inputs)


def finish_kernel(
    cols_ref,
    act_ref,
    att_ref,
    grad_ref,
    w_ref,
    tokens_ref,
    middle_ref,
    gains_in_ref,
    rows_ref,
    row_three_ref,
    cross_ref,
    qkv_ref,
    out_ref,
    tokens_grad_ref,
    gains_ref,
    far_ref,
    w,
    got,
    grad_in,
    total,
    part,
    side,
    lane,
    tail,
    mine,
    from_sp,
    from_side,
    from_line,
    w_done,
    own_done,
    swap_sent,
    swap_landed,
    sp_sent,
    sp_landed,
    gain_side,
    line_sent,
    line_landed,
    cross_sent,
    cross_landed,
    *sems,
):
    at = lax.axis_index("blk")
    me = lax.axis_index("sp")
    rows = lax.axis_size("blk") // 2
    line, column = at // 2, at % 2
    partner = at + 1 - 2 * column
    block = total.shape[0]
    size = tokens_ref.shape[0]
    units = cols_ref.shape[1]
    extra = block - size

    barrier = pltpu.get_barrier_semaphore()
    for step in range(1, 4):
        pl.semaphore_signal(
            barrier, inc=1, device_id={"sp": (me + step) % 4}, device_id_type=pl.DeviceIdType.MESH
        )

    def line_peer(step):
        return 2 * ((line + step) % rows) + column

    for peer in [partner] + [line_peer(step) for step in range(1, rows)]:
        pl.semaphore_signal(
            barrier, inc=1, device_id={"blk": peer}, device_id_type=pl.DeviceIdType.MESH
        )

    def load(member):
        span = pl.ds(pl.multiple_of(member * units, units), units)
        return pltpu.make_async_copy(w_ref.at[span, :], w.at[span, :], w_done.at[member])

    def rows_of(member):
        return cols_ref.at[pl.ds(pl.multiple_of(member * size, size), size), :]

    def swap(step):
        peer = (me + step) % 4
        return push_sp(
            rows_of(peer), got.at[4 - step], swap_sent.at[step], swap_landed.at[4 - step], peer
        )

    for step in range(4):
        load((me + step) % 4).start()
    keep = pltpu.make_async_copy(rows_of(me), got.at[0], own_done)
    keep.start()
    pl.semaphore_wait(barrier, 3 + rows)
    for step in (2, 1, 3):
        swap(step).start()
    over = carry(
        cross_ref, far_ref, far_ref.shape[1], cross_sent, cross_landed, (me + 2) % 4
    )
    over.start()
    keep.wait()

    def sp_gains(step):
        return push_sp(
            mine, from_sp.at[4 - step], sp_sent.at[step], sp_landed.at[4 - step], (me + step) % 4
        )

    def side_gains():
        return push(from_sp.at[0], from_side, gain_side.at[0], gain_side.at[1], partner)

    def line_gains(step):
        return push(
            from_line.at[0],
            from_line.at[rows - step],
            line_sent.at[step],
            line_landed.at[rows - step],
            line_peer(step),
        )

    def reduce(target):
        dims = (((0,), (0,)), ((), ()))
        wide_columns = pl.ds(pl.multiple_of(target * 2 * size, 2 * size), 2 * size)
        term = lax.dot_general(
            cols_ref[:, wide_columns], act_ref[...], dims, preferred_element_type=jnp.float32
        ).astype(jnp.bfloat16)
        columns = pl.ds(pl.multiple_of(target * 2 * extra, 2 * extra), 2 * extra)
        more = lax.dot_general(
            att_ref[:, columns], grad_ref[...], dims, preferred_element_type=jnp.float32
        ).astype(jnp.bfloat16)
        for half in range(2):
            start = pl.multiple_of((2 * target + half) * block, block)
            part[pl.ds(start, size), :] = term[half * size : (half + 1) * size]
            start = pl.multiple_of((2 * target + half) * block + size, extra)
            part[pl.ds(start, extra), :] = more[half * extra : (half + 1) * extra]

    def inputs_back():
        for step in (0, 1, 3, 2):
            member = (me + step) % 4
            load(member).wait()
            if step > 0:
                swap(4 - step).wait_recv()
            span = pl.ds(pl.multiple_of(member * units, units), units)
            term = jnp.dot(got[step], w[span, :], preferred_element_type=jnp.float32)
            if step == 0:
                grad_in[...] = term
            else:
                grad_in[...] += term
        normed, inverse = norm_parts(tokens_ref[...].astype(jnp.float32))
        grad_v, gain_row = norm_back(grad_in[...], normed, inverse, gains_in_ref[0:1, :])
        tokens_grad_ref[...] = (middle_ref[...] + grad_v).astype(jnp.bfloat16)
        mine[...] = rows_ref[...]
        mine[0:1, :] = gain_row[None, :]
        mine[3:4, :] = row_three_ref[...]
        for step in range(1, 4):
            sp_gains(step).start()

    def fill(step):
        pl.when(step == 2)(inputs_back)

        @pl.when(step == 3)
        def _():
            gains = mine[...]
            for other in range(1, 4):
                sp_gains(4 - other).wait_recv()
                gains = gains + from_sp[other]
            from_sp[0] = gains
            side_gains().start()

        @pl.when(step == 3)
        def _():
            side_gains().wait_recv()
            from_line[0] = from_sp[0] + from_side[...]
            for other in range(1, rows):
                line_gains(other).start()

    line_scatter(part, side, lane, tail, total, *sems, reduce, fill, split=True)
    qkv_ref[...] = total[:size]
    out_ref[...] = total[size:]
    gains = from_line[0]
    for other in range(1, rows):
        line_gains(rows - other).wait_recv()
        gains = gains + from_line[other]
    gains_ref[...] = gains
    for step in (1, 2, 3):
        swap(step).wait_send()
        sp_gains(step).wait_send()
    over.wait()
    side_gains().wait_send()
    for step in range(1, rows):
        line_gains(step).wait_send()


def finish(
    cols, act_block, attended, grad_block, w_qkv, tokens, grad_middle, gains, rows, row_three, cross
):
    blocks = lax.axis_size("blk")
    lines = blocks // 2
    size, width = tokens.shape
    block = (cols.shape[1] + attended.shape[1]) // blocks
    whole = pl.BlockSpec(memory_space=pltpu.VMEM)
    any_space = pl.BlockSpec(memory_space=pl.ANY)
    dma = pltpu.SemaphoreType.DMA
    small = rows.shape
    return pl.pallas_call(
        finish_kernel,
        out_shape=(
            jax.ShapeDtypeStruct((cols.shape[1] // blocks, width), jnp.float32),
            jax.ShapeDtypeStruct((attended.shape[1] // blocks, width), jnp.float32),
            jax.ShapeDtypeStruct((size, width), jnp.bfloat16),
            jax.ShapeDtypeStruct(small, jnp.float32),
            half_of(cross),
        ),
        in_specs=[whole] * 4 + [any_space] + [whole] * 5 + [any_space],
        out_specs=(whole, whole, whole, whole, any_space),
        scratch_shapes=[
            pltpu.VMEM(w_qkv.shape, jnp.bfloat16),
            pltpu.VMEM((4, size, cols.shape[1]), jnp.bfloat16),
            pltpu.VMEM((size, width), jnp.float32),
            pltpu.VMEM((block, width), jnp.float32),
            *lane_buffers(lines, block, width),
            pltpu.VMEM(small, jnp.float32),
            pltpu.VMEM((4, *small), jnp.float32),
            pltpu.VMEM(small, jnp.float32),
            pltpu.VMEM((lines, *small), jnp.float32),
            dma((4,)),
            dma,
            dma((4,)),
            dma((4,)),
            dma((4,)),
            dma((4,)),
            dma((2,)),
            dma((lines,)),
            dma((lines,)),
            dma,
            dma,
            *lane_sems(lines),
        ],
        compiler_params=pltpu.CompilerParams(
            collective_id=8, has_side_effects=True, vmem_limit_bytes=VMEM_BYTES
        ),
        cost_estimate=cost_of(85),
        name="finish",
    )(
        cols,
        act_block,
        attended,
        grad_block,
        w_qkv,
        tokens,
        grad_middle,
        gains,
        rows,
        row_three,
        cross,
    )


def weight_sums_wide(left, right):
    term = jnp.einsum("tc,td->cd", left, right, preferred_element_type=jnp.float32)
    return scatter_tokens(term)


def finish_wide(
    cols, act_block, attended, grad_block, w_qkv, tokens, grad_middle, gains, rows, row_three, cross
):
    (grad_act_in,) = exchange_project(cols, w_qkv, 7)
    normed, inverse = norm_parts(tokens.astype(jnp.float32))
    grad_v, gain_row = norm_back(grad_act_in, normed, inverse, gains[0])
    gains_all = lax.psum(
        jnp.concatenate([gain_row[None], rows[1:3], row_three, rows[4:]]), ("blk", "sp")
    )
    return (
        weight_sums_wide(cols, act_block),
        weight_sums_wide(attended, grad_block),
        (grad_middle + grad_v).astype(jnp.bfloat16),
        gains_all,
        None,
    )


def deliver_kernel(*refs):
    keep_ref, first_ref, last_ref, *others = refs
    ins, sum_ref, outs = others[:4], others[4], others[5:]
    half = first_ref.shape[1]
    for start, far_ref in ((0, first_ref), (half, last_ref)):
        rows = slice(start, start + half)
        sum_ref[:, rows] = keep_ref[:, rows].astype(jnp.float32) + far_ref[...].astype(
            jnp.float32
        )
    for source, target in zip(ins, outs):
        target[...] = source[...]


def deliver(keep, first, last, *results):
    kinds, units, width = keep.shape
    copies = [
        pl.BlockSpec((result.shape[0] // 2, width), lambda i: (jnp.minimum(i, 1), 0))
        for result in results
    ]
    sums = pl.BlockSpec((1, units, width), lambda i: (i, 0, 0))
    halves = pl.BlockSpec((1, units // 2, width), lambda i: (i, 0, 0))
    return pl.pallas_call(
        deliver_kernel,
        grid=(kinds,),
        out_shape=[jax.ShapeDtypeStruct(keep.shape, jnp.float32)]
        + [jax.ShapeDtypeStruct(result.shape, result.dtype) for result in results],
        in_specs=[sums, halves, halves] + copies,
        out_specs=[sums] + copies,
        compiler_params=pltpu.CompilerParams(vmem_limit_bytes=VMEM_BYTES),
        cost_estimate=cost_of(8),
        name="deliver",
    )(keep, first, last, *results)


def body(tokens, w_qkv, w_out, gains, w_ffn, cotangent):
    groups = lax.axis_size("sp")
    wide = lax.axis_size("blk") > 8
    act_block, projected = project_in(tokens, gains, w_qkv)
    attended_low, attended, totals, by_row, kv_all = attend(projected, HEADS // groups)
    attn, middle, act_ffn = exchange_project(attended_low, w_out, 5, (tokens, gains))
    w_parts = jnp.transpose(w_ffn, (1, 0, 2))
    result, grad_ffn, row_three, *kept = (ffn_forward_wide if wide else ffn_forward)(
        act_ffn, w_parts, middle, cotangent, gains
    )
    grad_act_ffn, ffn_part, cross = (ffn_back_wide if wide else ffn_back)(
        grad_ffn, kept, w_parts, groups
    )
    grad_block, scaled, delta, grad_middle, rows = project_back(
        grad_act_ffn, middle, attn, cotangent, gains, attended, by_row, totals, w_out
    )
    grad_cols, *far_first = attend_back(projected, scaled, delta, kv_all, cross)
    qkv_grad, out_grad, tokens_grad, gains_all, far_last = (finish_wide if wide else finish)(
        grad_cols,
        act_block,
        attended_low,
        grad_block,
        w_qkv,
        tokens,
        grad_middle,
        gains,
        rows,
        row_three,
        cross,
    )
    if wide:
        ffn_sum = ffn_part.astype(jnp.float32)
    else:
        ffn_sum, result, tokens_grad, qkv_grad, out_grad = deliver(
            ffn_part, *far_first, far_last, result, tokens_grad, qkv_grad, out_grad
        )
    ffn_grad = jnp.transpose(ffn_sum, (1, 0, 2))
    share = gains_all.shape[1] // (groups * lax.axis_size("blk"))
    place = lax.axis_index("sp") * lax.axis_size("blk") + lax.axis_index("blk")
    gains_grad = lax.dynamic_slice_in_dim(gains_all[:4], place * share, share, 1)
    return (result, tokens_grad, qkv_grad, out_grad, gains_grad, ffn_grad)


def solution(mesh):
    return jax.shard_map(
        body,
        mesh=mesh,
        in_specs=(
            P(("blk", "sp"), None),
            P(),
            P(),
            P(),
            P("blk", None, None),
            P(("blk", "sp"), None),
        ),
        out_specs=(
            P(("blk", "sp"), None),
            P(("blk", "sp"), None),
            P(("sp", "blk"), None),
            P(("sp", "blk"), None),
            P(None, ("sp", "blk")),
            P(("blk", "sp"), None, None),
        ),
        check_vma=False,
    )
```
